32 devices in a mesh: grp: 4 (over y, x), grid: 8 (over z, core).
Axes of the slice: x: 2, y: 2, z: 4, core: 2. Of those that a mesh axis runs over, the one named last changes fastest.
Arguments:
- orbitals: float32 [64, 262144], P('grp', 'grid'), may hold values from -6 to 6
- anchors: int32 [64, 3], replicated, may hold values from 0 to 31
- pair_slots: int32 [32, 4, 2], replicated, may hold values from -1 to 63, as said below
Outputs:
- exchange_term: float32 [64, 262144], P('grp', 'grid')
The draws below stay inside these ranges and needn't reach their ends.
Inputs may be any that keep to these rules, and one draw needn't show every extreme that they name: `pair_slots`: row k lists the pairs of owner k, the device with index k in the order grp, grid; its first slots hold pairs of two different orbital numbers and its other slots hold -1 in both columns. Exactly 64 slots hold pairs in all, no row holds more than 4, and some row holds exactly 4.
All inputs are finite; a program needn't handle non-finite values.
Results may differ from the reference program's by a relative error of at most 0.0003.
Values sent between devices are 32-bit elements; how exact they have to be, the bound alone decides.
A program may use at most 128 MiB of HBM per device.

```python
import jax
import jax.numpy as jnp
from jax import lax

B = 64
PAIR_DEV = 2
ITERS = 3
OWNERS = 32
NORB = 64
CAP = 4


def draw_pair_slots(key, part):
    order_key, first_key, gap_key = jax.random.split(jax.random.fold_in(key, 7), 3)
    position = jnp.argsort(jax.random.permutation(order_key, OWNERS))
    load = jnp.where(position < OWNERS // 4, CAP, jnp.where(position < 3 * OWNERS // 4, PAIR_DEV, 0))
    slot_idx = lax.broadcasted_iota(jnp.int32, (OWNERS, CAP), 1)
    filled = slot_idx < load[:, None]
    orbit_a = jax.random.randint(first_key, (OWNERS, CAP), 0, NORB)
    orbit_b = (orbit_a + jax.random.randint(gap_key, (OWNERS, CAP), 1, NORB)) % NORB
    paired = jnp.stack([orbit_a, orbit_b], -1)
    return jnp.where(filled[..., None], paired, -1).astype(jnp.int32)


def plant(drawn, stream_key, least, largest):
    place = [jax.random.randint(jax.random.fold_in(stream_key, axis), (), 0, length) for axis, length in enumerate(drawn.shape)]
    widest = drawn.shape.index(max(drawn.shape))
    next_to = place[:widest] + [(place[widest] + 1) % drawn.shape[widest]] + place[widest + 1:]
    return drawn.at[tuple(place)].set(least).at[tuple(next_to)].set(largest)


def block_scale(stream_key, dims, cuts, smallest, high):
    factor_of = 1.0
    for axis_at, parts in cuts:
        steps = jax.random.uniform(jax.random.fold_in(jax.random.fold_in(stream_key, 6), axis_at), (parts,), jnp.float32, smallest / len(cuts), high / len(cuts))
        factor_of = factor_of * jnp.repeat(jnp.exp(steps), dims[axis_at] // parts).reshape((-1,) + (1,) * (len(dims) - 1 - axis_at))
    return factor_of


def normal_values(key, shape, width, limit, cuts=(), kind=jnp.bfloat16):
    level = block_scale(key, shape, cuts, -0.22, 0.18) if cuts else 1.0
    values = jax.random.normal(key, shape, jnp.float32) * width * level
    return jnp.minimum(jnp.maximum(values, -limit), limit).astype(kind)


def setup_inputs(seed: int = 0) -> dict:
    keys = jax.random.split(jax.random.key(seed), 4)
    return {
        "orbitals": normal_values(keys[0], (NORB, B * B * B), 1.0, 6.0, ((0, 4), (1, 8)), jnp.float32),
        "anchors": plant(jax.random.randint(keys[1], (NORB, 3), 0, B // 2), jax.random.fold_in(keys[1], 1), 0, (B // 2) - 1).astype(jnp.int32),
        "pair_slots": draw_pair_slots(jax.random.fold_in(keys[3], 71), 0),
    }


def shift_field(field, offset, extent):
    plane_size = extent * extent
    padded_x = jnp.pad(field, ((extent, extent), (0, 0)))
    moved = lax.dynamic_slice_in_dim(padded_x, (extent - offset[0]).astype(jnp.int32), extent, 0)
    padded_yz = jnp.pad(moved, ((0, 0), (plane_size, plane_size)))
    linear = (offset[1] * extent + offset[2]).astype(jnp.int32)
    moved = lax.dynamic_slice_in_dim(padded_yz, (plane_size - linear).astype(jnp.int32), plane_size, 1)
    cells = lax.broadcasted_iota(jnp.int32, (1, plane_size), 1)
    coord_y = cells // extent - offset[1]
    coord_z = cells % extent - offset[2]
    inside = (coord_y >= 0) & (coord_y < extent) & (coord_z >= 0) & (coord_z < extent)
    return jnp.where(inside, moved, jnp.zeros_like(moved))


def operate(field, extent):
    padded_x = jnp.pad(field, ((1, 1), (0, 0)))
    beside = padded_x[2:] + padded_x[:-2]
    padded_y = jnp.pad(field, ((0, 0), (extent, extent)))
    beside = beside + padded_y[:, 2 * extent:] + padded_y[:, :-2 * extent]
    padded_z = jnp.pad(field, ((0, 0), (1, 1)))
    cells = lax.broadcasted_iota(jnp.int32, (1, field.shape[1]), 1) % extent
    upper_z = jnp.where(cells < extent - 1, padded_z[:, 2:], jnp.zeros_like(field))
    lower_z = jnp.where(cells > 0, padded_z[:, :-2], jnp.zeros_like(field))
    return 6.0 * field - beside - upper_z - lower_z


def conjugate(density, extent):
    potential = jnp.zeros_like(density)
    resid = density
    direction = density
    norm_now = jnp.sum(resid * resid)
    for turn in range(ITERS):
        image = operate(direction, extent)
        step_len = norm_now / jnp.sum(direction * image)
        potential = potential + step_len * direction
        resid = resid - step_len * image
        norm_next = jnp.sum(resid * resid)
        direction = resid + (norm_next / norm_now) * direction
        norm_now = norm_next
    return potential


def pair_terms(field_a, field_b, offset, extent):
    partner = shift_field(field_b, offset, extent)
    density = field_a * partner
    potential = conjugate(density, extent)
    term_a = potential * partner
    term_b = shift_field(potential * field_a, -offset, extent)
    return term_a, term_b


def reference(orbitals, anchors, pair_slots):
    extent = B
    slot_list = pair_slots.reshape(-1, 2)

    def add_pair(accum, slot_entry):
        filled = slot_entry[0] >= 0
        orbit_a = jnp.maximum(slot_entry[0], 0).astype(jnp.int32)
        orbit_b = jnp.maximum(slot_entry[1], 0).astype(jnp.int32)
        offset = anchors[orbit_b] - anchors[orbit_a]
        field_a = orbitals[orbit_a].reshape(extent, extent * extent)
        field_b = orbitals[orbit_b].reshape(extent, extent * extent)
        term_a, term_b = pair_terms(field_a, field_b, offset, extent)
        weight_flag = jnp.where(filled, 1.0, 0.0).astype(orbitals.dtype)
        accum = accum.at[orbit_a].add(weight_flag * term_a.reshape(-1))
        accum = accum.at[orbit_b].add(weight_flag * term_b.reshape(-1))
        return accum, None

    start = jnp.zeros(orbitals.shape, orbitals.dtype)
    accum, unused = lax.scan(add_pair, start, slot_list)
    return accum
```

```python
import functools
import math

import jax
import jax.numpy as jnp
from jax import lax
from jax.experimental import pallas as pl
from jax.experimental.pallas import tpu as pltpu
from jax.sharding import PartitionSpec as P

B = 64
PAIR_DEV = 2
ITERS = 3
MOST_CHUNKS = 2
LANES = 128
ROWS = B * B // LANES
PAD = 32
STEP = 4


def deal_evenly(pair_slots, owner_count, each_owner):
    flat_slots = pair_slots.reshape(-1, 2)
    filled = (flat_slots[:, 0] >= 0).astype(jnp.int32)
    position = jnp.cumsum(filled, dtype=jnp.int32) - filled
    wanted = lax.broadcasted_iota(jnp.int32, (owner_count, each_owner), 1) * owner_count
    wanted = (wanted + lax.broadcasted_iota(jnp.int32, (owner_count, each_owner), 0)).reshape(-1)
    matched = (position[None, :] == wanted[:, None]) & (filled[None, :] == 1)
    picked = jnp.sum(jnp.where(matched[:, :, None], flat_slots[None], 0), axis=1)
    return picked.reshape(owner_count, each_owner, 2)


def gather_kernel(ids_ref, src_ref, *out_refs):
    count, terms = out_refs[0].shape[:2]
    for slot, out_ref in enumerate(out_refs):
        def pick(dest, unused, slot=slot, out_ref=out_ref):
            for term in range(terms):
                out_ref[dest, term] = src_ref[ids_ref[(slot * count + dest) * terms + term]]
            return unused

        lax.fori_loop(0, count, pick, 0)


def gather_pieces(ids, pieces, slots, count):
    norb, rows, lanes = pieces.shape
    block = max(8, rows // 4)
    return pl.pallas_call(
        gather_kernel,
        grid_spec=pltpu.PrefetchScalarGridSpec(
            num_scalar_prefetch=1,
            grid=(rows // block,),
            in_specs=[pl.BlockSpec((norb, block, lanes), lambda i, ids: (0, i, 0))],
            out_specs=[pl.BlockSpec((count, 2, block, lanes), lambda i, ids: (0, 0, i, 0))] * slots,
        ),
        out_shape=[jax.ShapeDtypeStruct((count, 2, rows, lanes), jnp.float32)] * slots,
        cost_estimate=pl.CostEstimate(flops=0, bytes_accessed=8 * norb * rows * lanes, transcendentals=0),
        name="pick_pieces",
    )(ids, pieces)


def scatter_kernel(ids_ref, *refs):
    out_ref = refs[-1]
    out_ref[...] = jnp.zeros_like(out_ref)
    count, terms = refs[0].shape[:2]
    for slot, in_ref in enumerate(refs[:-1]):
        def add(dest, unused, slot=slot, in_ref=in_ref):
            for term in range(terms):
                orbit = ids_ref[(slot * count + dest) * terms + term]
                out_ref[orbit] = out_ref[orbit] + in_ref[dest, term]
            return unused

        lax.fori_loop(0, count, add, 0)


def scatter_pieces(ids, parts, norb):
    count, terms, rows, lanes = parts[0].shape
    block = max(8, rows // 4)
    return pl.pallas_call(
        scatter_kernel,
        grid_spec=pltpu.PrefetchScalarGridSpec(
            num_scalar_prefetch=1,
            grid=(rows // block,),
            in_specs=[pl.BlockSpec((count, terms, block, lanes), lambda i, ids: (0, 0, i, 0))] * len(parts),
            out_specs=pl.BlockSpec((norb, block, lanes), lambda i, ids: (0, i, 0)),
        ),
        out_shape=jax.ShapeDtypeStruct((norb, rows, lanes), jnp.float32),
        cost_estimate=pl.CostEstimate(flops=0, bytes_accessed=8 * norb * rows * lanes, transcendentals=0),
        name="add_pieces",
    )(ids, *parts)


def lane_ids(shape):
    return lax.broadcasted_iota(jnp.int32, shape, len(shape) - 1)


def shift_plane(plane, off_y, off_z):
    shape = plane.shape
    lane = lane_ids(shape)
    row = lax.broadcasted_iota(jnp.int32, shape, 0)
    linear = off_y * B + off_z
    across = jnp.bitwise_and(linear, LANES - 1)
    down = jnp.right_shift(linear, 7)
    turned = pltpu.roll(plane, across, 1)
    near = pltpu.roll(turned, jnp.bitwise_and(down, ROWS - 1), 0)
    far = pltpu.roll(turned, jnp.bitwise_and(down + 1, ROWS - 1), 0)
    moved = jnp.where(lane >= across, near, far)
    from_y = row * 2 + jnp.right_shift(lane, 6) - off_y
    from_z = jnp.bitwise_and(lane, B - 1) - off_z
    inside = (from_y >= 0) & (from_y < B) & (from_z >= 0) & (from_z < B)
    return jnp.where(inside, moved, 0.0)


def operate_plane(before, plane, after):
    shape = plane.shape
    lane = lane_ids(shape)
    row = lax.broadcasted_iota(jnp.int32, shape, 0)
    z = jnp.bitwise_and(lane, B - 1)
    upper_z = jnp.where(z < B - 1, pltpu.roll(plane, LANES - 1, 1), 0.0)
    lower_z = jnp.where(z > 0, pltpu.roll(plane, 1, 1), 0.0)
    half = pltpu.roll(plane, B, 1)
    down = jnp.where(row > 0, pltpu.roll(half, 1, 0), 0.0)
    up = jnp.where(row < ROWS - 1, pltpu.roll(half, ROWS - 1, 0), 0.0)
    beside = (before + after) + (half + jnp.where(lane < B, down, up))
    return 6.0 * plane - beside - upper_z - lower_z


def fold(values):
    return jnp.sum(values.reshape(ROWS // 8, 8, LANES), axis=0)


def total(acc):
    return jnp.sum(acc, axis=(0, 1), keepdims=True)


def solve_kernel(info_ref, *refs):
    chunks = (len(refs) - 6) // 2
    in_refs, out_refs = refs[:chunks], refs[chunks : 2 * chunks]
    wide, partner, direction, resid, image, potential = refs[2 * chunks :]
    count, terms, rows, lanes = in_refs[0].shape
    each = rows // ROWS
    dx, dy, dz = info_ref[0], info_ref[1], info_ref[2]
    keep = jnp.where(info_ref[3] > 0, 1.0, 0.0).astype(jnp.float32)
    edge = jnp.zeros((PAD, ROWS, LANES), jnp.float32)
    wide[pl.ds(0, PAD)] = edge
    wide[pl.ds(PAD + B, PAD)] = edge
    direction[0] = edge[0]
    direction[B + 1] = edge[0]
    none = jnp.zeros((8, LANES), jnp.float32)

    def place(owner, chunk, i):
        return (owner * chunks + chunk) * each + i

    def load(owner, unused):
        for chunk in range(chunks):
            for i in range(each):
                wide[PAD + place(owner, chunk, i)] = in_refs[chunk][owner, 1, pl.ds(i * ROWS, ROWS)]
        return unused

    lax.fori_loop(0, count, load, 0)

    def start(owner, acc):
        for chunk in range(chunks):
            for i in range(each):
                x = place(owner, chunk, i)
                other = shift_plane(wide[PAD + x - dx], dy, dz)
                partner[x] = other
                density = in_refs[chunk][owner, 0, pl.ds(i * ROWS, ROWS)] * other
                direction[x + 1] = density
                resid[x] = density
                acc = acc + fold(density * density)
        return acc

    norm_now = total(lax.fori_loop(0, count, start, none))

    for turn in range(ITERS):
        def apply(block, acc):
            for i in range(STEP):
                x = block * STEP + i
                plane = direction[x + 1]
                result = operate_plane(direction[x], plane, direction[x + 2])
                image[x] = result
                acc = acc + fold(plane * result)
            return acc

        step_len = norm_now / total(lax.fori_loop(0, B // STEP, apply, none))

        if turn == ITERS - 1:
            break

        def advance(block, acc):
            for i in range(STEP):
                x = block * STEP + i
                moved = step_len * direction[x + 1]
                potential[x] = moved if turn == 0 else potential[x] + moved
                left = resid[x] - step_len * image[x]
                resid[x] = left
                acc = acc + fold(left * left)
            return acc

        norm_next = total(lax.fori_loop(0, B // STEP, advance, none))
        ratio = norm_next / norm_now

        def renew(block, unused):
            for i in range(STEP):
                x = block * STEP + i
                direction[x + 1] = resid[x] + ratio * direction[x + 1]
            return unused

        lax.fori_loop(0, B // STEP, renew, 0)
        norm_now = norm_next

    def finish(owner, unused):
        for chunk in range(chunks):
            for i in range(each):
                x = place(owner, chunk, i)
                found = (potential[x] + step_len * direction[x + 1]) * keep
                out_refs[chunk][owner, 0, pl.ds(i * ROWS, ROWS)] = found * partner[x]
                wide[PAD + x] = found * in_refs[chunk][owner, 0, pl.ds(i * ROWS, ROWS)]
        return unused

    lax.fori_loop(0, count, finish, 0)

    def give_back(owner, unused):
        for chunk in range(chunks):
            for i in range(each):
                x = place(owner, chunk, i)
                out_refs[chunk][owner, 1, pl.ds(i * ROWS, ROWS)] = shift_plane(wide[PAD + x + dx], -dy, -dz)
        return unused

    lax.fori_loop(0, count, give_back, 0)


def solve_pair(info, parts):
    box = (B, ROWS, LANES)
    vmem = pl.BlockSpec(memory_space=pltpu.VMEM)
    return pl.pallas_call(
        solve_kernel,
        in_specs=[pl.BlockSpec(memory_space=pltpu.SMEM)] + [vmem] * len(parts),
        out_specs=[vmem] * len(parts),
        out_shape=[jax.ShapeDtypeStruct(p.shape, jnp.float32) for p in parts],
        scratch_shapes=[
            pltpu.VMEM((B + 2 * PAD, ROWS, LANES), jnp.float32),
            pltpu.VMEM(box, jnp.float32),
            pltpu.VMEM((B + 2, ROWS, LANES), jnp.float32),
            pltpu.VMEM(box, jnp.float32),
            pltpu.VMEM(box, jnp.float32),
            pltpu.VMEM(box, jnp.float32),
        ],
        compiler_params=pltpu.CompilerParams(vmem_limit_bytes=32 * 1024 * 1024),
        cost_estimate=pl.CostEstimate(flops=0, bytes_accessed=40 * 1024 * 1024, transcendentals=0),
        name="solve_pair",
    )(info, *parts)


def owner_body(orbitals, anchors, pair_slots):
    grid_count = lax.axis_size("grid")
    owner_count = lax.axis_size("grp") * grid_count
    group_idx = lax.axis_index("grp")
    place_idx = lax.axis_index("grid")
    assignment = deal_evenly(pair_slots, owner_count, PAIR_DEV)
    slots = assignment.shape[1]
    filled = assignment[..., 0] >= 0
    safe_ids = jnp.maximum(assignment, 0)
    group_table = lax.dynamic_slice_in_dim(safe_ids, group_idx * grid_count, grid_count, 0)
    ids = jnp.transpose(group_table, (1, 0, 2)).reshape(-1)
    owner_idx = group_idx * grid_count + place_idx
    own_pairs = safe_ids[owner_idx]
    offsets = anchors[own_pairs[:, 1]] - anchors[own_pairs[:, 0]]
    info = jnp.concatenate([offsets, filled[owner_idx].astype(jnp.int32)[:, None]], axis=1)

    norb_local, cells = orbitals.shape
    stacked = orbitals.reshape(norb_local, cells // LANES, LANES)
    chunks = math.gcd(MOST_CHUNKS, cells // (B * B))
    rows = stacked.shape[1] // chunks
    arrived = [[None] * chunks for _ in range(slots)]
    for chunk in range(chunks):
        pieces = lax.all_gather(stacked[:, chunk * rows : (chunk + 1) * rows], "grp", axis=0, tiled=True)
        outgoing = gather_pieces(ids, pieces, slots, grid_count)
        for slot in range(slots):
            arrived[slot][chunk] = lax.all_to_all(outgoing[slot], "grid", split_axis=0, concat_axis=0, tiled=True)
    returned = []
    for slot in range(slots):
        terms = solve_pair(info[slot], arrived[slot])
        returned.append(
            [lax.all_to_all(t, "grid", split_axis=0, concat_axis=0, tiled=True) for t in terms]
        )
    results = []
    for chunk in range(chunks):
        summed = scatter_pieces(ids, [r[chunk] for r in returned], anchors.shape[0])
        results.append(lax.psum_scatter(summed, "grp", scatter_dimension=0, tiled=True))
    return jnp.concatenate(results, axis=1).reshape(norb_local, cells)


MESH = pl.DeviceIdType.MESH
HALO = 3
WAVES = 4
SUB = 8


def remote(src, dst, send_sem, recv_sem, device):
    return pltpu.make_async_remote_copy(
        src_ref=src, dst_ref=dst, send_sem=send_sem, recv_sem=recv_sem, device_id=device, device_id_type=MESH
    )


def spot():
    grp = lax.axis_index("grp")
    place = lax.axis_index("grid")
    across = grp + 1 - 2 * lax.rem(grp, 2)
    along = lax.rem(grp + 2, 4)
    corner = lax.rem(across + 2, 4)
    return grp, place, across, along, corner


def greet(chips):
    grp, place, across, along, unused = spot()
    chip = place // 2
    core = lax.rem(place, 2)
    barrier = pltpu.get_barrier_semaphore()
    for device in ((across, place), (along, place), (grp, 2 * chip + 1 - core)):
        pl.semaphore_signal(barrier, inc=1, device_id=device, device_id_type=MESH)

    @pl.when(chip > 0)
    def below():
        pl.semaphore_signal(barrier, inc=1, device_id=(grp, place - 2), device_id_type=MESH)

    @pl.when(chip < chips - 1)
    def above():
        pl.semaphore_signal(barrier, inc=1, device_id=(grp, place + 2), device_id_type=MESH)

    ends = jnp.where(chip > 0, 1, 0) + jnp.where(chip < chips - 1, 1, 0)
    pl.semaphore_wait(barrier, 3 + ends)


class Relay:
    def __init__(self, wins, send_sem, recv_sem, signs, chips):
        self.wins, self.send_sem, self.recv_sem, self.signs, self.chips = wins, send_sem, recv_sem, signs, chips
        self.grp, self.place = lax.axis_index("grp"), lax.axis_index("grid")
        self.chip = self.place // 2
        self.core = lax.rem(self.place, 2)
        self.half = wins[0].shape[0] // 2
        self.planes = wins[0].shape[1] // 6

    def offset(self, sign, hop):
        return 2 * self.planes * (2 - hop if sign > 0 else hop)

    def region(self, chunk, side, hop, core):
        start = self.offset(self.signs[side], hop) + self.planes * core
        return self.wins[chunk].at[pl.ds(side * self.half, self.half), pl.ds(start, self.planes)]

    def comes(self, side, hop):
        source = self.chip - self.signs[side] * hop
        return source >= 0 if self.signs[side] > 0 else source < self.chips

    def goes(self, side, hop):
        source = self.chip + self.signs[side] - self.signs[side] * hop
        if self.signs[side] > 0:
            return (self.chip + 1 < self.chips) & (source >= 0)
        return (self.chip - 1 >= 0) & (source < self.chips)

    def onward(self, chunk, side, hop):
        here = self.region(chunk, side, hop - 1, self.core)
        there = self.region(chunk, side, hop, self.core)
        return remote(
            here, there, self.send_sem.at[chunk, side, hop - 1], self.recv_sem.at[chunk, side, hop - 1],
            (self.grp, self.place + 2 * self.signs[side]),
        )

    def arriving(self, chunk, side, hop):
        there = self.region(chunk, side, hop, self.core)
        return remote(
            there, there, self.send_sem.at[chunk, side, hop - 1], self.recv_sem.at[chunk, side, hop - 1],
            (self.grp, self.place + 2 * self.signs[side]),
        )

    def beside(self, chunk, side, hop, core):
        part = self.region(chunk, side, hop, core)
        return remote(
            part, part, self.send_sem.at[chunk, side, 2 + hop], self.recv_sem.at[chunk, side, 2 + hop],
            (self.grp, 2 * self.chip + 1 - self.core),
        )

    def clear(self):
        for side in range(2):
            for hop in (1, 2):
                start = self.offset(self.signs[side], hop)

                @pl.when(jnp.logical_not(self.comes(side, hop)))
                def fill(side=side, start=start):
                    for win in self.wins:
                        def zero(slot, unused, win=win):
                            win[slot, pl.ds(start, 2 * self.planes)] = jnp.zeros(
                                (2 * self.planes,) + win.shape[2:], jnp.float32
                            )
                            return unused

                        lax.fori_loop(side * self.half, (side + 1) * self.half, zero, 0)

    def begin(self, chunk):
        for side in range(2):
            self.beside(chunk, side, 0, self.core).start()

            @pl.when(self.goes(side, 1))
            def go(side=side):
                self.onward(chunk, side, 1).start()

    def first(self, chunk):
        for side in range(2):
            @pl.when(self.comes(side, 1))
            def got(side=side):
                self.arriving(chunk, side, 1).wait_recv()
                self.beside(chunk, side, 1, self.core).start()

            @pl.when(self.goes(side, 2))
            def go(side=side):
                self.onward(chunk, side, 2).start()

    def second(self, chunk):
        for side in range(2):
            @pl.when(self.comes(side, 2))
            def got(side=side):
                self.arriving(chunk, side, 2).wait_recv()
                self.beside(chunk, side, 2, self.core).start()

    def settle(self, chunk):
        for side in range(2):
            self.beside(chunk, side, 0, 1 - self.core).wait_recv()
            for hop in (1, 2):
                @pl.when(self.comes(side, hop))
                def got(side=side, hop=hop):
                    self.beside(chunk, side, hop, 1 - self.core).wait_recv()

    def drain(self):
        for chunk in range(len(self.wins)):
            for side in range(2):
                self.beside(chunk, side, 0, self.core).wait_send()
                for hop in (1, 2):
                    @pl.when(self.comes(side, hop))
                    def sent(chunk=chunk, side=side, hop=hop):
                        self.beside(chunk, side, hop, self.core).wait_send()

                    @pl.when(self.goes(side, hop))
                    def passed(chunk=chunk, side=side, hop=hop):
                        self.onward(chunk, side, hop).wait_send()


def bring_kernel(chips, tbl, orb, moved, fixed, *scratch):
    count = moved.shape[0]
    pools, wins = scratch[:count], scratch[count : 2 * count]
    own_sem, xy_send, xy_recv, z_send, z_recv = scratch[2 * count :]
    grp, place, across, along, corner = spot()
    core = lax.rem(place, 2)
    norb, planes = orb.shape[:2]
    part = norb // 2
    slots = moved.shape[1]
    relay = Relay(wins, z_send, z_recv, (1, -1), chips)

    def block(chunk, owner, start, size):
        return pools[chunk].at[pl.ds(owner * norb + start, size)]

    def stage(chunk):
        return pltpu.make_async_copy(
            orb.at[:, :, pl.ds(chunk * SUB, SUB)], block(chunk, grp, 0, norb), own_sem.at[chunk]
        )

    def hop(chunk, kind, owner, start, size, target):
        ref = block(chunk, owner, start, size)
        return remote(ref, ref, xy_send.at[chunk, kind], xy_recv.at[chunk, kind], (target, place))

    def direct(chunk, owners):
        return hop(chunk, 0, owners[0], 0, norb, across), hop(chunk, 1, owners[1], 0, norb, along)

    def turned(chunk, owners):
        return hop(chunk, 2, owners[0], 0, part, along), hop(chunk, 3, owners[1], part, part, across)

    for chunk in range(count):
        stage(chunk).start()
    greet(chips)
    relay.clear()

    def send_own(chunk):
        stage(chunk).wait()
        for copy in direct(chunk, (grp, grp)):
            copy.start()

    send_own(0)
    send_own(1)
    for step in range(count + 4):
        if step < count:
            for copy in direct(step, (across, along)):
                copy.wait_recv()
            for copy in turned(step, (across, along)):
                copy.start()
            if step + 2 < count:
                send_own(step + 2)
        chunk = step - 1
        if 0 <= chunk < count:
            for copy in turned(chunk, (corner, corner)):
                copy.wait_recv()
            for side in range(2):
                start = relay.offset(relay.signs[side], 0) + planes * core

                def pick(slot, unused, start=start, chunk=chunk):
                    wins[chunk][slot, pl.ds(start, planes)] = pools[chunk][tbl[0, slot]]
                    fixed[chunk, slot] = pools[chunk][tbl[1, slot]]
                    return unused

                lax.fori_loop(side * (slots // 2), (side + 1) * (slots // 2), pick, 0)
            relay.begin(chunk)
        chunk = step - 2
        if 0 <= chunk < count:
            relay.first(chunk)
        chunk = step - 3
        if 0 <= chunk < count:
            relay.second(chunk)
        chunk = step - 4
        if 0 <= chunk < count:
            relay.settle(chunk)

            def choose(slot, unused, chunk=chunk):
                first = tbl[2, slot] + planes * core
                for plane in range(planes):
                    moved[chunk, slot, plane] = wins[chunk][slot, first + plane]
                return unused

            lax.fori_loop(0, slots, choose, 0)
    for chunk in range(count):
        for copy in direct(chunk, (grp, grp)) + turned(chunk, (across, along)):
            copy.wait_send()
    relay.drain()


def bring(table, stacked, slots, groups, chips):
    norb, planes, rows, lanes = stacked.shape
    chunks = rows // SUB
    vmem = pl.BlockSpec(memory_space=pltpu.VMEM)
    dma = pltpu.SemaphoreType.DMA
    shape = jax.ShapeDtypeStruct((chunks, slots, planes, SUB, lanes), jnp.float32)
    return pl.pallas_call(
        functools.partial(bring_kernel, chips),
        in_specs=[pl.BlockSpec(memory_space=pltpu.SMEM), pl.BlockSpec(memory_space=pl.ANY)],
        out_specs=[vmem, vmem],
        out_shape=[shape, shape],
        scratch_shapes=[pltpu.VMEM((groups * norb, planes, SUB, lanes), jnp.float32)] * chunks
        + [pltpu.VMEM((slots, 6 * planes, SUB, lanes), jnp.float32)] * chunks
        + [dma((chunks,)), dma((chunks, 4)), dma((chunks, 4)), dma((chunks, 2, 5)), dma((chunks, 2, 5))],
        compiler_params=pltpu.CompilerParams(
            collective_id=0, has_side_effects=True, vmem_limit_bytes=48 * 1024 * 1024
        ),
        name="bring",
    )(table, stacked)


def pair_kernel(tbl, moved, fixed, dens, partner):
    slot = pl.program_id(0)
    second = tbl[3, slot] > 0
    dy, dz = tbl[4, slot], tbl[5, slot]

    for x in range(moved.shape[2]):
        left = moved[:, 0, x].reshape(ROWS, LANES)
        right = fixed[:, 0, x].reshape(ROWS, LANES)
        other = shift_plane(jnp.where(second, left, right), dy, dz)
        dens[0, x] = jnp.where(second, right, left) * other
        partner[0, x] = other


def pair_up(table, moved, fixed):
    chunks, slots, planes, sub, lanes = moved.shape
    tiled = pl.BlockSpec((chunks, 1, planes, sub, lanes), lambda i, t: (0, i, 0, 0, 0))
    plain = pl.BlockSpec((1, planes, ROWS, lanes), lambda i, t: (i, 0, 0, 0))
    shape = jax.ShapeDtypeStruct((slots, planes, ROWS, lanes), jnp.float32)
    return pl.pallas_call(
        pair_kernel,
        grid_spec=pltpu.PrefetchScalarGridSpec(
            num_scalar_prefetch=1, grid=(slots,), in_specs=[tiled, tiled], out_specs=[plain, plain]
        ),
        out_shape=[shape, shape],
        name="pair_up",
    )(table, moved, fixed)


def inner(plane):
    shape = plane.shape
    lane = lane_ids(shape)
    row = lax.broadcasted_iota(jnp.int32, shape, 0)
    z = jnp.bitwise_and(lane, B - 1)
    upper_z = jnp.where(z < B - 1, pltpu.roll(plane, LANES - 1, 1), 0.0)
    lower_z = jnp.where(z > 0, pltpu.roll(plane, 1, 1), 0.0)
    half = pltpu.roll(plane, B, 1)
    down = jnp.where(row > 0, pltpu.roll(half, 1, 0), 0.0)
    up = jnp.where(row < ROWS - 1, pltpu.roll(half, ROWS - 1, 0), 0.0)
    return 6.0 * plane - ((half + jnp.where(lane < B, down, up)) + (upper_z + lower_z))


def krylov_weights(m):
    a0 = m[0] / m[1]
    rr1 = a0 * a0 * m[2] - m[0]
    p, q = 1.0 + rr1 / m[0], -a0
    a1 = rr1 / (p * p * m[1] + 2.0 * p * q * m[2] + q * q * m[3])
    s1, s2 = -a0 - a1 * p, -a1 * q
    rr2 = (m[0] + s1 * s1 * m[2] + s2 * s2 * m[4]) + 2.0 * (s1 * m[1] + s2 * m[2] + s1 * s2 * m[3])
    b1 = rr2 / rr1
    e0, e1, e2 = 1.0 + b1 * p, s1 + b1 * q, s2
    bend = e0 * e0 * m[1] + e1 * e1 * m[3] + e2 * e2 * m[5]
    a2 = rr2 / (bend + 2.0 * (e0 * e1 * m[2] + e0 * e2 * m[3] + e1 * e2 * m[4]))
    return a0 + a1 * p + a2 * e0, a1 * q + a2 * e1, a2 * e2


def solve_slabs_kernel(places, tbl, dens, pot, wide, one, two, sums, gathered, weights, h_send, h_recv, s_send, s_recv):
    grp, place = lax.axis_index("grp"), lax.axis_index("grid")
    slots, planes = dens.shape[:2]
    first, last = HALO, HALO + planes - 1
    each = slots // WAVES
    barrier = pltpu.get_barrier_semaphore()
    for step in range(1, places):
        pl.semaphore_signal(
            barrier, inc=1, device_id=(grp, lax.rem(place + step, places)), device_id_type=MESH
        )
    pl.semaphore_wait(barrier, places - 1)

    def rise(wave):
        return remote(
            dens.at[pl.ds(wave * each, each), pl.ds(planes - HALO, HALO)],
            wide.at[pl.ds(wave * each, each), pl.ds(0, HALO)],
            h_send.at[wave, 0], h_recv.at[wave, 0], (grp, lax.rem(place + 1, places)),
        )

    def sink(wave):
        return remote(
            dens.at[pl.ds(wave * each, each), pl.ds(0, HALO)],
            wide.at[pl.ds(wave * each, each), pl.ds(HALO + planes, HALO)],
            h_send.at[wave, 1], h_recv.at[wave, 1], (grp, lax.rem(place + places - 1, places)),
        )

    lowest, highest = place == 0, place == places - 1
    for wave in range(WAVES):
        @pl.when(jnp.logical_not(highest))
        def send_up(wave=wave):
            rise(wave).start()

        @pl.when(jnp.logical_not(lowest))
        def send_down(wave=wave):
            sink(wave).start()

    blank = jnp.zeros((HALO, ROWS, LANES), jnp.float32)

    def copy_in(slot, unused):
        wide[slot, pl.ds(HALO, planes)] = dens[slot]
        one[slot, 1] = blank[0]
        one[slot, last + 3] = blank[0]
        one[slot, 0] = blank[0]
        return unused

    lax.fori_loop(0, slots, copy_in, 0)

    @pl.when(lowest)
    def no_below():
        def fill(slot, unused):
            wide[slot, pl.ds(0, HALO)] = blank
            return unused

        lax.fori_loop(0, slots, fill, 0)

    @pl.when(highest)
    def no_above():
        def fill(slot, unused):
            wide[slot, pl.ds(HALO + planes, HALO)] = blank
            return unused

        lax.fori_loop(0, slots, fill, 0)

    lane = lax.broadcasted_iota(jnp.int32, (1, LANES), 1)
    none = jnp.zeros((8, LANES), jnp.float32)

    def row_of(parts):
        row = jnp.zeros((1, LANES), jnp.float32)
        for at, part in parts:
            row = row + jnp.where(lane == at, total(part), 0.0)
        return row

    def work(slot, unused):
        low, high = tbl[6, slot], tbl[6, slot] + B

        def live(e):
            x = planes * place + e - HALO
            return jnp.where((x >= low) & (x < high), 1.0, 0.0).astype(jnp.float32)

        m0, m1, m2, m3, m4, m5 = none, none, none, none, none, none
        for e in range(first - 1, last + 3):
            value = live(e) * (inner(wide[slot, e]) - (wide[slot, e - 1] + wide[slot, e + 1]))
            one[slot, e] = value
            if first <= e <= last:
                source = wide[slot, e]
                m0 = m0 + fold(source * source)
                m1 = m1 + fold(source * value)
                m2 = m2 + fold(value * value)
        bent = None
        for e in range(first, last + 2):
            value = live(e) * (inner(one[slot, e]) - (one[slot, e - 1] + one[slot, e + 1]))
            two[slot, e] = value
            if e > first:
                m5 = m5 - 2.0 * fold(value * two[slot, e - 1])
            if e <= last:
                m3 = m3 + fold(one[slot, e] * value)
                m4 = m4 + fold(value * value)
                m5 = m5 + fold(value * inner(value))
        sums[pl.ds(slot, 1)] = row_of(enumerate((m0, m1, m2, m3, m4, m5)))
        return unused

    def rim(slot, spots, pairs):
        low, high = tbl[6, slot], tbl[6, slot] + B
        m2, m3, m4, m5 = none, none, none, none
        for e, fresh in spots:
            if fresh:
                x = planes * place + e - HALO
                alive = jnp.where((x >= low) & (x < high), 1.0, 0.0).astype(jnp.float32)
                two[slot, e] = alive * (inner(one[slot, e]) - (one[slot, e - 1] + one[slot, e + 1]))
        for e, fresh in spots:
            value, before = two[slot, e], one[slot, e]
            m2 = m2 + fold(before * before)
            m3 = m3 + fold(before * value)
            m4 = m4 + fold(value * value)
            m5 = m5 + fold(value * inner(value))
        for e in pairs:
            m5 = m5 - 2.0 * fold(two[slot, e] * two[slot, e + 1])
        sums[pl.ds(slot, 1)] = sums[pl.ds(slot, 1)] + row_of(((2, m2), (3, m3), (4, m4), (5, m5)))

    for wave in range(WAVES):
        @pl.when(jnp.logical_not(lowest))
        def got_below(wave=wave):
            rise(wave).wait_recv()

        @pl.when(jnp.logical_not(highest))
        def got_above(wave=wave):
            sink(wave).wait_recv()

        lax.fori_loop(wave * each, (wave + 1) * each, work, 0)

    @pl.when(lowest)
    def rim_below():
        def go(slot, unused):
            rim(slot, ((first - 2, True), (first - 1, True)), (first - 2, first - 1))
            return unused

        lax.fori_loop(0, slots, go, 0)

    @pl.when(highest)
    def rim_above():
        def go(slot, unused):
            rim(slot, ((last + 1, False), (last + 2, True)), (last + 1,))
            return unused

        lax.fori_loop(0, slots, go, 0)

    def tell(step):
        return remote(
            sums, gathered.at[place], s_send.at[step - 1], s_recv.at[step - 1],
            (grp, lax.rem(place + step, places)),
        )

    def hear(step):
        source = lax.rem(place + places - step, places)
        return remote(
            sums, gathered.at[source], s_send.at[step - 1], s_recv.at[step - 1],
            (grp, lax.rem(place + step, places)),
        )

    for step in range(1, places):
        tell(step).start()
    gathered[place] = sums[...]
    for step in range(1, places):
        hear(step).wait_recv()
    whole = gathered[0]
    for at in range(1, places):
        whole = whole + gathered[at]
    lanes = lax.broadcasted_iota(jnp.int32, whole.shape, 1)
    moments = [jnp.sum(jnp.where(lanes == at, whole, 0.0), axis=1, keepdims=True) for at in range(6)]
    for at, weight in enumerate(krylov_weights(moments)):
        weights[at] = jnp.broadcast_to(weight, whole.shape)

    def finish(slot, unused):
        w0, w1, w2 = [weights[at, pl.ds(slot, 1)] for at in range(3)]
        for x in range(planes):
            e = x + HALO
            pot[slot, x] = w0 * wide[slot, e] + w1 * one[slot, e] + w2 * two[slot, e]
        return unused

    lax.fori_loop(0, slots, finish, 0)
    for wave in range(WAVES):
        @pl.when(jnp.logical_not(highest))
        def sent_up(wave=wave):
            rise(wave).wait_send()

        @pl.when(jnp.logical_not(lowest))
        def sent_down(wave=wave):
            sink(wave).wait_send()

    for step in range(1, places):
        tell(step).wait_send()


def solve_slabs(table, dens, places):
    slots, planes, rows, lanes = dens.shape
    vmem = pl.BlockSpec(memory_space=pltpu.VMEM)
    dma = pltpu.SemaphoreType.DMA
    tall = pltpu.VMEM((slots, planes + 2 * HALO, rows, lanes), jnp.float32)
    return pl.pallas_call(
        functools.partial(solve_slabs_kernel, places),
        in_specs=[pl.BlockSpec(memory_space=pltpu.SMEM), vmem],
        out_specs=vmem,
        out_shape=jax.ShapeDtypeStruct(dens.shape, jnp.float32),
        scratch_shapes=[
            tall, tall, tall,
            pltpu.VMEM((slots, lanes), jnp.float32),
            pltpu.VMEM((places, slots, lanes), jnp.float32),
            pltpu.VMEM((3, slots, lanes), jnp.float32),
            dma((WAVES, 2)), dma((WAVES, 2)), dma((places - 1,)), dma((places - 1,)),
        ],
        compiler_params=pltpu.CompilerParams(
            collective_id=1, has_side_effects=True, vmem_limit_bytes=40 * 1024 * 1024
        ),
        name="solve_slabs",
    )(table, dens)


def term_kernel(tbl, pot, partner, moved, fixed, going, staying):
    slot = pl.program_id(0)
    second = tbl[3, slot] > 0
    dy, dz = tbl[4, slot], tbl[5, slot]
    chunks = going.shape[0]
    for x in range(pot.shape[1]):
        found = pot[0, x]
        left = moved[:, 0, x].reshape(ROWS, LANES)
        right = fixed[:, 0, x].reshape(ROWS, LANES)
        term_a = found * partner[0, x]
        term_b = shift_plane(found * jnp.where(second, right, left), -dy, -dz)
        going[:, 0, x] = jnp.where(second, term_b, term_a).reshape(chunks, SUB, LANES)
        staying[:, 0, x] = jnp.where(second, term_a, term_b).reshape(chunks, SUB, LANES)


def make_terms(table, pot, partner, moved, fixed):
    chunks, slots, planes, sub, lanes = moved.shape
    tiled = pl.BlockSpec((chunks, 1, planes, sub, lanes), lambda i, t: (0, i, 0, 0, 0))
    plain = pl.BlockSpec((1, planes, ROWS, lanes), lambda i, t: (i, 0, 0, 0))
    shape = jax.ShapeDtypeStruct(moved.shape, jnp.float32)
    return pl.pallas_call(
        term_kernel,
        grid_spec=pltpu.PrefetchScalarGridSpec(
            num_scalar_prefetch=1, grid=(slots,), in_specs=[plain, plain, tiled, tiled], out_specs=[tiled, tiled]
        ),
        out_shape=[shape, shape],
        name="make_terms",
    )(table, pot, partner, moved, fixed)


def hand_back_kernel(chips, tbl, last, going, staying, out, *scratch):
    count, slots = going.shape[:2]
    wins, chains, outs1, outs2, ins1, ins2 = [scratch[i * count : (i + 1) * count] for i in range(6)]
    xy_send, xy_recv, z_send, z_recv = scratch[6 * count :]
    grp, place, across, along, corner = spot()
    core = lax.rem(place, 2)
    norb, planes = out.shape[:2]
    part = norb // 2
    relay = Relay(wins, z_send, z_recv, (-1, 1), chips)
    greet(chips)
    relay.clear()

    def start(chunk):
        for side in range(2):
            at = relay.offset(relay.signs[side], 0) + planes * core

            def place_in(slot, unused, at=at):
                wins[chunk][slot, pl.ds(at, planes)] = going[chunk, slot]
                return unused

            lax.fori_loop(side * (slots // 2), (side + 1) * (slots // 2), place_in, 0)
        relay.begin(chunk)

    def swap(chunk, kind):
        src = (outs1 if kind < 2 else outs2)[chunk].at[kind % 2]
        dst = (ins1 if kind < 2 else ins2)[chunk].at[kind % 2]
        target = (across, along, along, across)[kind]
        return remote(src, dst, xy_send.at[chunk, kind], xy_recv.at[chunk, kind], (target, place))

    start(0)
    start(1)
    for step in range(count + 4):
        if step < count:
            relay.first(step)
            if step + 2 < count:
                start(step + 2)
        chunk = step - 1
        if 0 <= chunk < count:
            relay.second(chunk)
        chunk = step - 2
        if 0 <= chunk < count:
            relay.settle(chunk)
            chain = chains[chunk]
            chain[2 * slots] = jnp.zeros(chain.shape[1:], jnp.float32)

            def link_fixed(slot, unused, chain=chain, chunk=chunk):
                chain[slot] = staying[chunk, slot] + chain[tbl[8, slot]]
                return unused

            def link_moved(slot, unused, chain=chain, chunk=chunk):
                first = tbl[7, slot] + planes * core
                for plane in range(planes):
                    chain[slots + slot, plane] = wins[chunk][slot, first + plane] + chain[tbl[9, slot], plane]
                return unused

            lax.fori_loop(0, slots, link_fixed, 0)
            lax.fori_loop(0, slots, link_moved, 0)

            def pack(i, unused, chain=chain, chunk=chunk):
                outs1[chunk][0, i] = chain[last[across * norb + i]]
                outs1[chunk][0, part + i] = chain[last[corner * norb + i]]
                outs1[chunk][1, i] = chain[last[along * norb + part + i]]
                outs1[chunk][1, part + i] = chain[last[corner * norb + part + i]]
                return unused

            lax.fori_loop(0, part, pack, 0)
            swap(chunk, 0).start()
            swap(chunk, 1).start()
        chunk = step - 3
        if 0 <= chunk < count:
            chain = chains[chunk]
            swap(chunk, 0).wait_recv()

            def add_across(i, unused, chain=chain, chunk=chunk):
                outs2[chunk][0, i] = ins1[chunk][0, part + i] + chain[last[along * norb + i]]
                return unused

            lax.fori_loop(0, part, add_across, 0)
            swap(chunk, 2).start()
            swap(chunk, 1).wait_recv()

            def add_along(i, unused, chain=chain, chunk=chunk):
                outs2[chunk][1, i] = ins1[chunk][1, part + i] + chain[last[across * norb + part + i]]
                return unused

            lax.fori_loop(0, part, add_along, 0)
            swap(chunk, 3).start()
        chunk = step - 4
        if 0 <= chunk < count:
            chain = chains[chunk]
            swap(chunk, 2).wait_recv()
            swap(chunk, 3).wait_recv()
            for side in range(2):
                def keep(i, unused, side=side, chain=chain, chunk=chunk):
                    orbit = side * part + i
                    found = ins1[chunk][side, i] + ins2[chunk][side, i]
                    out[orbit, :, pl.ds(chunk * SUB, SUB)] = found + chain[last[grp * norb + orbit]]
                    return unused

                lax.fori_loop(0, part, keep, 0)
    for chunk in range(count):
        for kind in range(4):
            swap(chunk, kind).wait_send()
    relay.drain()


def hand_back(table, last, going, staying, norb, chips):
    chunks, slots, planes, sub, lanes = going.shape
    vmem = pl.BlockSpec(memory_space=pltpu.VMEM)
    smem = pl.BlockSpec(memory_space=pltpu.SMEM)
    dma = pltpu.SemaphoreType.DMA
    def room(*lead):
        return [pltpu.VMEM(lead + (planes, sub, lanes), jnp.float32)] * chunks
    wins = [pltpu.VMEM((slots, 6 * planes, sub, lanes), jnp.float32)] * chunks
    return pl.pallas_call(
        functools.partial(hand_back_kernel, chips),
        in_specs=[smem, smem, vmem, vmem],
        out_specs=vmem,
        out_shape=jax.ShapeDtypeStruct((norb, planes, chunks * sub, lanes), jnp.float32),
        scratch_shapes=wins + room(2 * slots + 1) + room(2, norb) + room(2, norb // 2)
        + room(2, norb) + room(2, norb // 2)
        + [dma((chunks, 4)), dma((chunks, 4)), dma((chunks, 2, 5)), dma((chunks, 2, 5))],
        compiler_params=pltpu.CompilerParams(
            collective_id=2, has_side_effects=True, vmem_limit_bytes=56 * 1024 * 1024
        ),
        name="hand_back",
    )(table, last, going, staying)


def slab_body(orbitals, anchors, pair_slots):
    groups, places = lax.axis_size("grp"), lax.axis_size("grid")
    norb_local, cells = orbitals.shape
    planes = cells // (B * B)
    each = PAIR_DEV * places
    assignment = deal_evenly(pair_slots, groups, each)
    pairs = assignment[lax.axis_index("grp")]
    offsets = anchors[pairs[:, 1]] - anchors[pairs[:, 0]]
    dx, dy, dz = offsets[:, 0], offsets[:, 1], offsets[:, 2]
    slot = lax.broadcasted_iota(jnp.int32, (each,), 0)
    rising = slot < each // 2
    second = jnp.where(rising, dx >= 0, dx <= 0)
    shift = jnp.where(second, dx, -dx)
    moved_id = jnp.where(second, pairs[:, 1], pairs[:, 0])
    fixed_id = jnp.where(second, pairs[:, 0], pairs[:, 1])
    terms = jnp.concatenate([fixed_id, moved_id])
    at = lax.broadcasted_iota(jnp.int32, (2 * each, 2 * each), 0)
    before = lax.broadcasted_iota(jnp.int32, (2 * each, 2 * each), 1)
    found = jnp.where((terms[:, None] == terms[None, :]) & (before < at), before, -1)
    prior = jnp.max(found, axis=1)
    prior = jnp.where(prior < 0, 2 * each, prior)
    norb = anchors.shape[0]
    orbit = lax.broadcasted_iota(jnp.int32, (norb, 2 * each), 0)
    index = lax.broadcasted_iota(jnp.int32, (norb, 2 * each), 1)
    last = jnp.max(jnp.where(terms[None, :] == orbit, index, -1), axis=1)
    last = jnp.where(last < 0, 2 * each, last)
    table = jnp.stack([
        moved_id, fixed_id,
        jnp.where(rising, 4 * planes, 0) - shift,
        second.astype(jnp.int32), dy, dz,
        jnp.where(second, 0, shift),
        jnp.where(rising, 0, 4 * planes) + shift,
        prior[:each], prior[each:],
    ])
    stacked = orbitals.reshape(norb_local, planes, ROWS, LANES)
    moved, fixed = bring(table, stacked, each, groups, places // 2)
    dens, partner = pair_up(table, moved, fixed)
    pot = solve_slabs(table, dens, places)
    going, staying = make_terms(table, pot, partner, moved, fixed)
    out = hand_back(table, last, going, staying, norb_local, places // 2)
    return out.reshape(norb_local, cells)


def slabs_fit(mesh):
    groups, places = mesh.shape["grp"], mesh.shape["grid"]
    return groups == 4 and places % 2 == 0 and 4 * (B // places) >= PAD


def solution(mesh):
    return jax.shard_map(
        slab_body if slabs_fit(mesh) else owner_body,
        mesh=mesh,
        in_specs=(P("grp", "grid"), P(), P()),
        out_specs=P("grp", "grid"),
        check_vma=False,
    )
```

```python
import functools
import math

import jax
import jax.numpy as jnp
from jax import lax
from jax.experimental import pallas as pl
from jax.experimental.pallas import tpu as pltpu
from jax.sharding import PartitionSpec as P

B = 64
PAIR_DEV = 2
ITERS = 3
MOST_CHUNKS = 2
LANES = 128
ROWS = B * B // LANES
PAD = 32
STEP = 4


def deal_evenly(pair_slots, owner_count, each_owner):
    flat_slots = pair_slots.reshape(-1, 2)
    filled = (flat_slots[:, 0] >= 0).astype(jnp.int32)
    position = jnp.cumsum(filled, dtype=jnp.int32) - filled
    wanted = lax.broadcasted_iota(jnp.int32, (owner_count, each_owner), 1) * owner_count
    wanted = (wanted + lax.broadcasted_iota(jnp.int32, (owner_count, each_owner), 0)).reshape(-1)
    matched = (position[None, :] == wanted[:, None]) & (filled[None, :] == 1)
    picked = jnp.sum(jnp.where(matched[:, :, None], flat_slots[None], 0), axis=1)
    return picked.reshape(owner_count, each_owner, 2)


def gather_kernel(ids_ref, src_ref, *out_refs):
    count, terms = out_refs[0].shape[:2]
    for slot, out_ref in enumerate(out_refs):
        def pick(dest, unused, slot=slot, out_ref=out_ref):
            for term in range(terms):
                out_ref[dest, term] = src_ref[ids_ref[(slot * count + dest) * terms + term]]
            return unused

        lax.fori_loop(0, count, pick, 0)


def gather_pieces(ids, pieces, slots, count):
    norb, rows, lanes = pieces.shape
    block = max(8, rows // 4)
    return pl.pallas_call(
        gather_kernel,
        grid_spec=pltpu.PrefetchScalarGridSpec(
            num_scalar_prefetch=1,
            grid=(rows // block,),
            in_specs=[pl.BlockSpec((norb, block, lanes), lambda i, ids: (0, i, 0))],
            out_specs=[pl.BlockSpec((count, 2, block, lanes), lambda i, ids: (0, 0, i, 0))] * slots,
        ),
        out_shape=[jax.ShapeDtypeStruct((count, 2, rows, lanes), jnp.float32)] * slots,
        cost_estimate=pl.CostEstimate(flops=0, bytes_accessed=8 * norb * rows * lanes, transcendentals=0),
        name="pick_pieces",
    )(ids, pieces)


def scatter_kernel(ids_ref, *refs):
    out_ref = refs[-1]
    out_ref[...] = jnp.zeros_like(out_ref)
    count, terms = refs[0].shape[:2]
    for slot, in_ref in enumerate(refs[:-1]):
        def add(dest, unused, slot=slot, in_ref=in_ref):
            for term in range(terms):
                orbit = ids_ref[(slot * count + dest) * terms + term]
                out_ref[orbit] = out_ref[orbit] + in_ref[dest, term]
            return unused

        lax.fori_loop(0, count, add, 0)


def scatter_pieces(ids, parts, norb):
    count, terms, rows, lanes = parts[0].shape
    block = max(8, rows // 4)
    return pl.pallas_call(
        scatter_kernel,
        grid_spec=pltpu.PrefetchScalarGridSpec(
            num_scalar_prefetch=1,
            grid=(rows // block,),
            in_specs=[pl.BlockSpec((count, terms, block, lanes), lambda i, ids: (0, 0, i, 0))] * len(parts),
            out_specs=pl.BlockSpec((norb, block, lanes), lambda i, ids: (0, i, 0)),
        ),
        out_shape=jax.ShapeDtypeStruct((norb, rows, lanes), jnp.float32),
        cost_estimate=pl.CostEstimate(flops=0, bytes_accessed=8 * norb * rows * lanes, transcendentals=0),
        name="add_pieces",
    )(ids, *parts)


def lane_ids(shape):
    return lax.broadcasted_iota(jnp.int32, shape, len(shape) - 1)


def shift_plane(plane, off_y, off_z):
    shape = plane.shape
    lane = lane_ids(shape)
    row = lax.broadcasted_iota(jnp.int32, shape, 0)
    linear = off_y * B + off_z
    across = jnp.bitwise_and(linear, LANES - 1)
    down = jnp.right_shift(linear, 7)
    turned = pltpu.roll(plane, across, 1)
    near = pltpu.roll(turned, jnp.bitwise_and(down, ROWS - 1), 0)
    far = pltpu.roll(turned, jnp.bitwise_and(down + 1, ROWS - 1), 0)
    moved = jnp.where(lane >= across, near, far)
    from_y = row * 2 + jnp.right_shift(lane, 6) - off_y
    from_z = jnp.bitwise_and(lane, B - 1) - off_z
    inside = (from_y >= 0) & (from_y < B) & (from_z >= 0) & (from_z < B)
    return jnp.where(inside, moved, 0.0)


def operate_plane(before, plane, after):
    shape = plane.shape
    lane = lane_ids(shape)
    row = lax.broadcasted_iota(jnp.int32, shape, 0)
    z = jnp.bitwise_and(lane, B - 1)
    upper_z = jnp.where(z < B - 1, pltpu.roll(plane, LANES - 1, 1), 0.0)
    lower_z = jnp.where(z > 0, pltpu.roll(plane, 1, 1), 0.0)
    half = pltpu.roll(plane, B, 1)
    down = jnp.where(row > 0, pltpu.roll(half, 1, 0), 0.0)
    up = jnp.where(row < ROWS - 1, pltpu.roll(half, ROWS - 1, 0), 0.0)
    beside = (before + after) + (half + jnp.where(lane < B, down, up))
    return 6.0 * plane - beside - upper_z - lower_z


def fold(values):
    return jnp.sum(values.reshape(ROWS // 8, 8, LANES), axis=0)


def total(acc):
    return jnp.sum(acc, axis=(0, 1), keepdims=True)


def solve_kernel(info_ref, *refs):
    chunks = (len(refs) - 6) // 2
    in_refs, out_refs = refs[:chunks], refs[chunks : 2 * chunks]
    wide, partner, direction, resid, image, potential = refs[2 * chunks :]
    count, terms, rows, lanes = in_refs[0].shape
    each = rows // ROWS
    dx, dy, dz = info_ref[0], info_ref[1], info_ref[2]
    keep = jnp.where(info_ref[3] > 0, 1.0, 0.0).astype(jnp.float32)
    edge = jnp.zeros((PAD, ROWS, LANES), jnp.float32)
    wide[pl.ds(0, PAD)] = edge
    wide[pl.ds(PAD + B, PAD)] = edge
    direction[0] = edge[0]
    direction[B + 1] = edge[0]
    none = jnp.zeros((8, LANES), jnp.float32)

    def place(owner, chunk, i):
        return (owner * chunks + chunk) * each + i

    def load(owner, unused):
        for chunk in range(chunks):
            for i in range(each):
                wide[PAD + place(owner, chunk, i)] = in_refs[chunk][owner, 1, pl.ds(i * ROWS, ROWS)]
        return unused

    lax.fori_loop(0, count, load, 0)

    def start(owner, acc):
        for chunk in range(chunks):
            for i in range(each):
                x = place(owner, chunk, i)
                other = shift_plane(wide[PAD + x - dx], dy, dz)
                partner[x] = other
                density = in_refs[chunk][owner, 0, pl.ds(i * ROWS, ROWS)] * other
                direction[x + 1] = density
                resid[x] = density
                acc = acc + fold(density * density)
        return acc

    norm_now = total(lax.fori_loop(0, count, start, none))

    for turn in range(ITERS):
        def apply(block, acc):
            for i in range(STEP):
                x = block * STEP + i
                plane = direction[x + 1]
                result = operate_plane(direction[x], plane, direction[x + 2])
                image[x] = result
                acc = acc + fold(plane * result)
            return acc

        step_len = norm_now / total(lax.fori_loop(0, B // STEP, apply, none))

        if turn == ITERS - 1:
            break

        def advance(block, acc):
            for i in range(STEP):
                x = block * STEP + i
                moved = step_len * direction[x + 1]
                potential[x] = moved if turn == 0 else potential[x] + moved
                left = resid[x] - step_len * image[x]
                resid[x] = left
                acc = acc + fold(left * left)
            return acc

        norm_next = total(lax.fori_loop(0, B // STEP, advance, none))
        ratio = norm_next / norm_now

        def renew(block, unused):
            for i in range(STEP):
                x = block * STEP + i
                direction[x + 1] = resid[x] + ratio * direction[x + 1]
            return unused

        lax.fori_loop(0, B // STEP, renew, 0)
        norm_now = norm_next

    def finish(owner, unused):
        for chunk in range(chunks):
            for i in range(each):
                x = place(owner, chunk, i)
                found = (potential[x] + step_len * direction[x + 1]) * keep
                out_refs[chunk][owner, 0, pl.ds(i * ROWS, ROWS)] = found * partner[x]
                wide[PAD + x] = found * in_refs[chunk][owner, 0, pl.ds(i * ROWS, ROWS)]
        return unused

    lax.fori_loop(0, count, finish, 0)

    def give_back(owner, unused):
        for chunk in range(chunks):
            for i in range(each):
                x = place(owner, chunk, i)
                out_refs[chunk][owner, 1, pl.ds(i * ROWS, ROWS)] = shift_plane(wide[PAD + x + dx], -dy, -dz)
        return unused

    lax.fori_loop(0, count, give_back, 0)


def solve_pair(info, parts):
    box = (B, ROWS, LANES)
    vmem = pl.BlockSpec(memory_space=pltpu.VMEM)
    return pl.pallas_call(
        solve_kernel,
        in_specs=[pl.BlockSpec(memory_space=pltpu.SMEM)] + [vmem] * len(parts),
        out_specs=[vmem] * len(parts),
        out_shape=[jax.ShapeDtypeStruct(p.shape, jnp.float32) for p in parts],
        scratch_shapes=[
            pltpu.VMEM((B + 2 * PAD, ROWS, LANES), jnp.float32),
            pltpu.VMEM(box, jnp.float32),
            pltpu.VMEM((B + 2, ROWS, LANES), jnp.float32),
            pltpu.VMEM(box, jnp.float32),
            pltpu.VMEM(box, jnp.float32),
            pltpu.VMEM(box, jnp.float32),
        ],
        compiler_params=pltpu.CompilerParams(vmem_limit_bytes=32 * 1024 * 1024),
        cost_estimate=pl.CostEstimate(flops=0, bytes_accessed=40 * 1024 * 1024, transcendentals=0),
        name="solve_pair",
    )(info, *parts)


def owner_body(orbitals, anchors, pair_slots):
    grid_count = lax.axis_size("grid")
    owner_count = lax.axis_size("grp") * grid_count
    group_idx = lax.axis_index("grp")
    place_idx = lax.axis_index("grid")
    assignment = deal_evenly(pair_slots, owner_count, PAIR_DEV)
    slots = assignment.shape[1]
    filled = assignment[..., 0] >= 0
    safe_ids = jnp.maximum(assignment, 0)
    group_table = lax.dynamic_slice_in_dim(safe_ids, group_idx * grid_count, grid_count, 0)
    ids = jnp.transpose(group_table, (1, 0, 2)).reshape(-1)
    owner_idx = group_idx * grid_count + place_idx
    own_pairs = safe_ids[owner_idx]
    offsets = anchors[own_pairs[:, 1]] - anchors[own_pairs[:, 0]]
    info = jnp.concatenate([offsets, filled[owner_idx].astype(jnp.int32)[:, None]], axis=1)

    norb_local, cells = orbitals.shape
    stacked = orbitals.reshape(norb_local, cells // LANES, LANES)
    chunks = math.gcd(MOST_CHUNKS, cells // (B * B))
    rows = stacked.shape[1] // chunks
    arrived = [[None] * chunks for _ in range(slots)]
    for chunk in range(chunks):
        pieces = lax.all_gather(stacked[:, chunk * rows : (chunk + 1) * rows], "grp", axis=0, tiled=True)
        outgoing = gather_pieces(ids, pieces, slots, grid_count)
        for slot in range(slots):
            arrived[slot][chunk] = lax.all_to_all(outgoing[slot], "grid", split_axis=0, concat_axis=0, tiled=True)
    returned = []
    for slot in range(slots):
        terms = solve_pair(info[slot], arrived[slot])
        returned.append(
            [lax.all_to_all(t, "grid", split_axis=0, concat_axis=0, tiled=True) for t in terms]
        )
    results = []
    for chunk in range(chunks):
        summed = scatter_pieces(ids, [r[chunk] for r in returned], anchors.shape[0])
        results.append(lax.psum_scatter(summed, "grp", scatter_dimension=0, tiled=True))
    return jnp.concatenate(results, axis=1).reshape(norb_local, cells)


MESH = pl.DeviceIdType.MESH
HALO = 3
WAVES = 4
SUB = 8


def remote(src, dst, send_sem, recv_sem, device):
    return pltpu.make_async_remote_copy(
        src_ref=src, dst_ref=dst, send_sem=send_sem, recv_sem=recv_sem, device_id=device, device_id_type=MESH
    )


def spot():
    grp = lax.axis_index("grp")
    place = lax.axis_index("grid")
    across = grp + 1 - 2 * lax.rem(grp, 2)
    along = lax.rem(grp + 2, 4)
    corner = lax.rem(across + 2, 4)
    return grp, place, across, along, corner


def greet(chips, wide=False):
    grp, place, across, along, corner = spot()
    chip = place // 2
    core = lax.rem(place, 2)
    barrier = pltpu.get_barrier_semaphore()
    peers = [(across, place), (along, place), (grp, 2 * chip + 1 - core)] + ([(corner, place)] if wide else [])
    for device in peers:
        pl.semaphore_signal(barrier, inc=1, device_id=device, device_id_type=MESH)

    @pl.when(chip > 0)
    def below():
        pl.semaphore_signal(barrier, inc=1, device_id=(grp, place - 2), device_id_type=MESH)

    @pl.when(chip < chips - 1)
    def above():
        pl.semaphore_signal(barrier, inc=1, device_id=(grp, place + 2), device_id_type=MESH)

    ends = jnp.where(chip > 0, 1, 0) + jnp.where(chip < chips - 1, 1, 0)
    pl.semaphore_wait(barrier, len(peers) + ends)


class Relay:
    def __init__(self, wins, send_sem, recv_sem, signs, chips, far, mid):
        self.wins, self.send_sem, self.recv_sem, self.signs, self.chips = wins, send_sem, recv_sem, signs, chips
        self.grp, self.place = lax.axis_index("grp"), lax.axis_index("grid")
        self.chip = self.place // 2
        self.core = lax.rem(self.place, 2)
        self.half = wins[0].shape[0] // 2
        self.planes = wins[0].shape[1] // 6
        self.far, self.mid = far, mid

    def offset(self, sign, hop):
        return 2 * self.planes * (2 - hop if sign > 0 else hop)

    def region(self, chunk, side, hop, core, size):
        start = self.offset(self.signs[side], hop) + self.planes * core
        return self.wins[chunk].at[pl.ds(side * self.half, size), pl.ds(start, self.planes)]

    def comes(self, side, hop):
        source = self.chip - self.signs[side] * hop
        return source >= 0 if self.signs[side] > 0 else source < self.chips

    def goes(self, side, hop):
        source = self.chip + self.signs[side] - self.signs[side] * hop
        if self.signs[side] > 0:
            return (self.chip + 1 < self.chips) & (source >= 0)
        return (self.chip - 1 >= 0) & (source < self.chips)

    def spans(self, side, hop, core, act):
        if hop == 0:
            act(self.half)
        elif hop == 2:
            act(self.far)
        elif self.mid == self.half:
            act(self.half)
        else:
            near = 1 if self.signs[side] > 0 else 0

            @pl.when(core == near)
            def whole():
                act(self.half)

            @pl.when(core != near)
            def some():
                act(self.mid)

    def onward(self, chunk, side, hop, size, here=None):
        source = self.region(chunk, side, hop - 1 if here is None else here, self.core, size)
        there = self.region(chunk, side, hop, self.core, size)
        return remote(
            source, there, self.send_sem.at[chunk, side, hop - 1], self.recv_sem.at[chunk, side, hop - 1],
            (self.grp, self.place + 2 * self.signs[side]),
        )

    def beside(self, chunk, side, hop, core, size):
        part = self.region(chunk, side, hop, core, size)
        return remote(
            part, part, self.send_sem.at[chunk, side, 2 + hop], self.recv_sem.at[chunk, side, 2 + hop],
            (self.grp, 2 * self.chip + 1 - self.core),
        )

    def clear(self):
        for side in range(2):
            for hop in (1, 2):
                start = self.offset(self.signs[side], hop)

                @pl.when(jnp.logical_not(self.comes(side, hop)))
                def fill(side=side, start=start):
                    for win in self.wins:
                        def zero(slot, unused, win=win):
                            win[slot, pl.ds(start, 2 * self.planes)] = jnp.zeros(
                                (2 * self.planes,) + win.shape[2:], jnp.float32
                            )
                            return unused

                        lax.fori_loop(side * self.half, (side + 1) * self.half, zero, 0)

    def pass_on(self, chunk, side, hop):
        @pl.when(self.goes(side, hop))
        def go():
            self.spans(side, hop, self.core, lambda size: self.onward(chunk, side, hop, size).start())

    def begin(self, chunk):
        for side in range(2):
            self.pass_on(chunk, side, 1)
            self.beside(chunk, side, 0, self.core, self.half).start()

    def take(self, chunk, side, hop):
        @pl.when(self.comes(side, hop))
        def got():
            def act(size):
                self.onward(chunk, side, hop, size, hop).wait_recv()

            self.spans(side, hop, self.core, act)

        if hop < 2:
            self.pass_on(chunk, side, hop + 1)

        @pl.when(self.comes(side, hop))
        def share():
            self.spans(side, hop, self.core, lambda size: self.beside(chunk, side, hop, self.core, size).start())

    def first(self, chunk):
        for side in range(2):
            self.take(chunk, side, 1)

    def second(self, chunk):
        for side in range(2):
            self.take(chunk, side, 2)

    def settle(self, chunk):
        other = 1 - self.core
        for side in range(2):
            self.beside(chunk, side, 0, other, self.half).wait_recv()
            for hop in (1, 2):
                @pl.when(self.comes(side, hop))
                def got(side=side, hop=hop):
                    self.spans(side, hop, other, lambda size: self.beside(chunk, side, hop, other, size).wait_recv())

    def drain(self):
        for chunk in range(len(self.wins)):
            for side in range(2):
                self.beside(chunk, side, 0, self.core, self.half).wait_send()
                for hop in (1, 2):
                    @pl.when(self.comes(side, hop))
                    def sent(chunk=chunk, side=side, hop=hop):
                        self.spans(
                            side, hop, self.core,
                            lambda size: self.beside(chunk, side, hop, self.core, size).wait_send(),
                        )

                    @pl.when(self.goes(side, hop))
                    def passed(chunk=chunk, side=side, hop=hop):
                        self.spans(
                            side, hop, self.core, lambda size: self.onward(chunk, side, hop, size).wait_send()
                        )


def bring_kernel(chips, tbl, orb, moved, fixed, *scratch):
    count = moved.shape[0]
    pools, wins = scratch[:count], scratch[count : 2 * count]
    own_sem, xy_send, xy_recv, z_send, z_recv = scratch[2 * count :]
    grp, place, across, along, corner = spot()
    core = lax.rem(place, 2)
    norb, planes = orb.shape[:2]
    part = norb // 2
    slots = moved.shape[1]
    relay = Relay(wins, z_send, z_recv, (1, -1), chips, slots // 2, slots // 2)

    def block(chunk, owner, start, size):
        return pools[chunk].at[pl.ds(owner * norb + start, size)]

    def stage(chunk):
        return pltpu.make_async_copy(
            orb.at[:, :, pl.ds(chunk * SUB, SUB)], block(chunk, grp, 0, norb), own_sem.at[chunk]
        )

    def hop(chunk, kind, owner, start, size, target):
        ref = block(chunk, owner, start, size)
        return remote(ref, ref, xy_send.at[chunk, kind], xy_recv.at[chunk, kind], (target, place))

    def direct(chunk, owners):
        return hop(chunk, 0, owners[0], 0, norb, across), hop(chunk, 1, owners[1], 0, norb, along)

    def turned(chunk, owners):
        return hop(chunk, 2, owners[0], 0, part, along), hop(chunk, 3, owners[1], part, part, across)

    for chunk in range(count):
        stage(chunk).start()
    greet(chips)
    relay.clear()

    def send_own(chunk):
        stage(chunk).wait()
        for copy in direct(chunk, (grp, grp)):
            copy.start()

    send_own(0)
    send_own(1)
    for step in range(count + 4):
        if step < count:
            for copy in direct(step, (across, along)):
                copy.wait_recv()
            for copy in turned(step, (across, along)):
                copy.start()
            if step + 2 < count:
                send_own(step + 2)
        chunk = step - 1
        if 0 <= chunk < count:
            for copy in turned(chunk, (corner, corner)):
                copy.wait_recv()
            for side in range(2):
                start = relay.offset(relay.signs[side], 0) + planes * core

                def pick(slot, unused, start=start, chunk=chunk):
                    wins[chunk][slot, pl.ds(start, planes)] = pools[chunk][tbl[0, slot]]
                    fixed[chunk, slot] = pools[chunk][tbl[1, slot]]
                    return unused

                lax.fori_loop(side * (slots // 2), (side + 1) * (slots // 2), pick, 0)
            relay.begin(chunk)
        chunk = step - 2
        if 0 <= chunk < count:
            relay.first(chunk)
        chunk = step - 3
        if 0 <= chunk < count:
            relay.second(chunk)
        chunk = step - 4
        if 0 <= chunk < count:
            relay.settle(chunk)

            def choose(slot, unused, chunk=chunk):
                first = tbl[2, slot] + planes * core
                for plane in range(planes):
                    moved[chunk, slot, plane] = wins[chunk][slot, first + plane]
                return unused

            lax.fori_loop(0, slots, choose, 0)
    for chunk in range(count):
        for copy in direct(chunk, (grp, grp)) + turned(chunk, (across, along)):
            copy.wait_send()
    relay.drain()


def bring(table, stacked, slots, groups, chips):
    norb, planes, rows, lanes = stacked.shape
    chunks = rows // SUB
    vmem = pl.BlockSpec(memory_space=pltpu.VMEM)
    dma = pltpu.SemaphoreType.DMA
    shape = jax.ShapeDtypeStruct((chunks, slots, planes, SUB, lanes), jnp.float32)
    return pl.pallas_call(
        functools.partial(bring_kernel, chips),
        in_specs=[pl.BlockSpec(memory_space=pltpu.SMEM), pl.BlockSpec(memory_space=pl.ANY)],
        out_specs=[vmem, vmem],
        out_shape=[shape, shape],
        scratch_shapes=[pltpu.VMEM((groups * norb, planes, SUB, lanes), jnp.float32)] * chunks
        + [pltpu.VMEM((slots, 6 * planes, SUB, lanes), jnp.float32)] * chunks
        + [dma((chunks,)), dma((chunks, 4)), dma((chunks, 4)), dma((chunks, 2, 5)), dma((chunks, 2, 5))],
        compiler_params=pltpu.CompilerParams(
            collective_id=0, has_side_effects=True, vmem_limit_bytes=48 * 1024 * 1024
        ),
        name="bring",
    )(table, stacked)


def pair_kernel(tbl, moved, fixed, dens, partner):
    def go(slot, unused):
        second = tbl[3, slot] > 0
        dy, dz = tbl[4, slot], tbl[5, slot]
        for x in range(moved.shape[2]):
            left = moved[:, slot, x].reshape(ROWS, LANES)
            right = fixed[:, slot, x].reshape(ROWS, LANES)
            other = shift_plane(jnp.where(second, left, right), dy, dz)
            dens[slot, x] = jnp.where(second, right, left) * other
            partner[slot, x] = other
        return unused

    lax.fori_loop(0, moved.shape[1], go, 0)


def pair_up(table, moved, fixed):
    chunks, slots, planes, sub, lanes = moved.shape
    vmem = pl.BlockSpec(memory_space=pltpu.VMEM)
    shape = jax.ShapeDtypeStruct((slots, planes, ROWS, lanes), jnp.float32)
    return pl.pallas_call(
        pair_kernel,
        in_specs=[pl.BlockSpec(memory_space=pltpu.SMEM), vmem, vmem],
        out_specs=[vmem, vmem],
        out_shape=[shape, shape],
        compiler_params=pltpu.CompilerParams(vmem_limit_bytes=24 * 1024 * 1024),
        name="pair_up",
    )(table, moved, fixed)


def inner(plane):
    shape = plane.shape
    lane = lane_ids(shape)
    row = lax.broadcasted_iota(jnp.int32, shape, 0)
    z = jnp.bitwise_and(lane, B - 1)
    upper_z = jnp.where(z < B - 1, pltpu.roll(plane, LANES - 1, 1), 0.0)
    lower_z = jnp.where(z > 0, pltpu.roll(plane, 1, 1), 0.0)
    half = pltpu.roll(plane, B, 1)
    down = jnp.where(row > 0, pltpu.roll(half, 1, 0), 0.0)
    up = jnp.where(row < ROWS - 1, pltpu.roll(half, ROWS - 1, 0), 0.0)
    return 6.0 * plane - ((half + jnp.where(lane < B, down, up)) + (upper_z + lower_z))


def krylov_weights(m):
    a0 = m[0] / m[1]
    rr1 = a0 * a0 * m[2] - m[0]
    p, q = 1.0 + rr1 / m[0], -a0
    a1 = rr1 / (p * p * m[1] + 2.0 * p * q * m[2] + q * q * m[3])
    s1, s2 = -a0 - a1 * p, -a1 * q
    rr2 = (m[0] + s1 * s1 * m[2] + s2 * s2 * m[4]) + 2.0 * (s1 * m[1] + s2 * m[2] + s1 * s2 * m[3])
    b1 = rr2 / rr1
    e0, e1, e2 = 1.0 + b1 * p, s1 + b1 * q, s2
    bend = e0 * e0 * m[1] + e1 * e1 * m[3] + e2 * e2 * m[5]
    a2 = rr2 / (bend + 2.0 * (e0 * e1 * m[2] + e0 * e2 * m[3] + e1 * e2 * m[4]))
    return a0 + a1 * p + a2 * e0, a1 * q + a2 * e1, a2 * e2


def solve_slabs_kernel(places, tbl, dens, pot, wide, one, two, sums, gathered, weights, h_send, h_recv, s_send, s_recv):
    grp, place = lax.axis_index("grp"), lax.axis_index("grid")
    slots, planes = dens.shape[:2]
    first, last = HALO, HALO + planes - 1
    each = slots // WAVES
    barrier = pltpu.get_barrier_semaphore()
    for step in range(1, places):
        pl.semaphore_signal(
            barrier, inc=1, device_id=(grp, lax.rem(place + step, places)), device_id_type=MESH
        )
    pl.semaphore_wait(barrier, places - 1)

    def rise(wave):
        return remote(
            dens.at[pl.ds(wave * each, each), pl.ds(planes - HALO, HALO)],
            wide.at[pl.ds(wave * each, each), pl.ds(0, HALO)],
            h_send.at[wave, 0], h_recv.at[wave, 0], (grp, lax.rem(place + 1, places)),
        )

    def sink(wave):
        return remote(
            dens.at[pl.ds(wave * each, each), pl.ds(0, HALO)],
            wide.at[pl.ds(wave * each, each), pl.ds(HALO + planes, HALO)],
            h_send.at[wave, 1], h_recv.at[wave, 1], (grp, lax.rem(place + places - 1, places)),
        )

    lowest, highest = place == 0, place == places - 1
    for wave in range(WAVES):
        @pl.when(jnp.logical_not(highest))
        def send_up(wave=wave):
            rise(wave).start()

        @pl.when(jnp.logical_not(lowest))
        def send_down(wave=wave):
            sink(wave).start()

    blank = jnp.zeros((HALO, ROWS, LANES), jnp.float32)

    def copy_in(slot, unused):
        wide[slot, pl.ds(HALO, planes)] = dens[slot]
        one[slot, 1] = blank[0]
        one[slot, last + 3] = blank[0]
        one[slot, 0] = blank[0]
        return unused

    lax.fori_loop(0, slots, copy_in, 0)

    @pl.when(lowest)
    def no_below():
        def fill(slot, unused):
            wide[slot, pl.ds(0, HALO)] = blank
            return unused

        lax.fori_loop(0, slots, fill, 0)

    @pl.when(highest)
    def no_above():
        def fill(slot, unused):
            wide[slot, pl.ds(HALO + planes, HALO)] = blank
            return unused

        lax.fori_loop(0, slots, fill, 0)

    lane = lax.broadcasted_iota(jnp.int32, (1, LANES), 1)
    none = jnp.zeros((8, LANES), jnp.float32)

    def row_of(parts):
        row = jnp.zeros((1, LANES), jnp.float32)
        for at, part in parts:
            row = row + jnp.where(lane == at, total(part), 0.0)
        return row

    def work(slot, unused):
        low, high = tbl[6, slot], tbl[6, slot] + B

        def live(e):
            x = planes * place + e - HALO
            return jnp.where((x >= low) & (x < high), 1.0, 0.0).astype(jnp.float32)

        m0, m1, m2, m3, m4, m5 = none, none, none, none, none, none
        for e in range(first - 1, last + 3):
            value = live(e) * (inner(wide[slot, e]) - (wide[slot, e - 1] + wide[slot, e + 1]))
            one[slot, e] = value
            if first <= e <= last:
                source = wide[slot, e]
                m0 = m0 + fold(source * source)
                m1 = m1 + fold(source * value)
                m2 = m2 + fold(value * value)
        bent = None
        for e in range(first, last + 2):
            value = live(e) * (inner(one[slot, e]) - (one[slot, e - 1] + one[slot, e + 1]))
            two[slot, e] = value
            if e > first:
                m5 = m5 - 2.0 * fold(value * two[slot, e - 1])
            if e <= last:
                m3 = m3 + fold(one[slot, e] * value)
                m4 = m4 + fold(value * value)
                m5 = m5 + fold(value * inner(value))
        sums[pl.ds(slot, 1)] = row_of(enumerate((m0, m1, m2, m3, m4, m5)))
        return unused

    def rim(slot, spots, pairs):
        low, high = tbl[6, slot], tbl[6, slot] + B
        m2, m3, m4, m5 = none, none, none, none
        for e, fresh in spots:
            if fresh:
                x = planes * place + e - HALO
                alive = jnp.where((x >= low) & (x < high), 1.0, 0.0).astype(jnp.float32)
                two[slot, e] = alive * (inner(one[slot, e]) - (one[slot, e - 1] + one[slot, e + 1]))
        for e, fresh in spots:
            value, before = two[slot, e], one[slot, e]
            m2 = m2 + fold(before * before)
            m3 = m3 + fold(before * value)
            m4 = m4 + fold(value * value)
            m5 = m5 + fold(value * inner(value))
        for e in pairs:
            m5 = m5 - 2.0 * fold(two[slot, e] * two[slot, e + 1])
        sums[pl.ds(slot, 1)] = sums[pl.ds(slot, 1)] + row_of(((2, m2), (3, m3), (4, m4), (5, m5)))

    for wave in range(WAVES):
        @pl.when(jnp.logical_not(lowest))
        def got_below(wave=wave):
            rise(wave).wait_recv()

        @pl.when(jnp.logical_not(highest))
        def got_above(wave=wave):
            sink(wave).wait_recv()

        lax.fori_loop(wave * each, (wave + 1) * each, work, 0)

    @pl.when(lowest)
    def rim_below():
        def go(slot, unused):
            rim(slot, ((first - 2, True), (first - 1, True)), (first - 2, first - 1))
            return unused

        lax.fori_loop(0, slots, go, 0)

    @pl.when(highest)
    def rim_above():
        def go(slot, unused):
            rim(slot, ((last + 1, False), (last + 2, True)), (last + 1,))
            return unused

        lax.fori_loop(0, slots, go, 0)

    def tell(step):
        return remote(
            sums, gathered.at[place], s_send.at[step - 1], s_recv.at[step - 1],
            (grp, lax.rem(place + step, places)),
        )

    def hear(step):
        source = lax.rem(place + places - step, places)
        return remote(
            sums, gathered.at[source], s_send.at[step - 1], s_recv.at[step - 1],
            (grp, lax.rem(place + step, places)),
        )

    for step in range(1, places):
        tell(step).start()
    gathered[place] = sums[...]
    for step in range(1, places):
        hear(step).wait_recv()
    whole = gathered[0]
    for at in range(1, places):
        whole = whole + gathered[at]
    lanes = lax.broadcasted_iota(jnp.int32, whole.shape, 1)
    moments = [jnp.sum(jnp.where(lanes == at, whole, 0.0), axis=1, keepdims=True) for at in range(6)]
    for at, weight in enumerate(krylov_weights(moments)):
        weights[at] = jnp.broadcast_to(weight, whole.shape)

    def finish(slot, unused):
        w0, w1, w2 = [weights[at, pl.ds(slot, 1)] for at in range(3)]
        for x in range(planes):
            e = x + HALO
            pot[slot, x] = w0 * wide[slot, e] + w1 * one[slot, e] + w2 * two[slot, e]
        return unused

    lax.fori_loop(0, slots, finish, 0)
    for wave in range(WAVES):
        @pl.when(jnp.logical_not(highest))
        def sent_up(wave=wave):
            rise(wave).wait_send()

        @pl.when(jnp.logical_not(lowest))
        def sent_down(wave=wave):
            sink(wave).wait_send()

    for step in range(1, places):
        tell(step).wait_send()


def solve_slabs(table, dens, places, ident):
    slots, planes, rows, lanes = dens.shape
    vmem = pl.BlockSpec(memory_space=pltpu.VMEM)
    dma = pltpu.SemaphoreType.DMA
    tall = pltpu.VMEM((slots, planes + 2 * HALO, rows, lanes), jnp.float32)
    return pl.pallas_call(
        functools.partial(solve_slabs_kernel, places),
        in_specs=[pl.BlockSpec(memory_space=pltpu.SMEM), vmem],
        out_specs=vmem,
        out_shape=jax.ShapeDtypeStruct(dens.shape, jnp.float32),
        scratch_shapes=[
            tall, tall, tall,
            pltpu.VMEM((slots, lanes), jnp.float32),
            pltpu.VMEM((places, slots, lanes), jnp.float32),
            pltpu.VMEM((3, slots, lanes), jnp.float32),
            dma((WAVES, 2)), dma((WAVES, 2)), dma((places - 1,)), dma((places - 1,)),
        ],
        compiler_params=pltpu.CompilerParams(
            collective_id=ident, has_side_effects=True, vmem_limit_bytes=40 * 1024 * 1024
        ),
        name="solve_slabs",
    )(table, dens)


def term_kernel(tbl, pot, partner, moved, fixed, going, staying):
    chunks = going.shape[0]

    def go(slot, unused):
        second = tbl[3, slot] > 0
        dy, dz = tbl[4, slot], tbl[5, slot]
        for x in range(pot.shape[1]):
            found = pot[slot, x]
            left = moved[:, slot, x].reshape(ROWS, LANES)
            right = fixed[:, slot, x].reshape(ROWS, LANES)
            term_a = found * partner[slot, x]
            term_b = shift_plane(found * jnp.where(second, right, left), -dy, -dz)
            going[:, slot, x] = jnp.where(second, term_b, term_a).reshape(chunks, SUB, LANES)
            staying[:, slot, x] = jnp.where(second, term_a, term_b).reshape(chunks, SUB, LANES)
        return unused

    lax.fori_loop(0, pot.shape[0], go, 0)


def make_terms(table, pot, partner, moved, fixed):
    vmem = pl.BlockSpec(memory_space=pltpu.VMEM)
    shape = jax.ShapeDtypeStruct(moved.shape, jnp.float32)
    return pl.pallas_call(
        term_kernel,
        in_specs=[pl.BlockSpec(memory_space=pltpu.SMEM)] + [vmem] * 4,
        out_specs=[vmem, vmem],
        out_shape=[shape, shape],
        compiler_params=pltpu.CompilerParams(vmem_limit_bytes=24 * 1024 * 1024),
        name="make_terms",
    )(table, pot, partner, moved, fixed)


def hand_back_kernel(chips, tbl, last, going, staying, out, *scratch):
    count, slots = going.shape[:2]
    wins, chains, outs1, outs2, ins1, ins2 = [scratch[i * count : (i + 1) * count] for i in range(6)]
    xy_send, xy_recv, z_send, z_recv = scratch[6 * count :]
    grp, place, across, along, corner = spot()
    core = lax.rem(place, 2)
    norb, planes = out.shape[:2]
    part = norb // 2
    relay = Relay(wins, z_send, z_recv, (-1, 1), chips, slots // 2, slots // 2)
    greet(chips)
    relay.clear()

    def start(chunk):
        for side in range(2):
            at = relay.offset(relay.signs[side], 0) + planes * core

            def place_in(slot, unused, at=at):
                wins[chunk][slot, pl.ds(at, planes)] = going[chunk, slot]
                return unused

            lax.fori_loop(side * (slots // 2), (side + 1) * (slots // 2), place_in, 0)
        relay.begin(chunk)

    def swap(chunk, kind):
        src = (outs1 if kind < 2 else outs2)[chunk].at[kind % 2]
        dst = (ins1 if kind < 2 else ins2)[chunk].at[kind % 2]
        target = (across, along, along, across)[kind]
        return remote(src, dst, xy_send.at[chunk, kind], xy_recv.at[chunk, kind], (target, place))

    start(0)
    start(1)
    for step in range(count + 4):
        if step < count:
            relay.first(step)
            if step + 2 < count:
                start(step + 2)
        chunk = step - 1
        if 0 <= chunk < count:
            relay.second(chunk)
        chunk = step - 2
        if 0 <= chunk < count:
            relay.settle(chunk)
            chain = chains[chunk]
            chain[2 * slots] = jnp.zeros(chain.shape[1:], jnp.float32)

            def link_fixed(slot, unused, chain=chain, chunk=chunk):
                chain[slot] = staying[chunk, slot] + chain[tbl[8, slot]]
                return unused

            def link_moved(slot, unused, chain=chain, chunk=chunk):
                first = tbl[7, slot] + planes * core
                for plane in range(planes):
                    chain[slots + slot, plane] = wins[chunk][slot, first + plane] + chain[tbl[9, slot], plane]
                return unused

            lax.fori_loop(0, slots, link_fixed, 0)
            lax.fori_loop(0, slots, link_moved, 0)

            def pack(i, unused, chain=chain, chunk=chunk):
                outs1[chunk][0, i] = chain[last[across * norb + i]]
                outs1[chunk][0, part + i] = chain[last[corner * norb + i]]
                outs1[chunk][1, i] = chain[last[along * norb + part + i]]
                outs1[chunk][1, part + i] = chain[last[corner * norb + part + i]]
                return unused

            lax.fori_loop(0, part, pack, 0)
            swap(chunk, 0).start()
            swap(chunk, 1).start()
        chunk = step - 3
        if 0 <= chunk < count:
            chain = chains[chunk]
            swap(chunk, 0).wait_recv()

            def add_across(i, unused, chain=chain, chunk=chunk):
                outs2[chunk][0, i] = ins1[chunk][0, part + i] + chain[last[along * norb + i]]
                return unused

            lax.fori_loop(0, part, add_across, 0)
            swap(chunk, 2).start()
            swap(chunk, 1).wait_recv()

            def add_along(i, unused, chain=chain, chunk=chunk):
                outs2[chunk][1, i] = ins1[chunk][1, part + i] + chain[last[across * norb + part + i]]
                return unused

            lax.fori_loop(0, part, add_along, 0)
            swap(chunk, 3).start()
        chunk = step - 4
        if 0 <= chunk < count:
            chain = chains[chunk]
            swap(chunk, 2).wait_recv()
            swap(chunk, 3).wait_recv()
            for side in range(2):
                def keep(i, unused, side=side, chain=chain, chunk=chunk):
                    orbit = side * part + i
                    found = ins1[chunk][side, i] + ins2[chunk][side, i]
                    out[orbit, :, pl.ds(chunk * SUB, SUB)] = found + chain[last[grp * norb + orbit]]
                    return unused

                lax.fori_loop(0, part, keep, 0)
    for chunk in range(count):
        for kind in range(4):
            swap(chunk, kind).wait_send()
    relay.drain()


def hand_back(table, last, going, staying, norb, chips):
    chunks, slots, planes, sub, lanes = going.shape
    vmem = pl.BlockSpec(memory_space=pltpu.VMEM)
    smem = pl.BlockSpec(memory_space=pltpu.SMEM)
    dma = pltpu.SemaphoreType.DMA
    def room(*lead):
        return [pltpu.VMEM(lead + (planes, sub, lanes), jnp.float32)] * chunks
    wins = [pltpu.VMEM((slots, 6 * planes, sub, lanes), jnp.float32)] * chunks
    return pl.pallas_call(
        functools.partial(hand_back_kernel, chips),
        in_specs=[smem, smem, vmem, vmem],
        out_specs=vmem,
        out_shape=jax.ShapeDtypeStruct((norb, planes, chunks * sub, lanes), jnp.float32),
        scratch_shapes=wins + room(2 * slots + 1) + room(2, norb) + room(2, norb // 2)
        + room(2, norb) + room(2, norb // 2)
        + [dma((chunks, 4)), dma((chunks, 4)), dma((chunks, 2, 5)), dma((chunks, 2, 5))],
        compiler_params=pltpu.CompilerParams(
            collective_id=2, has_side_effects=True, vmem_limit_bytes=56 * 1024 * 1024
        ),
        name="hand_back",
    )(table, last, going, staying)


def plan_kernel(cap, planes, me_ref, anchors, pairs, tbl, links, fits, spots, lists, tallies, counts):
    groups = 4
    orbits = anchors.shape[0] // 3
    local = orbits // groups
    entries = pairs.shape[0] // 2
    each = tbl.shape[1]
    half = each // 2
    extra = (groups - 1) * cap
    final = extra
    prior = final + local + extra
    ends = prior + extra
    worst = 1 << 20
    me = me_ref[0]

    def reset(o, unused):
        for h in range(groups):
            spots[h * orbits + o] = jnp.where(o // local == h, o - h * local, -1)
        return unused

    lax.fori_loop(0, orbits, reset, 0)
    for i in range(2 * groups):
        tallies[i] = 0
    for i in range(groups * groups):
        counts[i] = 0

    def clean(i, unused):
        links[i] = 0
        links[prior + i] = extra
        return unused

    lax.fori_loop(0, extra, clean, 0)

    def close(i, unused):
        links[final + i] = 2 * each
        return unused

    lax.fori_loop(0, local + extra, close, 0)

    def close_own(i, unused):
        links[ends + i] = extra
        return unused

    lax.fori_loop(0, local, close_own, 0)

    def sort(i, tails):
        a, b = pairs[2 * i], pairs[2 * i + 1]
        filled = a >= 0
        reach = jnp.abs(anchors[3 * jnp.maximum(b, 0)] - anchors[3 * jnp.maximum(a, 0)])
        kind = jnp.where(reach > 2 * planes, 0, jnp.where(reach > planes, 1, 2))
        tail = jnp.where(kind == 0, tails[0], jnp.where(kind == 1, tails[1], tails[2]))

        @pl.when(filled)
        def put():
            lists[kind * entries + tail] = i

        return tuple(tails[k] + jnp.where(filled & (kind == k), 1, 0) for k in range(3))

    zero = jnp.int32(0)
    tails = lax.fori_loop(0, entries, sort, (zero, zero, zero))
    fits[0] = 1

    for kind, limit in enumerate((half // 2, 3 * half // 4, half)):
        def deal(i, unused, kind=kind, limit=limit):
            entry = lists[kind * entries + i]
            a, b = pairs[2 * entry], pairs[2 * entry + 1]
            group_a, group_b = a // local, b // local
            best, column, side, slot = jnp.int32(worst), zero, zero, zero
            for h in range(groups):
                new_a, new_b = spots[h * orbits + a] < 0, spots[h * orbits + b] < 0
                need_a = jnp.where(new_a, counts[h * groups + jnp.bitwise_xor(group_a, h)] + 1, 0)
                need_b = jnp.where(new_b, counts[h * groups + jnp.bitwise_xor(group_b, h)] + 1, 0)
                need_b = need_b + jnp.where(new_a & new_b & (group_a == group_b), 1, 0)
                need = jnp.maximum(need_a, need_b)
                up, down = tallies[2 * h], tallies[2 * h + 1]
                taken = jnp.minimum(up, down)
                cost = jnp.where(new_a, 2, 0) + jnp.where(new_b, 2, 0) + need + taken
                score = jnp.where((taken < limit) & (need <= cap), cost, worst)
                better = score < best
                best = jnp.where(better, score, best)
                column = jnp.where(better, h, column)
                side = jnp.where(better, jnp.where(down < up, 1, 0), side)
                slot = jnp.where(better, taken, slot)

            @pl.when(best >= worst)
            def fail():
                fits[0] = 0

            @pl.when(best < worst)
            def seat():
                tallies[2 * column + side] = slot + 1
                for orbit, group in ((a, group_a), (b, group_b)):
                    @pl.when(spots[column * orbits + orbit] < 0)
                    def fetch(orbit=orbit, group=group):
                        turn = jnp.bitwise_xor(group, column)
                        taken = counts[column * groups + turn]
                        spots[column * orbits + orbit] = local + (turn - 1) * cap + taken
                        counts[column * groups + turn] = taken + 1

                        @pl.when(group == me)
                        def note():
                            links[(turn - 1) * cap + taken] = orbit - group * local

                @pl.when(column == me)
                def fill():
                    at = side * half + slot
                    spot_a, spot_b = spots[column * orbits + a], spots[column * orbits + b]
                    dx = anchors[3 * b] - anchors[3 * a]
                    rising = side == 0
                    second = jnp.where(rising, dx, -dx) >= 0
                    shift = jnp.where(second, dx, -dx)
                    tbl[0, at] = jnp.where(second, spot_b, spot_a)
                    tbl[1, at] = jnp.where(second, spot_a, spot_b)
                    tbl[2, at] = jnp.where(rising, 4 * planes, 0) - shift
                    tbl[3, at] = jnp.where(second, 1, 0)
                    tbl[4, at] = anchors[3 * b + 1] - anchors[3 * a + 1]
                    tbl[5, at] = anchors[3 * b + 2] - anchors[3 * a + 2]
                    tbl[6, at] = jnp.where(second, 0, shift)
                    tbl[7, at] = jnp.where(rising, 0, 4 * planes) + shift

            return unused

        lax.fori_loop(0, tails[kind], deal, 0)

    @pl.when(fits[0] > 0)
    def chain():
        for row, base in ((1, 0), (0, each)):
            def link(slot, unused, row=row, base=base):
                at = final + tbl[row, slot]
                tbl[9 - row, slot] = links[at]
                links[at] = base + slot
                return unused

            lax.fori_loop(0, each, link, 0)
        for turn in range(1, groups):
            def hook(i, unused, turn=turn):
                at = (turn - 1) * cap + i
                end = ends + links[at]
                links[prior + at] = links[end]
                links[end] = at
                return unused

            lax.fori_loop(0, counts[jnp.bitwise_xor(me, turn) * groups + turn], hook, 0)


def make_plan(me, anchors, pair_slots, cap, each, planes):
    orbits = anchors.shape[0]
    entries = pair_slots.shape[0] * pair_slots.shape[1]
    smem = pl.BlockSpec(memory_space=pltpu.SMEM)
    local = orbits // 4
    return pl.pallas_call(
        functools.partial(plan_kernel, cap, planes),
        in_specs=[smem] * 3,
        out_specs=[smem] * 3,
        out_shape=[
            jax.ShapeDtypeStruct((10, each), jnp.int32),
            jax.ShapeDtypeStruct((9 * cap + 2 * local,), jnp.int32),
            jax.ShapeDtypeStruct((1,), jnp.int32),
        ],
        scratch_shapes=[
            pltpu.SMEM((4 * orbits,), jnp.int32), pltpu.SMEM((3 * entries,), jnp.int32),
            pltpu.SMEM((8,), jnp.int32), pltpu.SMEM((16,), jnp.int32),
        ],
        name="plan",
    )(me, anchors.reshape(-1), pair_slots.reshape(-1))


def fetch_kernel(chips, cap, tbl, links, orb, moved, fixed, *scratch):
    count = moved.shape[0]
    owns, parcels, pools, wins = [scratch[i * count : (i + 1) * count] for i in range(4)]
    own_sem, xy_send, xy_recv, z_send, z_recv = scratch[4 * count :]
    grp, place, across, along, corner = spot()
    core = lax.rem(place, 2)
    norb, planes = orb.shape[:2]
    slots = moved.shape[1]
    half = slots // 2
    relay = Relay(wins, z_send, z_recv, (1, -1), chips, half // 2, 3 * half // 4)

    def stage(chunk, kind):
        dst = owns[chunk] if kind == 0 else pools[chunk].at[pl.ds(0, norb)]
        return pltpu.make_async_copy(orb.at[:, :, pl.ds(chunk * SUB, SUB)], dst, own_sem.at[chunk, kind])

    def parcel(chunk, kind):
        return remote(
            parcels[chunk].at[pl.ds(kind * cap, cap)], pools[chunk].at[pl.ds(norb + kind * cap, cap)],
            xy_send.at[chunk, kind], xy_recv.at[chunk, kind], ((across, along, corner)[kind], place),
        )

    for chunk in range(count):
        stage(chunk, 0).start()
    for chunk in range(count):
        stage(chunk, 1).start()
    greet(chips, True)

    def pack(chunk):
        stage(chunk, 0).wait()

        def put(i, unused):
            parcels[chunk][i] = owns[chunk][links[i]]
            return unused

        lax.fori_loop(0, 3 * cap, put, 0)

    def send(chunk):
        for kind in (2, 0, 1):
            parcel(chunk, kind).start()

    pack(0)
    for chunk in range(1, count):
        pack(chunk)
        send(chunk - 1)
    send(count - 1)
    relay.clear()
    for step in range(count + 3):
        chunk = step
        if chunk < count:
            stage(chunk, 1).wait()
            for kind in range(3):
                parcel(chunk, kind).wait_recv()
            for side in range(2):
                start = relay.offset(relay.signs[side], 0) + planes * core

                def pick(slot, unused, start=start, chunk=chunk):
                    wins[chunk][slot, pl.ds(start, planes)] = pools[chunk][tbl[0, slot]]
                    return unused

                lax.fori_loop(side * half, (side + 1) * half, pick, 0)

            def hold(slot, unused, chunk=chunk):
                fixed[chunk, slot] = pools[chunk][tbl[1, slot]]
                return unused

            lax.fori_loop(0, slots, hold, 0)
            relay.begin(chunk)
        chunk = step - 1
        if 0 <= chunk < count:
            relay.first(chunk)
        chunk = step - 2
        if 0 <= chunk < count:
            relay.second(chunk)
        chunk = step - 3
        if 0 <= chunk < count:
            relay.settle(chunk)

            def choose(slot, unused, chunk=chunk):
                first = tbl[2, slot] + planes * core
                for plane in range(planes):
                    moved[chunk, slot, plane] = wins[chunk][slot, first + plane]
                return unused

            lax.fori_loop(0, slots, choose, 0)
    for chunk in range(count):
        for kind in range(3):
            parcel(chunk, kind).wait_send()
    relay.drain()


def fetch(table, links, stacked, slots, chips, cap):
    norb, planes, rows, lanes = stacked.shape
    chunks = rows // SUB
    vmem = pl.BlockSpec(memory_space=pltpu.VMEM)
    smem = pl.BlockSpec(memory_space=pltpu.SMEM)
    dma = pltpu.SemaphoreType.DMA
    shape = jax.ShapeDtypeStruct((chunks, slots, planes, SUB, lanes), jnp.float32)

    def room(count, deep=planes):
        return [pltpu.VMEM((count, deep, SUB, lanes), jnp.float32)] * chunks

    return pl.pallas_call(
        functools.partial(fetch_kernel, chips, cap),
        in_specs=[smem, smem, pl.BlockSpec(memory_space=pl.ANY)],
        out_specs=[vmem, vmem],
        out_shape=[shape, shape],
        scratch_shapes=room(norb) + room(3 * cap) + room(norb + 3 * cap) + room(slots, 6 * planes)
        + [dma((chunks, 2)), dma((chunks, 3)), dma((chunks, 3)), dma((chunks, 2, 5)), dma((chunks, 2, 5))],
        compiler_params=pltpu.CompilerParams(
            collective_id=3, has_side_effects=True, vmem_limit_bytes=48 * 1024 * 1024
        ),
        name="fetch",
    )(table, links, stacked)


def give_kernel(chips, cap, tbl, links, going, staying, out, *scratch):
    count, slots = going.shape[:2]
    wins, chains, parcels, backs, tallied = [scratch[i * count : (i + 1) * count] for i in range(5)]
    xy_send, xy_recv, z_send, z_recv = scratch[5 * count :]
    grp, place, across, along, corner = spot()
    core = lax.rem(place, 2)
    norb, planes = out.shape[:2]
    half = slots // 2
    extra = 3 * cap
    final = extra
    prior = final + norb + extra
    ends = prior + extra
    relay = Relay(wins, z_send, z_recv, (-1, 1), chips, half // 2, 3 * half // 4)
    greet(chips, True)

    def load(chunk):
        for side in range(2):
            at = relay.offset(relay.signs[side], 0) + planes * core

            def place_in(slot, unused, at=at):
                wins[chunk][slot, pl.ds(at, planes)] = going[chunk, slot]
                return unused

            lax.fori_loop(side * half, (side + 1) * half, place_in, 0)

    def parcel(chunk, kind):
        return remote(
            parcels[chunk].at[pl.ds(kind * cap, cap)], backs[chunk].at[pl.ds(kind * cap, cap)],
            xy_send.at[chunk, kind], xy_recv.at[chunk, kind], ((across, along, corner)[kind], place),
        )

    load(0)
    load(1)
    relay.begin(0)
    for chunk in range(2, count):
        load(chunk)
    relay.begin(1)
    relay.clear()
    for step in range(count + 3):
        if step < count:
            relay.first(step)
            if step + 2 < count:
                relay.begin(step + 2)
        chunk = step - 1
        if 0 <= chunk < count:
            relay.second(chunk)
        chunk = step - 2
        if 0 <= chunk < count:
            relay.settle(chunk)
            chain = chains[chunk]
            chain[2 * slots] = jnp.zeros(chain.shape[1:], jnp.float32)

            def link_fixed(slot, unused, chain=chain, chunk=chunk):
                chain[slot] = staying[chunk, slot] + chain[tbl[8, slot]]
                return unused

            def link_moved(slot, unused, chain=chain, chunk=chunk):
                first = tbl[7, slot] + planes * core
                for plane in range(planes):
                    chain[slots + slot, plane] = wins[chunk][slot, first + plane] + chain[tbl[9, slot], plane]
                return unused

            lax.fori_loop(0, slots, link_fixed, 0)
            lax.fori_loop(0, slots, link_moved, 0)

            def pack(i, unused, chain=chain, chunk=chunk):
                parcels[chunk][i] = chain[links[final + norb + i]]
                return unused

            lax.fori_loop(0, extra, pack, 0)
            for kind in (2, 0, 1):
                parcel(chunk, kind).start()
        chunk = step - 3
        if 0 <= chunk < count:
            total_of = tallied[chunk]
            total_of[extra] = jnp.zeros(total_of.shape[1:], jnp.float32)
            for kind in range(3):
                parcel(chunk, kind).wait_recv()

            def gather(i, unused, total_of=total_of, chunk=chunk):
                total_of[i] = backs[chunk][i] + total_of[links[prior + i]]
                return unused

            lax.fori_loop(0, extra, gather, 0)

            def keep(orbit, unused, total_of=total_of, chunk=chunk):
                found = total_of[links[ends + orbit]] + chains[chunk][links[final + orbit]]
                out[orbit, :, pl.ds(chunk * SUB, SUB)] = found
                return unused

            lax.fori_loop(0, norb, keep, 0)
    for chunk in range(count):
        for kind in range(3):
            parcel(chunk, kind).wait_send()
    relay.drain()


def give(table, links, going, staying, norb, chips, cap):
    chunks, slots, planes, sub, lanes = going.shape
    vmem = pl.BlockSpec(memory_space=pltpu.VMEM)
    smem = pl.BlockSpec(memory_space=pltpu.SMEM)
    dma = pltpu.SemaphoreType.DMA

    def room(count, deep=planes):
        return [pltpu.VMEM((count, deep, sub, lanes), jnp.float32)] * chunks

    return pl.pallas_call(
        functools.partial(give_kernel, chips, cap),
        in_specs=[smem, smem, vmem, vmem],
        out_specs=vmem,
        out_shape=jax.ShapeDtypeStruct((norb, planes, chunks * sub, lanes), jnp.float32),
        scratch_shapes=room(slots, 6 * planes) + room(2 * slots + 1) + room(3 * cap) + room(3 * cap)
        + room(3 * cap + 1) + [dma((chunks, 3)), dma((chunks, 3)), dma((chunks, 2, 5)), dma((chunks, 2, 5))],
        compiler_params=pltpu.CompilerParams(
            collective_id=4, has_side_effects=True, vmem_limit_bytes=48 * 1024 * 1024
        ),
        name="give",
    )(table, links, going, staying)


def full_tables(anchors, pair_slots, planes, groups, each):
    assignment = deal_evenly(pair_slots, groups, each)
    pairs = assignment[lax.axis_index("grp")]
    offsets = anchors[pairs[:, 1]] - anchors[pairs[:, 0]]
    dx, dy, dz = offsets[:, 0], offsets[:, 1], offsets[:, 2]
    slot = lax.broadcasted_iota(jnp.int32, (each,), 0)
    rising = slot < each // 2
    second = jnp.where(rising, dx >= 0, dx <= 0)
    shift = jnp.where(second, dx, -dx)
    moved_id = jnp.where(second, pairs[:, 1], pairs[:, 0])
    fixed_id = jnp.where(second, pairs[:, 0], pairs[:, 1])
    terms = jnp.concatenate([fixed_id, moved_id])
    at = lax.broadcasted_iota(jnp.int32, (2 * each, 2 * each), 0)
    before = lax.broadcasted_iota(jnp.int32, (2 * each, 2 * each), 1)
    found = jnp.where((terms[:, None] == terms[None, :]) & (before < at), before, -1)
    prior = jnp.max(found, axis=1)
    prior = jnp.where(prior < 0, 2 * each, prior)
    norb = anchors.shape[0]
    orbit = lax.broadcasted_iota(jnp.int32, (norb, 2 * each), 0)
    index = lax.broadcasted_iota(jnp.int32, (norb, 2 * each), 1)
    last = jnp.max(jnp.where(terms[None, :] == orbit, index, -1), axis=1)
    last = jnp.where(last < 0, 2 * each, last)
    table = jnp.stack([
        moved_id, fixed_id,
        jnp.where(rising, 4 * planes, 0) - shift,
        second.astype(jnp.int32), dy, dz,
        jnp.where(second, 0, shift),
        jnp.where(rising, 0, 4 * planes) + shift,
        prior[:each], prior[each:],
    ])
    return table, last


def slab_body(orbitals, anchors, pair_slots):
    groups, places = lax.axis_size("grp"), lax.axis_size("grid")
    norb_local, cells = orbitals.shape
    planes = cells // (B * B)
    each = PAIR_DEV * places
    chips = places // 2
    cap = 7 * norb_local // 16
    me = jnp.full((1,), lax.axis_index("grp"), jnp.int32)
    plan, links, fits = make_plan(me, anchors, pair_slots, cap, each, planes)
    stacked = orbitals.reshape(norb_local, planes, ROWS, LANES)

    def lean(stacked, anchors, pair_slots, plan, links):
        moved, fixed = fetch(plan, links, stacked, each, chips, cap)
        dens, partner = pair_up(plan, moved, fixed)
        pot = solve_slabs(plan, dens, places, 1)
        going, staying = make_terms(plan, pot, partner, moved, fixed)
        return give(plan, links, going, staying, norb_local, chips, cap)

    def full(stacked, anchors, pair_slots, plan, links):
        table, last = full_tables(anchors, pair_slots, planes, groups, each)
        moved, fixed = bring(table, stacked, each, groups, chips)
        dens, partner = pair_up(table, moved, fixed)
        pot = solve_slabs(table, dens, places, 5)
        going, staying = make_terms(table, pot, partner, moved, fixed)
        return hand_back(table, last, going, staying, norb_local, chips)

    out = lax.cond(fits[0] > 0, lean, full, stacked, anchors, pair_slots, plan, links)
    return out.reshape(norb_local, cells)


def slabs_fit(mesh):
    groups, places = mesh.shape["grp"], mesh.shape["grid"]
    return groups == 4 and places % 2 == 0 and 4 * (B // places) >= PAD


def solution(mesh):
    return jax.shard_map(
        slab_body if slabs_fit(mesh) else owner_body,
        mesh=mesh,
        in_specs=(P("grp", "grid"), P(), P()),
        out_specs=P("grp", "grid"),
        check_vma=False,
    )
```

```python
import functools
import math

import jax
import jax.numpy as jnp
from jax import lax
from jax.experimental import pallas as pl
from jax.experimental.pallas import tpu as pltpu
from jax.sharding import PartitionSpec as P

B = 64
PAIR_DEV = 2
ITERS = 3
MOST_CHUNKS = 2
LANES = 128
ROWS = B * B // LANES
PAD = 32
STEP = 4


def deal_evenly(pair_slots, owner_count, each_owner):
    flat_slots = pair_slots.reshape(-1, 2)
    filled = (flat_slots[:, 0] >= 0).astype(jnp.int32)
    position = jnp.cumsum(filled, dtype=jnp.int32) - filled
    wanted = lax.broadcasted_iota(jnp.int32, (owner_count, each_owner), 1) * owner_count
    wanted = (wanted + lax.broadcasted_iota(jnp.int32, (owner_count, each_owner), 0)).reshape(-1)
    matched = (position[None, :] == wanted[:, None]) & (filled[None, :] == 1)
    picked = jnp.sum(jnp.where(matched[:, :, None], flat_slots[None], 0), axis=1)
    return picked.reshape(owner_count, each_owner, 2)


def gather_kernel(ids_ref, src_ref, *out_refs):
    count, terms = out_refs[0].shape[:2]
    for slot, out_ref in enumerate(out_refs):
        def pick(dest, unused, slot=slot, out_ref=out_ref):
            for term in range(terms):
                out_ref[dest, term] = src_ref[ids_ref[(slot * count + dest) * terms + term]]
            return unused

        lax.fori_loop(0, count, pick, 0)


def gather_pieces(ids, pieces, slots, count):
    norb, rows, lanes = pieces.shape
    block = max(8, rows // 4)
    return pl.pallas_call(
        gather_kernel,
        grid_spec=pltpu.PrefetchScalarGridSpec(
            num_scalar_prefetch=1,
            grid=(rows // block,),
            in_specs=[pl.BlockSpec((norb, block, lanes), lambda i, ids: (0, i, 0))],
            out_specs=[pl.BlockSpec((count, 2, block, lanes), lambda i, ids: (0, 0, i, 0))] * slots,
        ),
        out_shape=[jax.ShapeDtypeStruct((count, 2, rows, lanes), jnp.float32)] * slots,
        cost_estimate=pl.CostEstimate(flops=0, bytes_accessed=8 * norb * rows * lanes, transcendentals=0),
        name="pick_pieces",
    )(ids, pieces)


def scatter_kernel(ids_ref, *refs):
    out_ref = refs[-1]
    out_ref[...] = jnp.zeros_like(out_ref)
    count, terms = refs[0].shape[:2]
    for slot, in_ref in enumerate(refs[:-1]):
        def add(dest, unused, slot=slot, in_ref=in_ref):
            for term in range(terms):
                orbit = ids_ref[(slot * count + dest) * terms + term]
                out_ref[orbit] = out_ref[orbit] + in_ref[dest, term]
            return unused

        lax.fori_loop(0, count, add, 0)


def scatter_pieces(ids, parts, norb):
    count, terms, rows, lanes = parts[0].shape
    block = max(8, rows // 4)
    return pl.pallas_call(
        scatter_kernel,
        grid_spec=pltpu.PrefetchScalarGridSpec(
            num_scalar_prefetch=1,
            grid=(rows // block,),
            in_specs=[pl.BlockSpec((count, terms, block, lanes), lambda i, ids: (0, 0, i, 0))] * len(parts),
            out_specs=pl.BlockSpec((norb, block, lanes), lambda i, ids: (0, i, 0)),
        ),
        out_shape=jax.ShapeDtypeStruct((norb, rows, lanes), jnp.float32),
        cost_estimate=pl.CostEstimate(flops=0, bytes_accessed=8 * norb * rows * lanes, transcendentals=0),
        name="add_pieces",
    )(ids, *parts)


def lane_ids(shape):
    return lax.broadcasted_iota(jnp.int32, shape, len(shape) - 1)


def shift_plane(plane, off_y, off_z):
    shape = plane.shape
    lane = lane_ids(shape)
    row = lax.broadcasted_iota(jnp.int32, shape, 0)
    linear = off_y * B + off_z
    across = jnp.bitwise_and(linear, LANES - 1)
    down = jnp.right_shift(linear, 7)
    turned = pltpu.roll(plane, across, 1)
    near = pltpu.roll(turned, jnp.bitwise_and(down, ROWS - 1), 0)
    far = pltpu.roll(turned, jnp.bitwise_and(down + 1, ROWS - 1), 0)
    moved = jnp.where(lane >= across, near, far)
    from_y = row * 2 + jnp.right_shift(lane, 6) - off_y
    from_z = jnp.bitwise_and(lane, B - 1) - off_z
    inside = (from_y >= 0) & (from_y < B) & (from_z >= 0) & (from_z < B)
    return jnp.where(inside, moved, 0.0)


def operate_plane(before, plane, after):
    shape = plane.shape
    lane = lane_ids(shape)
    row = lax.broadcasted_iota(jnp.int32, shape, 0)
    z = jnp.bitwise_and(lane, B - 1)
    upper_z = jnp.where(z < B - 1, pltpu.roll(plane, LANES - 1, 1), 0.0)
    lower_z = jnp.where(z > 0, pltpu.roll(plane, 1, 1), 0.0)
    half = pltpu.roll(plane, B, 1)
    down = jnp.where(row > 0, pltpu.roll(half, 1, 0), 0.0)
    up = jnp.where(row < ROWS - 1, pltpu.roll(half, ROWS - 1, 0), 0.0)
    beside = (before + after) + (half + jnp.where(lane < B, down, up))
    return 6.0 * plane - beside - upper_z - lower_z


def fold(values):
    return jnp.sum(values.reshape(ROWS // 8, 8, LANES), axis=0)


def total(acc):
    return jnp.sum(acc, axis=(0, 1), keepdims=True)


def solve_kernel(info_ref, *refs):
    chunks = (len(refs) - 6) // 2
    in_refs, out_refs = refs[:chunks], refs[chunks : 2 * chunks]
    wide, partner, direction, resid, image, potential = refs[2 * chunks :]
    count, terms, rows, lanes = in_refs[0].shape
    each = rows // ROWS
    dx, dy, dz = info_ref[0], info_ref[1], info_ref[2]
    keep = jnp.where(info_ref[3] > 0, 1.0, 0.0).astype(jnp.float32)
    edge = jnp.zeros((PAD, ROWS, LANES), jnp.float32)
    wide[pl.ds(0, PAD)] = edge
    wide[pl.ds(PAD + B, PAD)] = edge
    direction[0] = edge[0]
    direction[B + 1] = edge[0]
    none = jnp.zeros((8, LANES), jnp.float32)

    def place(owner, chunk, i):
        return (owner * chunks + chunk) * each + i

    def load(owner, unused):
        for chunk in range(chunks):
            for i in range(each):
                wide[PAD + place(owner, chunk, i)] = in_refs[chunk][owner, 1, pl.ds(i * ROWS, ROWS)]
        return unused

    lax.fori_loop(0, count, load, 0)

    def start(owner, acc):
        for chunk in range(chunks):
            for i in range(each):
                x = place(owner, chunk, i)
                other = shift_plane(wide[PAD + x - dx], dy, dz)
                partner[x] = other
                density = in_refs[chunk][owner, 0, pl.ds(i * ROWS, ROWS)] * other
                direction[x + 1] = density
                resid[x] = density
                acc = acc + fold(density * density)
        return acc

    norm_now = total(lax.fori_loop(0, count, start, none))

    for turn in range(ITERS):
        def apply(block, acc):
            for i in range(STEP):
                x = block * STEP + i
                plane = direction[x + 1]
                result = operate_plane(direction[x], plane, direction[x + 2])
                image[x] = result
                acc = acc + fold(plane * result)
            return acc

        step_len = norm_now / total(lax.fori_loop(0, B // STEP, apply, none))

        if turn == ITERS - 1:
            break

        def advance(block, acc):
            for i in range(STEP):
                x = block * STEP + i
                moved = step_len * direction[x + 1]
                potential[x] = moved if turn == 0 else potential[x] + moved
                left = resid[x] - step_len * image[x]
                resid[x] = left
                acc = acc + fold(left * left)
            return acc

        norm_next = total(lax.fori_loop(0, B // STEP, advance, none))
        ratio = norm_next / norm_now

        def renew(block, unused):
            for i in range(STEP):
                x = block * STEP + i
                direction[x + 1] = resid[x] + ratio * direction[x + 1]
            return unused

        lax.fori_loop(0, B // STEP, renew, 0)
        norm_now = norm_next

    def finish(owner, unused):
        for chunk in range(chunks):
            for i in range(each):
                x = place(owner, chunk, i)
                found = (potential[x] + step_len * direction[x + 1]) * keep
                out_refs[chunk][owner, 0, pl.ds(i * ROWS, ROWS)] = found * partner[x]
                wide[PAD + x] = found * in_refs[chunk][owner, 0, pl.ds(i * ROWS, ROWS)]
        return unused

    lax.fori_loop(0, count, finish, 0)

    def give_back(owner, unused):
        for chunk in range(chunks):
            for i in range(each):
                x = place(owner, chunk, i)
                out_refs[chunk][owner, 1, pl.ds(i * ROWS, ROWS)] = shift_plane(wide[PAD + x + dx], -dy, -dz)
        return unused

    lax.fori_loop(0, count, give_back, 0)


def solve_pair(info, parts):
    box = (B, ROWS, LANES)
    vmem = pl.BlockSpec(memory_space=pltpu.VMEM)
    return pl.pallas_call(
        solve_kernel,
        in_specs=[pl.BlockSpec(memory_space=pltpu.SMEM)] + [vmem] * len(parts),
        out_specs=[vmem] * len(parts),
        out_shape=[jax.ShapeDtypeStruct(p.shape, jnp.float32) for p in parts],
        scratch_shapes=[
            pltpu.VMEM((B + 2 * PAD, ROWS, LANES), jnp.float32),
            pltpu.VMEM(box, jnp.float32),
            pltpu.VMEM((B + 2, ROWS, LANES), jnp.float32),
            pltpu.VMEM(box, jnp.float32),
            pltpu.VMEM(box, jnp.float32),
            pltpu.VMEM(box, jnp.float32),
        ],
        compiler_params=pltpu.CompilerParams(vmem_limit_bytes=32 * 1024 * 1024),
        cost_estimate=pl.CostEstimate(flops=0, bytes_accessed=40 * 1024 * 1024, transcendentals=0),
        name="solve_pair",
    )(info, *parts)


def owner_body(orbitals, anchors, pair_slots):
    grid_count = lax.axis_size("grid")
    owner_count = lax.axis_size("grp") * grid_count
    group_idx = lax.axis_index("grp")
    place_idx = lax.axis_index("grid")
    assignment = deal_evenly(pair_slots, owner_count, PAIR_DEV)
    slots = assignment.shape[1]
    filled = assignment[..., 0] >= 0
    safe_ids = jnp.maximum(assignment, 0)
    group_table = lax.dynamic_slice_in_dim(safe_ids, group_idx * grid_count, grid_count, 0)
    ids = jnp.transpose(group_table, (1, 0, 2)).reshape(-1)
    owner_idx = group_idx * grid_count + place_idx
    own_pairs = safe_ids[owner_idx]
    offsets = anchors[own_pairs[:, 1]] - anchors[own_pairs[:, 0]]
    info = jnp.concatenate([offsets, filled[owner_idx].astype(jnp.int32)[:, None]], axis=1)

    norb_local, cells = orbitals.shape
    stacked = orbitals.reshape(norb_local, cells // LANES, LANES)
    chunks = math.gcd(MOST_CHUNKS, cells // (B * B))
    rows = stacked.shape[1] // chunks
    arrived = [[None] * chunks for _ in range(slots)]
    for chunk in range(chunks):
        pieces = lax.all_gather(stacked[:, chunk * rows : (chunk + 1) * rows], "grp", axis=0, tiled=True)
        outgoing = gather_pieces(ids, pieces, slots, grid_count)
        for slot in range(slots):
            arrived[slot][chunk] = lax.all_to_all(outgoing[slot], "grid", split_axis=0, concat_axis=0, tiled=True)
    returned = []
    for slot in range(slots):
        terms = solve_pair(info[slot], arrived[slot])
        returned.append(
            [lax.all_to_all(t, "grid", split_axis=0, concat_axis=0, tiled=True) for t in terms]
        )
    results = []
    for chunk in range(chunks):
        summed = scatter_pieces(ids, [r[chunk] for r in returned], anchors.shape[0])
        results.append(lax.psum_scatter(summed, "grp", scatter_dimension=0, tiled=True))
    return jnp.concatenate(results, axis=1).reshape(norb_local, cells)


MESH = pl.DeviceIdType.MESH
HALO = 3
WAVES = 4
TRIALS = 12
SUB = 8


def remote(src, dst, send_sem, recv_sem, device):
    return pltpu.make_async_remote_copy(
        src_ref=src, dst_ref=dst, send_sem=send_sem, recv_sem=recv_sem, device_id=device, device_id_type=MESH
    )


def spot():
    grp = lax.axis_index("grp")
    place = lax.axis_index("grid")
    across = grp + 1 - 2 * lax.rem(grp, 2)
    along = lax.rem(grp + 2, 4)
    corner = lax.rem(across + 2, 4)
    return grp, place, across, along, corner


def greet(chips, wide=False):
    grp, place, across, along, corner = spot()
    chip = place // 2
    core = lax.rem(place, 2)
    barrier = pltpu.get_barrier_semaphore()
    peers = [(across, place), (along, place), (grp, 2 * chip + 1 - core)] + ([(corner, place)] if wide else [])
    for device in peers:
        pl.semaphore_signal(barrier, inc=1, device_id=device, device_id_type=MESH)

    @pl.when(chip > 0)
    def below():
        pl.semaphore_signal(barrier, inc=1, device_id=(grp, place - 2), device_id_type=MESH)

    @pl.when(chip < chips - 1)
    def above():
        pl.semaphore_signal(barrier, inc=1, device_id=(grp, place + 2), device_id_type=MESH)

    ends = jnp.where(chip > 0, 1, 0) + jnp.where(chip < chips - 1, 1, 0)
    pl.semaphore_wait(barrier, len(peers) + ends)


class Relay:
    def __init__(self, wins, send_sem, recv_sem, signs, chips, marks):
        self.wins, self.send_sem, self.recv_sem, self.signs, self.chips = wins, send_sem, recv_sem, signs, chips
        self.grp, self.place = lax.axis_index("grp"), lax.axis_index("grid")
        self.chip = self.place // 2
        self.core = lax.rem(self.place, 2)
        self.half = wins[0].shape[0] // 2
        self.planes = wins[0].shape[1] // 6
        self.deep, self.far, self.mid = marks

    def offset(self, sign, hop):
        return 2 * self.planes * (2 - hop if sign > 0 else hop)

    def region(self, chunk, side, hop, core, size):
        start = self.offset(self.signs[side], hop) + self.planes * core
        return self.wins[chunk].at[pl.ds(side * self.half, size), pl.ds(start, self.planes)]

    def comes(self, side, hop):
        source = self.chip - self.signs[side] * hop
        return source >= 0 if self.signs[side] > 0 else source < self.chips

    def goes(self, side, hop):
        source = self.chip + self.signs[side] - self.signs[side] * hop
        if self.signs[side] > 0:
            return (self.chip + 1 < self.chips) & (source >= 0)
        return (self.chip - 1 >= 0) & (source < self.chips)

    def spans(self, side, hop, core, act):
        if hop == 0:
            act(self.half)
        else:
            near = 1 if self.signs[side] > 0 else 0
            most, least = (self.half, self.mid) if hop == 1 else (self.far, self.deep)
            if most == least:
                act(most)
                return

            @pl.when(core == near)
            def whole():
                act(most)

            @pl.when(core != near)
            def some():
                act(least)

    def onward(self, chunk, side, hop, size, here=None):
        source = self.region(chunk, side, hop - 1 if here is None else here, self.core, size)
        there = self.region(chunk, side, hop, self.core, size)
        return remote(
            source, there, self.send_sem.at[chunk, side, hop - 1], self.recv_sem.at[chunk, side, hop - 1],
            (self.grp, self.place + 2 * self.signs[side]),
        )

    def beside(self, chunk, side, hop, core, size):
        part = self.region(chunk, side, hop, core, size)
        return remote(
            part, part, self.send_sem.at[chunk, side, 2 + hop], self.recv_sem.at[chunk, side, 2 + hop],
            (self.grp, 2 * self.chip + 1 - self.core),
        )

    def clear(self):
        for side in range(2):
            for hop in (1, 2):
                start = self.offset(self.signs[side], hop)

                @pl.when(jnp.logical_not(self.comes(side, hop)))
                def fill(side=side, start=start):
                    for win in self.wins:
                        def zero(slot, unused, win=win):
                            win[slot, pl.ds(start, 2 * self.planes)] = jnp.zeros(
                                (2 * self.planes,) + win.shape[2:], jnp.float32
                            )
                            return unused

                        lax.fori_loop(side * self.half, (side + 1) * self.half, zero, 0)

    def pass_on(self, chunk, side, hop):
        @pl.when(self.goes(side, hop))
        def go():
            self.spans(side, hop, self.core, lambda size: self.onward(chunk, side, hop, size).start())

    def begin(self, chunk):
        for side in range(2):
            self.pass_on(chunk, side, 1)
            self.beside(chunk, side, 0, self.core, self.half).start()

    def take(self, chunk, side, hop):
        @pl.when(self.comes(side, hop))
        def got():
            def act(size):
                self.onward(chunk, side, hop, size, hop).wait_recv()

            self.spans(side, hop, self.core, act)

        if hop < 2:
            self.pass_on(chunk, side, hop + 1)

        @pl.when(self.comes(side, hop))
        def share():
            self.spans(side, hop, self.core, lambda size: self.beside(chunk, side, hop, self.core, size).start())

    def first(self, chunk):
        for side in range(2):
            self.take(chunk, side, 1)

    def second(self, chunk):
        for side in range(2):
            self.take(chunk, side, 2)

    def settle(self, chunk):
        other = 1 - self.core
        for side in range(2):
            self.beside(chunk, side, 0, other, self.half).wait_recv()
            for hop in (1, 2):
                @pl.when(self.comes(side, hop))
                def got(side=side, hop=hop):
                    self.spans(side, hop, other, lambda size: self.beside(chunk, side, hop, other, size).wait_recv())

    def drain(self):
        for chunk in range(len(self.wins)):
            for side in range(2):
                self.beside(chunk, side, 0, self.core, self.half).wait_send()
                for hop in (1, 2):
                    @pl.when(self.comes(side, hop))
                    def sent(chunk=chunk, side=side, hop=hop):
                        self.spans(
                            side, hop, self.core,
                            lambda size: self.beside(chunk, side, hop, self.core, size).wait_send(),
                        )

                    @pl.when(self.goes(side, hop))
                    def passed(chunk=chunk, side=side, hop=hop):
                        self.spans(
                            side, hop, self.core, lambda size: self.onward(chunk, side, hop, size).wait_send()
                        )


def bring_kernel(chips, tbl, orb, moved, fixed, *scratch):
    count = moved.shape[0]
    pools, wins = scratch[:count], scratch[count : 2 * count]
    own_sem, xy_send, xy_recv, z_send, z_recv = scratch[2 * count :]
    grp, place, across, along, corner = spot()
    core = lax.rem(place, 2)
    norb, planes = orb.shape[:2]
    part = norb // 2
    slots = moved.shape[1]
    relay = Relay(wins, z_send, z_recv, (1, -1), chips, (slots // 2,) * 3)

    def block(chunk, owner, start, size):
        return pools[chunk].at[pl.ds(owner * norb + start, size)]

    def stage(chunk):
        return pltpu.make_async_copy(
            orb.at[:, :, pl.ds(chunk * SUB, SUB)], block(chunk, grp, 0, norb), own_sem.at[chunk]
        )

    def hop(chunk, kind, owner, start, size, target):
        ref = block(chunk, owner, start, size)
        return remote(ref, ref, xy_send.at[chunk, kind], xy_recv.at[chunk, kind], (target, place))

    def direct(chunk, owners):
        return hop(chunk, 0, owners[0], 0, norb, across), hop(chunk, 1, owners[1], 0, norb, along)

    def turned(chunk, owners):
        return hop(chunk, 2, owners[0], 0, part, along), hop(chunk, 3, owners[1], part, part, across)

    for chunk in range(count):
        stage(chunk).start()
    greet(chips)
    relay.clear()

    def send_own(chunk):
        stage(chunk).wait()
        for copy in direct(chunk, (grp, grp)):
            copy.start()

    send_own(0)
    send_own(1)
    for step in range(count + 4):
        if step < count:
            for copy in direct(step, (across, along)):
                copy.wait_recv()
            for copy in turned(step, (across, along)):
                copy.start()
            if step + 2 < count:
                send_own(step + 2)
        chunk = step - 1
        if 0 <= chunk < count:
            for copy in turned(chunk, (corner, corner)):
                copy.wait_recv()
            for side in range(2):
                start = relay.offset(relay.signs[side], 0) + planes * core

                def pick(slot, unused, start=start, chunk=chunk):
                    wins[chunk][slot, pl.ds(start, planes)] = pools[chunk][tbl[0, slot]]
                    fixed[chunk, slot] = pools[chunk][tbl[1, slot]]
                    return unused

                lax.fori_loop(side * (slots // 2), (side + 1) * (slots // 2), pick, 0)
            relay.begin(chunk)
        chunk = step - 2
        if 0 <= chunk < count:
            relay.first(chunk)
        chunk = step - 3
        if 0 <= chunk < count:
            relay.second(chunk)
        chunk = step - 4
        if 0 <= chunk < count:
            relay.settle(chunk)

            def choose(slot, unused, chunk=chunk):
                first = tbl[2, slot] + planes * core
                for plane in range(planes):
                    moved[chunk, slot, plane] = wins[chunk][slot, first + plane]
                return unused

            lax.fori_loop(0, slots, choose, 0)
    for chunk in range(count):
        for copy in direct(chunk, (grp, grp)) + turned(chunk, (across, along)):
            copy.wait_send()
    relay.drain()


def bring(table, stacked, slots, groups, chips):
    norb, planes, rows, lanes = stacked.shape
    chunks = rows // SUB
    vmem = pl.BlockSpec(memory_space=pltpu.VMEM)
    dma = pltpu.SemaphoreType.DMA
    shape = jax.ShapeDtypeStruct((chunks, slots, planes, SUB, lanes), jnp.float32)
    return pl.pallas_call(
        functools.partial(bring_kernel, chips),
        in_specs=[pl.BlockSpec(memory_space=pltpu.SMEM), pl.BlockSpec(memory_space=pl.ANY)],
        out_specs=[vmem, vmem],
        out_shape=[shape, shape],
        scratch_shapes=[pltpu.VMEM((groups * norb, planes, SUB, lanes), jnp.float32)] * chunks
        + [pltpu.VMEM((slots, 6 * planes, SUB, lanes), jnp.float32)] * chunks
        + [dma((chunks,)), dma((chunks, 4)), dma((chunks, 4)), dma((chunks, 2, 5)), dma((chunks, 2, 5))],
        compiler_params=pltpu.CompilerParams(
            collective_id=0, has_side_effects=True, vmem_limit_bytes=48 * 1024 * 1024
        ),
        name="bring",
    )(table, stacked)


def pair_kernel(tbl, moved, fixed, dens, partner):
    def go(slot, unused):
        second = tbl[3, slot] > 0
        dy, dz = tbl[4, slot], tbl[5, slot]
        for x in range(moved.shape[2]):
            left = moved[:, slot, x].reshape(ROWS, LANES)
            right = fixed[:, slot, x].reshape(ROWS, LANES)
            other = shift_plane(jnp.where(second, left, right), dy, dz)
            dens[slot, x] = jnp.where(second, right, left) * other
            partner[slot, x] = other
        return unused

    lax.fori_loop(0, moved.shape[1], go, 0)


def pair_up(table, moved, fixed):
    chunks, slots, planes, sub, lanes = moved.shape
    vmem = pl.BlockSpec(memory_space=pltpu.VMEM)
    shape = jax.ShapeDtypeStruct((slots, planes, ROWS, lanes), jnp.float32)
    return pl.pallas_call(
        pair_kernel,
        in_specs=[pl.BlockSpec(memory_space=pltpu.SMEM), vmem, vmem],
        out_specs=[vmem, vmem],
        out_shape=[shape, shape],
        compiler_params=pltpu.CompilerParams(vmem_limit_bytes=24 * 1024 * 1024),
        name="pair_up",
    )(table, moved, fixed)


def inner(plane):
    shape = plane.shape
    lane = lane_ids(shape)
    row = lax.broadcasted_iota(jnp.int32, shape, 0)
    z = jnp.bitwise_and(lane, B - 1)
    upper_z = jnp.where(z < B - 1, pltpu.roll(plane, LANES - 1, 1), 0.0)
    lower_z = jnp.where(z > 0, pltpu.roll(plane, 1, 1), 0.0)
    half = pltpu.roll(plane, B, 1)
    down = jnp.where(row > 0, pltpu.roll(half, 1, 0), 0.0)
    up = jnp.where(row < ROWS - 1, pltpu.roll(half, ROWS - 1, 0), 0.0)
    return 6.0 * plane - ((half + jnp.where(lane < B, down, up)) + (upper_z + lower_z))


def krylov_weights(m):
    a0 = m[0] / m[1]
    rr1 = a0 * a0 * m[2] - m[0]
    p, q = 1.0 + rr1 / m[0], -a0
    a1 = rr1 / (p * p * m[1] + 2.0 * p * q * m[2] + q * q * m[3])
    s1, s2 = -a0 - a1 * p, -a1 * q
    rr2 = (m[0] + s1 * s1 * m[2] + s2 * s2 * m[4]) + 2.0 * (s1 * m[1] + s2 * m[2] + s1 * s2 * m[3])
    b1 = rr2 / rr1
    e0, e1, e2 = 1.0 + b1 * p, s1 + b1 * q, s2
    bend = e0 * e0 * m[1] + e1 * e1 * m[3] + e2 * e2 * m[5]
    a2 = rr2 / (bend + 2.0 * (e0 * e1 * m[2] + e0 * e2 * m[3] + e1 * e2 * m[4]))
    return a0 + a1 * p + a2 * e0, a1 * q + a2 * e1, a2 * e2


def solve_slabs_kernel(places, tbl, dens, pot, wide, one, two, sums, gathered, weights, h_send, h_recv, s_send, s_recv):
    grp, place = lax.axis_index("grp"), lax.axis_index("grid")
    slots, planes = dens.shape[:2]
    first, last = HALO, HALO + planes - 1
    each = slots // WAVES
    barrier = pltpu.get_barrier_semaphore()
    for step in range(1, places):
        pl.semaphore_signal(
            barrier, inc=1, device_id=(grp, lax.rem(place + step, places)), device_id_type=MESH
        )
    pl.semaphore_wait(barrier, places - 1)

    def rise(wave):
        return remote(
            dens.at[pl.ds(wave * each, each), pl.ds(planes - HALO + 1, HALO - 1)],
            wide.at[pl.ds(wave * each, each), pl.ds(1, HALO - 1)],
            h_send.at[wave, 0], h_recv.at[wave, 0], (grp, lax.rem(place + 1, places)),
        )

    def sink(wave):
        return remote(
            dens.at[pl.ds(wave * each, each), pl.ds(0, HALO)],
            wide.at[pl.ds(wave * each, each), pl.ds(HALO + planes, HALO)],
            h_send.at[wave, 1], h_recv.at[wave, 1], (grp, lax.rem(place + places - 1, places)),
        )

    lowest, highest = place == 0, place == places - 1
    for wave in range(WAVES):
        @pl.when(jnp.logical_not(highest))
        def send_up(wave=wave):
            rise(wave).start()

        @pl.when(jnp.logical_not(lowest))
        def send_down(wave=wave):
            sink(wave).start()

    blank = jnp.zeros((HALO, ROWS, LANES), jnp.float32)

    def copy_in(slot, unused):
        wide[slot, pl.ds(HALO, planes)] = dens[slot]
        one[slot, 1] = blank[0]
        one[slot, last + 3] = blank[0]
        one[slot, 0] = blank[0]
        return unused

    lax.fori_loop(0, slots, copy_in, 0)

    @pl.when(lowest)
    def no_below():
        def fill(slot, unused):
            wide[slot, pl.ds(0, HALO)] = blank
            return unused

        lax.fori_loop(0, slots, fill, 0)

    @pl.when(highest)
    def no_above():
        def fill(slot, unused):
            wide[slot, pl.ds(HALO + planes, HALO)] = blank
            return unused

        lax.fori_loop(0, slots, fill, 0)

    lane = lax.broadcasted_iota(jnp.int32, (1, LANES), 1)
    none = jnp.zeros((8, LANES), jnp.float32)

    def row_of(parts):
        row = jnp.zeros((1, LANES), jnp.float32)
        for at, part in parts:
            row = row + jnp.where(lane == at, total(part), 0.0)
        return row

    def work(slot, unused):
        low, high = tbl[6, slot], tbl[6, slot] + B

        def live(e):
            x = planes * place + e - HALO
            return jnp.where((x >= low) & (x < high), 1.0, 0.0).astype(jnp.float32)

        m0, m1, m2, m3, m4, m5 = none, none, none, none, none, none
        for e in range(first - 1, last + 3):
            value = live(e) * (inner(wide[slot, e]) - (wide[slot, e - 1] + wide[slot, e + 1]))
            one[slot, e] = value
            if first <= e <= last:
                source = wide[slot, e]
                m0 = m0 + fold(source * source)
                m1 = m1 + fold(source * value)
                m2 = m2 + fold(value * value)
        bent = None
        for e in range(first, last + 2):
            value = live(e) * (inner(one[slot, e]) - (one[slot, e - 1] + one[slot, e + 1]))
            two[slot, e] = value
            if e > first:
                m5 = m5 - 2.0 * fold(value * two[slot, e - 1])
            if e <= last:
                m3 = m3 + fold(one[slot, e] * value)
                m4 = m4 + fold(value * value)
                m5 = m5 + fold(value * inner(value))
        sums[pl.ds(slot, 1)] = row_of(enumerate((m0, m1, m2, m3, m4, m5)))
        return unused

    def rim(slot, spots, pairs):
        low, high = tbl[6, slot], tbl[6, slot] + B
        m2, m3, m4, m5 = none, none, none, none
        for e, fresh in spots:
            if fresh:
                x = planes * place + e - HALO
                alive = jnp.where((x >= low) & (x < high), 1.0, 0.0).astype(jnp.float32)
                two[slot, e] = alive * (inner(one[slot, e]) - (one[slot, e - 1] + one[slot, e + 1]))
        for e, fresh in spots:
            value, before = two[slot, e], one[slot, e]
            m2 = m2 + fold(before * before)
            m3 = m3 + fold(before * value)
            m4 = m4 + fold(value * value)
            m5 = m5 + fold(value * inner(value))
        for e in pairs:
            m5 = m5 - 2.0 * fold(two[slot, e] * two[slot, e + 1])
        sums[pl.ds(slot, 1)] = sums[pl.ds(slot, 1)] + row_of(((2, m2), (3, m3), (4, m4), (5, m5)))

    for wave in range(WAVES):
        @pl.when(jnp.logical_not(lowest))
        def got_below(wave=wave):
            rise(wave).wait_recv()

        @pl.when(jnp.logical_not(highest))
        def got_above(wave=wave):
            sink(wave).wait_recv()

        lax.fori_loop(wave * each, (wave + 1) * each, work, 0)

    @pl.when(lowest)
    def rim_below():
        def go(slot, unused):
            rim(slot, ((first - 2, True), (first - 1, True)), (first - 2, first - 1))
            return unused

        lax.fori_loop(0, slots, go, 0)

    @pl.when(highest)
    def rim_above():
        def go(slot, unused):
            rim(slot, ((last + 1, False), (last + 2, True)), (last + 1,))
            return unused

        lax.fori_loop(0, slots, go, 0)

    def tell(step):
        return remote(
            sums, gathered.at[place], s_send.at[step - 1], s_recv.at[step - 1],
            (grp, lax.rem(place + step, places)),
        )

    def hear(step):
        source = lax.rem(place + places - step, places)
        return remote(
            sums, gathered.at[source], s_send.at[step - 1], s_recv.at[step - 1],
            (grp, lax.rem(place + step, places)),
        )

    for step in range(1, places):
        tell(step).start()
    gathered[place] = sums[...]
    for step in range(1, places):
        hear(step).wait_recv()
    whole = gathered[0]
    for at in range(1, places):
        whole = whole + gathered[at]
    lanes = lax.broadcasted_iota(jnp.int32, whole.shape, 1)
    moments = [jnp.sum(jnp.where(lanes == at, whole, 0.0), axis=1, keepdims=True) for at in range(6)]
    for at, weight in enumerate(krylov_weights(moments)):
        weights[at] = jnp.broadcast_to(weight, whole.shape)

    def finish(slot, unused):
        w0, w1, w2 = [weights[at, pl.ds(slot, 1)] for at in range(3)]
        for x in range(planes):
            e = x + HALO
            pot[slot, x] = w0 * wide[slot, e] + w1 * one[slot, e] + w2 * two[slot, e]
        return unused

    lax.fori_loop(0, slots, finish, 0)
    for wave in range(WAVES):
        @pl.when(jnp.logical_not(highest))
        def sent_up(wave=wave):
            rise(wave).wait_send()

        @pl.when(jnp.logical_not(lowest))
        def sent_down(wave=wave):
            sink(wave).wait_send()

    for step in range(1, places):
        tell(step).wait_send()


def solve_slabs(table, dens, places, ident):
    slots, planes, rows, lanes = dens.shape
    vmem = pl.BlockSpec(memory_space=pltpu.VMEM)
    dma = pltpu.SemaphoreType.DMA
    tall = pltpu.VMEM((slots, planes + 2 * HALO, rows, lanes), jnp.float32)
    return pl.pallas_call(
        functools.partial(solve_slabs_kernel, places),
        in_specs=[pl.BlockSpec(memory_space=pltpu.SMEM), vmem],
        out_specs=vmem,
        out_shape=jax.ShapeDtypeStruct(dens.shape, jnp.float32),
        scratch_shapes=[
            tall, tall, tall,
            pltpu.VMEM((slots, lanes), jnp.float32),
            pltpu.VMEM((places, slots, lanes), jnp.float32),
            pltpu.VMEM((3, slots, lanes), jnp.float32),
            dma((WAVES, 2)), dma((WAVES, 2)), dma((places - 1,)), dma((places - 1,)),
        ],
        compiler_params=pltpu.CompilerParams(
            collective_id=ident, has_side_effects=True, vmem_limit_bytes=40 * 1024 * 1024
        ),
        name="solve_slabs",
    )(table, dens)


def term_kernel(tbl, pot, partner, moved, fixed, going, staying):
    chunks = going.shape[0]

    def go(slot, unused):
        second = tbl[3, slot] > 0
        dy, dz = tbl[4, slot], tbl[5, slot]
        for x in range(pot.shape[1]):
            found = pot[slot, x]
            left = moved[:, slot, x].reshape(ROWS, LANES)
            right = fixed[:, slot, x].reshape(ROWS, LANES)
            term_a = found * partner[slot, x]
            term_b = shift_plane(found * jnp.where(second, right, left), -dy, -dz)
            going[:, slot, x] = jnp.where(second, term_b, term_a).reshape(chunks, SUB, LANES)
            staying[:, slot, x] = jnp.where(second, term_a, term_b).reshape(chunks, SUB, LANES)
        return unused

    lax.fori_loop(0, pot.shape[0], go, 0)


def make_terms(table, pot, partner, moved, fixed):
    vmem = pl.BlockSpec(memory_space=pltpu.VMEM)
    shape = jax.ShapeDtypeStruct(moved.shape, jnp.float32)
    return pl.pallas_call(
        term_kernel,
        in_specs=[pl.BlockSpec(memory_space=pltpu.SMEM)] + [vmem] * 4,
        out_specs=[vmem, vmem],
        out_shape=[shape, shape],
        compiler_params=pltpu.CompilerParams(vmem_limit_bytes=24 * 1024 * 1024),
        name="make_terms",
    )(table, pot, partner, moved, fixed)


def hand_back_kernel(chips, tbl, last, going, staying, out, *scratch):
    count, slots = going.shape[:2]
    wins, chains, outs1, outs2, ins1, ins2 = [scratch[i * count : (i + 1) * count] for i in range(6)]
    xy_send, xy_recv, z_send, z_recv = scratch[6 * count :]
    grp, place, across, along, corner = spot()
    core = lax.rem(place, 2)
    norb, planes = out.shape[:2]
    part = norb // 2
    relay = Relay(wins, z_send, z_recv, (-1, 1), chips, (slots // 2,) * 3)
    greet(chips)
    relay.clear()

    def start(chunk):
        for side in range(2):
            at = relay.offset(relay.signs[side], 0) + planes * core

            def place_in(slot, unused, at=at):
                wins[chunk][slot, pl.ds(at, planes)] = going[chunk, slot]
                return unused

            lax.fori_loop(side * (slots // 2), (side + 1) * (slots // 2), place_in, 0)
        relay.begin(chunk)

    def swap(chunk, kind):
        src = (outs1 if kind < 2 else outs2)[chunk].at[kind % 2]
        dst = (ins1 if kind < 2 else ins2)[chunk].at[kind % 2]
        target = (across, along, along, across)[kind]
        return remote(src, dst, xy_send.at[chunk, kind], xy_recv.at[chunk, kind], (target, place))

    start(0)
    start(1)
    for step in range(count + 4):
        if step < count:
            relay.first(step)
            if step + 2 < count:
                start(step + 2)
        chunk = step - 1
        if 0 <= chunk < count:
            relay.second(chunk)
        chunk = step - 2
        if 0 <= chunk < count:
            relay.settle(chunk)
            chain = chains[chunk]
            chain[2 * slots] = jnp.zeros(chain.shape[1:], jnp.float32)

            def link_fixed(slot, unused, chain=chain, chunk=chunk):
                chain[slot] = staying[chunk, slot] + chain[tbl[8, slot]]
                return unused

            def link_moved(slot, unused, chain=chain, chunk=chunk):
                first = tbl[7, slot] + planes * core
                for plane in range(planes):
                    chain[slots + slot, plane] = wins[chunk][slot, first + plane] + chain[tbl[9, slot], plane]
                return unused

            lax.fori_loop(0, slots, link_fixed, 0)
            lax.fori_loop(0, slots, link_moved, 0)

            def pack(i, unused, chain=chain, chunk=chunk):
                outs1[chunk][0, i] = chain[last[across * norb + i]]
                outs1[chunk][0, part + i] = chain[last[corner * norb + i]]
                outs1[chunk][1, i] = chain[last[along * norb + part + i]]
                outs1[chunk][1, part + i] = chain[last[corner * norb + part + i]]
                return unused

            lax.fori_loop(0, part, pack, 0)
            swap(chunk, 0).start()
            swap(chunk, 1).start()
        chunk = step - 3
        if 0 <= chunk < count:
            chain = chains[chunk]
            swap(chunk, 0).wait_recv()

            def add_across(i, unused, chain=chain, chunk=chunk):
                outs2[chunk][0, i] = ins1[chunk][0, part + i] + chain[last[along * norb + i]]
                return unused

            lax.fori_loop(0, part, add_across, 0)
            swap(chunk, 2).start()
            swap(chunk, 1).wait_recv()

            def add_along(i, unused, chain=chain, chunk=chunk):
                outs2[chunk][1, i] = ins1[chunk][1, part + i] + chain[last[across * norb + part + i]]
                return unused

            lax.fori_loop(0, part, add_along, 0)
            swap(chunk, 3).start()
        chunk = step - 4
        if 0 <= chunk < count:
            chain = chains[chunk]
            swap(chunk, 2).wait_recv()
            swap(chunk, 3).wait_recv()
            for side in range(2):
                def keep(i, unused, side=side, chain=chain, chunk=chunk):
                    orbit = side * part + i
                    found = ins1[chunk][side, i] + ins2[chunk][side, i]
                    out[orbit, :, pl.ds(chunk * SUB, SUB)] = found + chain[last[grp * norb + orbit]]
                    return unused

                lax.fori_loop(0, part, keep, 0)
    for chunk in range(count):
        for kind in range(4):
            swap(chunk, kind).wait_send()
    relay.drain()


def hand_back(table, last, going, staying, norb, chips):
    chunks, slots, planes, sub, lanes = going.shape
    vmem = pl.BlockSpec(memory_space=pltpu.VMEM)
    smem = pl.BlockSpec(memory_space=pltpu.SMEM)
    dma = pltpu.SemaphoreType.DMA
    def room(*lead):
        return [pltpu.VMEM(lead + (planes, sub, lanes), jnp.float32)] * chunks
    wins = [pltpu.VMEM((slots, 6 * planes, sub, lanes), jnp.float32)] * chunks
    return pl.pallas_call(
        functools.partial(hand_back_kernel, chips),
        in_specs=[smem, smem, vmem, vmem],
        out_specs=vmem,
        out_shape=jax.ShapeDtypeStruct((norb, planes, chunks * sub, lanes), jnp.float32),
        scratch_shapes=wins + room(2 * slots + 1) + room(2, norb) + room(2, norb // 2)
        + room(2, norb) + room(2, norb // 2)
        + [dma((chunks, 4)), dma((chunks, 4)), dma((chunks, 2, 5)), dma((chunks, 2, 5))],
        compiler_params=pltpu.CompilerParams(
            collective_id=2, has_side_effects=True, vmem_limit_bytes=56 * 1024 * 1024
        ),
        name="hand_back",
    )(table, last, going, staying)


def plan_kernel(cap, planes, me_ref, anchors, pairs, tbl, links, fits, spots, masks, lists, mine, counts):
    groups = 4
    orbits = anchors.shape[1]
    local = orbits // groups
    depth, unused, owners = pairs.shape
    entries = depth * owners
    each = tbl.shape[1]
    half = each // 2
    extra = (groups - 1) * cap
    final = extra
    prior = final + local + extra
    ends = prior + extra
    spare = ends + local
    worst = 1 << 20
    me = me_ref[0]

    def group_of(orbit):
        if local & (local - 1) == 0:
            return jnp.right_shift(orbit, local.bit_length() - 1)
        return orbit // local

    def unpack(code):
        return jnp.bitwise_and(code, 1023), jnp.bitwise_and(jnp.right_shift(code, 10), 1023)

    def clean(i, unused):
        links[i] = 0
        links[prior + i] = extra
        return unused

    def close(i, unused):
        links[final + i] = 2 * each
        return unused

    def own(i, unused):
        links[ends + i] = extra
        spots[me * local + i] = i
        return unused

    lax.fori_loop(0, extra, clean, 0, unroll=5)
    lax.fori_loop(0, local + extra, close, 0)
    lax.fori_loop(0, local, own, 0, unroll=4)

    def sort(i, tails, layer):
        a, b = pairs[layer, 0, i], pairs[layer, 1, i]
        filled = a >= 0
        dx = anchors[0, jnp.maximum(b, 0)] - anchors[0, jnp.maximum(a, 0)]
        reach = jnp.abs(dx)
        kind = 3 - sum(jnp.where(reach > planes * k, 1, 0) for k in (1, 2, 3))
        tail = jnp.where(kind == 0, tails[0], jnp.where(kind == 1, tails[1], jnp.where(kind == 2, tails[2], tails[3])))
        code = a + jnp.left_shift(b, 10) + jnp.left_shift(dx + B, 20)
        lists[jnp.where(filled, kind * entries + tail, 4 * entries)] = code
        return tuple(tails[k] + jnp.where(filled & (kind == k), 1, 0) for k in range(4))

    zero = jnp.int32(0)
    tails = (zero,) * 4
    for layer in range(depth):
        tails = lax.fori_loop(0, owners, functools.partial(sort, layer=layer), tails, unroll=4)
    fits[0] = 0

    def trial(turn):
        def reset(i, unused):
            for g in range(groups):
                masks[g * local + i] = 1 << g
            return unused

        lax.fori_loop(0, local, reset, 0, unroll=4)
        state = (zero,) * (groups + 2)
        for kind, limit in enumerate((half // 4, half // 2, 3 * half // 4, half)):
            size = tails[kind]
            base = lax.rem(turn * 5, jnp.maximum(size, 1))
            flip = jnp.bitwise_and(turn, 1) > 0

            def deal(i, state, kind=kind, limit=limit, size=size, base=base, flip=flip):
                filled, tally, bad = state[:groups], state[groups], state[groups + 1]
                at = i + base
                at = jnp.where(at >= size, at - size, at)
                code = lists[kind * entries + jnp.where(flip, size - 1 - at, at)]
                a, b = unpack(code)
                mask_a, mask_b = masks[a], masks[b]
                group_a, group_b = group_of(a), group_of(b)
                same = jnp.where(group_a == group_b, 1, 0)

                def needs(h, count):
                    new_a = 1 - jnp.bitwise_and(jnp.right_shift(mask_a, h), 1)
                    new_b = 1 - jnp.bitwise_and(jnp.right_shift(mask_b, h), 1)
                    step_a = jnp.left_shift(jnp.bitwise_xor(group_a, h), 2)
                    step_b = jnp.left_shift(jnp.bitwise_xor(group_b, h), 2)
                    had_a = jnp.bitwise_and(jnp.right_shift(count, step_a), 15)
                    had_b = jnp.bitwise_and(jnp.right_shift(count, step_b), 15) + new_a * same
                    return new_a, new_b, step_a, step_b, had_a, had_b

                best = jnp.int32(worst)
                for h in range(groups):
                    new_a, new_b, unused_a, unused_b, had_a, had_b = needs(h, filled[h])
                    need = jnp.maximum(new_a * (had_a + 1), new_b * (had_b + 1))
                    up = jnp.bitwise_and(jnp.right_shift(tally, 8 * h), 15)
                    down = jnp.bitwise_and(jnp.right_shift(tally, 8 * h + 4), 15)
                    taken = jnp.minimum(up, down)
                    side = jnp.where(down < up, 32, 0)
                    cost = jnp.left_shift(2 * (new_a + new_b) + need + taken, 8) + (side + taken + (h << 6))
                    best = jnp.minimum(best, jnp.where((taken < limit) & (need <= cap), cost, worst))
                good = best < worst
                flag = jnp.where(good, 1, 0)
                column = jnp.bitwise_and(jnp.right_shift(best, 6), 3)
                side = jnp.bitwise_and(jnp.right_shift(best, 5), 1)
                slot = jnp.bitwise_and(best, 31)
                count = filled[0]
                for h in range(1, groups):
                    count = jnp.where(column == h, filled[h], count)
                new_a, new_b, step_a, step_b, had_a, had_b = needs(column, count)
                grown = count + flag * (jnp.left_shift(new_a, step_a) + jnp.left_shift(new_b, step_b))
                masks[a] = jnp.bitwise_or(mask_a, jnp.left_shift(flag, column))
                masks[b] = jnp.bitwise_or(mask_b, jnp.left_shift(flag, column))
                here = good & (column == me)
                mine[jnp.where(here, side * half + slot, each)] = code
                for orbit, group, new, had in ((a, group_a, new_a, had_a), (b, group_b, new_b, had_b)):
                    at = (jnp.bitwise_xor(group, column) - 1) * cap + had
                    spots[jnp.where(here & (new > 0), orbit, orbits)] = local + at
                    links[jnp.where(good & (new > 0) & (group == me), at, spare)] = orbit - group * local
                kept = tuple(jnp.where(column == h, grown, filled[h]) for h in range(groups))
                tally = tally + jnp.left_shift(flag, 8 * column + 4 * side)
                return kept + (tally, jnp.bitwise_or(bad, 1 - flag))

            state = lax.fori_loop(0, size, deal, state)
        for h in range(groups):
            counts[h] = state[h]
        fits[0] = 1 - state[groups + 1]

    def attempt(turn, unused):
        @pl.when(fits[0] == 0)
        def go():
            trial(turn)

        return unused

    lax.fori_loop(0, TRIALS, attempt, 0)

    @pl.when(fits[0] > 0)
    def settle():
        def fill(at, unused):
            code = mine[at]
            a, b = unpack(code)
            dx = jnp.right_shift(code, 20) - B
            spot_a, spot_b = spots[a], spots[b]
            rising = at < half
            second = jnp.where(rising, dx, -dx) >= 0
            shift = jnp.where(second, dx, -dx)
            tbl[0, at] = jnp.where(second, spot_b, spot_a)
            tbl[1, at] = jnp.where(second, spot_a, spot_b)
            tbl[2, at] = jnp.where(rising, 4 * planes, 0) - shift
            tbl[3, at] = jnp.where(second, 1, 0)
            tbl[4, at] = anchors[1, b] - anchors[1, a]
            tbl[5, at] = anchors[2, b] - anchors[2, a]
            tbl[6, at] = jnp.where(second, 0, shift)
            tbl[7, at] = jnp.where(rising, 0, 4 * planes) + shift
            return unused

        lax.fori_loop(0, each, fill, 0, unroll=2)
        for row, base in ((1, 0), (0, each)):
            def link(slot, unused, row=row, base=base):
                at = final + tbl[row, slot]
                tbl[9 - row, slot] = links[at]
                links[at] = base + slot
                return unused

            lax.fori_loop(0, each, link, 0)
        for turn in range(1, groups):
            def hook(i, unused, turn=turn):
                at = (turn - 1) * cap + i
                end = ends + links[at]
                links[prior + at] = links[end]
                links[end] = at
                return unused

            sent = jnp.bitwise_and(jnp.right_shift(counts[jnp.bitwise_xor(me, turn)], 4 * turn), 15)
            lax.fori_loop(0, sent, hook, 0)


def make_plan(anchors, pair_slots, cap, each, planes):
    orbits = anchors.shape[0]
    entries = pair_slots.shape[0] * pair_slots.shape[1]
    smem = pl.BlockSpec(memory_space=pltpu.SMEM)
    local = orbits // 4
    me = jnp.full((1,), lax.axis_index("grp"), jnp.int32)
    return pl.pallas_call(
        functools.partial(plan_kernel, cap, planes),
        in_specs=[smem] * 3,
        out_specs=[smem] * 3,
        out_shape=[
            jax.ShapeDtypeStruct((10, each), jnp.int32),
            jax.ShapeDtypeStruct((9 * cap + 2 * local + 1,), jnp.int32),
            jax.ShapeDtypeStruct((1,), jnp.int32),
        ],
        scratch_shapes=[
            pltpu.SMEM((orbits + 1,), jnp.int32), pltpu.SMEM((orbits,), jnp.int32),
            pltpu.SMEM((4 * entries + 1,), jnp.int32), pltpu.SMEM((each + 1,), jnp.int32),
            pltpu.SMEM((4,), jnp.int32),
        ],
        name="plan",
    )(me, anchors.T, jnp.transpose(pair_slots, (1, 2, 0)))


def fetch_kernel(chips, cap, tbl, links, orb, moved, fixed, *scratch):
    count = moved.shape[0]
    owns, parcels, pools, wins = [scratch[i * count : (i + 1) * count] for i in range(4)]
    own_sem, xy_send, xy_recv, z_send, z_recv = scratch[4 * count :]
    grp, place, across, along, corner = spot()
    core = lax.rem(place, 2)
    norb, planes = orb.shape[:2]
    slots = moved.shape[1]
    half = slots // 2
    relay = Relay(wins, z_send, z_recv, (1, -1), chips, (half // 4, half // 2, 3 * half // 4))

    def stage(chunk, kind):
        dst = owns[chunk] if kind == 0 else pools[chunk].at[pl.ds(0, norb)]
        return pltpu.make_async_copy(orb.at[:, :, pl.ds(chunk * SUB, SUB)], dst, own_sem.at[chunk, kind])

    def parcel(chunk, kind):
        return remote(
            parcels[chunk].at[pl.ds(kind * cap, cap)], pools[chunk].at[pl.ds(norb + kind * cap, cap)],
            xy_send.at[chunk, kind], xy_recv.at[chunk, kind], ((across, along, corner)[kind], place),
        )

    for chunk in range(count):
        stage(chunk, 0).start()
    for chunk in range(count):
        stage(chunk, 1).start()
    greet(chips, True)

    def pack(chunk):
        stage(chunk, 0).wait()

        def put(i, unused):
            parcels[chunk][i] = owns[chunk][links[i]]
            return unused

        lax.fori_loop(0, 3 * cap, put, 0)

    def send(chunk):
        for kind in (2, 0, 1):
            parcel(chunk, kind).start()

    pack(0)
    for chunk in range(1, count):
        pack(chunk)
        send(chunk - 1)
    send(count - 1)
    relay.clear()
    for step in range(count + 3):
        chunk = step
        if chunk < count:
            stage(chunk, 1).wait()
            for kind in range(3):
                parcel(chunk, kind).wait_recv()
            for side in range(2):
                start = relay.offset(relay.signs[side], 0) + planes * core

                def pick(slot, unused, start=start, chunk=chunk):
                    wins[chunk][slot, pl.ds(start, planes)] = pools[chunk][tbl[0, slot]]
                    return unused

                lax.fori_loop(side * half, (side + 1) * half, pick, 0)

            def hold(slot, unused, chunk=chunk):
                fixed[chunk, slot] = pools[chunk][tbl[1, slot]]
                return unused

            lax.fori_loop(0, slots, hold, 0)
            relay.begin(chunk)
        chunk = step - 1
        if 0 <= chunk < count:
            relay.first(chunk)
        chunk = step - 2
        if 0 <= chunk < count:
            relay.second(chunk)
        chunk = step - 3
        if 0 <= chunk < count:
            relay.settle(chunk)

            def choose(slot, unused, chunk=chunk):
                first = tbl[2, slot] + planes * core
                for plane in range(planes):
                    moved[chunk, slot, plane] = wins[chunk][slot, first + plane]
                return unused

            lax.fori_loop(0, slots, choose, 0)
    for chunk in range(count):
        for kind in range(3):
            parcel(chunk, kind).wait_send()
    relay.drain()


def fetch(table, links, stacked, slots, chips, cap):
    norb, planes, rows, lanes = stacked.shape
    chunks = rows // SUB
    vmem = pl.BlockSpec(memory_space=pltpu.VMEM)
    smem = pl.BlockSpec(memory_space=pltpu.SMEM)
    dma = pltpu.SemaphoreType.DMA
    shape = jax.ShapeDtypeStruct((chunks, slots, planes, SUB, lanes), jnp.float32)

    def room(count, deep=planes):
        return [pltpu.VMEM((count, deep, SUB, lanes), jnp.float32)] * chunks

    return pl.pallas_call(
        functools.partial(fetch_kernel, chips, cap),
        in_specs=[smem, smem, pl.BlockSpec(memory_space=pl.ANY)],
        out_specs=[vmem, vmem],
        out_shape=[shape, shape],
        scratch_shapes=room(norb) + room(3 * cap) + room(norb + 3 * cap) + room(slots, 6 * planes)
        + [dma((chunks, 2)), dma((chunks, 3)), dma((chunks, 3)), dma((chunks, 2, 5)), dma((chunks, 2, 5))],
        compiler_params=pltpu.CompilerParams(
            collective_id=3, has_side_effects=True, vmem_limit_bytes=48 * 1024 * 1024
        ),
        name="fetch",
    )(table, links, stacked)


def give_kernel(chips, cap, tbl, links, going, staying, out, *scratch):
    count, slots = going.shape[:2]
    wins, chains, parcels, backs, tallied = [scratch[i * count : (i + 1) * count] for i in range(5)]
    xy_send, xy_recv, z_send, z_recv = scratch[5 * count :]
    grp, place, across, along, corner = spot()
    core = lax.rem(place, 2)
    norb, planes = out.shape[:2]
    half = slots // 2
    extra = 3 * cap
    final = extra
    prior = final + norb + extra
    ends = prior + extra
    relay = Relay(wins, z_send, z_recv, (-1, 1), chips, (half // 4, half // 2, 3 * half // 4))
    greet(chips, True)

    def load(chunk):
        for side in range(2):
            at = relay.offset(relay.signs[side], 0) + planes * core

            def place_in(slot, unused, at=at):
                wins[chunk][slot, pl.ds(at, planes)] = going[chunk, slot]
                return unused

            lax.fori_loop(side * half, (side + 1) * half, place_in, 0)

    def parcel(chunk, kind):
        return remote(
            parcels[chunk].at[pl.ds(kind * cap, cap)], backs[chunk].at[pl.ds(kind * cap, cap)],
            xy_send.at[chunk, kind], xy_recv.at[chunk, kind], ((across, along, corner)[kind], place),
        )

    load(0)
    load(1)
    relay.begin(0)
    for chunk in range(2, count):
        load(chunk)
    relay.begin(1)
    relay.clear()
    for step in range(count + 3):
        if step < count:
            relay.first(step)
            if step + 2 < count:
                relay.begin(step + 2)
        chunk = step - 1
        if 0 <= chunk < count:
            relay.second(chunk)
        chunk = step - 2
        if 0 <= chunk < count:
            relay.settle(chunk)
            chain = chains[chunk]
            chain[2 * slots] = jnp.zeros(chain.shape[1:], jnp.float32)

            def link_fixed(slot, unused, chain=chain, chunk=chunk):
                chain[slot] = staying[chunk, slot] + chain[tbl[8, slot]]
                return unused

            def link_moved(slot, unused, chain=chain, chunk=chunk):
                first = tbl[7, slot] + planes * core
                for plane in range(planes):
                    chain[slots + slot, plane] = wins[chunk][slot, first + plane] + chain[tbl[9, slot], plane]
                return unused

            lax.fori_loop(0, slots, link_fixed, 0)
            lax.fori_loop(0, slots, link_moved, 0)

            def pack(i, unused, chain=chain, chunk=chunk):
                parcels[chunk][i] = chain[links[final + norb + i]]
                return unused

            lax.fori_loop(0, extra, pack, 0)
            for kind in (2, 0, 1):
                parcel(chunk, kind).start()
        chunk = step - 3
        if 0 <= chunk < count:
            total_of = tallied[chunk]
            total_of[extra] = jnp.zeros(total_of.shape[1:], jnp.float32)
            for kind in range(3):
                parcel(chunk, kind).wait_recv()

            def gather(i, unused, total_of=total_of, chunk=chunk):
                total_of[i] = backs[chunk][i] + total_of[links[prior + i]]
                return unused

            lax.fori_loop(0, extra, gather, 0)

            def keep(orbit, unused, total_of=total_of, chunk=chunk):
                found = total_of[links[ends + orbit]] + chains[chunk][links[final + orbit]]
                out[orbit, :, pl.ds(chunk * SUB, SUB)] = found
                return unused

            lax.fori_loop(0, norb, keep, 0)
    for chunk in range(count):
        for kind in range(3):
            parcel(chunk, kind).wait_send()
    relay.drain()


def give(table, links, going, staying, norb, chips, cap):
    chunks, slots, planes, sub, lanes = going.shape
    vmem = pl.BlockSpec(memory_space=pltpu.VMEM)
    smem = pl.BlockSpec(memory_space=pltpu.SMEM)
    dma = pltpu.SemaphoreType.DMA

    def room(count, deep=planes):
        return [pltpu.VMEM((count, deep, sub, lanes), jnp.float32)] * chunks

    return pl.pallas_call(
        functools.partial(give_kernel, chips, cap),
        in_specs=[smem, smem, vmem, vmem],
        out_specs=vmem,
        out_shape=jax.ShapeDtypeStruct((norb, planes, chunks * sub, lanes), jnp.float32),
        scratch_shapes=room(slots, 6 * planes) + room(2 * slots + 1) + room(3 * cap) + room(3 * cap)
        + room(3 * cap + 1) + [dma((chunks, 3)), dma((chunks, 3)), dma((chunks, 2, 5)), dma((chunks, 2, 5))],
        compiler_params=pltpu.CompilerParams(
            collective_id=4, has_side_effects=True, vmem_limit_bytes=48 * 1024 * 1024
        ),
        name="give",
    )(table, links, going, staying)


def full_tables(anchors, pair_slots, planes, groups, each):
    assignment = deal_evenly(pair_slots, groups, each)
    pairs = assignment[lax.axis_index("grp")]
    offsets = anchors[pairs[:, 1]] - anchors[pairs[:, 0]]
    dx, dy, dz = offsets[:, 0], offsets[:, 1], offsets[:, 2]
    slot = lax.broadcasted_iota(jnp.int32, (each,), 0)
    rising = slot < each // 2
    second = jnp.where(rising, dx >= 0, dx <= 0)
    shift = jnp.where(second, dx, -dx)
    moved_id = jnp.where(second, pairs[:, 1], pairs[:, 0])
    fixed_id = jnp.where(second, pairs[:, 0], pairs[:, 1])
    terms = jnp.concatenate([fixed_id, moved_id])
    at = lax.broadcasted_iota(jnp.int32, (2 * each, 2 * each), 0)
    before = lax.broadcasted_iota(jnp.int32, (2 * each, 2 * each), 1)
    found = jnp.where((terms[:, None] == terms[None, :]) & (before < at), before, -1)
    prior = jnp.max(found, axis=1)
    prior = jnp.where(prior < 0, 2 * each, prior)
    norb = anchors.shape[0]
    orbit = lax.broadcasted_iota(jnp.int32, (norb, 2 * each), 0)
    index = lax.broadcasted_iota(jnp.int32, (norb, 2 * each), 1)
    last = jnp.max(jnp.where(terms[None, :] == orbit, index, -1), axis=1)
    last = jnp.where(last < 0, 2 * each, last)
    table = jnp.stack([
        moved_id, fixed_id,
        jnp.where(rising, 4 * planes, 0) - shift,
        second.astype(jnp.int32), dy, dz,
        jnp.where(second, 0, shift),
        jnp.where(rising, 0, 4 * planes) + shift,
        prior[:each], prior[each:],
    ])
    return table, last


def slab_body(orbitals, anchors, pair_slots):
    groups, places = lax.axis_size("grp"), lax.axis_size("grid")
    norb_local, cells = orbitals.shape
    planes = cells // (B * B)
    each = PAIR_DEV * places
    chips = places // 2
    cap = 5 * norb_local // 16
    plan, links, fits = make_plan(anchors, pair_slots, cap, each, planes)
    stacked = orbitals.reshape(norb_local, planes, ROWS, LANES)

    def lean(stacked, anchors, pair_slots, plan, links):
        moved, fixed = fetch(plan, links, stacked, each, chips, cap)
        dens, partner = pair_up(plan, moved, fixed)
        pot = solve_slabs(plan, dens, places, 1)
        going, staying = make_terms(plan, pot, partner, moved, fixed)
        return give(plan, links, going, staying, norb_local, chips, cap)

    def full(stacked, anchors, pair_slots, plan, links):
        table, last = full_tables(anchors, pair_slots, planes, groups, each)
        moved, fixed = bring(table, stacked, each, groups, chips)
        dens, partner = pair_up(table, moved, fixed)
        pot = solve_slabs(table, dens, places, 5)
        going, staying = make_terms(table, pot, partner, moved, fixed)
        return hand_back(table, last, going, staying, norb_local, chips)

    out = lax.cond(fits[0] > 0, lean, full, stacked, anchors, pair_slots, plan, links)
    return out.reshape(norb_local, cells)


def slabs_fit(mesh):
    groups, places = mesh.shape["grp"], mesh.shape["grid"]
    return groups == 4 and places % 2 == 0 and 4 * (B // places) >= PAD


def solution(mesh):
    return jax.shard_map(
        slab_body if slabs_fit(mesh) else owner_body,
        mesh=mesh,
        in_specs=(P("grp", "grid"), P(), P()),
        out_specs=P("grp", "grid"),
        check_vma=False,
    )
```

```python
import functools
import math

import jax
import jax.numpy as jnp
from jax import lax
from jax.experimental import pallas as pl
from jax.experimental.pallas import tpu as pltpu
from jax.sharding import PartitionSpec as P

B = 64
PAIR_DEV = 2
ITERS = 3
MOST_CHUNKS = 2
LANES = 128
ROWS = B * B // LANES
PAD = 32
STEP = 4


def deal_evenly(pair_slots, owner_count, each_owner):
    flat_slots = pair_slots.reshape(-1, 2)
    filled = (flat_slots[:, 0] >= 0).astype(jnp.int32)
    position = jnp.cumsum(filled, dtype=jnp.int32) - filled
    wanted = lax.broadcasted_iota(jnp.int32, (owner_count, each_owner), 1) * owner_count
    wanted = (wanted + lax.broadcasted_iota(jnp.int32, (owner_count, each_owner), 0)).reshape(-1)
    matched = (position[None, :] == wanted[:, None]) & (filled[None, :] == 1)
    picked = jnp.sum(jnp.where(matched[:, :, None], flat_slots[None], 0), axis=1)
    return picked.reshape(owner_count, each_owner, 2)


def gather_kernel(ids_ref, src_ref, *out_refs):
    count, terms = out_refs[0].shape[:2]
    for slot, out_ref in enumerate(out_refs):
        def pick(dest, unused, slot=slot, out_ref=out_ref):
            for term in range(terms):
                out_ref[dest, term] = src_ref[ids_ref[(slot * count + dest) * terms + term]]
            return unused

        lax.fori_loop(0, count, pick, 0)


def gather_pieces(ids, pieces, slots, count):
    norb, rows, lanes = pieces.shape
    block = max(8, rows // 4)
    return pl.pallas_call(
        gather_kernel,
        grid_spec=pltpu.PrefetchScalarGridSpec(
            num_scalar_prefetch=1,
            grid=(rows // block,),
            in_specs=[pl.BlockSpec((norb, block, lanes), lambda i, ids: (0, i, 0))],
            out_specs=[pl.BlockSpec((count, 2, block, lanes), lambda i, ids: (0, 0, i, 0))] * slots,
        ),
        out_shape=[jax.ShapeDtypeStruct((count, 2, rows, lanes), jnp.float32)] * slots,
        cost_estimate=pl.CostEstimate(flops=0, bytes_accessed=8 * norb * rows * lanes, transcendentals=0),
        name="pick_pieces",
    )(ids, pieces)


def scatter_kernel(ids_ref, *refs):
    out_ref = refs[-1]
    out_ref[...] = jnp.zeros_like(out_ref)
    count, terms = refs[0].shape[:2]
    for slot, in_ref in enumerate(refs[:-1]):
        def add(dest, unused, slot=slot, in_ref=in_ref):
            for term in range(terms):
                orbit = ids_ref[(slot * count + dest) * terms + term]
                out_ref[orbit] = out_ref[orbit] + in_ref[dest, term]
            return unused

        lax.fori_loop(0, count, add, 0)


def scatter_pieces(ids, parts, norb):
    count, terms, rows, lanes = parts[0].shape
    block = max(8, rows // 4)
    return pl.pallas_call(
        scatter_kernel,
        grid_spec=pltpu.PrefetchScalarGridSpec(
            num_scalar_prefetch=1,
            grid=(rows // block,),
            in_specs=[pl.BlockSpec((count, terms, block, lanes), lambda i, ids: (0, 0, i, 0))] * len(parts),
            out_specs=pl.BlockSpec((norb, block, lanes), lambda i, ids: (0, i, 0)),
        ),
        out_shape=jax.ShapeDtypeStruct((norb, rows, lanes), jnp.float32),
        cost_estimate=pl.CostEstimate(flops=0, bytes_accessed=8 * norb * rows * lanes, transcendentals=0),
        name="add_pieces",
    )(ids, *parts)


def lane_ids(shape):
    return lax.broadcasted_iota(jnp.int32, shape, len(shape) - 1)


def shift_plane(plane, off_y, off_z):
    shape = plane.shape
    lane = lane_ids(shape)
    row = lax.broadcasted_iota(jnp.int32, shape, 0)
    linear = off_y * B + off_z
    across = jnp.bitwise_and(linear, LANES - 1)
    down = jnp.right_shift(linear, 7)
    turned = pltpu.roll(plane, across, 1)
    near = pltpu.roll(turned, jnp.bitwise_and(down, ROWS - 1), 0)
    far = pltpu.roll(turned, jnp.bitwise_and(down + 1, ROWS - 1), 0)
    moved = jnp.where(lane >= across, near, far)
    from_y = row * 2 + jnp.right_shift(lane, 6) - off_y
    from_z = jnp.bitwise_and(lane, B - 1) - off_z
    inside = (from_y >= 0) & (from_y < B) & (from_z >= 0) & (from_z < B)
    return jnp.where(inside, moved, 0.0)


def operate_plane(before, plane, after):
    shape = plane.shape
    lane = lane_ids(shape)
    row = lax.broadcasted_iota(jnp.int32, shape, 0)
    z = jnp.bitwise_and(lane, B - 1)
    upper_z = jnp.where(z < B - 1, pltpu.roll(plane, LANES - 1, 1), 0.0)
    lower_z = jnp.where(z > 0, pltpu.roll(plane, 1, 1), 0.0)
    half = pltpu.roll(plane, B, 1)
    down = jnp.where(row > 0, pltpu.roll(half, 1, 0), 0.0)
    up = jnp.where(row < ROWS - 1, pltpu.roll(half, ROWS - 1, 0), 0.0)
    beside = (before + after) + (half + jnp.where(lane < B, down, up))
    return 6.0 * plane - beside - upper_z - lower_z


def fold(values):
    return jnp.sum(values.reshape(ROWS // 8, 8, LANES), axis=0)


def total(acc):
    return jnp.sum(acc, axis=(0, 1), keepdims=True)


def solve_kernel(info_ref, *refs):
    chunks = (len(refs) - 6) // 2
    in_refs, out_refs = refs[:chunks], refs[chunks : 2 * chunks]
    wide, partner, direction, resid, image, potential = refs[2 * chunks :]
    count, terms, rows, lanes = in_refs[0].shape
    each = rows // ROWS
    dx, dy, dz = info_ref[0], info_ref[1], info_ref[2]
    keep = jnp.where(info_ref[3] > 0, 1.0, 0.0).astype(jnp.float32)
    edge = jnp.zeros((PAD, ROWS, LANES), jnp.float32)
    wide[pl.ds(0, PAD)] = edge
    wide[pl.ds(PAD + B, PAD)] = edge
    direction[0] = edge[0]
    direction[B + 1] = edge[0]
    none = jnp.zeros((8, LANES), jnp.float32)

    def place(owner, chunk, i):
        return (owner * chunks + chunk) * each + i

    def load(owner, unused):
        for chunk in range(chunks):
            for i in range(each):
                wide[PAD + place(owner, chunk, i)] = in_refs[chunk][owner, 1, pl.ds(i * ROWS, ROWS)]
        return unused

    lax.fori_loop(0, count, load, 0)

    def start(owner, acc):
        for chunk in range(chunks):
            for i in range(each):
                x = place(owner, chunk, i)
                other = shift_plane(wide[PAD + x - dx], dy, dz)
                partner[x] = other
                density = in_refs[chunk][owner, 0, pl.ds(i * ROWS, ROWS)] * other
                direction[x + 1] = density
                resid[x] = density
                acc = acc + fold(density * density)
        return acc

    norm_now = total(lax.fori_loop(0, count, start, none))

    for turn in range(ITERS):
        def apply(block, acc):
            for i in range(STEP):
                x = block * STEP + i
                plane = direction[x + 1]
                result = operate_plane(direction[x], plane, direction[x + 2])
                image[x] = result
                acc = acc + fold(plane * result)
            return acc

        step_len = norm_now / total(lax.fori_loop(0, B // STEP, apply, none))

        if turn == ITERS - 1:
            break

        def advance(block, acc):
            for i in range(STEP):
                x = block * STEP + i
                moved = step_len * direction[x + 1]
                potential[x] = moved if turn == 0 else potential[x] + moved
                left = resid[x] - step_len * image[x]
                resid[x] = left
                acc = acc + fold(left * left)
            return acc

        norm_next = total(lax.fori_loop(0, B // STEP, advance, none))
        ratio = norm_next / norm_now

        def renew(block, unused):
            for i in range(STEP):
                x = block * STEP + i
                direction[x + 1] = resid[x] + ratio * direction[x + 1]
            return unused

        lax.fori_loop(0, B // STEP, renew, 0)
        norm_now = norm_next

    def finish(owner, unused):
        for chunk in range(chunks):
            for i in range(each):
                x = place(owner, chunk, i)
                found = (potential[x] + step_len * direction[x + 1]) * keep
                out_refs[chunk][owner, 0, pl.ds(i * ROWS, ROWS)] = found * partner[x]
                wide[PAD + x] = found * in_refs[chunk][owner, 0, pl.ds(i * ROWS, ROWS)]
        return unused

    lax.fori_loop(0, count, finish, 0)

    def give_back(owner, unused):
        for chunk in range(chunks):
            for i in range(each):
                x = place(owner, chunk, i)
                out_refs[chunk][owner, 1, pl.ds(i * ROWS, ROWS)] = shift_plane(wide[PAD + x + dx], -dy, -dz)
        return unused

    lax.fori_loop(0, count, give_back, 0)


def solve_pair(info, parts):
    box = (B, ROWS, LANES)
    vmem = pl.BlockSpec(memory_space=pltpu.VMEM)
    return pl.pallas_call(
        solve_kernel,
        in_specs=[pl.BlockSpec(memory_space=pltpu.SMEM)] + [vmem] * len(parts),
        out_specs=[vmem] * len(parts),
        out_shape=[jax.ShapeDtypeStruct(p.shape, jnp.float32) for p in parts],
        scratch_shapes=[
            pltpu.VMEM((B + 2 * PAD, ROWS, LANES), jnp.float32),
            pltpu.VMEM(box, jnp.float32),
            pltpu.VMEM((B + 2, ROWS, LANES), jnp.float32),
            pltpu.VMEM(box, jnp.float32),
            pltpu.VMEM(box, jnp.float32),
            pltpu.VMEM(box, jnp.float32),
        ],
        compiler_params=pltpu.CompilerParams(vmem_limit_bytes=32 * 1024 * 1024),
        cost_estimate=pl.CostEstimate(flops=0, bytes_accessed=40 * 1024 * 1024, transcendentals=0),
        name="solve_pair",
    )(info, *parts)


def owner_body(orbitals, anchors, pair_slots):
    grid_count = lax.axis_size("grid")
    owner_count = lax.axis_size("grp") * grid_count
    group_idx = lax.axis_index("grp")
    place_idx = lax.axis_index("grid")
    assignment = deal_evenly(pair_slots, owner_count, PAIR_DEV)
    slots = assignment.shape[1]
    filled = assignment[..., 0] >= 0
    safe_ids = jnp.maximum(assignment, 0)
    group_table = lax.dynamic_slice_in_dim(safe_ids, group_idx * grid_count, grid_count, 0)
    ids = jnp.transpose(group_table, (1, 0, 2)).reshape(-1)
    owner_idx = group_idx * grid_count + place_idx
    own_pairs = safe_ids[owner_idx]
    offsets = anchors[own_pairs[:, 1]] - anchors[own_pairs[:, 0]]
    info = jnp.concatenate([offsets, filled[owner_idx].astype(jnp.int32)[:, None]], axis=1)

    norb_local, cells = orbitals.shape
    stacked = orbitals.reshape(norb_local, cells // LANES, LANES)
    chunks = math.gcd(MOST_CHUNKS, cells // (B * B))
    rows = stacked.shape[1] // chunks
    arrived = [[None] * chunks for _ in range(slots)]
    for chunk in range(chunks):
        pieces = lax.all_gather(stacked[:, chunk * rows : (chunk + 1) * rows], "grp", axis=0, tiled=True)
        outgoing = gather_pieces(ids, pieces, slots, grid_count)
        for slot in range(slots):
            arrived[slot][chunk] = lax.all_to_all(outgoing[slot], "grid", split_axis=0, concat_axis=0, tiled=True)
    returned = []
    for slot in range(slots):
        terms = solve_pair(info[slot], arrived[slot])
        returned.append(
            [lax.all_to_all(t, "grid", split_axis=0, concat_axis=0, tiled=True) for t in terms]
        )
    results = []
    for chunk in range(chunks):
        summed = scatter_pieces(ids, [r[chunk] for r in returned], anchors.shape[0])
        results.append(lax.psum_scatter(summed, "grp", scatter_dimension=0, tiled=True))
    return jnp.concatenate(results, axis=1).reshape(norb_local, cells)


MESH = pl.DeviceIdType.MESH
HALO = 3
WAVES = 4
TRIALS = 12
SUB = 8


def remote(src, dst, send_sem, recv_sem, device):
    return pltpu.make_async_remote_copy(
        src_ref=src, dst_ref=dst, send_sem=send_sem, recv_sem=recv_sem, device_id=device, device_id_type=MESH
    )


def spot():
    grp = lax.axis_index("grp")
    place = lax.axis_index("grid")
    across = grp + 1 - 2 * lax.rem(grp, 2)
    along = lax.rem(grp + 2, 4)
    corner = lax.rem(across + 2, 4)
    return grp, place, across, along, corner


def greet(chips, wide=False):
    grp, place, across, along, corner = spot()
    chip = place // 2
    core = lax.rem(place, 2)
    barrier = pltpu.get_barrier_semaphore()
    peers = [(across, place), (along, place), (grp, 2 * chip + 1 - core)] + ([(corner, place)] if wide else [])
    for device in peers:
        pl.semaphore_signal(barrier, inc=1, device_id=device, device_id_type=MESH)

    @pl.when(chip > 0)
    def below():
        pl.semaphore_signal(barrier, inc=1, device_id=(grp, place - 2), device_id_type=MESH)

    @pl.when(chip < chips - 1)
    def above():
        pl.semaphore_signal(barrier, inc=1, device_id=(grp, place + 2), device_id_type=MESH)

    ends = jnp.where(chip > 0, 1, 0) + jnp.where(chip < chips - 1, 1, 0)
    pl.semaphore_wait(barrier, len(peers) + ends)


class Relay:
    def __init__(self, wins, send_sem, recv_sem, signs, chips, marks):
        self.wins, self.send_sem, self.recv_sem, self.signs, self.chips = wins, send_sem, recv_sem, signs, chips
        self.grp, self.place = lax.axis_index("grp"), lax.axis_index("grid")
        self.chip = self.place // 2
        self.core = lax.rem(self.place, 2)
        self.half = wins[0].shape[0] // 2
        self.planes = wins[0].shape[1] // 6
        self.deep, self.far, self.mid = marks

    def offset(self, sign, hop):
        return 2 * self.planes * (2 - hop if sign > 0 else hop)

    def region(self, chunk, side, hop, core, size):
        start = self.offset(self.signs[side], hop) + self.planes * core
        return self.wins[chunk].at[pl.ds(side * self.half, size), pl.ds(start, self.planes)]

    def comes(self, side, hop):
        source = self.chip - self.signs[side] * hop
        return source >= 0 if self.signs[side] > 0 else source < self.chips

    def goes(self, side, hop):
        source = self.chip + self.signs[side] - self.signs[side] * hop
        if self.signs[side] > 0:
            return (self.chip + 1 < self.chips) & (source >= 0)
        return (self.chip - 1 >= 0) & (source < self.chips)

    def spans(self, side, hop, core, act):
        if hop == 0:
            act(self.half)
        else:
            near = 1 if self.signs[side] > 0 else 0
            most, least = (self.half, self.mid) if hop == 1 else (self.far, self.deep)
            if most == least:
                act(most)
                return

            @pl.when(core == near)
            def whole():
                act(most)

            @pl.when(core != near)
            def some():
                act(least)

    def onward(self, chunk, side, hop, size, here=None):
        source = self.region(chunk, side, hop - 1 if here is None else here, self.core, size)
        there = self.region(chunk, side, hop, self.core, size)
        return remote(
            source, there, self.send_sem.at[chunk, side, hop - 1], self.recv_sem.at[chunk, side, hop - 1],
            (self.grp, self.place + 2 * self.signs[side]),
        )

    def beside(self, chunk, side, hop, core, size):
        part = self.region(chunk, side, hop, core, size)
        return remote(
            part, part, self.send_sem.at[chunk, side, 2 + hop], self.recv_sem.at[chunk, side, 2 + hop],
            (self.grp, 2 * self.chip + 1 - self.core),
        )

    def clear(self):
        for side in range(2):
            for hop in (1, 2):
                start = self.offset(self.signs[side], hop)

                @pl.when(jnp.logical_not(self.comes(side, hop)))
                def fill(side=side, start=start):
                    for win in self.wins:
                        def zero(slot, unused, win=win):
                            win[slot, pl.ds(start, 2 * self.planes)] = jnp.zeros(
                                (2 * self.planes,) + win.shape[2:], jnp.float32
                            )
                            return unused

                        lax.fori_loop(side * self.half, (side + 1) * self.half, zero, 0)

    def pass_on(self, chunk, side, hop):
        @pl.when(self.goes(side, hop))
        def go():
            self.spans(side, hop, self.core, lambda size: self.onward(chunk, side, hop, size).start())

    def begin(self, chunk):
        for side in range(2):
            self.pass_on(chunk, side, 1)
            self.beside(chunk, side, 0, self.core, self.half).start()

    def take(self, chunk, side, hop):
        @pl.when(self.comes(side, hop))
        def got():
            def act(size):
                self.onward(chunk, side, hop, size, hop).wait_recv()

            self.spans(side, hop, self.core, act)

        if hop < 2:
            self.pass_on(chunk, side, hop + 1)

        @pl.when(self.comes(side, hop))
        def share():
            self.spans(side, hop, self.core, lambda size: self.beside(chunk, side, hop, self.core, size).start())

    def first(self, chunk):
        for side in range(2):
            self.take(chunk, side, 1)

    def second(self, chunk):
        for side in range(2):
            self.take(chunk, side, 2)

    def settle(self, chunk):
        other = 1 - self.core
        for side in range(2):
            self.beside(chunk, side, 0, other, self.half).wait_recv()
            for hop in (1, 2):
                @pl.when(self.comes(side, hop))
                def got(side=side, hop=hop):
                    self.spans(side, hop, other, lambda size: self.beside(chunk, side, hop, other, size).wait_recv())

    def drain(self):
        for chunk in range(len(self.wins)):
            for side in range(2):
                self.beside(chunk, side, 0, self.core, self.half).wait_send()
                for hop in (1, 2):
                    @pl.when(self.comes(side, hop))
                    def sent(chunk=chunk, side=side, hop=hop):
                        self.spans(
                            side, hop, self.core,
                            lambda size: self.beside(chunk, side, hop, self.core, size).wait_send(),
                        )

                    @pl.when(self.goes(side, hop))
                    def passed(chunk=chunk, side=side, hop=hop):
                        self.spans(
                            side, hop, self.core, lambda size: self.onward(chunk, side, hop, size).wait_send()
                        )


def bring_kernel(chips, tbl, orb, moved, fixed, *scratch):
    count = moved.shape[0]
    pools, wins = scratch[:count], scratch[count : 2 * count]
    own_sem, xy_send, xy_recv, z_send, z_recv = scratch[2 * count :]
    grp, place, across, along, corner = spot()
    core = lax.rem(place, 2)
    norb, planes = orb.shape[:2]
    part = norb // 2
    slots = moved.shape[1]
    relay = Relay(wins, z_send, z_recv, (1, -1), chips, (slots // 2,) * 3)

    def block(chunk, owner, start, size):
        return pools[chunk].at[pl.ds(owner * norb + start, size)]

    def stage(chunk):
        return pltpu.make_async_copy(
            orb.at[:, :, pl.ds(chunk * SUB, SUB)], block(chunk, grp, 0, norb), own_sem.at[chunk]
        )

    def hop(chunk, kind, owner, start, size, target):
        ref = block(chunk, owner, start, size)
        return remote(ref, ref, xy_send.at[chunk, kind], xy_recv.at[chunk, kind], (target, place))

    def direct(chunk, owners):
        return hop(chunk, 0, owners[0], 0, norb, across), hop(chunk, 1, owners[1], 0, norb, along)

    def turned(chunk, owners):
        return hop(chunk, 2, owners[0], 0, part, along), hop(chunk, 3, owners[1], part, part, across)

    for chunk in range(count):
        stage(chunk).start()
    greet(chips)
    relay.clear()

    def send_own(chunk):
        stage(chunk).wait()
        for copy in direct(chunk, (grp, grp)):
            copy.start()

    send_own(0)
    send_own(1)
    for step in range(count + 4):
        if step < count:
            for copy in direct(step, (across, along)):
                copy.wait_recv()
            for copy in turned(step, (across, along)):
                copy.start()
            if step + 2 < count:
                send_own(step + 2)
        chunk = step - 1
        if 0 <= chunk < count:
            for copy in turned(chunk, (corner, corner)):
                copy.wait_recv()
            for side in range(2):
                start = relay.offset(relay.signs[side], 0) + planes * core

                def pick(slot, unused, start=start, chunk=chunk):
                    wins[chunk][slot, pl.ds(start, planes)] = pools[chunk][tbl[0, slot]]
                    fixed[chunk, slot] = pools[chunk][tbl[1, slot]]
                    return unused

                lax.fori_loop(side * (slots // 2), (side + 1) * (slots // 2), pick, 0)
            relay.begin(chunk)
        chunk = step - 2
        if 0 <= chunk < count:
            relay.first(chunk)
        chunk = step - 3
        if 0 <= chunk < count:
            relay.second(chunk)
        chunk = step - 4
        if 0 <= chunk < count:
            relay.settle(chunk)

            def choose(slot, unused, chunk=chunk):
                first = tbl[2, slot] + planes * core
                for plane in range(planes):
                    moved[chunk, slot, plane] = wins[chunk][slot, first + plane]
                return unused

            lax.fori_loop(0, slots, choose, 0)
    for chunk in range(count):
        for copy in direct(chunk, (grp, grp)) + turned(chunk, (across, along)):
            copy.wait_send()
    relay.drain()


def bring(table, stacked, slots, groups, chips):
    norb, planes, rows, lanes = stacked.shape
    chunks = rows // SUB
    vmem = pl.BlockSpec(memory_space=pltpu.VMEM)
    dma = pltpu.SemaphoreType.DMA
    shape = jax.ShapeDtypeStruct((chunks, slots, planes, SUB, lanes), jnp.float32)
    return pl.pallas_call(
        functools.partial(bring_kernel, chips),
        in_specs=[pl.BlockSpec(memory_space=pltpu.SMEM), pl.BlockSpec(memory_space=pl.ANY)],
        out_specs=[vmem, vmem],
        out_shape=[shape, shape],
        scratch_shapes=[pltpu.VMEM((groups * norb, planes, SUB, lanes), jnp.float32)] * chunks
        + [pltpu.VMEM((slots, 6 * planes, SUB, lanes), jnp.float32)] * chunks
        + [dma((chunks,)), dma((chunks, 4)), dma((chunks, 4)), dma((chunks, 2, 5)), dma((chunks, 2, 5))],
        compiler_params=pltpu.CompilerParams(
            collective_id=0, has_side_effects=True, vmem_limit_bytes=48 * 1024 * 1024
        ),
        name="bring",
    )(table, stacked)


def pair_kernel(tbl, moved, fixed, dens, partner):
    def go(slot, unused):
        second = tbl[3, slot] > 0
        dy, dz = tbl[4, slot], tbl[5, slot]
        for x in range(moved.shape[2]):
            left = moved[:, slot, x].reshape(ROWS, LANES)
            right = fixed[:, slot, x].reshape(ROWS, LANES)
            other = shift_plane(jnp.where(second, left, right), dy, dz)
            dens[slot, x] = jnp.where(second, right, left) * other
            partner[slot, x] = other
        return unused

    lax.fori_loop(0, moved.shape[1], go, 0)


def pair_up(table, moved, fixed):
    chunks, slots, planes, sub, lanes = moved.shape
    vmem = pl.BlockSpec(memory_space=pltpu.VMEM)
    shape = jax.ShapeDtypeStruct((slots, planes, ROWS, lanes), jnp.float32)
    return pl.pallas_call(
        pair_kernel,
        in_specs=[pl.BlockSpec(memory_space=pltpu.SMEM), vmem, vmem],
        out_specs=[vmem, vmem],
        out_shape=[shape, shape],
        compiler_params=pltpu.CompilerParams(vmem_limit_bytes=24 * 1024 * 1024),
        name="pair_up",
    )(table, moved, fixed)


def inner(plane):
    shape = plane.shape
    lane = lane_ids(shape)
    row = lax.broadcasted_iota(jnp.int32, shape, 0)
    z = jnp.bitwise_and(lane, B - 1)
    upper_z = jnp.where(z < B - 1, pltpu.roll(plane, LANES - 1, 1), 0.0)
    lower_z = jnp.where(z > 0, pltpu.roll(plane, 1, 1), 0.0)
    half = pltpu.roll(plane, B, 1)
    down = jnp.where(row > 0, pltpu.roll(half, 1, 0), 0.0)
    up = jnp.where(row < ROWS - 1, pltpu.roll(half, ROWS - 1, 0), 0.0)
    return 6.0 * plane - ((half + jnp.where(lane < B, down, up)) + (upper_z + lower_z))


def krylov_weights(m):
    a0 = m[0] / m[1]
    rr1 = a0 * a0 * m[2] - m[0]
    p, q = 1.0 + rr1 / m[0], -a0
    a1 = rr1 / (p * p * m[1] + 2.0 * p * q * m[2] + q * q * m[3])
    s1, s2 = -a0 - a1 * p, -a1 * q
    rr2 = (m[0] + s1 * s1 * m[2] + s2 * s2 * m[4]) + 2.0 * (s1 * m[1] + s2 * m[2] + s1 * s2 * m[3])
    b1 = rr2 / rr1
    e0, e1, e2 = 1.0 + b1 * p, s1 + b1 * q, s2
    bend = e0 * e0 * m[1] + e1 * e1 * m[3] + e2 * e2 * m[5]
    a2 = rr2 / (bend + 2.0 * (e0 * e1 * m[2] + e0 * e2 * m[3] + e1 * e2 * m[4]))
    return a0 + a1 * p + a2 * e0, a1 * q + a2 * e1, a2 * e2


def solve_slabs_kernel(places, tbl, dens, pot, wide, one, two, sums, gathered, weights, h_send, h_recv, s_send, s_recv):
    grp, place = lax.axis_index("grp"), lax.axis_index("grid")
    slots, planes = dens.shape[:2]
    first, last = HALO, HALO + planes - 1
    each = slots // WAVES
    barrier = pltpu.get_barrier_semaphore()
    for step in range(1, places):
        pl.semaphore_signal(
            barrier, inc=1, device_id=(grp, lax.rem(place + step, places)), device_id_type=MESH
        )
    pl.semaphore_wait(barrier, places - 1)

    def rise(wave):
        return remote(
            dens.at[pl.ds(wave * each, each), pl.ds(planes - HALO + 1, HALO - 1)],
            wide.at[pl.ds(wave * each, each), pl.ds(1, HALO - 1)],
            h_send.at[wave, 0], h_recv.at[wave, 0], (grp, lax.rem(place + 1, places)),
        )

    def sink(wave):
        return remote(
            dens.at[pl.ds(wave * each, each), pl.ds(0, HALO)],
            wide.at[pl.ds(wave * each, each), pl.ds(HALO + planes, HALO)],
            h_send.at[wave, 1], h_recv.at[wave, 1], (grp, lax.rem(place + places - 1, places)),
        )

    lowest, highest = place == 0, place == places - 1
    for wave in range(WAVES):
        @pl.when(jnp.logical_not(highest))
        def send_up(wave=wave):
            rise(wave).start()

        @pl.when(jnp.logical_not(lowest))
        def send_down(wave=wave):
            sink(wave).start()

    blank = jnp.zeros((HALO, ROWS, LANES), jnp.float32)

    def copy_in(slot, unused):
        wide[slot, pl.ds(HALO, planes)] = dens[slot]
        one[slot, 1] = blank[0]
        one[slot, last + 3] = blank[0]
        one[slot, 0] = blank[0]
        return unused

    lax.fori_loop(0, slots, copy_in, 0)

    @pl.when(lowest)
    def no_below():
        def fill(slot, unused):
            wide[slot, pl.ds(0, HALO)] = blank
            return unused

        lax.fori_loop(0, slots, fill, 0)

    @pl.when(highest)
    def no_above():
        def fill(slot, unused):
            wide[slot, pl.ds(HALO + planes, HALO)] = blank
            return unused

        lax.fori_loop(0, slots, fill, 0)

    lane = lax.broadcasted_iota(jnp.int32, (1, LANES), 1)
    none = jnp.zeros((8, LANES), jnp.float32)

    def row_of(parts):
        row = jnp.zeros((1, LANES), jnp.float32)
        for at, part in parts:
            row = row + jnp.where(lane == at, total(part), 0.0)
        return row

    def work(slot, unused):
        low, high = tbl[6, slot], tbl[6, slot] + B

        def live(e):
            x = planes * place + e - HALO
            return jnp.where((x >= low) & (x < high), 1.0, 0.0).astype(jnp.float32)

        m0, m1, m2, m3, m4, m5 = none, none, none, none, none, none
        for e in range(first - 1, last + 3):
            value = live(e) * (inner(wide[slot, e]) - (wide[slot, e - 1] + wide[slot, e + 1]))
            one[slot, e] = value
            if first <= e <= last:
                source = wide[slot, e]
                m0 = m0 + fold(source * source)
                m1 = m1 + fold(source * value)
                m2 = m2 + fold(value * value)
        bent = None
        for e in range(first, last + 2):
            value = live(e) * (inner(one[slot, e]) - (one[slot, e - 1] + one[slot, e + 1]))
            two[slot, e] = value
            if e > first:
                m5 = m5 - 2.0 * fold(value * two[slot, e - 1])
            if e <= last:
                m3 = m3 + fold(one[slot, e] * value)
                m4 = m4 + fold(value * value)
                m5 = m5 + fold(value * inner(value))
        sums[pl.ds(slot, 1)] = row_of(enumerate((m0, m1, m2, m3, m4, m5)))
        return unused

    def rim(slot, spots, pairs):
        low, high = tbl[6, slot], tbl[6, slot] + B
        m2, m3, m4, m5 = none, none, none, none
        for e, fresh in spots:
            if fresh:
                x = planes * place + e - HALO
                alive = jnp.where((x >= low) & (x < high), 1.0, 0.0).astype(jnp.float32)
                two[slot, e] = alive * (inner(one[slot, e]) - (one[slot, e - 1] + one[slot, e + 1]))
        for e, fresh in spots:
            value, before = two[slot, e], one[slot, e]
            m2 = m2 + fold(before * before)
            m3 = m3 + fold(before * value)
            m4 = m4 + fold(value * value)
            m5 = m5 + fold(value * inner(value))
        for e in pairs:
            m5 = m5 - 2.0 * fold(two[slot, e] * two[slot, e + 1])
        sums[pl.ds(slot, 1)] = sums[pl.ds(slot, 1)] + row_of(((2, m2), (3, m3), (4, m4), (5, m5)))

    for wave in range(WAVES):
        @pl.when(jnp.logical_not(lowest))
        def got_below(wave=wave):
            rise(wave).wait_recv()

        @pl.when(jnp.logical_not(highest))
        def got_above(wave=wave):
            sink(wave).wait_recv()

        lax.fori_loop(wave * each, (wave + 1) * each, work, 0)

    @pl.when(lowest)
    def rim_below():
        def go(slot, unused):
            rim(slot, ((first - 2, True), (first - 1, True)), (first - 2, first - 1))
            return unused

        lax.fori_loop(0, slots, go, 0)

    @pl.when(highest)
    def rim_above():
        def go(slot, unused):
            rim(slot, ((last + 1, False), (last + 2, True)), (last + 1,))
            return unused

        lax.fori_loop(0, slots, go, 0)

    def tell(step):
        return remote(
            sums, gathered.at[place], s_send.at[step - 1], s_recv.at[step - 1],
            (grp, lax.rem(place + step, places)),
        )

    def hear(step):
        source = lax.rem(place + places - step, places)
        return remote(
            sums, gathered.at[source], s_send.at[step - 1], s_recv.at[step - 1],
            (grp, lax.rem(place + step, places)),
        )

    for step in range(1, places):
        tell(step).start()
    gathered[place] = sums[...]
    for step in range(1, places):
        hear(step).wait_recv()
    whole = gathered[0]
    for at in range(1, places):
        whole = whole + gathered[at]
    lanes = lax.broadcasted_iota(jnp.int32, whole.shape, 1)
    moments = [jnp.sum(jnp.where(lanes == at, whole, 0.0), axis=1, keepdims=True) for at in range(6)]
    for at, weight in enumerate(krylov_weights(moments)):
        weights[at] = jnp.broadcast_to(weight, whole.shape)

    def finish(slot, unused):
        w0, w1, w2 = [weights[at, pl.ds(slot, 1)] for at in range(3)]
        for x in range(planes):
            e = x + HALO
            pot[slot, x] = w0 * wide[slot, e] + w1 * one[slot, e] + w2 * two[slot, e]
        return unused

    lax.fori_loop(0, slots, finish, 0)
    for wave in range(WAVES):
        @pl.when(jnp.logical_not(highest))
        def sent_up(wave=wave):
            rise(wave).wait_send()

        @pl.when(jnp.logical_not(lowest))
        def sent_down(wave=wave):
            sink(wave).wait_send()

    for step in range(1, places):
        tell(step).wait_send()


def solve_slabs(table, dens, places, ident):
    slots, planes, rows, lanes = dens.shape
    vmem = pl.BlockSpec(memory_space=pltpu.VMEM)
    dma = pltpu.SemaphoreType.DMA
    tall = pltpu.VMEM((slots, planes + 2 * HALO, rows, lanes), jnp.float32)
    return pl.pallas_call(
        functools.partial(solve_slabs_kernel, places),
        in_specs=[pl.BlockSpec(memory_space=pltpu.SMEM), vmem],
        out_specs=vmem,
        out_shape=jax.ShapeDtypeStruct(dens.shape, jnp.float32),
        scratch_shapes=[
            tall, tall, tall,
            pltpu.VMEM((slots, lanes), jnp.float32),
            pltpu.VMEM((places, slots, lanes), jnp.float32),
            pltpu.VMEM((3, slots, lanes), jnp.float32),
            dma((WAVES, 2)), dma((WAVES, 2)), dma((places - 1,)), dma((places - 1,)),
        ],
        compiler_params=pltpu.CompilerParams(
            collective_id=ident, has_side_effects=True, vmem_limit_bytes=40 * 1024 * 1024
        ),
        name="solve_slabs",
    )(table, dens)


def term_kernel(tbl, pot, partner, moved, fixed, going, staying):
    chunks = going.shape[0]

    def go(slot, unused):
        second = tbl[3, slot] > 0
        dy, dz = tbl[4, slot], tbl[5, slot]
        for x in range(pot.shape[1]):
            found = pot[slot, x]
            left = moved[:, slot, x].reshape(ROWS, LANES)
            right = fixed[:, slot, x].reshape(ROWS, LANES)
            term_a = found * partner[slot, x]
            term_b = shift_plane(found * jnp.where(second, right, left), -dy, -dz)
            going[:, slot, x] = jnp.where(second, term_b, term_a).reshape(chunks, SUB, LANES)
            staying[:, slot, x] = jnp.where(second, term_a, term_b).reshape(chunks, SUB, LANES)
        return unused

    lax.fori_loop(0, pot.shape[0], go, 0)


def make_terms(table, pot, partner, moved, fixed):
    vmem = pl.BlockSpec(memory_space=pltpu.VMEM)
    shape = jax.ShapeDtypeStruct(moved.shape, jnp.float32)
    return pl.pallas_call(
        term_kernel,
        in_specs=[pl.BlockSpec(memory_space=pltpu.SMEM)] + [vmem] * 4,
        out_specs=[vmem, vmem],
        out_shape=[shape, shape],
        compiler_params=pltpu.CompilerParams(vmem_limit_bytes=24 * 1024 * 1024),
        name="make_terms",
    )(table, pot, partner, moved, fixed)


def hand_back_kernel(chips, tbl, last, going, staying, out, *scratch):
    count, slots = going.shape[:2]
    wins, chains, outs1, outs2, ins1, ins2 = [scratch[i * count : (i + 1) * count] for i in range(6)]
    xy_send, xy_recv, z_send, z_recv = scratch[6 * count :]
    grp, place, across, along, corner = spot()
    core = lax.rem(place, 2)
    norb, planes = out.shape[:2]
    part = norb // 2
    relay = Relay(wins, z_send, z_recv, (-1, 1), chips, (slots // 2,) * 3)
    greet(chips)
    relay.clear()

    def start(chunk):
        for side in range(2):
            at = relay.offset(relay.signs[side], 0) + planes * core

            def place_in(slot, unused, at=at):
                wins[chunk][slot, pl.ds(at, planes)] = going[chunk, slot]
                return unused

            lax.fori_loop(side * (slots // 2), (side + 1) * (slots // 2), place_in, 0)
        relay.begin(chunk)

    def swap(chunk, kind):
        src = (outs1 if kind < 2 else outs2)[chunk].at[kind % 2]
        dst = (ins1 if kind < 2 else ins2)[chunk].at[kind % 2]
        target = (across, along, along, across)[kind]
        return remote(src, dst, xy_send.at[chunk, kind], xy_recv.at[chunk, kind], (target, place))

    start(0)
    start(1)
    for step in range(count + 4):
        if step < count:
            relay.first(step)
            if step + 2 < count:
                start(step + 2)
        chunk = step - 1
        if 0 <= chunk < count:
            relay.second(chunk)
        chunk = step - 2
        if 0 <= chunk < count:
            relay.settle(chunk)
            chain = chains[chunk]
            chain[2 * slots] = jnp.zeros(chain.shape[1:], jnp.float32)

            def link_fixed(slot, unused, chain=chain, chunk=chunk):
                chain[slot] = staying[chunk, slot] + chain[tbl[8, slot]]
                return unused

            def link_moved(slot, unused, chain=chain, chunk=chunk):
                first = tbl[7, slot] + planes * core
                for plane in range(planes):
                    chain[slots + slot, plane] = wins[chunk][slot, first + plane] + chain[tbl[9, slot], plane]
                return unused

            lax.fori_loop(0, slots, link_fixed, 0)
            lax.fori_loop(0, slots, link_moved, 0)

            def pack(i, unused, chain=chain, chunk=chunk):
                outs1[chunk][0, i] = chain[last[across * norb + i]]
                outs1[chunk][0, part + i] = chain[last[corner * norb + i]]
                outs1[chunk][1, i] = chain[last[along * norb + part + i]]
                outs1[chunk][1, part + i] = chain[last[corner * norb + part + i]]
                return unused

            lax.fori_loop(0, part, pack, 0)
            swap(chunk, 0).start()
            swap(chunk, 1).start()
        chunk = step - 3
        if 0 <= chunk < count:
            chain = chains[chunk]
            swap(chunk, 0).wait_recv()

            def add_across(i, unused, chain=chain, chunk=chunk):
                outs2[chunk][0, i] = ins1[chunk][0, part + i] + chain[last[along * norb + i]]
                return unused

            lax.fori_loop(0, part, add_across, 0)
            swap(chunk, 2).start()
            swap(chunk, 1).wait_recv()

            def add_along(i, unused, chain=chain, chunk=chunk):
                outs2[chunk][1, i] = ins1[chunk][1, part + i] + chain[last[across * norb + part + i]]
                return unused

            lax.fori_loop(0, part, add_along, 0)
            swap(chunk, 3).start()
        chunk = step - 4
        if 0 <= chunk < count:
            chain = chains[chunk]
            swap(chunk, 2).wait_recv()
            swap(chunk, 3).wait_recv()
            for side in range(2):
                def keep(i, unused, side=side, chain=chain, chunk=chunk):
                    orbit = side * part + i
                    found = ins1[chunk][side, i] + ins2[chunk][side, i]
                    out[orbit, :, pl.ds(chunk * SUB, SUB)] = found + chain[last[grp * norb + orbit]]
                    return unused

                lax.fori_loop(0, part, keep, 0)
    for chunk in range(count):
        for kind in range(4):
            swap(chunk, kind).wait_send()
    relay.drain()


def hand_back(table, last, going, staying, norb, chips):
    chunks, slots, planes, sub, lanes = going.shape
    vmem = pl.BlockSpec(memory_space=pltpu.VMEM)
    smem = pl.BlockSpec(memory_space=pltpu.SMEM)
    dma = pltpu.SemaphoreType.DMA
    def room(*lead):
        return [pltpu.VMEM(lead + (planes, sub, lanes), jnp.float32)] * chunks
    wins = [pltpu.VMEM((slots, 6 * planes, sub, lanes), jnp.float32)] * chunks
    return pl.pallas_call(
        functools.partial(hand_back_kernel, chips),
        in_specs=[smem, smem, vmem, vmem],
        out_specs=vmem,
        out_shape=jax.ShapeDtypeStruct((norb, planes, chunks * sub, lanes), jnp.float32),
        scratch_shapes=wins + room(2 * slots + 1) + room(2, norb) + room(2, norb // 2)
        + room(2, norb) + room(2, norb // 2)
        + [dma((chunks, 4)), dma((chunks, 4)), dma((chunks, 2, 5)), dma((chunks, 2, 5))],
        compiler_params=pltpu.CompilerParams(
            collective_id=2, has_side_effects=True, vmem_limit_bytes=56 * 1024 * 1024
        ),
        name="hand_back",
    )(table, last, going, staying)


def plan_kernel(cap, planes, me_ref, anchors, pairs, tbl, links, fits, spots, masks, lists, mine, counts):
    groups = 4
    orbits = anchors.shape[1]
    local = orbits // groups
    depth, unused, owners = pairs.shape
    entries = depth * owners
    each = tbl.shape[1]
    half = each // 2
    extra = (groups - 1) * cap
    final = extra
    prior = final + local + extra
    ends = prior + extra
    spare = ends + local
    worst = 1 << 20
    me = me_ref[0]

    def group_of(orbit):
        if local & (local - 1) == 0:
            return jnp.right_shift(orbit, local.bit_length() - 1)
        return orbit // local

    def unpack(code):
        return jnp.bitwise_and(code, 1023), jnp.bitwise_and(jnp.right_shift(code, 10), 1023)

    def clean(i, unused):
        links[i] = 0
        links[prior + i] = extra
        return unused

    def close(i, unused):
        links[final + i] = 2 * each
        return unused

    def own(i, unused):
        links[ends + i] = extra
        spots[me * local + i] = i
        return unused

    lax.fori_loop(0, extra, clean, 0, unroll=5)
    lax.fori_loop(0, local + extra, close, 0)
    lax.fori_loop(0, local, own, 0, unroll=4)

    def sort(i, tails, layer):
        a, b = pairs[layer, 0, i], pairs[layer, 1, i]
        filled = a >= 0
        dx = anchors[0, jnp.maximum(b, 0)] - anchors[0, jnp.maximum(a, 0)]
        reach = jnp.abs(dx)
        kind = 3 - sum(jnp.where(reach > planes * k, 1, 0) for k in (1, 2, 3))
        tail = jnp.where(kind == 0, tails[0], jnp.where(kind == 1, tails[1], jnp.where(kind == 2, tails[2], tails[3])))
        code = a + jnp.left_shift(b, 10) + jnp.left_shift(dx + B, 20)
        lists[jnp.where(filled, kind * entries + tail, 4 * entries)] = code
        return tuple(tails[k] + jnp.where(filled & (kind == k), 1, 0) for k in range(4))

    zero = jnp.int32(0)
    tails = (zero,) * 4
    for layer in range(depth):
        tails = lax.fori_loop(0, owners, functools.partial(sort, layer=layer), tails, unroll=4)
    fits[0] = 0

    def trial(turn):
        def reset(i, unused):
            for g in range(groups):
                masks[g * local + i] = 1 << g
            return unused

        lax.fori_loop(0, local, reset, 0, unroll=4)
        state = (zero,) * (groups + 2)
        for kind, limit in enumerate((half // 4, half // 2, 3 * half // 4, half)):
            size = tails[kind]
            base = lax.rem(turn * 5, jnp.maximum(size, 1))
            flip = jnp.bitwise_and(turn, 1) > 0

            def deal(i, state, kind=kind, limit=limit, size=size, base=base, flip=flip):
                filled, tally, bad = state[:groups], state[groups], state[groups + 1]
                at = i + base
                at = jnp.where(at >= size, at - size, at)
                code = lists[kind * entries + jnp.where(flip, size - 1 - at, at)]
                a, b = unpack(code)
                mask_a, mask_b = masks[a], masks[b]
                group_a, group_b = group_of(a), group_of(b)
                same = jnp.where(group_a == group_b, 1, 0)

                def needs(h, count):
                    new_a = 1 - jnp.bitwise_and(jnp.right_shift(mask_a, h), 1)
                    new_b = 1 - jnp.bitwise_and(jnp.right_shift(mask_b, h), 1)
                    step_a = jnp.left_shift(jnp.bitwise_xor(group_a, h), 2)
                    step_b = jnp.left_shift(jnp.bitwise_xor(group_b, h), 2)
                    had_a = jnp.bitwise_and(jnp.right_shift(count, step_a), 15)
                    had_b = jnp.bitwise_and(jnp.right_shift(count, step_b), 15) + new_a * same
                    return new_a, new_b, step_a, step_b, had_a, had_b

                best = jnp.int32(worst)
                for h in range(groups):
                    new_a, new_b, unused_a, unused_b, had_a, had_b = needs(h, filled[h])
                    need = jnp.maximum(new_a * (had_a + 1), new_b * (had_b + 1))
                    up = jnp.bitwise_and(jnp.right_shift(tally, 8 * h), 15)
                    down = jnp.bitwise_and(jnp.right_shift(tally, 8 * h + 4), 15)
                    taken = jnp.minimum(up, down)
                    side = jnp.where(down < up, 32, 0)
                    cost = jnp.left_shift(2 * (new_a + new_b) + need + taken, 8) + (side + taken + (h << 6))
                    best = jnp.minimum(best, jnp.where((taken < limit) & (need <= cap), cost, worst))
                good = best < worst
                flag = jnp.where(good, 1, 0)
                column = jnp.bitwise_and(jnp.right_shift(best, 6), 3)
                side = jnp.bitwise_and(jnp.right_shift(best, 5), 1)
                slot = jnp.bitwise_and(best, 31)
                count = filled[0]
                for h in range(1, groups):
                    count = jnp.where(column == h, filled[h], count)
                new_a, new_b, step_a, step_b, had_a, had_b = needs(column, count)
                grown = count + flag * (jnp.left_shift(new_a, step_a) + jnp.left_shift(new_b, step_b))
                masks[a] = jnp.bitwise_or(mask_a, jnp.left_shift(flag, column))
                masks[b] = jnp.bitwise_or(mask_b, jnp.left_shift(flag, column))
                here = good & (column == me)
                mine[jnp.where(here, side * half + slot, each)] = code
                for orbit, group, new, had in ((a, group_a, new_a, had_a), (b, group_b, new_b, had_b)):
                    at = (jnp.bitwise_xor(group, column) - 1) * cap + had
                    spots[jnp.where(here & (new > 0), orbit, orbits)] = local + at
                    links[jnp.where(good & (new > 0) & (group == me), at, spare)] = orbit - group * local
                kept = tuple(jnp.where(column == h, grown, filled[h]) for h in range(groups))
                tally = tally + jnp.left_shift(flag, 8 * column + 4 * side)
                return kept + (tally, jnp.bitwise_or(bad, 1 - flag))

            state = lax.fori_loop(0, size, deal, state)
        for h in range(groups):
            counts[h] = state[h]
        fits[0] = 1 - state[groups + 1]

    def attempt(turn, unused):
        @pl.when(fits[0] == 0)
        def go():
            trial(turn)

        return unused

    lax.fori_loop(0, TRIALS, attempt, 0)

    @pl.when(fits[0] > 0)
    def settle():
        def fill(at, unused):
            code = mine[at]
            a, b = unpack(code)
            dx = jnp.right_shift(code, 20) - B
            spot_a, spot_b = spots[a], spots[b]
            rising = at < half
            second = jnp.where(rising, dx, -dx) >= 0
            shift = jnp.where(second, dx, -dx)
            tbl[0, at] = jnp.where(second, spot_b, spot_a)
            tbl[1, at] = jnp.where(second, spot_a, spot_b)
            tbl[2, at] = jnp.where(rising, 4 * planes, 0) - shift
            tbl[3, at] = jnp.where(second, 1, 0)
            tbl[4, at] = anchors[1, b] - anchors[1, a]
            tbl[5, at] = anchors[2, b] - anchors[2, a]
            tbl[6, at] = jnp.where(second, 0, shift)
            tbl[7, at] = jnp.where(rising, 0, 4 * planes) + shift
            return unused

        lax.fori_loop(0, each, fill, 0, unroll=2)
        for row, base in ((1, 0), (0, each)):
            def link(slot, unused, row=row, base=base):
                at = final + tbl[row, slot]
                tbl[9 - row, slot] = links[at]
                links[at] = base + slot
                return unused

            lax.fori_loop(0, each, link, 0)
        for turn in range(1, groups):
            def hook(i, unused, turn=turn):
                at = (turn - 1) * cap + i
                end = ends + links[at]
                links[prior + at] = links[end]
                links[end] = at
                return unused

            sent = jnp.bitwise_and(jnp.right_shift(counts[jnp.bitwise_xor(me, turn)], 4 * turn), 15)
            lax.fori_loop(0, sent, hook, 0)


def make_plan(anchors, pair_slots, cap, each, planes):
    orbits = anchors.shape[0]
    entries = pair_slots.shape[0] * pair_slots.shape[1]
    smem = pl.BlockSpec(memory_space=pltpu.SMEM)
    local = orbits // 4
    me = jnp.full((1,), lax.axis_index("grp"), jnp.int32)
    return pl.pallas_call(
        functools.partial(plan_kernel, cap, planes),
        in_specs=[smem] * 3,
        out_specs=[smem] * 3,
        out_shape=[
            jax.ShapeDtypeStruct((10, each), jnp.int32),
            jax.ShapeDtypeStruct((9 * cap + 2 * local + 1,), jnp.int32),
            jax.ShapeDtypeStruct((1,), jnp.int32),
        ],
        scratch_shapes=[
            pltpu.SMEM((orbits + 1,), jnp.int32), pltpu.SMEM((orbits,), jnp.int32),
            pltpu.SMEM((4 * entries + 1,), jnp.int32), pltpu.SMEM((each + 1,), jnp.int32),
            pltpu.SMEM((4,), jnp.int32),
        ],
        name="plan",
    )(me, anchors.T, jnp.transpose(pair_slots, (1, 2, 0)))


def coupled(plane):
    shape = plane.shape
    lane = lane_ids(shape)
    row = lax.broadcasted_iota(jnp.int32, shape, 0)
    lower_z = jnp.where(jnp.bitwise_and(lane, B - 1) > 0, pltpu.roll(plane, 1, 1), 0.0)
    half = pltpu.roll(plane, B, 1)
    down = jnp.where(row > 0, pltpu.roll(half, 1, 0), 0.0)
    return 3.0 * plane - lower_z - jnp.where(lane < B, down, half)


def lean_kernel(chips, cap, tbl, links, orb, out, *scratch):
    count = out.shape[2] // SUB
    owns, parcels, pools, wins, wins_back, chains, parcels_back, backs, tallied = [
        scratch[i * count : (i + 1) * count] for i in range(9)
    ]
    partner, wide, one, two, staying, held, sums, gathered, weights = scratch[9 * count : 9 * count + 9]
    (own_sem, xy_send, xy_recv, z_send, z_recv, yx_send, yx_recv, zb_send, zb_recv,
     h_send, h_recv, s_send, s_recv) = scratch[9 * count + 9 :]
    grp, place, across, along, corner = spot()
    core = lax.rem(place, 2)
    places = 2 * chips
    norb, planes = out.shape[:2]
    slots = partner.shape[0]
    half = slots // 2
    first, last = HALO, HALO + planes - 1
    each = slots // WAVES
    marks = (half // 4, half // 2, 3 * half // 4)
    relay = Relay(wins, z_send, z_recv, (1, -1), chips, marks)
    relay_back = Relay(wins_back, zb_send, zb_recv, (-1, 1), chips, marks)
    lowest, highest = place == 0, place == places - 1

    def stage(chunk, kind):
        dst = owns[chunk] if kind == 0 else pools[chunk].at[pl.ds(0, norb)]
        return pltpu.make_async_copy(orb.at[:, :, pl.ds(chunk * SUB, SUB)], dst, own_sem.at[chunk, kind])

    for kind in range(2):
        for chunk in range(count):
            stage(chunk, kind).start()
    barrier = pltpu.get_barrier_semaphore()
    for step in range(1, places):
        pl.semaphore_signal(
            barrier, inc=1, device_id=(grp, lax.rem(place + step, places)), device_id_type=MESH
        )
    for target in (across, along, corner):
        pl.semaphore_signal(barrier, inc=1, device_id=(target, place), device_id_type=MESH)

    def parcel(chunk, kind):
        return remote(
            parcels[chunk].at[pl.ds(kind * cap, cap)], pools[chunk].at[pl.ds(norb + kind * cap, cap)],
            xy_send.at[chunk, kind], xy_recv.at[chunk, kind], ((across, along, corner)[kind], place),
        )

    def pack(chunk):
        stage(chunk, 0).wait()

        def put(i, unused):
            parcels[chunk][i] = owns[chunk][links[i]]
            return unused

        lax.fori_loop(0, 3 * cap, put, 0)

    def send(chunk):
        for kind in (2, 0, 1):
            parcel(chunk, kind).start()

    pack(0)
    pl.semaphore_wait(barrier, places + 2)
    for chunk in range(1, count):
        pack(chunk)
        send(chunk - 1)
    send(count - 1)
    relay.clear()
    relay_back.clear()
    blank = jnp.zeros((HALO, ROWS, LANES), jnp.float32)

    def clear(slot, unused):
        for e in (0, 1, last + 3):
            one[slot, e] = blank[0]
        return unused

    lax.fori_loop(0, slots, clear, 0)

    @pl.when(lowest)
    def no_below():
        def fill(slot, unused):
            wide[slot, pl.ds(0, HALO)] = blank
            return unused

        lax.fori_loop(0, slots, fill, 0)

    @pl.when(highest)
    def no_above():
        def fill(slot, unused):
            wide[slot, pl.ds(HALO + planes, HALO)] = blank
            return unused

        lax.fori_loop(0, slots, fill, 0)

    for step in range(count + 3):
        chunk = step
        if chunk < count:
            stage(chunk, 1).wait()
            for kind in range(3):
                parcel(chunk, kind).wait_recv()
            for side in range(2):
                start = relay.offset(relay.signs[side], 0) + planes * core

                def pick(slot, unused, start=start, chunk=chunk):
                    wins[chunk][slot, pl.ds(start, planes)] = pools[chunk][tbl[0, slot]]
                    return unused

                lax.fori_loop(side * half, (side + 1) * half, pick, 0)
            relay.begin(chunk)
        chunk = step - 1
        if 0 <= chunk < count:
            relay.first(chunk)
        chunk = step - 2
        if 0 <= chunk < count:
            relay.second(chunk)
        chunk = step - 3
        if 0 <= chunk < count:
            relay.settle(chunk)

    def couple_of(slot, x):
        at = tbl[2, slot] + planes * core + x
        held_at = tbl[1, slot]
        left = jnp.concatenate([win[slot, at] for win in wins], axis=0)
        right = jnp.concatenate([pool[held_at, x] for pool in pools], axis=0)
        return left, right

    def rise(wave):
        return remote(
            wide.at[pl.ds(wave * each, each), pl.ds(last - HALO + 2, HALO - 1)],
            wide.at[pl.ds(wave * each, each), pl.ds(1, HALO - 1)],
            h_send.at[wave, 0], h_recv.at[wave, 0], (grp, lax.rem(place + 1, places)),
        )

    def sink(wave):
        return remote(
            wide.at[pl.ds(wave * each, each), pl.ds(first, HALO)],
            wide.at[pl.ds(wave * each, each), pl.ds(last + 1, HALO)],
            h_send.at[wave, 1], h_recv.at[wave, 1], (grp, lax.rem(place + places - 1, places)),
        )

    def edges(wave):
        @pl.when(jnp.logical_not(highest))
        def send_up():
            rise(wave).start()

        @pl.when(jnp.logical_not(lowest))
        def send_down():
            sink(wave).start()

    def make(slot, unused):
        second = tbl[3, slot] > 0
        dy, dz = tbl[4, slot], tbl[5, slot]
        for x in range(planes):
            left, right = couple_of(slot, x)
            other = shift_plane(jnp.where(second, left, right), dy, dz)
            wide[slot, x + HALO] = jnp.where(second, right, left) * other
            partner[slot, x] = other
        return unused

    none = jnp.zeros((8, LANES), jnp.float32)
    lane = lax.broadcasted_iota(jnp.int32, (1, LANES), 1)

    def row_of(parts):
        row = jnp.zeros((1, LANES), jnp.float32)
        for at, part in parts:
            row = row + jnp.where(lane == at, total(part), 0.0)
        return row

    def live(slot, e):
        x = planes * place + e - HALO
        low = tbl[6, slot]
        return jnp.where((x >= low) & (x < low + B), 1.0, 0.0).astype(jnp.float32)

    def raise_one(slot, e, acc):
        source = wide[slot, e]
        value = live(slot, e) * (inner(source) - (wide[slot, e - 1] + wide[slot, e + 1]))
        one[slot, e] = value
        if first <= e <= last:
            acc[1] = acc[1] + fold(source * value)
            acc[2] = acc[2] + fold(value * value)

    def raise_two(slot, e):
        source = one[slot, e]
        two[slot, e] = live(slot, e) * (inner(source) - (one[slot, e - 1] + one[slot, e + 1]))

    def measure_two(slot, e, acc, below):
        value = two[slot, e]
        acc[3] = acc[3] + fold(one[slot, e] * value)
        acc[4] = acc[4] + fold(value * value)
        bent = coupled(value)
        acc[5] = acc[5] + fold(value * (bent - two[slot, e - 1] if below else bent))

    def work_inside(slot, unused):
        acc = [none] * 6
        for e in range(first, last + 1):
            source = wide[slot, e]
            acc[0] = acc[0] + fold(source * source)
        for e in range(first + 1, last):
            raise_one(slot, e, acc)
        for e in range(first + 2, last - 1):
            raise_two(slot, e)
            measure_two(slot, e, acc, e > first + 2)
        for at in range(6):
            held[slot, at] = acc[at]
        return unused

    def work_edges(slot, unused):
        acc = [held[slot, at] for at in range(6)]
        for e in (first - 1, first, last, last + 1, last + 2):
            raise_one(slot, e, acc)
        for e in (first, first + 1, last - 1, last, last + 1):
            raise_two(slot, e)
        for e in (first, first + 1, last - 1, last):
            measure_two(slot, e, acc, e > first)
        acc[5] = acc[5] - fold(two[slot, first + 2] * two[slot, first + 1])
        acc[5] = acc[5] - fold(two[slot, last + 1] * two[slot, last])
        acc[5] = 2.0 * acc[5]
        sums[pl.ds(slot, 1)] = row_of(enumerate(acc))
        return unused

    def rim(slot, fresh, spots, pairs):
        for e in fresh:
            raise_two(slot, e)
        m2, m3, m4, m5 = none, none, none, none
        for e in spots:
            value, before = two[slot, e], one[slot, e]
            m2 = m2 + fold(before * before)
            m3 = m3 + fold(before * value)
            m4 = m4 + fold(value * value)
            m5 = m5 + fold(value * coupled(value))
        for e in pairs:
            m5 = m5 - fold(two[slot, e] * two[slot, e + 1])
        sums[pl.ds(slot, 1)] = sums[pl.ds(slot, 1)] + row_of(((2, m2), (3, m3), (4, m4), (5, 2.0 * m5)))

    lax.fori_loop(0, each, make, 0)
    for wave in range(1, WAVES):
        lax.fori_loop(wave * each, (wave + 1) * each, make, 0)
        edges(wave - 1)
    edges(WAVES - 1)
    lax.fori_loop(0, slots, work_inside, 0)
    for wave in range(WAVES):
        @pl.when(jnp.logical_not(lowest))
        def got_below(wave=wave):
            rise(wave).wait_recv()

        @pl.when(jnp.logical_not(highest))
        def got_above(wave=wave):
            sink(wave).wait_recv()

        lax.fori_loop(wave * each, (wave + 1) * each, work_edges, 0)

    @pl.when(lowest)
    def rim_below():
        def go(slot, unused):
            rim(slot, (first - 2, first - 1), (first - 2, first - 1), (first - 2, first - 1))
            return unused

        lax.fori_loop(0, slots, go, 0)

    @pl.when(highest)
    def rim_above():
        def go(slot, unused):
            rim(slot, (last + 2,), (last + 1, last + 2), (last + 1,))
            return unused

        lax.fori_loop(0, slots, go, 0)

    def tell(step, at):
        return remote(
            sums, gathered.at[at], s_send.at[step - 1], s_recv.at[step - 1],
            (grp, lax.rem(place + step, places)),
        )

    for step in range(1, places):
        tell(step, place).start()
    gathered[place] = sums[...]
    for step in range(1, places):
        tell(step, lax.rem(place + places - step, places)).wait_recv()
    whole = gathered[0]
    for at in range(1, places):
        whole = whole + gathered[at]
    lanes = lax.broadcasted_iota(jnp.int32, whole.shape, 1)
    moments = [jnp.sum(jnp.where(lanes == at, whole, 0.0), axis=1, keepdims=True) for at in range(6)]
    for at, weight in enumerate(krylov_weights(moments)):
        weights[at] = jnp.broadcast_to(weight, whole.shape)

    for side in range(2):
        start = relay_back.offset(relay_back.signs[side], 0) + planes * core

        def finish(slot, unused, start=start):
            second = tbl[3, slot] > 0
            dy, dz = tbl[4, slot], tbl[5, slot]
            w0, w1, w2 = [weights[at, pl.ds(slot, 1)] for at in range(3)]
            for x in range(planes):
                e = x + HALO
                found = w0 * wide[slot, e] + w1 * one[slot, e] + w2 * two[slot, e]
                left, right = couple_of(slot, x)
                term_a = found * partner[slot, x]
                term_b = shift_plane(found * jnp.where(second, right, left), -dy, -dz)
                going = jnp.where(second, term_b, term_a)
                stays = jnp.where(second, term_a, term_b)
                for chunk in range(count):
                    wins_back[chunk][slot, start + x] = going[chunk * SUB : (chunk + 1) * SUB]
                    staying[chunk, slot, x] = stays[chunk * SUB : (chunk + 1) * SUB]
            return unused

        lax.fori_loop(side * half, (side + 1) * half, finish, 0)

    extra = 3 * cap
    final = extra
    prior = final + norb + extra
    ends = prior + extra

    def reply(chunk, kind):
        return remote(
            parcels_back[chunk].at[pl.ds(kind * cap, cap)], backs[chunk].at[pl.ds(kind * cap, cap)],
            yx_send.at[chunk, kind], yx_recv.at[chunk, kind], ((across, along, corner)[kind], place),
        )

    relay_back.begin(0)
    relay_back.begin(1)
    for step in range(count + 3):
        if step < count:
            relay_back.first(step)
            if step + 2 < count:
                relay_back.begin(step + 2)
        chunk = step - 1
        if 0 <= chunk < count:
            relay_back.second(chunk)
        chunk = step - 2
        if 0 <= chunk < count:
            relay_back.settle(chunk)
            chain = chains[chunk]
            chain[2 * slots] = jnp.zeros(chain.shape[1:], jnp.float32)

            def link_fixed(slot, unused, chain=chain, chunk=chunk):
                chain[slot] = staying[chunk, slot] + chain[tbl[8, slot]]
                return unused

            def link_moved(slot, unused, chain=chain, chunk=chunk):
                at = tbl[7, slot] + planes * core
                for plane in range(planes):
                    chain[slots + slot, plane] = wins_back[chunk][slot, at + plane] + chain[tbl[9, slot], plane]
                return unused

            lax.fori_loop(0, slots, link_fixed, 0)
            lax.fori_loop(0, slots, link_moved, 0)

            def wrap(i, unused, chain=chain, chunk=chunk):
                parcels_back[chunk][i] = chain[links[final + norb + i]]
                return unused

            lax.fori_loop(0, extra, wrap, 0)
            for kind in (2, 0, 1):
                reply(chunk, kind).start()
        chunk = step - 3
        if 0 <= chunk < count:
            total_of = tallied[chunk]
            total_of[extra] = jnp.zeros(total_of.shape[1:], jnp.float32)
            for kind in range(3):
                reply(chunk, kind).wait_recv()

            def gather(i, unused, total_of=total_of, chunk=chunk):
                total_of[i] = backs[chunk][i] + total_of[links[prior + i]]
                return unused

            lax.fori_loop(0, extra, gather, 0)

            def keep(orbit, unused, total_of=total_of, chunk=chunk):
                found = total_of[links[ends + orbit]] + chains[chunk][links[final + orbit]]
                out[orbit, :, pl.ds(chunk * SUB, SUB)] = found
                return unused

            lax.fori_loop(0, norb, keep, 0)
    for chunk in range(count):
        for kind in range(3):
            parcel(chunk, kind).wait_send()
            reply(chunk, kind).wait_send()
    for wave in range(WAVES):
        @pl.when(jnp.logical_not(highest))
        def sent_up(wave=wave):
            rise(wave).wait_send()

        @pl.when(jnp.logical_not(lowest))
        def sent_down(wave=wave):
            sink(wave).wait_send()

    for step in range(1, places):
        tell(step, place).wait_send()
    relay.drain()
    relay_back.drain()


def run_lean(table, links, stacked, slots, chips, cap):
    norb, planes, rows, lanes = stacked.shape
    chunks = rows // SUB
    places = 2 * chips
    smem = pl.BlockSpec(memory_space=pltpu.SMEM)
    dma = pltpu.SemaphoreType.DMA

    def room(count, deep=planes):
        return [pltpu.VMEM((count, deep, SUB, lanes), jnp.float32)] * chunks

    tall = pltpu.VMEM((slots, planes + 2 * HALO, rows, lanes), jnp.float32)
    xy, z = dma((chunks, 3)), dma((chunks, 2, 5))
    return pl.pallas_call(
        functools.partial(lean_kernel, chips, cap),
        in_specs=[smem, smem, pl.BlockSpec(memory_space=pl.ANY)],
        out_specs=pl.BlockSpec(memory_space=pltpu.VMEM),
        out_shape=jax.ShapeDtypeStruct(stacked.shape, jnp.float32),
        scratch_shapes=room(norb) + room(3 * cap) + room(norb + 3 * cap) + room(slots, 6 * planes)
        + room(slots, 6 * planes) + room(2 * slots + 1) + room(3 * cap) + room(3 * cap) + room(3 * cap + 1)
        + [
            pltpu.VMEM((slots, planes, rows, lanes), jnp.float32), tall, tall, tall,
            pltpu.VMEM((chunks, slots, planes, SUB, lanes), jnp.float32),
            pltpu.VMEM((slots, 6, 8, lanes), jnp.float32),
            pltpu.VMEM((slots, lanes), jnp.float32),
            pltpu.VMEM((places, slots, lanes), jnp.float32),
            pltpu.VMEM((3, slots, lanes), jnp.float32),
            dma((chunks, 2)), xy, xy, z, z, xy, xy, z, z,
            dma((WAVES, 2)), dma((WAVES, 2)), dma((places - 1,)), dma((places - 1,)),
        ],
        compiler_params=pltpu.CompilerParams(
            collective_id=3, has_side_effects=True, vmem_limit_bytes=67043328
        ),
        name="lean",
    )(table, links, stacked)


def full_tables(anchors, pair_slots, planes, groups, each):
    assignment = deal_evenly(pair_slots, groups, each)
    pairs = assignment[lax.axis_index("grp")]
    offsets = anchors[pairs[:, 1]] - anchors[pairs[:, 0]]
    dx, dy, dz = offsets[:, 0], offsets[:, 1], offsets[:, 2]
    slot = lax.broadcasted_iota(jnp.int32, (each,), 0)
    rising = slot < each // 2
    second = jnp.where(rising, dx >= 0, dx <= 0)
    shift = jnp.where(second, dx, -dx)
    moved_id = jnp.where(second, pairs[:, 1], pairs[:, 0])
    fixed_id = jnp.where(second, pairs[:, 0], pairs[:, 1])
    terms = jnp.concatenate([fixed_id, moved_id])
    at = lax.broadcasted_iota(jnp.int32, (2 * each, 2 * each), 0)
    before = lax.broadcasted_iota(jnp.int32, (2 * each, 2 * each), 1)
    found = jnp.where((terms[:, None] == terms[None, :]) & (before < at), before, -1)
    prior = jnp.max(found, axis=1)
    prior = jnp.where(prior < 0, 2 * each, prior)
    norb = anchors.shape[0]
    orbit = lax.broadcasted_iota(jnp.int32, (norb, 2 * each), 0)
    index = lax.broadcasted_iota(jnp.int32, (norb, 2 * each), 1)
    last = jnp.max(jnp.where(terms[None, :] == orbit, index, -1), axis=1)
    last = jnp.where(last < 0, 2 * each, last)
    table = jnp.stack([
        moved_id, fixed_id,
        jnp.where(rising, 4 * planes, 0) - shift,
        second.astype(jnp.int32), dy, dz,
        jnp.where(second, 0, shift),
        jnp.where(rising, 0, 4 * planes) + shift,
        prior[:each], prior[each:],
    ])
    return table, last


def slab_body(orbitals, anchors, pair_slots):
    groups, places = lax.axis_size("grp"), lax.axis_size("grid")
    norb_local, cells = orbitals.shape
    planes = cells // (B * B)
    each = PAIR_DEV * places
    chips = places // 2
    cap = 5 * norb_local // 16
    plan, links, fits = make_plan(anchors, pair_slots, cap, each, planes)
    stacked = orbitals.reshape(norb_local, planes, ROWS, LANES)

    def lean(stacked, anchors, pair_slots, plan, links):
        return run_lean(plan, links, stacked, each, chips, cap)

    def full(stacked, anchors, pair_slots, plan, links):
        table, last = full_tables(anchors, pair_slots, planes, groups, each)
        moved, fixed = bring(table, stacked, each, groups, chips)
        dens, partner = pair_up(table, moved, fixed)
        pot = solve_slabs(table, dens, places, 5)
        going, staying = make_terms(table, pot, partner, moved, fixed)
        return hand_back(table, last, going, staying, norb_local, chips)

    out = lax.cond(fits[0] > 0, lean, full, stacked, anchors, pair_slots, plan, links)
    return out.reshape(norb_local, cells)


def slabs_fit(mesh):
    groups, places = mesh.shape["grp"], mesh.shape["grid"]
    return groups == 4 and places % 2 == 0 and 4 * (B // places) >= PAD


def solution(mesh):
    return jax.shard_map(
        slab_body if slabs_fit(mesh) else owner_body,
        mesh=mesh,
        in_specs=(P("grp", "grid"), P(), P()),
        out_specs=P("grp", "grid"),
        check_vma=False,
    )
```

```python
import functools
import math

import jax
import jax.numpy as jnp
from jax import lax
from jax.experimental import pallas as pl
from jax.experimental.pallas import tpu as pltpu
from jax.sharding import PartitionSpec as P

B = 64
PAIR_DEV = 2
ITERS = 3
MOST_CHUNKS = 2
LANES = 128
ROWS = B * B // LANES
PAD = 32
STEP = 4


def deal_evenly(pair_slots, owner_count, each_owner):
    flat_slots = pair_slots.reshape(-1, 2)
    filled = (flat_slots[:, 0] >= 0).astype(jnp.int32)
    position = jnp.cumsum(filled, dtype=jnp.int32) - filled
    wanted = lax.broadcasted_iota(jnp.int32, (owner_count, each_owner), 1) * owner_count
    wanted = (wanted + lax.broadcasted_iota(jnp.int32, (owner_count, each_owner), 0)).reshape(-1)
    matched = (position[None, :] == wanted[:, None]) & (filled[None, :] == 1)
    picked = jnp.sum(jnp.where(matched[:, :, None], flat_slots[None], 0), axis=1)
    return picked.reshape(owner_count, each_owner, 2)


def gather_kernel(ids_ref, src_ref, *out_refs):
    count, terms = out_refs[0].shape[:2]
    for slot, out_ref in enumerate(out_refs):
        def pick(dest, unused, slot=slot, out_ref=out_ref):
            for term in range(terms):
                out_ref[dest, term] = src_ref[ids_ref[(slot * count + dest) * terms + term]]
            return unused

        lax.fori_loop(0, count, pick, 0)


def gather_pieces(ids, pieces, slots, count):
    norb, rows, lanes = pieces.shape
    block = max(8, rows // 4)
    return pl.pallas_call(
        gather_kernel,
        grid_spec=pltpu.PrefetchScalarGridSpec(
            num_scalar_prefetch=1,
            grid=(rows // block,),
            in_specs=[pl.BlockSpec((norb, block, lanes), lambda i, ids: (0, i, 0))],
            out_specs=[pl.BlockSpec((count, 2, block, lanes), lambda i, ids: (0, 0, i, 0))] * slots,
        ),
        out_shape=[jax.ShapeDtypeStruct((count, 2, rows, lanes), jnp.float32)] * slots,
        cost_estimate=pl.CostEstimate(flops=0, bytes_accessed=8 * norb * rows * lanes, transcendentals=0),
        name="pick_pieces",
    )(ids, pieces)


def scatter_kernel(ids_ref, *refs):
    out_ref = refs[-1]
    out_ref[...] = jnp.zeros_like(out_ref)
    count, terms = refs[0].shape[:2]
    for slot, in_ref in enumerate(refs[:-1]):
        def add(dest, unused, slot=slot, in_ref=in_ref):
            for term in range(terms):
                orbit = ids_ref[(slot * count + dest) * terms + term]
                out_ref[orbit] = out_ref[orbit] + in_ref[dest, term]
            return unused

        lax.fori_loop(0, count, add, 0)


def scatter_pieces(ids, parts, norb):
    count, terms, rows, lanes = parts[0].shape
    block = max(8, rows // 4)
    return pl.pallas_call(
        scatter_kernel,
        grid_spec=pltpu.PrefetchScalarGridSpec(
            num_scalar_prefetch=1,
            grid=(rows // block,),
            in_specs=[pl.BlockSpec((count, terms, block, lanes), lambda i, ids: (0, 0, i, 0))] * len(parts),
            out_specs=pl.BlockSpec((norb, block, lanes), lambda i, ids: (0, i, 0)),
        ),
        out_shape=jax.ShapeDtypeStruct((norb, rows, lanes), jnp.float32),
        cost_estimate=pl.CostEstimate(flops=0, bytes_accessed=8 * norb * rows * lanes, transcendentals=0),
        name="add_pieces",
    )(ids, *parts)


def lane_ids(shape):
    return lax.broadcasted_iota(jnp.int32, shape, len(shape) - 1)


def shift_plane(plane, off_y, off_z):
    shape = plane.shape
    lane = lane_ids(shape)
    row = lax.broadcasted_iota(jnp.int32, shape, 0)
    linear = off_y * B + off_z
    across = jnp.bitwise_and(linear, LANES - 1)
    down = jnp.right_shift(linear, 7)
    turned = pltpu.roll(plane, across, 1)
    near = pltpu.roll(turned, jnp.bitwise_and(down, ROWS - 1), 0)
    far = pltpu.roll(turned, jnp.bitwise_and(down + 1, ROWS - 1), 0)
    moved = jnp.where(lane >= across, near, far)
    from_y = row * 2 + jnp.right_shift(lane, 6) - off_y
    from_z = jnp.bitwise_and(lane, B - 1) - off_z
    inside = (from_y >= 0) & (from_y < B) & (from_z >= 0) & (from_z < B)
    return jnp.where(inside, moved, 0.0)


def operate_plane(before, plane, after):
    shape = plane.shape
    lane = lane_ids(shape)
    row = lax.broadcasted_iota(jnp.int32, shape, 0)
    z = jnp.bitwise_and(lane, B - 1)
    upper_z = jnp.where(z < B - 1, pltpu.roll(plane, LANES - 1, 1), 0.0)
    lower_z = jnp.where(z > 0, pltpu.roll(plane, 1, 1), 0.0)
    half = pltpu.roll(plane, B, 1)
    down = jnp.where(row > 0, pltpu.roll(half, 1, 0), 0.0)
    up = jnp.where(row < ROWS - 1, pltpu.roll(half, ROWS - 1, 0), 0.0)
    beside = (before + after) + (half + jnp.where(lane < B, down, up))
    return 6.0 * plane - beside - upper_z - lower_z


def fold(values):
    return jnp.sum(values.reshape(ROWS // 8, 8, LANES), axis=0)


def total(acc):
    return jnp.sum(acc, axis=(0, 1), keepdims=True)


def solve_kernel(info_ref, *refs):
    chunks = (len(refs) - 6) // 2
    in_refs, out_refs = refs[:chunks], refs[chunks : 2 * chunks]
    wide, partner, direction, resid, image, potential = refs[2 * chunks :]
    count, terms, rows, lanes = in_refs[0].shape
    each = rows // ROWS
    dx, dy, dz = info_ref[0], info_ref[1], info_ref[2]
    keep = jnp.where(info_ref[3] > 0, 1.0, 0.0).astype(jnp.float32)
    edge = jnp.zeros((PAD, ROWS, LANES), jnp.float32)
    wide[pl.ds(0, PAD)] = edge
    wide[pl.ds(PAD + B, PAD)] = edge
    direction[0] = edge[0]
    direction[B + 1] = edge[0]
    none = jnp.zeros((8, LANES), jnp.float32)

    def place(owner, chunk, i):
        return (owner * chunks + chunk) * each + i

    def load(owner, unused):
        for chunk in range(chunks):
            for i in range(each):
                wide[PAD + place(owner, chunk, i)] = in_refs[chunk][owner, 1, pl.ds(i * ROWS, ROWS)]
        return unused

    lax.fori_loop(0, count, load, 0)

    def start(owner, acc):
        for chunk in range(chunks):
            for i in range(each):
                x = place(owner, chunk, i)
                other = shift_plane(wide[PAD + x - dx], dy, dz)
                partner[x] = other
                density = in_refs[chunk][owner, 0, pl.ds(i * ROWS, ROWS)] * other
                direction[x + 1] = density
                resid[x] = density
                acc = acc + fold(density * density)
        return acc

    norm_now = total(lax.fori_loop(0, count, start, none))

    for turn in range(ITERS):
        def apply(block, acc):
            for i in range(STEP):
                x = block * STEP + i
                plane = direction[x + 1]
                result = operate_plane(direction[x], plane, direction[x + 2])
                image[x] = result
                acc = acc + fold(plane * result)
            return acc

        step_len = norm_now / total(lax.fori_loop(0, B // STEP, apply, none))

        if turn == ITERS - 1:
            break

        def advance(block, acc):
            for i in range(STEP):
                x = block * STEP + i
                moved = step_len * direction[x + 1]
                potential[x] = moved if turn == 0 else potential[x] + moved
                left = resid[x] - step_len * image[x]
                resid[x] = left
                acc = acc + fold(left * left)
            return acc

        norm_next = total(lax.fori_loop(0, B // STEP, advance, none))
        ratio = norm_next / norm_now

        def renew(block, unused):
            for i in range(STEP):
                x = block * STEP + i
                direction[x + 1] = resid[x] + ratio * direction[x + 1]
            return unused

        lax.fori_loop(0, B // STEP, renew, 0)
        norm_now = norm_next

    def finish(owner, unused):
        for chunk in range(chunks):
            for i in range(each):
                x = place(owner, chunk, i)
                found = (potential[x] + step_len * direction[x + 1]) * keep
                out_refs[chunk][owner, 0, pl.ds(i * ROWS, ROWS)] = found * partner[x]
                wide[PAD + x] = found * in_refs[chunk][owner, 0, pl.ds(i * ROWS, ROWS)]
        return unused

    lax.fori_loop(0, count, finish, 0)

    def give_back(owner, unused):
        for chunk in range(chunks):
            for i in range(each):
                x = place(owner, chunk, i)
                out_refs[chunk][owner, 1, pl.ds(i * ROWS, ROWS)] = shift_plane(wide[PAD + x + dx], -dy, -dz)
        return unused

    lax.fori_loop(0, count, give_back, 0)


def solve_pair(info, parts):
    box = (B, ROWS, LANES)
    vmem = pl.BlockSpec(memory_space=pltpu.VMEM)
    return pl.pallas_call(
        solve_kernel,
        in_specs=[pl.BlockSpec(memory_space=pltpu.SMEM)] + [vmem] * len(parts),
        out_specs=[vmem] * len(parts),
        out_shape=[jax.ShapeDtypeStruct(p.shape, jnp.float32) for p in parts],
        scratch_shapes=[
            pltpu.VMEM((B + 2 * PAD, ROWS, LANES), jnp.float32),
            pltpu.VMEM(box, jnp.float32),
            pltpu.VMEM((B + 2, ROWS, LANES), jnp.float32),
            pltpu.VMEM(box, jnp.float32),
            pltpu.VMEM(box, jnp.float32),
            pltpu.VMEM(box, jnp.float32),
        ],
        compiler_params=pltpu.CompilerParams(vmem_limit_bytes=32 * 1024 * 1024),
        cost_estimate=pl.CostEstimate(flops=0, bytes_accessed=40 * 1024 * 1024, transcendentals=0),
        name="solve_pair",
    )(info, *parts)


def owner_body(orbitals, anchors, pair_slots):
    grid_count = lax.axis_size("grid")
    owner_count = lax.axis_size("grp") * grid_count
    group_idx = lax.axis_index("grp")
    place_idx = lax.axis_index("grid")
    assignment = deal_evenly(pair_slots, owner_count, PAIR_DEV)
    slots = assignment.shape[1]
    filled = assignment[..., 0] >= 0
    safe_ids = jnp.maximum(assignment, 0)
    group_table = lax.dynamic_slice_in_dim(safe_ids, group_idx * grid_count, grid_count, 0)
    ids = jnp.transpose(group_table, (1, 0, 2)).reshape(-1)
    owner_idx = group_idx * grid_count + place_idx
    own_pairs = safe_ids[owner_idx]
    offsets = anchors[own_pairs[:, 1]] - anchors[own_pairs[:, 0]]
    info = jnp.concatenate([offsets, filled[owner_idx].astype(jnp.int32)[:, None]], axis=1)

    norb_local, cells = orbitals.shape
    stacked = orbitals.reshape(norb_local, cells // LANES, LANES)
    chunks = math.gcd(MOST_CHUNKS, cells // (B * B))
    rows = stacked.shape[1] // chunks
    arrived = [[None] * chunks for _ in range(slots)]
    for chunk in range(chunks):
        pieces = lax.all_gather(stacked[:, chunk * rows : (chunk + 1) * rows], "grp", axis=0, tiled=True)
        outgoing = gather_pieces(ids, pieces, slots, grid_count)
        for slot in range(slots):
            arrived[slot][chunk] = lax.all_to_all(outgoing[slot], "grid", split_axis=0, concat_axis=0, tiled=True)
    returned = []
    for slot in range(slots):
        terms = solve_pair(info[slot], arrived[slot])
        returned.append(
            [lax.all_to_all(t, "grid", split_axis=0, concat_axis=0, tiled=True) for t in terms]
        )
    results = []
    for chunk in range(chunks):
        summed = scatter_pieces(ids, [r[chunk] for r in returned], anchors.shape[0])
        results.append(lax.psum_scatter(summed, "grp", scatter_dimension=0, tiled=True))
    return jnp.concatenate(results, axis=1).reshape(norb_local, cells)


MESH = pl.DeviceIdType.MESH
HALO = 3
WAVES = 4
TRIALS = 12
SUB = 8


def remote(src, dst, send_sem, recv_sem, device):
    return pltpu.make_async_remote_copy(
        src_ref=src, dst_ref=dst, send_sem=send_sem, recv_sem=recv_sem, device_id=device, device_id_type=MESH
    )


def spot():
    grp = lax.axis_index("grp")
    place = lax.axis_index("grid")
    across = grp + 1 - 2 * lax.rem(grp, 2)
    along = lax.rem(grp + 2, 4)
    corner = lax.rem(across + 2, 4)
    return grp, place, across, along, corner


def greet(chips, wide=False):
    grp, place, across, along, corner = spot()
    chip = place // 2
    core = lax.rem(place, 2)
    barrier = pltpu.get_barrier_semaphore()
    peers = [(across, place), (along, place), (grp, 2 * chip + 1 - core)] + ([(corner, place)] if wide else [])
    for device in peers:
        pl.semaphore_signal(barrier, inc=1, device_id=device, device_id_type=MESH)

    @pl.when(chip > 0)
    def below():
        pl.semaphore_signal(barrier, inc=1, device_id=(grp, place - 2), device_id_type=MESH)

    @pl.when(chip < chips - 1)
    def above():
        pl.semaphore_signal(barrier, inc=1, device_id=(grp, place + 2), device_id_type=MESH)

    ends = jnp.where(chip > 0, 1, 0) + jnp.where(chip < chips - 1, 1, 0)
    pl.semaphore_wait(barrier, len(peers) + ends)


class Relay:
    def __init__(self, wins, send_sem, recv_sem, signs, chips, marks):
        self.wins, self.send_sem, self.recv_sem, self.signs, self.chips = wins, send_sem, recv_sem, signs, chips
        self.grp, self.place = lax.axis_index("grp"), lax.axis_index("grid")
        self.chip = self.place // 2
        self.core = lax.rem(self.place, 2)
        self.half = wins[0].shape[0] // 2
        self.planes = wins[0].shape[1] // 6
        self.deep, self.far, self.mid = marks

    def offset(self, sign, hop):
        return 2 * self.planes * (2 - hop if sign > 0 else hop)

    def region(self, chunk, side, hop, core, size):
        start = self.offset(self.signs[side], hop) + self.planes * core
        return self.wins[chunk].at[pl.ds(side * self.half, size), pl.ds(start, self.planes)]

    def comes(self, side, hop):
        source = self.chip - self.signs[side] * hop
        return source >= 0 if self.signs[side] > 0 else source < self.chips

    def goes(self, side, hop):
        source = self.chip + self.signs[side] - self.signs[side] * hop
        if self.signs[side] > 0:
            return (self.chip + 1 < self.chips) & (source >= 0)
        return (self.chip - 1 >= 0) & (source < self.chips)

    def spans(self, side, hop, core, act):
        if hop == 0:
            act(self.half)
        else:
            near = 1 if self.signs[side] > 0 else 0
            most, least = (self.half, self.mid) if hop == 1 else (self.far, self.deep)
            if most == least:
                act(most)
                return

            @pl.when(core == near)
            def whole():
                act(most)

            @pl.when(core != near)
            def some():
                act(least)

    def onward(self, chunk, side, hop, size, here=None):
        source = self.region(chunk, side, hop - 1 if here is None else here, self.core, size)
        there = self.region(chunk, side, hop, self.core, size)
        return remote(
            source, there, self.send_sem.at[chunk, side, hop - 1], self.recv_sem.at[chunk, side, hop - 1],
            (self.grp, self.place + 2 * self.signs[side]),
        )

    def beside(self, chunk, side, hop, core, size):
        part = self.region(chunk, side, hop, core, size)
        return remote(
            part, part, self.send_sem.at[chunk, side, 2 + hop], self.recv_sem.at[chunk, side, 2 + hop],
            (self.grp, 2 * self.chip + 1 - self.core),
        )

    def clear(self):
        for side in range(2):
            for hop in (1, 2):
                start = self.offset(self.signs[side], hop)

                @pl.when(jnp.logical_not(self.comes(side, hop)))
                def fill(side=side, start=start):
                    for win in self.wins:
                        def zero(slot, unused, win=win):
                            win[slot, pl.ds(start, 2 * self.planes)] = jnp.zeros(
                                (2 * self.planes,) + win.shape[2:], jnp.float32
                            )
                            return unused

                        lax.fori_loop(side * self.half, (side + 1) * self.half, zero, 0)

    def pass_on(self, chunk, side, hop):
        @pl.when(self.goes(side, hop))
        def go():
            self.spans(side, hop, self.core, lambda size: self.onward(chunk, side, hop, size).start())

    def begin(self, chunk):
        for side in range(2):
            self.pass_on(chunk, side, 1)
            self.beside(chunk, side, 0, self.core, self.half).start()

    def take(self, chunk, side, hop):
        @pl.when(self.comes(side, hop))
        def got():
            def act(size):
                self.onward(chunk, side, hop, size, hop).wait_recv()

            self.spans(side, hop, self.core, act)

        if hop < 2:
            self.pass_on(chunk, side, hop + 1)

        @pl.when(self.comes(side, hop))
        def share():
            self.spans(side, hop, self.core, lambda size: self.beside(chunk, side, hop, self.core, size).start())

    def first(self, chunk):
        for side in range(2):
            self.take(chunk, side, 1)

    def second(self, chunk):
        for side in range(2):
            self.take(chunk, side, 2)

    def settle(self, chunk):
        other = 1 - self.core
        for side in range(2):
            self.beside(chunk, side, 0, other, self.half).wait_recv()
            for hop in (1, 2):
                @pl.when(self.comes(side, hop))
                def got(side=side, hop=hop):
                    self.spans(side, hop, other, lambda size: self.beside(chunk, side, hop, other, size).wait_recv())

    def drain(self):
        for chunk in range(len(self.wins)):
            for side in range(2):
                self.beside(chunk, side, 0, self.core, self.half).wait_send()
                for hop in (1, 2):
                    @pl.when(self.comes(side, hop))
                    def sent(chunk=chunk, side=side, hop=hop):
                        self.spans(
                            side, hop, self.core,
                            lambda size: self.beside(chunk, side, hop, self.core, size).wait_send(),
                        )

                    @pl.when(self.goes(side, hop))
                    def passed(chunk=chunk, side=side, hop=hop):
                        self.spans(
                            side, hop, self.core, lambda size: self.onward(chunk, side, hop, size).wait_send()
                        )


def bring_kernel(chips, tbl, orb, moved, fixed, *scratch):
    count = moved.shape[0]
    pools, wins = scratch[:count], scratch[count : 2 * count]
    own_sem, xy_send, xy_recv, z_send, z_recv = scratch[2 * count :]
    grp, place, across, along, corner = spot()
    core = lax.rem(place, 2)
    norb, planes = orb.shape[:2]
    part = norb // 2
    slots = moved.shape[1]
    relay = Relay(wins, z_send, z_recv, (1, -1), chips, (slots // 2,) * 3)

    def block(chunk, owner, start, size):
        return pools[chunk].at[pl.ds(owner * norb + start, size)]

    def stage(chunk):
        return pltpu.make_async_copy(
            orb.at[:, :, pl.ds(chunk * SUB, SUB)], block(chunk, grp, 0, norb), own_sem.at[chunk]
        )

    def hop(chunk, kind, owner, start, size, target):
        ref = block(chunk, owner, start, size)
        return remote(ref, ref, xy_send.at[chunk, kind], xy_recv.at[chunk, kind], (target, place))

    def direct(chunk, owners):
        return hop(chunk, 0, owners[0], 0, norb, across), hop(chunk, 1, owners[1], 0, norb, along)

    def turned(chunk, owners):
        return hop(chunk, 2, owners[0], 0, part, along), hop(chunk, 3, owners[1], part, part, across)

    for chunk in range(count):
        stage(chunk).start()
    greet(chips)
    relay.clear()

    def send_own(chunk):
        stage(chunk).wait()
        for copy in direct(chunk, (grp, grp)):
            copy.start()

    send_own(0)
    send_own(1)
    for step in range(count + 4):
        if step < count:
            for copy in direct(step, (across, along)):
                copy.wait_recv()
            for copy in turned(step, (across, along)):
                copy.start()
            if step + 2 < count:
                send_own(step + 2)
        chunk = step - 1
        if 0 <= chunk < count:
            for copy in turned(chunk, (corner, corner)):
                copy.wait_recv()
            for side in range(2):
                start = relay.offset(relay.signs[side], 0) + planes * core

                def pick(slot, unused, start=start, chunk=chunk):
                    wins[chunk][slot, pl.ds(start, planes)] = pools[chunk][tbl[0, slot]]
                    fixed[chunk, slot] = pools[chunk][tbl[1, slot]]
                    return unused

                lax.fori_loop(side * (slots // 2), (side + 1) * (slots // 2), pick, 0)
            relay.begin(chunk)
        chunk = step - 2
        if 0 <= chunk < count:
            relay.first(chunk)
        chunk = step - 3
        if 0 <= chunk < count:
            relay.second(chunk)
        chunk = step - 4
        if 0 <= chunk < count:
            relay.settle(chunk)

            def choose(slot, unused, chunk=chunk):
                first = tbl[2, slot] + planes * core
                for plane in range(planes):
                    moved[chunk, slot, plane] = wins[chunk][slot, first + plane]
                return unused

            lax.fori_loop(0, slots, choose, 0)
    for chunk in range(count):
        for copy in direct(chunk, (grp, grp)) + turned(chunk, (across, along)):
            copy.wait_send()
    relay.drain()


def bring(table, stacked, slots, groups, chips):
    norb, planes, rows, lanes = stacked.shape
    chunks = rows // SUB
    vmem = pl.BlockSpec(memory_space=pltpu.VMEM)
    dma = pltpu.SemaphoreType.DMA
    shape = jax.ShapeDtypeStruct((chunks, slots, planes, SUB, lanes), jnp.float32)
    return pl.pallas_call(
        functools.partial(bring_kernel, chips),
        in_specs=[pl.BlockSpec(memory_space=pltpu.SMEM), pl.BlockSpec(memory_space=pl.ANY)],
        out_specs=[vmem, vmem],
        out_shape=[shape, shape],
        scratch_shapes=[pltpu.VMEM((groups * norb, planes, SUB, lanes), jnp.float32)] * chunks
        + [pltpu.VMEM((slots, 6 * planes, SUB, lanes), jnp.float32)] * chunks
        + [dma((chunks,)), dma((chunks, 4)), dma((chunks, 4)), dma((chunks, 2, 5)), dma((chunks, 2, 5))],
        compiler_params=pltpu.CompilerParams(
            collective_id=0, has_side_effects=True, vmem_limit_bytes=48 * 1024 * 1024
        ),
        name="bring",
    )(table, stacked)


def pair_kernel(tbl, moved, fixed, dens, partner):
    def go(slot, unused):
        second = tbl[3, slot] > 0
        dy, dz = tbl[4, slot], tbl[5, slot]
        for x in range(moved.shape[2]):
            left = moved[:, slot, x].reshape(ROWS, LANES)
            right = fixed[:, slot, x].reshape(ROWS, LANES)
            other = shift_plane(jnp.where(second, left, right), dy, dz)
            dens[slot, x] = jnp.where(second, right, left) * other
            partner[slot, x] = other
        return unused

    lax.fori_loop(0, moved.shape[1], go, 0)


def pair_up(table, moved, fixed):
    chunks, slots, planes, sub, lanes = moved.shape
    vmem = pl.BlockSpec(memory_space=pltpu.VMEM)
    shape = jax.ShapeDtypeStruct((slots, planes, ROWS, lanes), jnp.float32)
    return pl.pallas_call(
        pair_kernel,
        in_specs=[pl.BlockSpec(memory_space=pltpu.SMEM), vmem, vmem],
        out_specs=[vmem, vmem],
        out_shape=[shape, shape],
        compiler_params=pltpu.CompilerParams(vmem_limit_bytes=24 * 1024 * 1024),
        name="pair_up",
    )(table, moved, fixed)


def inner(plane):
    shape = plane.shape
    lane = lane_ids(shape)
    row = lax.broadcasted_iota(jnp.int32, shape, 0)
    z = jnp.bitwise_and(lane, B - 1)
    upper_z = jnp.where(z < B - 1, pltpu.roll(plane, LANES - 1, 1), 0.0)
    lower_z = jnp.where(z > 0, pltpu.roll(plane, 1, 1), 0.0)
    half = pltpu.roll(plane, B, 1)
    down = jnp.where(row > 0, pltpu.roll(half, 1, 0), 0.0)
    up = jnp.where(row < ROWS - 1, pltpu.roll(half, ROWS - 1, 0), 0.0)
    return 6.0 * plane - ((half + jnp.where(lane < B, down, up)) + (upper_z + lower_z))


def krylov_weights(m):
    a0 = m[0] / m[1]
    rr1 = a0 * a0 * m[2] - m[0]
    p, q = 1.0 + rr1 / m[0], -a0
    a1 = rr1 / (p * p * m[1] + 2.0 * p * q * m[2] + q * q * m[3])
    s1, s2 = -a0 - a1 * p, -a1 * q
    rr2 = (m[0] + s1 * s1 * m[2] + s2 * s2 * m[4]) + 2.0 * (s1 * m[1] + s2 * m[2] + s1 * s2 * m[3])
    b1 = rr2 / rr1
    e0, e1, e2 = 1.0 + b1 * p, s1 + b1 * q, s2
    bend = e0 * e0 * m[1] + e1 * e1 * m[3] + e2 * e2 * m[5]
    a2 = rr2 / (bend + 2.0 * (e0 * e1 * m[2] + e0 * e2 * m[3] + e1 * e2 * m[4]))
    return a0 + a1 * p + a2 * e0, a1 * q + a2 * e1, a2 * e2


def solve_slabs_kernel(places, tbl, dens, pot, wide, one, two, sums, gathered, weights, h_send, h_recv, s_send, s_recv):
    grp, place = lax.axis_index("grp"), lax.axis_index("grid")
    slots, planes = dens.shape[:2]
    first, last = HALO, HALO + planes - 1
    each = slots // WAVES
    barrier = pltpu.get_barrier_semaphore()
    for step in range(1, places):
        pl.semaphore_signal(
            barrier, inc=1, device_id=(grp, lax.rem(place + step, places)), device_id_type=MESH
        )
    pl.semaphore_wait(barrier, places - 1)

    def rise(wave):
        return remote(
            dens.at[pl.ds(wave * each, each), pl.ds(planes - HALO + 1, HALO - 1)],
            wide.at[pl.ds(wave * each, each), pl.ds(1, HALO - 1)],
            h_send.at[wave, 0], h_recv.at[wave, 0], (grp, lax.rem(place + 1, places)),
        )

    def sink(wave):
        return remote(
            dens.at[pl.ds(wave * each, each), pl.ds(0, HALO)],
            wide.at[pl.ds(wave * each, each), pl.ds(HALO + planes, HALO)],
            h_send.at[wave, 1], h_recv.at[wave, 1], (grp, lax.rem(place + places - 1, places)),
        )

    lowest, highest = place == 0, place == places - 1
    for wave in range(WAVES):
        @pl.when(jnp.logical_not(highest))
        def send_up(wave=wave):
            rise(wave).start()

        @pl.when(jnp.logical_not(lowest))
        def send_down(wave=wave):
            sink(wave).start()

    blank = jnp.zeros((HALO, ROWS, LANES), jnp.float32)

    def copy_in(slot, unused):
        wide[slot, pl.ds(HALO, planes)] = dens[slot]
        one[slot, 1] = blank[0]
        one[slot, last + 3] = blank[0]
        one[slot, 0] = blank[0]
        return unused

    lax.fori_loop(0, slots, copy_in, 0)

    @pl.when(lowest)
    def no_below():
        def fill(slot, unused):
            wide[slot, pl.ds(0, HALO)] = blank
            return unused

        lax.fori_loop(0, slots, fill, 0)

    @pl.when(highest)
    def no_above():
        def fill(slot, unused):
            wide[slot, pl.ds(HALO + planes, HALO)] = blank
            return unused

        lax.fori_loop(0, slots, fill, 0)

    lane = lax.broadcasted_iota(jnp.int32, (1, LANES), 1)
    none = jnp.zeros((8, LANES), jnp.float32)

    def row_of(parts):
        row = jnp.zeros((1, LANES), jnp.float32)
        for at, part in parts:
            row = row + jnp.where(lane == at, total(part), 0.0)
        return row

    def work(slot, unused):
        low, high = tbl[6, slot], tbl[6, slot] + B

        def live(e):
            x = planes * place + e - HALO
            return jnp.where((x >= low) & (x < high), 1.0, 0.0).astype(jnp.float32)

        m0, m1, m2, m3, m4, m5 = none, none, none, none, none, none
        for e in range(first - 1, last + 3):
            value = live(e) * (inner(wide[slot, e]) - (wide[slot, e - 1] + wide[slot, e + 1]))
            one[slot, e] = value
            if first <= e <= last:
                source = wide[slot, e]
                m0 = m0 + fold(source * source)
                m1 = m1 + fold(source * value)
                m2 = m2 + fold(value * value)
        bent = None
        for e in range(first, last + 2):
            value = live(e) * (inner(one[slot, e]) - (one[slot, e - 1] + one[slot, e + 1]))
            two[slot, e] = value
            if e > first:
                m5 = m5 - 2.0 * fold(value * two[slot, e - 1])
            if e <= last:
                m3 = m3 + fold(one[slot, e] * value)
                m4 = m4 + fold(value * value)
                m5 = m5 + fold(value * inner(value))
        sums[pl.ds(slot, 1)] = row_of(enumerate((m0, m1, m2, m3, m4, m5)))
        return unused

    def rim(slot, spots, pairs):
        low, high = tbl[6, slot], tbl[6, slot] + B
        m2, m3, m4, m5 = none, none, none, none
        for e, fresh in spots:
            if fresh:
                x = planes * place + e - HALO
                alive = jnp.where((x >= low) & (x < high), 1.0, 0.0).astype(jnp.float32)
                two[slot, e] = alive * (inner(one[slot, e]) - (one[slot, e - 1] + one[slot, e + 1]))
        for e, fresh in spots:
            value, before = two[slot, e], one[slot, e]
            m2 = m2 + fold(before * before)
            m3 = m3 + fold(before * value)
            m4 = m4 + fold(value * value)
            m5 = m5 + fold(value * inner(value))
        for e in pairs:
            m5 = m5 - 2.0 * fold(two[slot, e] * two[slot, e + 1])
        sums[pl.ds(slot, 1)] = sums[pl.ds(slot, 1)] + row_of(((2, m2), (3, m3), (4, m4), (5, m5)))

    for wave in range(WAVES):
        @pl.when(jnp.logical_not(lowest))
        def got_below(wave=wave):
            rise(wave).wait_recv()

        @pl.when(jnp.logical_not(highest))
        def got_above(wave=wave):
            sink(wave).wait_recv()

        lax.fori_loop(wave * each, (wave + 1) * each, work, 0)

    @pl.when(lowest)
    def rim_below():
        def go(slot, unused):
            rim(slot, ((first - 2, True), (first - 1, True)), (first - 2, first - 1))
            return unused

        lax.fori_loop(0, slots, go, 0)

    @pl.when(highest)
    def rim_above():
        def go(slot, unused):
            rim(slot, ((last + 1, False), (last + 2, True)), (last + 1,))
            return unused

        lax.fori_loop(0, slots, go, 0)

    def tell(step):
        return remote(
            sums, gathered.at[place], s_send.at[step - 1], s_recv.at[step - 1],
            (grp, lax.rem(place + step, places)),
        )

    def hear(step):
        source = lax.rem(place + places - step, places)
        return remote(
            sums, gathered.at[source], s_send.at[step - 1], s_recv.at[step - 1],
            (grp, lax.rem(place + step, places)),
        )

    for step in range(1, places):
        tell(step).start()
    gathered[place] = sums[...]
    for step in range(1, places):
        hear(step).wait_recv()
    whole = gathered[0]
    for at in range(1, places):
        whole = whole + gathered[at]
    lanes = lax.broadcasted_iota(jnp.int32, whole.shape, 1)
    moments = [jnp.sum(jnp.where(lanes == at, whole, 0.0), axis=1, keepdims=True) for at in range(6)]
    for at, weight in enumerate(krylov_weights(moments)):
        weights[at] = jnp.broadcast_to(weight, whole.shape)

    def finish(slot, unused):
        w0, w1, w2 = [weights[at, pl.ds(slot, 1)] for at in range(3)]
        for x in range(planes):
            e = x + HALO
            pot[slot, x] = w0 * wide[slot, e] + w1 * one[slot, e] + w2 * two[slot, e]
        return unused

    lax.fori_loop(0, slots, finish, 0)
    for wave in range(WAVES):
        @pl.when(jnp.logical_not(highest))
        def sent_up(wave=wave):
            rise(wave).wait_send()

        @pl.when(jnp.logical_not(lowest))
        def sent_down(wave=wave):
            sink(wave).wait_send()

    for step in range(1, places):
        tell(step).wait_send()


def solve_slabs(table, dens, places, ident):
    slots, planes, rows, lanes = dens.shape
    vmem = pl.BlockSpec(memory_space=pltpu.VMEM)
    dma = pltpu.SemaphoreType.DMA
    tall = pltpu.VMEM((slots, planes + 2 * HALO, rows, lanes), jnp.float32)
    return pl.pallas_call(
        functools.partial(solve_slabs_kernel, places),
        in_specs=[pl.BlockSpec(memory_space=pltpu.SMEM), vmem],
        out_specs=vmem,
        out_shape=jax.ShapeDtypeStruct(dens.shape, jnp.float32),
        scratch_shapes=[
            tall, tall, tall,
            pltpu.VMEM((slots, lanes), jnp.float32),
            pltpu.VMEM((places, slots, lanes), jnp.float32),
            pltpu.VMEM((3, slots, lanes), jnp.float32),
            dma((WAVES, 2)), dma((WAVES, 2)), dma((places - 1,)), dma((places - 1,)),
        ],
        compiler_params=pltpu.CompilerParams(
            collective_id=ident, has_side_effects=True, vmem_limit_bytes=40 * 1024 * 1024
        ),
        name="solve_slabs",
    )(table, dens)


def term_kernel(tbl, pot, partner, moved, fixed, going, staying):
    chunks = going.shape[0]

    def go(slot, unused):
        second = tbl[3, slot] > 0
        dy, dz = tbl[4, slot], tbl[5, slot]
        for x in range(pot.shape[1]):
            found = pot[slot, x]
            left = moved[:, slot, x].reshape(ROWS, LANES)
            right = fixed[:, slot, x].reshape(ROWS, LANES)
            term_a = found * partner[slot, x]
            term_b = shift_plane(found * jnp.where(second, right, left), -dy, -dz)
            going[:, slot, x] = jnp.where(second, term_b, term_a).reshape(chunks, SUB, LANES)
            staying[:, slot, x] = jnp.where(second, term_a, term_b).reshape(chunks, SUB, LANES)
        return unused

    lax.fori_loop(0, pot.shape[0], go, 0)


def make_terms(table, pot, partner, moved, fixed):
    vmem = pl.BlockSpec(memory_space=pltpu.VMEM)
    shape = jax.ShapeDtypeStruct(moved.shape, jnp.float32)
    return pl.pallas_call(
        term_kernel,
        in_specs=[pl.BlockSpec(memory_space=pltpu.SMEM)] + [vmem] * 4,
        out_specs=[vmem, vmem],
        out_shape=[shape, shape],
        compiler_params=pltpu.CompilerParams(vmem_limit_bytes=24 * 1024 * 1024),
        name="make_terms",
    )(table, pot, partner, moved, fixed)


def hand_back_kernel(chips, tbl, last, going, staying, out, *scratch):
    count, slots = going.shape[:2]
    wins, chains, outs1, outs2, ins1, ins2 = [scratch[i * count : (i + 1) * count] for i in range(6)]
    xy_send, xy_recv, z_send, z_recv = scratch[6 * count :]
    grp, place, across, along, corner = spot()
    core = lax.rem(place, 2)
    norb, planes = out.shape[:2]
    part = norb // 2
    relay = Relay(wins, z_send, z_recv, (-1, 1), chips, (slots // 2,) * 3)
    greet(chips)
    relay.clear()

    def start(chunk):
        for side in range(2):
            at = relay.offset(relay.signs[side], 0) + planes * core

            def place_in(slot, unused, at=at):
                wins[chunk][slot, pl.ds(at, planes)] = going[chunk, slot]
                return unused

            lax.fori_loop(side * (slots // 2), (side + 1) * (slots // 2), place_in, 0)
        relay.begin(chunk)

    def swap(chunk, kind):
        src = (outs1 if kind < 2 else outs2)[chunk].at[kind % 2]
        dst = (ins1 if kind < 2 else ins2)[chunk].at[kind % 2]
        target = (across, along, along, across)[kind]
        return remote(src, dst, xy_send.at[chunk, kind], xy_recv.at[chunk, kind], (target, place))

    start(0)
    start(1)
    for step in range(count + 4):
        if step < count:
            relay.first(step)
            if step + 2 < count:
                start(step + 2)
        chunk = step - 1
        if 0 <= chunk < count:
            relay.second(chunk)
        chunk = step - 2
        if 0 <= chunk < count:
            relay.settle(chunk)
            chain = chains[chunk]
            chain[2 * slots] = jnp.zeros(chain.shape[1:], jnp.float32)

            def link_fixed(slot, unused, chain=chain, chunk=chunk):
                chain[slot] = staying[chunk, slot] + chain[tbl[8, slot]]
                return unused

            def link_moved(slot, unused, chain=chain, chunk=chunk):
                first = tbl[7, slot] + planes * core
                for plane in range(planes):
                    chain[slots + slot, plane] = wins[chunk][slot, first + plane] + chain[tbl[9, slot], plane]
                return unused

            lax.fori_loop(0, slots, link_fixed, 0)
            lax.fori_loop(0, slots, link_moved, 0)

            def pack(i, unused, chain=chain, chunk=chunk):
                outs1[chunk][0, i] = chain[last[across * norb + i]]
                outs1[chunk][0, part + i] = chain[last[corner * norb + i]]
                outs1[chunk][1, i] = chain[last[along * norb + part + i]]
                outs1[chunk][1, part + i] = chain[last[corner * norb + part + i]]
                return unused

            lax.fori_loop(0, part, pack, 0)
            swap(chunk, 0).start()
            swap(chunk, 1).start()
        chunk = step - 3
        if 0 <= chunk < count:
            chain = chains[chunk]
            swap(chunk, 0).wait_recv()

            def add_across(i, unused, chain=chain, chunk=chunk):
                outs2[chunk][0, i] = ins1[chunk][0, part + i] + chain[last[along * norb + i]]
                return unused

            lax.fori_loop(0, part, add_across, 0)
            swap(chunk, 2).start()
            swap(chunk, 1).wait_recv()

            def add_along(i, unused, chain=chain, chunk=chunk):
                outs2[chunk][1, i] = ins1[chunk][1, part + i] + chain[last[across * norb + part + i]]
                return unused

            lax.fori_loop(0, part, add_along, 0)
            swap(chunk, 3).start()
        chunk = step - 4
        if 0 <= chunk < count:
            chain = chains[chunk]
            swap(chunk, 2).wait_recv()
            swap(chunk, 3).wait_recv()
            for side in range(2):
                def keep(i, unused, side=side, chain=chain, chunk=chunk):
                    orbit = side * part + i
                    found = ins1[chunk][side, i] + ins2[chunk][side, i]
                    out[orbit, :, pl.ds(chunk * SUB, SUB)] = found + chain[last[grp * norb + orbit]]
                    return unused

                lax.fori_loop(0, part, keep, 0)
    for chunk in range(count):
        for kind in range(4):
            swap(chunk, kind).wait_send()
    relay.drain()


def hand_back(table, last, going, staying, norb, chips):
    chunks, slots, planes, sub, lanes = going.shape
    vmem = pl.BlockSpec(memory_space=pltpu.VMEM)
    smem = pl.BlockSpec(memory_space=pltpu.SMEM)
    dma = pltpu.SemaphoreType.DMA
    def room(*lead):
        return [pltpu.VMEM(lead + (planes, sub, lanes), jnp.float32)] * chunks
    wins = [pltpu.VMEM((slots, 6 * planes, sub, lanes), jnp.float32)] * chunks
    return pl.pallas_call(
        functools.partial(hand_back_kernel, chips),
        in_specs=[smem, smem, vmem, vmem],
        out_specs=vmem,
        out_shape=jax.ShapeDtypeStruct((norb, planes, chunks * sub, lanes), jnp.float32),
        scratch_shapes=wins + room(2 * slots + 1) + room(2, norb) + room(2, norb // 2)
        + room(2, norb) + room(2, norb // 2)
        + [dma((chunks, 4)), dma((chunks, 4)), dma((chunks, 2, 5)), dma((chunks, 2, 5))],
        compiler_params=pltpu.CompilerParams(
            collective_id=2, has_side_effects=True, vmem_limit_bytes=56 * 1024 * 1024
        ),
        name="hand_back",
    )(table, last, going, staying)


def plan_kernel(cap, planes, me_ref, anchors, pairs, tbl, links, fits, spots, masks, lists, mine, counts):
    groups = 4
    orbits = anchors.shape[1]
    local = orbits // groups
    depth, unused, owners = pairs.shape
    entries = depth * owners
    each = tbl.shape[1]
    half = each // 2
    extra = (groups - 1) * cap
    final = extra
    prior = final + local + extra
    ends = prior + extra
    spare = ends + local
    worst = 1 << 20
    me = me_ref[0]

    def unpack(code):
        return jnp.bitwise_and(code, 1023), jnp.bitwise_and(jnp.right_shift(code, 10), 1023)

    def clean(i, unused):
        links[i] = 0
        links[prior + i] = extra
        return unused

    def close(i, unused):
        links[final + i] = 2 * each
        return unused

    def own(i, unused):
        links[ends + i] = extra
        spots[me * local + i] = i
        return unused

    lax.fori_loop(0, extra, clean, 0, unroll=5)
    lax.fori_loop(0, local + extra, close, 0, unroll=4)
    lax.fori_loop(0, local, own, 0, unroll=4)

    def sort(i, tails, layer):
        a, b = pairs[layer, 0, i], pairs[layer, 1, i]
        filled = jnp.where(a >= 0, 1, 0)
        dx = anchors[0, jnp.maximum(b, 0)] - anchors[0, jnp.maximum(a, 0)]
        reach = jnp.abs(dx)
        kind = 3 - sum(jnp.where(reach > planes * k, 1, 0) for k in (1, 2, 3))
        step = jnp.left_shift(kind, 3)
        tail = jnp.bitwise_and(jnp.right_shift(tails, step), 255)
        code = a + jnp.left_shift(b, 10) + jnp.left_shift(dx + B, 20)
        lists[jnp.where(filled > 0, kind * entries + tail, 4 * entries)] = code
        return tails + jnp.left_shift(filled, step)

    zero = jnp.int32(0)
    packed = zero
    for layer in range(depth):
        packed = lax.fori_loop(0, owners, functools.partial(sort, layer=layer), packed, unroll=8)
    tails = [jnp.bitwise_and(jnp.right_shift(packed, 8 * k), 255) for k in range(4)]
    fits[0] = 0

    def trial(turn):
        def reset(i, unused):
            for g in range(groups):
                masks[g * local + i] = (15 - (1 << g)) + (g << 10)
            return unused

        lax.fori_loop(0, local, reset, 0, unroll=8)
        state = (zero,) * (groups + 1)
        for kind, limit in enumerate((half // 4, half // 2, 3 * half // 4, half)):
            size = tails[kind]
            base = lax.rem(turn * 5, jnp.maximum(size, 1))
            flip = jnp.bitwise_and(turn, 1) > 0

            def deal(i, state, kind=kind, limit=limit, size=size, base=base, flip=flip):
                filled, bad = state[:groups], state[groups]
                at = i + base
                at = jnp.where(at >= size, at - size, at)
                code = lists[kind * entries + jnp.where(flip, size - 1 - at, at)]
                a, b = unpack(code)
                word_a, word_b = masks[a], masks[b]
                step_a, step_b = jnp.right_shift(word_a, 8), jnp.right_shift(word_b, 8)
                same = jnp.where(step_a == step_b, 1, 0)

                def needs(h, count):
                    new_a = jnp.bitwise_and(jnp.right_shift(word_a, h), 1)
                    new_b = jnp.bitwise_and(jnp.right_shift(word_b, h), 1)
                    had_a = jnp.bitwise_and(jnp.right_shift(count, step_a), 15)
                    had_b = jnp.bitwise_and(jnp.right_shift(count, step_b), 15) + jnp.bitwise_and(new_a, same)
                    return new_a, new_b, had_a, had_b

                best = jnp.int32(worst)
                for h in range(groups):
                    new_a, new_b, had_a, had_b = needs(h, filled[h])
                    need = jnp.maximum(jnp.where(new_a > 0, had_a + 1, 0), jnp.where(new_b > 0, had_b + 1, 0))
                    up = jnp.bitwise_and(jnp.right_shift(filled[h], 16), 15)
                    down = jnp.right_shift(filled[h], 20)
                    taken = jnp.minimum(up, down)
                    side = jnp.where(down < up, 32 + (h << 6), h << 6)
                    cost = jnp.left_shift(2 * (new_a + new_b) + need + taken, 8) + (side + taken)
                    best = jnp.minimum(best, jnp.where((taken < limit) & (need <= cap), cost, worst))
                good = best < worst
                flag = jnp.where(good, 1, 0)
                column = jnp.bitwise_and(jnp.right_shift(best, 6), 3)
                side = jnp.bitwise_and(jnp.right_shift(best, 5), 1)
                slot = jnp.bitwise_and(best, 31)
                count = filled[0]
                for h in range(1, groups):
                    count = jnp.where(column == h, filled[h], count)
                new_a, new_b, had_a, had_b = needs(column, count)
                grown = jnp.left_shift(new_a, step_a) + jnp.left_shift(new_b, step_b)
                grown = jnp.where(good, count + grown + jnp.left_shift(1, 16 + 4 * side), count)
                masks[a] = word_a - jnp.where(good, jnp.left_shift(new_a, column), 0)
                masks[b] = word_b - jnp.where(good, jnp.left_shift(new_b, column), 0)
                here = good & (column == me)
                mine[jnp.where(here, side * half + slot, each)] = code
                for orbit, step, new, had in ((a, step_a, new_a, had_a), (b, step_b, new_b, had_b)):
                    group = jnp.right_shift(step, 2)
                    at = (jnp.bitwise_xor(group, column) - 1) * cap + had
                    spots[jnp.where(here & (new > 0), orbit, orbits)] = local + at
                    links[jnp.where(good & (new > 0) & (group == me), at, spare)] = orbit - group * local
                kept = tuple(jnp.where(column == h, grown, filled[h]) for h in range(groups))
                return kept + (jnp.bitwise_or(bad, 1 - flag),)

            state = lax.fori_loop(0, size, deal, state)
        for h in range(groups):
            counts[h] = state[h]
        fits[0] = 1 - state[groups]

    def attempt(turn, unused):
        @pl.when(fits[0] == 0)
        def go():
            trial(turn)

        return unused

    lax.fori_loop(0, TRIALS, attempt, 0)

    @pl.when(fits[0] > 0)
    def settle():
        def fill(at, unused):
            code = mine[at]
            a, b = unpack(code)
            dx = jnp.right_shift(code, 20) - B
            spot_a, spot_b = spots[a], spots[b]
            rising = at < half
            second = jnp.where(rising, dx, -dx) >= 0
            shift = jnp.where(second, dx, -dx)
            tbl[0, at] = jnp.where(second, spot_b, spot_a)
            tbl[1, at] = jnp.where(second, spot_a, spot_b)
            tbl[2, at] = jnp.where(rising, 4 * planes, 0) - shift
            tbl[3, at] = jnp.where(second, 1, 0)
            tbl[4, at] = anchors[1, b] - anchors[1, a]
            tbl[5, at] = anchors[2, b] - anchors[2, a]
            tbl[6, at] = jnp.where(second, 0, shift)
            tbl[7, at] = jnp.where(rising, 0, 4 * planes) + shift
            return unused

        lax.fori_loop(0, each, fill, 0, unroll=2)
        for row, base in ((1, 0), (0, each)):
            def link(slot, unused, row=row, base=base):
                at = final + tbl[row, slot]
                tbl[9 - row, slot] = links[at]
                links[at] = base + slot
                return unused

            lax.fori_loop(0, each, link, 0)
        for turn in range(1, groups):
            def hook(i, unused, turn=turn):
                at = (turn - 1) * cap + i
                end = ends + links[at]
                links[prior + at] = links[end]
                links[end] = at
                return unused

            sent = jnp.bitwise_and(jnp.right_shift(counts[jnp.bitwise_xor(me, turn)], 4 * me), 15)
            lax.fori_loop(0, sent, hook, 0)


def make_plan(anchors, pair_slots, cap, each, planes):
    orbits = anchors.shape[0]
    entries = pair_slots.shape[0] * pair_slots.shape[1]
    smem = pl.BlockSpec(memory_space=pltpu.SMEM)
    local = orbits // 4
    me = jnp.full((1,), lax.axis_index("grp"), jnp.int32)
    return pl.pallas_call(
        functools.partial(plan_kernel, cap, planes),
        in_specs=[smem] * 3,
        out_specs=[smem] * 3,
        out_shape=[
            jax.ShapeDtypeStruct((10, each), jnp.int32),
            jax.ShapeDtypeStruct((9 * cap + 2 * local + 1,), jnp.int32),
            jax.ShapeDtypeStruct((1,), jnp.int32),
        ],
        scratch_shapes=[
            pltpu.SMEM((orbits + 1,), jnp.int32), pltpu.SMEM((orbits,), jnp.int32),
            pltpu.SMEM((4 * entries + 1,), jnp.int32), pltpu.SMEM((each + 1,), jnp.int32),
            pltpu.SMEM((4,), jnp.int32),
        ],
        name="plan",
    )(me, anchors.T, jnp.transpose(pair_slots, (1, 2, 0)))


def coupled(plane):
    shape = plane.shape
    lane = lane_ids(shape)
    row = lax.broadcasted_iota(jnp.int32, shape, 0)
    lower_z = jnp.where(jnp.bitwise_and(lane, B - 1) > 0, pltpu.roll(plane, 1, 1), 0.0)
    half = pltpu.roll(plane, B, 1)
    down = jnp.where(row > 0, pltpu.roll(half, 1, 0), 0.0)
    return 3.0 * plane - lower_z - jnp.where(lane < B, down, half)


def lean_kernel(chips, cap, tbl, links, orb, out, *scratch):
    count = out.shape[2]
    raws, owns, parcels, pools, wins, wins_back, chains, parcels_back, backs, tallied = [
        scratch[i * count : (i + 1) * count] for i in range(10)
    ]
    partner, wide, one, two, staying, held, sums, gathered, weights = scratch[10 * count : 10 * count + 9]
    (own_sem, xy_send, xy_recv, z_send, z_recv, yx_send, yx_recv, zb_send, zb_recv,
     h_send, h_recv, s_send, s_recv) = scratch[10 * count + 9 :]
    grp, place, across, along, corner = spot()
    core = lax.rem(place, 2)
    places = 2 * chips
    tiles, planes = orb.shape[:2]
    deep = orb.shape[4]
    norb = tiles * deep
    slots = partner.shape[0]
    half = slots // 2
    first, last = HALO, HALO + planes - 1
    each = slots // WAVES
    marks = (half // 4, half // 2, 3 * half // 4)
    relay = Relay(wins, z_send, z_recv, (1, -1), chips, marks)
    relay_back = Relay(wins_back, zb_send, zb_recv, (-1, 1), chips, marks)
    lowest, highest = place == 0, place == places - 1

    def stage(chunk):
        return pltpu.make_async_copy(orb.at[:, :, chunk], raws[chunk], own_sem.at[chunk])

    for chunk in range(count):
        stage(chunk).start()
    barrier = pltpu.get_barrier_semaphore()
    for step in range(1, places):
        pl.semaphore_signal(
            barrier, inc=1, device_id=(grp, lax.rem(place + step, places)), device_id_type=MESH
        )
    for target in (across, along, corner):
        pl.semaphore_signal(barrier, inc=1, device_id=(target, place), device_id_type=MESH)

    def parcel(chunk, kind):
        return remote(
            parcels[chunk].at[pl.ds(kind * cap, cap)], pools[chunk].at[pl.ds(norb + kind * cap, cap)],
            xy_send.at[chunk, kind], xy_recv.at[chunk, kind], ((across, along, corner)[kind], place),
        )

    def pack(chunk):
        stage(chunk).wait()

        def untile(plane, unused):
            for tile in range(tiles):
                for row in range(deep):
                    piece = raws[chunk][tile, plane, :, row, :]
                    owns[chunk][tile * deep + row, plane] = piece
                    pools[chunk][tile * deep + row, plane] = piece
            return unused

        lax.fori_loop(0, planes, untile, 0)

        def put(i, unused):
            parcels[chunk][i] = owns[chunk][links[i]]
            return unused

        lax.fori_loop(0, 3 * cap, put, 0)

    def send(chunk):
        for kind in (2, 0, 1):
            parcel(chunk, kind).start()

    pack(0)
    pl.semaphore_wait(barrier, places + 2)
    for chunk in range(1, count):
        pack(chunk)
        send(chunk - 1)
    send(count - 1)
    relay.clear()
    relay_back.clear()
    blank = jnp.zeros((HALO, ROWS, LANES), jnp.float32)

    def clear(slot, unused):
        for e in (0, 1, last + 3):
            one[slot, e] = blank[0]
        return unused

    lax.fori_loop(0, slots, clear, 0)

    @pl.when(lowest)
    def no_below():
        def fill(slot, unused):
            wide[slot, pl.ds(0, HALO)] = blank
            return unused

        lax.fori_loop(0, slots, fill, 0)

    @pl.when(highest)
    def no_above():
        def fill(slot, unused):
            wide[slot, pl.ds(HALO + planes, HALO)] = blank
            return unused

        lax.fori_loop(0, slots, fill, 0)

    for step in range(count + 3):
        chunk = step
        if chunk < count:
            for kind in range(3):
                parcel(chunk, kind).wait_recv()
            for side in range(2):
                start = relay.offset(relay.signs[side], 0) + planes * core

                def pick(slot, unused, start=start, chunk=chunk):
                    wins[chunk][slot, pl.ds(start, planes)] = pools[chunk][tbl[0, slot]]
                    return unused

                lax.fori_loop(side * half, (side + 1) * half, pick, 0)
            relay.begin(chunk)
        chunk = step - 1
        if 0 <= chunk < count:
            relay.first(chunk)
        chunk = step - 2
        if 0 <= chunk < count:
            relay.second(chunk)
        chunk = step - 3
        if 0 <= chunk < count:
            relay.settle(chunk)

    def couple_of(slot, x):
        at = tbl[2, slot] + planes * core + x
        held_at = tbl[1, slot]
        left = jnp.concatenate([win[slot, at] for win in wins], axis=0)
        right = jnp.concatenate([pool[held_at, x] for pool in pools], axis=0)
        return left, right

    def rise(wave):
        return remote(
            wide.at[pl.ds(wave * each, each), pl.ds(last - HALO + 2, HALO - 1)],
            wide.at[pl.ds(wave * each, each), pl.ds(1, HALO - 1)],
            h_send.at[wave, 0], h_recv.at[wave, 0], (grp, lax.rem(place + 1, places)),
        )

    def sink(wave):
        return remote(
            wide.at[pl.ds(wave * each, each), pl.ds(first, HALO)],
            wide.at[pl.ds(wave * each, each), pl.ds(last + 1, HALO)],
            h_send.at[wave, 1], h_recv.at[wave, 1], (grp, lax.rem(place + places - 1, places)),
        )

    def edges(wave):
        @pl.when(jnp.logical_not(highest))
        def send_up():
            rise(wave).start()

        @pl.when(jnp.logical_not(lowest))
        def send_down():
            sink(wave).start()

    def make(slot, unused):
        second = tbl[3, slot] > 0
        dy, dz = tbl[4, slot], tbl[5, slot]
        for x in range(planes):
            left, right = couple_of(slot, x)
            other = shift_plane(jnp.where(second, left, right), dy, dz)
            wide[slot, x + HALO] = jnp.where(second, right, left) * other
            partner[slot, x] = other
        return unused

    none = jnp.zeros((8, LANES), jnp.float32)
    lane = lax.broadcasted_iota(jnp.int32, (1, LANES), 1)

    def row_of(parts):
        row = jnp.zeros((1, LANES), jnp.float32)
        for at, part in parts:
            row = row + jnp.where(lane == at, total(part), 0.0)
        return row

    def live(slot, e):
        x = planes * place + e - HALO
        low = tbl[6, slot]
        return jnp.where((x >= low) & (x < low + B), 1.0, 0.0).astype(jnp.float32)

    def raise_one(slot, e, acc):
        source = wide[slot, e]
        value = live(slot, e) * (inner(source) - (wide[slot, e - 1] + wide[slot, e + 1]))
        one[slot, e] = value
        if first <= e <= last:
            acc[1] = acc[1] + fold(source * value)
            acc[2] = acc[2] + fold(value * value)

    def raise_two(slot, e):
        source = one[slot, e]
        two[slot, e] = live(slot, e) * (inner(source) - (one[slot, e - 1] + one[slot, e + 1]))

    def measure_two(slot, e, acc, below):
        value = two[slot, e]
        acc[3] = acc[3] + fold(one[slot, e] * value)
        acc[4] = acc[4] + fold(value * value)
        bent = coupled(value)
        acc[5] = acc[5] + fold(value * (bent - two[slot, e - 1] if below else bent))

    def work_inside(slot, unused):
        acc = [none] * 6
        for e in range(first, last + 1):
            source = wide[slot, e]
            acc[0] = acc[0] + fold(source * source)
        for e in range(first + 1, last):
            raise_one(slot, e, acc)
        for e in range(first + 2, last - 1):
            raise_two(slot, e)
            measure_two(slot, e, acc, e > first + 2)
        for at in range(6):
            held[slot, at] = acc[at]
        return unused

    def work_edges(slot, unused):
        acc = [held[slot, at] for at in range(6)]
        for e in (first - 1, first, last, last + 1, last + 2):
            raise_one(slot, e, acc)
        for e in (first, first + 1, last - 1, last, last + 1):
            raise_two(slot, e)
        for e in (first, first + 1, last - 1, last):
            measure_two(slot, e, acc, e > first)
        acc[5] = acc[5] - fold(two[slot, first + 2] * two[slot, first + 1])
        acc[5] = acc[5] - fold(two[slot, last + 1] * two[slot, last])
        acc[5] = 2.0 * acc[5]
        sums[pl.ds(slot, 1)] = row_of(enumerate(acc))
        return unused

    def rim(slot, fresh, spots, pairs):
        for e in fresh:
            raise_two(slot, e)
        m2, m3, m4, m5 = none, none, none, none
        for e in spots:
            value, before = two[slot, e], one[slot, e]
            m2 = m2 + fold(before * before)
            m3 = m3 + fold(before * value)
            m4 = m4 + fold(value * value)
            m5 = m5 + fold(value * coupled(value))
        for e in pairs:
            m5 = m5 - fold(two[slot, e] * two[slot, e + 1])
        sums[pl.ds(slot, 1)] = sums[pl.ds(slot, 1)] + row_of(((2, m2), (3, m3), (4, m4), (5, 2.0 * m5)))

    lax.fori_loop(0, each, make, 0)
    for wave in range(1, WAVES):
        lax.fori_loop(wave * each, (wave + 1) * each, make, 0)
        edges(wave - 1)
    edges(WAVES - 1)
    lax.fori_loop(0, slots, work_inside, 0)
    for wave in range(WAVES):
        @pl.when(jnp.logical_not(lowest))
        def got_below(wave=wave):
            rise(wave).wait_recv()

        @pl.when(jnp.logical_not(highest))
        def got_above(wave=wave):
            sink(wave).wait_recv()

        lax.fori_loop(wave * each, (wave + 1) * each, work_edges, 0)

    @pl.when(lowest)
    def rim_below():
        def go(slot, unused):
            rim(slot, (first - 2, first - 1), (first - 2, first - 1), (first - 2, first - 1))
            return unused

        lax.fori_loop(0, slots, go, 0)

    @pl.when(highest)
    def rim_above():
        def go(slot, unused):
            rim(slot, (last + 2,), (last + 1, last + 2), (last + 1,))
            return unused

        lax.fori_loop(0, slots, go, 0)

    def tell(step, at):
        return remote(
            sums, gathered.at[at], s_send.at[step - 1], s_recv.at[step - 1],
            (grp, lax.rem(place + step, places)),
        )

    for step in range(1, places):
        tell(step, place).start()
    gathered[place] = sums[...]
    for step in range(1, places):
        tell(step, lax.rem(place + places - step, places)).wait_recv()
    whole = gathered[0]
    for at in range(1, places):
        whole = whole + gathered[at]
    lanes = lax.broadcasted_iota(jnp.int32, whole.shape, 1)
    moments = [jnp.sum(jnp.where(lanes == at, whole, 0.0), axis=1, keepdims=True) for at in range(6)]
    for at, weight in enumerate(krylov_weights(moments)):
        weights[at] = jnp.broadcast_to(weight, whole.shape)

    for side in range(2):
        start = relay_back.offset(relay_back.signs[side], 0) + planes * core

        def finish(slot, unused, start=start):
            second = tbl[3, slot] > 0
            dy, dz = tbl[4, slot], tbl[5, slot]
            w0, w1, w2 = [weights[at, pl.ds(slot, 1)] for at in range(3)]
            for x in range(planes):
                e = x + HALO
                found = w0 * wide[slot, e] + w1 * one[slot, e] + w2 * two[slot, e]
                left, right = couple_of(slot, x)
                term_a = found * partner[slot, x]
                term_b = shift_plane(found * jnp.where(second, right, left), -dy, -dz)
                going = jnp.where(second, term_b, term_a)
                stays = jnp.where(second, term_a, term_b)
                for chunk in range(count):
                    wins_back[chunk][slot, start + x] = going[chunk * SUB : (chunk + 1) * SUB]
                    staying[chunk, slot, x] = stays[chunk * SUB : (chunk + 1) * SUB]
            return unused

        lax.fori_loop(side * half, (side + 1) * half, finish, 0)

    extra = 3 * cap
    final = extra
    prior = final + norb + extra
    ends = prior + extra

    def reply(chunk, kind):
        return remote(
            parcels_back[chunk].at[pl.ds(kind * cap, cap)], backs[chunk].at[pl.ds(kind * cap, cap)],
            yx_send.at[chunk, kind], yx_recv.at[chunk, kind], ((across, along, corner)[kind], place),
        )

    relay_back.begin(0)
    relay_back.begin(1)
    for step in range(count + 3):
        if step < count:
            relay_back.first(step)
            if step + 2 < count:
                relay_back.begin(step + 2)
        chunk = step - 1
        if 0 <= chunk < count:
            relay_back.second(chunk)
        chunk = step - 2
        if 0 <= chunk < count:
            relay_back.settle(chunk)
            chain = chains[chunk]
            chain[2 * slots] = jnp.zeros(chain.shape[1:], jnp.float32)

            def link_fixed(slot, unused, chain=chain, chunk=chunk):
                chain[slot] = staying[chunk, slot] + chain[tbl[8, slot]]
                return unused

            def link_moved(slot, unused, chain=chain, chunk=chunk):
                at = tbl[7, slot] + planes * core
                for plane in range(planes):
                    chain[slots + slot, plane] = wins_back[chunk][slot, at + plane] + chain[tbl[9, slot], plane]
                return unused

            lax.fori_loop(0, slots, link_fixed, 0)
            lax.fori_loop(0, slots, link_moved, 0)

            def wrap(i, unused, chain=chain, chunk=chunk):
                parcels_back[chunk][i] = chain[links[final + norb + i]]
                return unused

            lax.fori_loop(0, extra, wrap, 0)
            for kind in (2, 0, 1):
                reply(chunk, kind).start()
        chunk = step - 3
        if 0 <= chunk < count:
            total_of = tallied[chunk]
            total_of[extra] = jnp.zeros(total_of.shape[1:], jnp.float32)
            for kind in range(3):
                reply(chunk, kind).wait_recv()

            def gather(i, unused, total_of=total_of, chunk=chunk):
                total_of[i] = backs[chunk][i] + total_of[links[prior + i]]
                return unused

            lax.fori_loop(0, extra, gather, 0)

            for orbit in range(norb):
                found = total_of[links[ends + orbit]] + chains[chunk][links[final + orbit]]
                for plane in range(planes):
                    out[orbit // deep, plane, chunk, :, orbit % deep, :] = found[plane]
    for chunk in range(count):
        for kind in range(3):
            parcel(chunk, kind).wait_send()
            reply(chunk, kind).wait_send()
    for wave in range(WAVES):
        @pl.when(jnp.logical_not(highest))
        def sent_up(wave=wave):
            rise(wave).wait_send()

        @pl.when(jnp.logical_not(lowest))
        def sent_down(wave=wave):
            sink(wave).wait_send()

    for step in range(1, places):
        tell(step, place).wait_send()
    relay.drain()
    relay_back.drain()


def run_lean(table, links, tiled, slots, chips, cap):
    tiles, planes, chunks, unused, deep, lanes = tiled.shape
    norb, rows = tiles * deep, chunks * SUB
    places = 2 * chips
    smem = pl.BlockSpec(memory_space=pltpu.SMEM)
    dma = pltpu.SemaphoreType.DMA

    def room(count, deep=planes):
        return [pltpu.VMEM((count, deep, SUB, lanes), jnp.float32)] * chunks

    tall = pltpu.VMEM((slots, planes + 2 * HALO, rows, lanes), jnp.float32)
    xy, z = dma((chunks, 3)), dma((chunks, 2, 5))
    return pl.pallas_call(
        functools.partial(lean_kernel, chips, cap),
        in_specs=[smem, smem, pl.BlockSpec(memory_space=pl.ANY)],
        out_specs=pl.BlockSpec(memory_space=pltpu.VMEM),
        out_shape=jax.ShapeDtypeStruct(tiled.shape, jnp.float32),
        scratch_shapes=[pltpu.VMEM((tiles, planes, SUB, deep, lanes), jnp.float32)] * chunks
        + room(norb) + room(3 * cap) + room(norb + 3 * cap) + room(slots, 6 * planes)
        + room(slots, 6 * planes) + room(2 * slots + 1) + room(3 * cap) + room(3 * cap) + room(3 * cap + 1)
        + [
            pltpu.VMEM((slots, planes, rows, lanes), jnp.float32), tall, tall, tall,
            pltpu.VMEM((chunks, slots, planes, SUB, lanes), jnp.float32),
            pltpu.VMEM((slots, 6, 8, lanes), jnp.float32),
            pltpu.VMEM((slots, lanes), jnp.float32),
            pltpu.VMEM((places, slots, lanes), jnp.float32),
            pltpu.VMEM((3, slots, lanes), jnp.float32),
            dma((chunks,)), xy, xy, z, z, xy, xy, z, z,
            dma((WAVES, 2)), dma((WAVES, 2)), dma((places - 1,)), dma((places - 1,)),
        ],
        compiler_params=pltpu.CompilerParams(
            collective_id=3, has_side_effects=True, vmem_limit_bytes=67043328
        ),
        name="lean",
    )(table, links, tiled)


def full_tables(anchors, pair_slots, planes, groups, each):
    assignment = deal_evenly(pair_slots, groups, each)
    pairs = assignment[lax.axis_index("grp")]
    offsets = anchors[pairs[:, 1]] - anchors[pairs[:, 0]]
    dx, dy, dz = offsets[:, 0], offsets[:, 1], offsets[:, 2]
    slot = lax.broadcasted_iota(jnp.int32, (each,), 0)
    rising = slot < each // 2
    second = jnp.where(rising, dx >= 0, dx <= 0)
    shift = jnp.where(second, dx, -dx)
    moved_id = jnp.where(second, pairs[:, 1], pairs[:, 0])
    fixed_id = jnp.where(second, pairs[:, 0], pairs[:, 1])
    terms = jnp.concatenate([fixed_id, moved_id])
    at = lax.broadcasted_iota(jnp.int32, (2 * each, 2 * each), 0)
    before = lax.broadcasted_iota(jnp.int32, (2 * each, 2 * each), 1)
    found = jnp.where((terms[:, None] == terms[None, :]) & (before < at), before, -1)
    prior = jnp.max(found, axis=1)
    prior = jnp.where(prior < 0, 2 * each, prior)
    norb = anchors.shape[0]
    orbit = lax.broadcasted_iota(jnp.int32, (norb, 2 * each), 0)
    index = lax.broadcasted_iota(jnp.int32, (norb, 2 * each), 1)
    last = jnp.max(jnp.where(terms[None, :] == orbit, index, -1), axis=1)
    last = jnp.where(last < 0, 2 * each, last)
    table = jnp.stack([
        moved_id, fixed_id,
        jnp.where(rising, 4 * planes, 0) - shift,
        second.astype(jnp.int32), dy, dz,
        jnp.where(second, 0, shift),
        jnp.where(rising, 0, 4 * planes) + shift,
        prior[:each], prior[each:],
    ])
    return table, last


def slab_body(orbitals, anchors, pair_slots):
    groups, places = lax.axis_size("grp"), lax.axis_size("grid")
    norb_local, cells = orbitals.shape
    planes = cells // (B * B)
    each = PAIR_DEV * places
    chips = places // 2
    cap = 5 * norb_local // 16
    plan, links, fits = make_plan(anchors, pair_slots, cap, each, planes)
    deep = math.gcd(norb_local, 8)

    def lean(orbitals, anchors, pair_slots, plan, links):
        tiled = orbitals.reshape(norb_local // deep, deep, planes, ROWS // SUB, SUB, LANES)
        out = run_lean(plan, links, jnp.transpose(tiled, (0, 2, 3, 4, 1, 5)), each, chips, cap)
        return jnp.transpose(out, (0, 4, 1, 2, 3, 5)).reshape(norb_local, cells)

    def full(orbitals, anchors, pair_slots, plan, links):
        stacked = orbitals.reshape(norb_local, planes, ROWS, LANES)
        table, last = full_tables(anchors, pair_slots, planes, groups, each)
        moved, fixed = bring(table, stacked, each, groups, chips)
        dens, partner = pair_up(table, moved, fixed)
        pot = solve_slabs(table, dens, places, 5)
        going, staying = make_terms(table, pot, partner, moved, fixed)
        out = hand_back(table, last, going, staying, norb_local, chips)
        return out.reshape(norb_local, cells)

    return lax.cond(fits[0] > 0, lean, full, orbitals, anchors, pair_slots, plan, links)


def slabs_fit(mesh):
    groups, places = mesh.shape["grp"], mesh.shape["grid"]
    return groups == 4 and places % 2 == 0 and 4 * (B // places) >= PAD


def solution(mesh):
    return jax.shard_map(
        slab_body if slabs_fit(mesh) else owner_body,
        mesh=mesh,
        in_specs=(P("grp", "grid"), P(), P()),
        out_specs=P("grp", "grid"),
        check_vma=False,
    )
```

```python
import functools
import math

import jax
import jax.numpy as jnp
from jax import lax
from jax.experimental import pallas as pl
from jax.experimental.pallas import tpu as pltpu
from jax.sharding import PartitionSpec as P

B = 64
PAIR_DEV = 2
ITERS = 3
MOST_CHUNKS = 2
LANES = 128
ROWS = B * B // LANES
PAD = 32
STEP = 4


def deal_evenly(pair_slots, owner_count, each_owner):
    flat_slots = pair_slots.reshape(-1, 2)
    filled = (flat_slots[:, 0] >= 0).astype(jnp.int32)
    position = jnp.cumsum(filled, dtype=jnp.int32) - filled
    wanted = lax.broadcasted_iota(jnp.int32, (owner_count, each_owner), 1) * owner_count
    wanted = (wanted + lax.broadcasted_iota(jnp.int32, (owner_count, each_owner), 0)).reshape(-1)
    matched = (position[None, :] == wanted[:, None]) & (filled[None, :] == 1)
    picked = jnp.sum(jnp.where(matched[:, :, None], flat_slots[None], 0), axis=1)
    return picked.reshape(owner_count, each_owner, 2)


def gather_kernel(ids_ref, src_ref, *out_refs):
    count, terms = out_refs[0].shape[:2]
    for slot, out_ref in enumerate(out_refs):
        def pick(dest, unused, slot=slot, out_ref=out_ref):
            for term in range(terms):
                out_ref[dest, term] = src_ref[ids_ref[(slot * count + dest) * terms + term]]
            return unused

        lax.fori_loop(0, count, pick, 0)


def gather_pieces(ids, pieces, slots, count):
    norb, rows, lanes = pieces.shape
    block = max(8, rows // 4)
    return pl.pallas_call(
        gather_kernel,
        grid_spec=pltpu.PrefetchScalarGridSpec(
            num_scalar_prefetch=1,
            grid=(rows // block,),
            in_specs=[pl.BlockSpec((norb, block, lanes), lambda i, ids: (0, i, 0))],
            out_specs=[pl.BlockSpec((count, 2, block, lanes), lambda i, ids: (0, 0, i, 0))] * slots,
        ),
        out_shape=[jax.ShapeDtypeStruct((count, 2, rows, lanes), jnp.float32)] * slots,
        cost_estimate=pl.CostEstimate(flops=0, bytes_accessed=8 * norb * rows * lanes, transcendentals=0),
        name="pick_pieces",
    )(ids, pieces)


def scatter_kernel(ids_ref, *refs):
    out_ref = refs[-1]
    out_ref[...] = jnp.zeros_like(out_ref)
    count, terms = refs[0].shape[:2]
    for slot, in_ref in enumerate(refs[:-1]):
        def add(dest, unused, slot=slot, in_ref=in_ref):
            for term in range(terms):
                orbit = ids_ref[(slot * count + dest) * terms + term]
                out_ref[orbit] = out_ref[orbit] + in_ref[dest, term]
            return unused

        lax.fori_loop(0, count, add, 0)


def scatter_pieces(ids, parts, norb):
    count, terms, rows, lanes = parts[0].shape
    block = max(8, rows // 4)
    return pl.pallas_call(
        scatter_kernel,
        grid_spec=pltpu.PrefetchScalarGridSpec(
            num_scalar_prefetch=1,
            grid=(rows // block,),
            in_specs=[pl.BlockSpec((count, terms, block, lanes), lambda i, ids: (0, 0, i, 0))] * len(parts),
            out_specs=pl.BlockSpec((norb, block, lanes), lambda i, ids: (0, i, 0)),
        ),
        out_shape=jax.ShapeDtypeStruct((norb, rows, lanes), jnp.float32),
        cost_estimate=pl.CostEstimate(flops=0, bytes_accessed=8 * norb * rows * lanes, transcendentals=0),
        name="add_pieces",
    )(ids, *parts)


def lane_ids(shape):
    return lax.broadcasted_iota(jnp.int32, shape, len(shape) - 1)


def shift_plane(plane, off_y, off_z):
    shape = plane.shape
    lane = lane_ids(shape)
    row = lax.broadcasted_iota(jnp.int32, shape, 0)
    linear = off_y * B + off_z
    across = jnp.bitwise_and(linear, LANES - 1)
    down = jnp.right_shift(linear, 7)
    turned = pltpu.roll(plane, across, 1)
    near = pltpu.roll(turned, jnp.bitwise_and(down, ROWS - 1), 0)
    far = pltpu.roll(turned, jnp.bitwise_and(down + 1, ROWS - 1), 0)
    moved = jnp.where(lane >= across, near, far)
    from_y = row * 2 + jnp.right_shift(lane, 6) - off_y
    from_z = jnp.bitwise_and(lane, B - 1) - off_z
    inside = (from_y >= 0) & (from_y < B) & (from_z >= 0) & (from_z < B)
    return jnp.where(inside, moved, 0.0)


def operate_plane(before, plane, after):
    shape = plane.shape
    lane = lane_ids(shape)
    row = lax.broadcasted_iota(jnp.int32, shape, 0)
    z = jnp.bitwise_and(lane, B - 1)
    upper_z = jnp.where(z < B - 1, pltpu.roll(plane, LANES - 1, 1), 0.0)
    lower_z = jnp.where(z > 0, pltpu.roll(plane, 1, 1), 0.0)
    half = pltpu.roll(plane, B, 1)
    down = jnp.where(row > 0, pltpu.roll(half, 1, 0), 0.0)
    up = jnp.where(row < ROWS - 1, pltpu.roll(half, ROWS - 1, 0), 0.0)
    beside = (before + after) + (half + jnp.where(lane < B, down, up))
    return 6.0 * plane - beside - upper_z - lower_z


def fold(values):
    return jnp.sum(values.reshape(ROWS // 8, 8, LANES), axis=0)


def total(acc):
    return jnp.sum(acc, axis=(0, 1), keepdims=True)


def solve_kernel(info_ref, *refs):
    chunks = (len(refs) - 6) // 2
    in_refs, out_refs = refs[:chunks], refs[chunks : 2 * chunks]
    wide, partner, direction, resid, image, potential = refs[2 * chunks :]
    count, terms, rows, lanes = in_refs[0].shape
    each = rows // ROWS
    dx, dy, dz = info_ref[0], info_ref[1], info_ref[2]
    keep = jnp.where(info_ref[3] > 0, 1.0, 0.0).astype(jnp.float32)
    edge = jnp.zeros((PAD, ROWS, LANES), jnp.float32)
    wide[pl.ds(0, PAD)] = edge
    wide[pl.ds(PAD + B, PAD)] = edge
    direction[0] = edge[0]
    direction[B + 1] = edge[0]
    none = jnp.zeros((8, LANES), jnp.float32)

    def place(owner, chunk, i):
        return (owner * chunks + chunk) * each + i

    def load(owner, unused):
        for chunk in range(chunks):
            for i in range(each):
                wide[PAD + place(owner, chunk, i)] = in_refs[chunk][owner, 1, pl.ds(i * ROWS, ROWS)]
        return unused

    lax.fori_loop(0, count, load, 0)

    def start(owner, acc):
        for chunk in range(chunks):
            for i in range(each):
                x = place(owner, chunk, i)
                other = shift_plane(wide[PAD + x - dx], dy, dz)
                partner[x] = other
                density = in_refs[chunk][owner, 0, pl.ds(i * ROWS, ROWS)] * other
                direction[x + 1] = density
                resid[x] = density
                acc = acc + fold(density * density)
        return acc

    norm_now = total(lax.fori_loop(0, count, start, none))

    for turn in range(ITERS):
        def apply(block, acc):
            for i in range(STEP):
                x = block * STEP + i
                plane = direction[x + 1]
                result = operate_plane(direction[x], plane, direction[x + 2])
                image[x] = result
                acc = acc + fold(plane * result)
            return acc

        step_len = norm_now / total(lax.fori_loop(0, B // STEP, apply, none))

        if turn == ITERS - 1:
            break

        def advance(block, acc):
            for i in range(STEP):
                x = block * STEP + i
                moved = step_len * direction[x + 1]
                potential[x] = moved if turn == 0 else potential[x] + moved
                left = resid[x] - step_len * image[x]
                resid[x] = left
                acc = acc + fold(left * left)
            return acc

        norm_next = total(lax.fori_loop(0, B // STEP, advance, none))
        ratio = norm_next / norm_now

        def renew(block, unused):
            for i in range(STEP):
                x = block * STEP + i
                direction[x + 1] = resid[x] + ratio * direction[x + 1]
            return unused

        lax.fori_loop(0, B // STEP, renew, 0)
        norm_now = norm_next

    def finish(owner, unused):
        for chunk in range(chunks):
            for i in range(each):
                x = place(owner, chunk, i)
                found = (potential[x] + step_len * direction[x + 1]) * keep
                out_refs[chunk][owner, 0, pl.ds(i * ROWS, ROWS)] = found * partner[x]
                wide[PAD + x] = found * in_refs[chunk][owner, 0, pl.ds(i * ROWS, ROWS)]
        return unused

    lax.fori_loop(0, count, finish, 0)

    def give_back(owner, unused):
        for chunk in range(chunks):
            for i in range(each):
                x = place(owner, chunk, i)
                out_refs[chunk][owner, 1, pl.ds(i * ROWS, ROWS)] = shift_plane(wide[PAD + x + dx], -dy, -dz)
        return unused

    lax.fori_loop(0, count, give_back, 0)


def solve_pair(info, parts):
    box = (B, ROWS, LANES)
    vmem = pl.BlockSpec(memory_space=pltpu.VMEM)
    return pl.pallas_call(
        solve_kernel,
        in_specs=[pl.BlockSpec(memory_space=pltpu.SMEM)] + [vmem] * len(parts),
        out_specs=[vmem] * len(parts),
        out_shape=[jax.ShapeDtypeStruct(p.shape, jnp.float32) for p in parts],
        scratch_shapes=[
            pltpu.VMEM((B + 2 * PAD, ROWS, LANES), jnp.float32),
            pltpu.VMEM(box, jnp.float32),
            pltpu.VMEM((B + 2, ROWS, LANES), jnp.float32),
            pltpu.VMEM(box, jnp.float32),
            pltpu.VMEM(box, jnp.float32),
            pltpu.VMEM(box, jnp.float32),
        ],
        compiler_params=pltpu.CompilerParams(vmem_limit_bytes=32 * 1024 * 1024),
        cost_estimate=pl.CostEstimate(flops=0, bytes_accessed=40 * 1024 * 1024, transcendentals=0),
        name="solve_pair",
    )(info, *parts)


def owner_body(orbitals, anchors, pair_slots):
    grid_count = lax.axis_size("grid")
    owner_count = lax.axis_size("grp") * grid_count
    group_idx = lax.axis_index("grp")
    place_idx = lax.axis_index("grid")
    assignment = deal_evenly(pair_slots, owner_count, PAIR_DEV)
    slots = assignment.shape[1]
    filled = assignment[..., 0] >= 0
    safe_ids = jnp.maximum(assignment, 0)
    group_table = lax.dynamic_slice_in_dim(safe_ids, group_idx * grid_count, grid_count, 0)
    ids = jnp.transpose(group_table, (1, 0, 2)).reshape(-1)
    owner_idx = group_idx * grid_count + place_idx
    own_pairs = safe_ids[owner_idx]
    offsets = anchors[own_pairs[:, 1]] - anchors[own_pairs[:, 0]]
    info = jnp.concatenate([offsets, filled[owner_idx].astype(jnp.int32)[:, None]], axis=1)

    norb_local, cells = orbitals.shape
    stacked = orbitals.reshape(norb_local, cells // LANES, LANES)
    chunks = math.gcd(MOST_CHUNKS, cells // (B * B))
    rows = stacked.shape[1] // chunks
    arrived = [[None] * chunks for _ in range(slots)]
    for chunk in range(chunks):
        pieces = lax.all_gather(stacked[:, chunk * rows : (chunk + 1) * rows], "grp", axis=0, tiled=True)
        outgoing = gather_pieces(ids, pieces, slots, grid_count)
        for slot in range(slots):
            arrived[slot][chunk] = lax.all_to_all(outgoing[slot], "grid", split_axis=0, concat_axis=0, tiled=True)
    returned = []
    for slot in range(slots):
        terms = solve_pair(info[slot], arrived[slot])
        returned.append(
            [lax.all_to_all(t, "grid", split_axis=0, concat_axis=0, tiled=True) for t in terms]
        )
    results = []
    for chunk in range(chunks):
        summed = scatter_pieces(ids, [r[chunk] for r in returned], anchors.shape[0])
        results.append(lax.psum_scatter(summed, "grp", scatter_dimension=0, tiled=True))
    return jnp.concatenate(results, axis=1).reshape(norb_local, cells)


MESH = pl.DeviceIdType.MESH
HALO = 3
WAVES = 4
TRIALS = 12
SUB = 8


def remote(src, dst, send_sem, recv_sem, device):
    return pltpu.make_async_remote_copy(
        src_ref=src, dst_ref=dst, send_sem=send_sem, recv_sem=recv_sem, device_id=device, device_id_type=MESH
    )


def spot():
    grp = lax.axis_index("grp")
    place = lax.axis_index("grid")
    across = grp + 1 - 2 * lax.rem(grp, 2)
    along = lax.rem(grp + 2, 4)
    corner = lax.rem(across + 2, 4)
    return grp, place, across, along, corner


def greet(chips, wide=False):
    grp, place, across, along, corner = spot()
    chip = place // 2
    core = lax.rem(place, 2)
    barrier = pltpu.get_barrier_semaphore()
    peers = [(across, place), (along, place), (grp, 2 * chip + 1 - core)] + ([(corner, place)] if wide else [])
    for device in peers:
        pl.semaphore_signal(barrier, inc=1, device_id=device, device_id_type=MESH)

    @pl.when(chip > 0)
    def below():
        pl.semaphore_signal(barrier, inc=1, device_id=(grp, place - 2), device_id_type=MESH)

    @pl.when(chip < chips - 1)
    def above():
        pl.semaphore_signal(barrier, inc=1, device_id=(grp, place + 2), device_id_type=MESH)

    ends = jnp.where(chip > 0, 1, 0) + jnp.where(chip < chips - 1, 1, 0)
    pl.semaphore_wait(barrier, len(peers) + ends)


class Relay:
    def __init__(self, wins, send_sem, recv_sem, signs, chips, marks):
        self.wins, self.send_sem, self.recv_sem, self.signs, self.chips = wins, send_sem, recv_sem, signs, chips
        self.grp, self.place = lax.axis_index("grp"), lax.axis_index("grid")
        self.chip = self.place // 2
        self.core = lax.rem(self.place, 2)
        self.half = wins[0].shape[0] // 2
        self.planes = wins[0].shape[1] // 6
        self.deep, self.far, self.mid = marks

    def offset(self, sign, hop):
        return 2 * self.planes * (2 - hop if sign > 0 else hop)

    def region(self, chunk, side, hop, core, size, skip=0):
        start = self.offset(self.signs[side], hop) + self.planes * core
        return self.wins[chunk].at[pl.ds(side * self.half + skip, size), pl.ds(start, self.planes)]

    def comes(self, side, hop):
        source = self.chip - self.signs[side] * hop
        return source >= 0 if self.signs[side] > 0 else source < self.chips

    def goes(self, side, hop):
        source = self.chip + self.signs[side] - self.signs[side] * hop
        if self.signs[side] > 0:
            return (self.chip + 1 < self.chips) & (source >= 0)
        return (self.chip - 1 >= 0) & (source < self.chips)

    def spans(self, side, hop, core, act):
        if hop == 0:
            act(self.half)
        else:
            near = 1 if self.signs[side] > 0 else 0
            most, least = (self.half, self.mid) if hop == 1 else (self.far, self.deep)
            if most == least:
                act(most)
                return

            @pl.when(core == near)
            def whole():
                act(most)

            @pl.when(core != near)
            def some():
                act(least)

    def onward(self, chunk, side, hop, size, here=None):
        source = self.region(chunk, side, hop - 1 if here is None else here, self.core, size)
        there = self.region(chunk, side, hop, self.core, size)
        return remote(
            source, there, self.send_sem.at[chunk, side, hop - 1], self.recv_sem.at[chunk, side, hop - 1],
            (self.grp, self.place + 2 * self.signs[side]),
        )

    def rest(self, chunk, side, act, here=0):
        def copy(size):
            source = self.region(chunk, side, here, self.core, size - self.far, self.far)
            there = self.region(chunk, side, 1, self.core, size - self.far, self.far)
            act(remote(
                source, there, self.send_sem.at[chunk, side, 5], self.recv_sem.at[chunk, side, 5],
                (self.grp, self.place + 2 * self.signs[side]),
            ))

        if self.far < self.half:
            self.spans(side, 1, self.core, copy)

    def ahead(self, side, hop, act):
        if hop == 1:
            act(self.far)
        else:
            self.spans(side, hop, self.core, act)

    def beside(self, chunk, side, hop, core, size):
        part = self.region(chunk, side, hop, core, size)
        return remote(
            part, part, self.send_sem.at[chunk, side, 2 + hop], self.recv_sem.at[chunk, side, 2 + hop],
            (self.grp, 2 * self.chip + 1 - self.core),
        )

    def clear(self):
        for side in range(2):
            for hop in (1, 2):
                start = self.offset(self.signs[side], hop)

                @pl.when(jnp.logical_not(self.comes(side, hop)))
                def fill(side=side, start=start):
                    for win in self.wins:
                        def zero(slot, unused, win=win):
                            win[slot, pl.ds(start, 2 * self.planes)] = jnp.zeros(
                                (2 * self.planes,) + win.shape[2:], jnp.float32
                            )
                            return unused

                        lax.fori_loop(side * self.half, (side + 1) * self.half, zero, 0)

    def pass_on(self, chunk, side, hop):
        @pl.when(self.goes(side, hop))
        def go():
            self.ahead(side, hop, lambda size: self.onward(chunk, side, hop, size).start())
            if hop == 1:
                self.rest(chunk, side, lambda copy: copy.start())

    def begin(self, chunk, sides=(0, 1)):
        for side in sides:
            self.pass_on(chunk, side, 1)
        for side in sides:
            self.beside(chunk, side, 0, self.core, self.half).start()

    def arrive(self, chunk, side, hop):
        @pl.when(self.comes(side, hop))
        def got():
            self.ahead(side, hop, lambda size: self.onward(chunk, side, hop, size, hop).wait_recv())

    def spread(self, chunk, side, hop):
        @pl.when(self.comes(side, hop))
        def share():
            if hop == 1:
                self.rest(chunk, side, lambda copy: copy.wait_recv(), 1)
            self.spans(side, hop, self.core, lambda size: self.beside(chunk, side, hop, self.core, size).start())

    def first(self, chunk):
        for side in range(2):
            self.arrive(chunk, side, 1)
            self.pass_on(chunk, side, 2)

    def share(self, chunk):
        for side in range(2):
            self.spread(chunk, side, 1)

    def second(self, chunk):
        for side in range(2):
            self.arrive(chunk, side, 2)
            self.spread(chunk, side, 2)

    def settle(self, chunk):
        other = 1 - self.core
        for side in range(2):
            self.beside(chunk, side, 0, other, self.half).wait_recv()
            for hop in (1, 2):
                @pl.when(self.comes(side, hop))
                def got(side=side, hop=hop):
                    self.spans(side, hop, other, lambda size: self.beside(chunk, side, hop, other, size).wait_recv())

    def drain(self):
        for chunk in range(len(self.wins)):
            for side in range(2):
                self.beside(chunk, side, 0, self.core, self.half).wait_send()
                for hop in (1, 2):
                    @pl.when(self.comes(side, hop))
                    def sent(chunk=chunk, side=side, hop=hop):
                        self.spans(
                            side, hop, self.core,
                            lambda size: self.beside(chunk, side, hop, self.core, size).wait_send(),
                        )

                    @pl.when(self.goes(side, hop))
                    def passed(chunk=chunk, side=side, hop=hop):
                        self.ahead(side, hop, lambda size: self.onward(chunk, side, hop, size).wait_send())
                        if hop == 1:
                            self.rest(chunk, side, lambda copy: copy.wait_send())


def bring_kernel(chips, tbl, orb, moved, fixed, *scratch):
    count = moved.shape[0]
    pools, wins = scratch[:count], scratch[count : 2 * count]
    own_sem, xy_send, xy_recv, z_send, z_recv = scratch[2 * count :]
    grp, place, across, along, corner = spot()
    core = lax.rem(place, 2)
    norb, planes = orb.shape[:2]
    part = norb // 2
    slots = moved.shape[1]
    relay = Relay(wins, z_send, z_recv, (1, -1), chips, (slots // 2,) * 3)

    def block(chunk, owner, start, size):
        return pools[chunk].at[pl.ds(owner * norb + start, size)]

    def stage(chunk):
        return pltpu.make_async_copy(
            orb.at[:, :, pl.ds(chunk * SUB, SUB)], block(chunk, grp, 0, norb), own_sem.at[chunk]
        )

    def hop(chunk, kind, owner, start, size, target):
        ref = block(chunk, owner, start, size)
        return remote(ref, ref, xy_send.at[chunk, kind], xy_recv.at[chunk, kind], (target, place))

    def direct(chunk, owners):
        return hop(chunk, 0, owners[0], 0, norb, across), hop(chunk, 1, owners[1], 0, norb, along)

    def turned(chunk, owners):
        return hop(chunk, 2, owners[0], 0, part, along), hop(chunk, 3, owners[1], part, part, across)

    for chunk in range(count):
        stage(chunk).start()
    greet(chips)
    relay.clear()

    def send_own(chunk):
        stage(chunk).wait()
        for copy in direct(chunk, (grp, grp)):
            copy.start()

    send_own(0)
    send_own(1)
    for step in range(count + 4):
        if step < count:
            for copy in direct(step, (across, along)):
                copy.wait_recv()
            for copy in turned(step, (across, along)):
                copy.start()
            if step + 2 < count:
                send_own(step + 2)
        chunk = step - 1
        if 0 <= chunk < count:
            for copy in turned(chunk, (corner, corner)):
                copy.wait_recv()
            for side in range(2):
                start = relay.offset(relay.signs[side], 0) + planes * core

                def pick(slot, unused, start=start, chunk=chunk):
                    wins[chunk][slot, pl.ds(start, planes)] = pools[chunk][tbl[0, slot]]
                    fixed[chunk, slot] = pools[chunk][tbl[1, slot]]
                    return unused

                lax.fori_loop(side * (slots // 2), (side + 1) * (slots // 2), pick, 0)
            relay.begin(chunk)
        chunk = step - 2
        if 0 <= chunk < count:
            relay.first(chunk)
            relay.share(chunk)
        chunk = step - 3
        if 0 <= chunk < count:
            relay.second(chunk)
        chunk = step - 4
        if 0 <= chunk < count:
            relay.settle(chunk)

            def choose(slot, unused, chunk=chunk):
                first = tbl[2, slot] + planes * core
                for plane in range(planes):
                    moved[chunk, slot, plane] = wins[chunk][slot, first + plane]
                return unused

            lax.fori_loop(0, slots, choose, 0)
    for chunk in range(count):
        for copy in direct(chunk, (grp, grp)) + turned(chunk, (across, along)):
            copy.wait_send()
    relay.drain()


def bring(table, stacked, slots, groups, chips):
    norb, planes, rows, lanes = stacked.shape
    chunks = rows // SUB
    vmem = pl.BlockSpec(memory_space=pltpu.VMEM)
    dma = pltpu.SemaphoreType.DMA
    shape = jax.ShapeDtypeStruct((chunks, slots, planes, SUB, lanes), jnp.float32)
    return pl.pallas_call(
        functools.partial(bring_kernel, chips),
        in_specs=[pl.BlockSpec(memory_space=pltpu.SMEM), pl.BlockSpec(memory_space=pl.ANY)],
        out_specs=[vmem, vmem],
        out_shape=[shape, shape],
        scratch_shapes=[pltpu.VMEM((groups * norb, planes, SUB, lanes), jnp.float32)] * chunks
        + [pltpu.VMEM((slots, 6 * planes, SUB, lanes), jnp.float32)] * chunks
        + [dma((chunks,)), dma((chunks, 4)), dma((chunks, 4)), dma((chunks, 2, 6)), dma((chunks, 2, 6))],
        compiler_params=pltpu.CompilerParams(
            collective_id=0, has_side_effects=True, vmem_limit_bytes=48 * 1024 * 1024
        ),
        name="bring",
    )(table, stacked)


def pair_kernel(tbl, moved, fixed, dens, partner):
    def go(slot, unused):
        second = tbl[3, slot] > 0
        dy, dz = tbl[4, slot], tbl[5, slot]
        for x in range(moved.shape[2]):
            left = moved[:, slot, x].reshape(ROWS, LANES)
            right = fixed[:, slot, x].reshape(ROWS, LANES)
            other = shift_plane(jnp.where(second, left, right), dy, dz)
            dens[slot, x] = jnp.where(second, right, left) * other
            partner[slot, x] = other
        return unused

    lax.fori_loop(0, moved.shape[1], go, 0)


def pair_up(table, moved, fixed):
    chunks, slots, planes, sub, lanes = moved.shape
    vmem = pl.BlockSpec(memory_space=pltpu.VMEM)
    shape = jax.ShapeDtypeStruct((slots, planes, ROWS, lanes), jnp.float32)
    return pl.pallas_call(
        pair_kernel,
        in_specs=[pl.BlockSpec(memory_space=pltpu.SMEM), vmem, vmem],
        out_specs=[vmem, vmem],
        out_shape=[shape, shape],
        compiler_params=pltpu.CompilerParams(vmem_limit_bytes=24 * 1024 * 1024),
        name="pair_up",
    )(table, moved, fixed)


def inner(plane):
    shape = plane.shape
    lane = lane_ids(shape)
    row = lax.broadcasted_iota(jnp.int32, shape, 0)
    z = jnp.bitwise_and(lane, B - 1)
    upper_z = jnp.where(z < B - 1, pltpu.roll(plane, LANES - 1, 1), 0.0)
    lower_z = jnp.where(z > 0, pltpu.roll(plane, 1, 1), 0.0)
    half = pltpu.roll(plane, B, 1)
    down = jnp.where(row > 0, pltpu.roll(half, 1, 0), 0.0)
    up = jnp.where(row < ROWS - 1, pltpu.roll(half, ROWS - 1, 0), 0.0)
    return 6.0 * plane - ((half + jnp.where(lane < B, down, up)) + (upper_z + lower_z))


def krylov_weights(m):
    a0 = m[0] / m[1]
    rr1 = a0 * a0 * m[2] - m[0]
    p, q = 1.0 + rr1 / m[0], -a0
    a1 = rr1 / (p * p * m[1] + 2.0 * p * q * m[2] + q * q * m[3])
    s1, s2 = -a0 - a1 * p, -a1 * q
    rr2 = (m[0] + s1 * s1 * m[2] + s2 * s2 * m[4]) + 2.0 * (s1 * m[1] + s2 * m[2] + s1 * s2 * m[3])
    b1 = rr2 / rr1
    e0, e1, e2 = 1.0 + b1 * p, s1 + b1 * q, s2
    bend = e0 * e0 * m[1] + e1 * e1 * m[3] + e2 * e2 * m[5]
    a2 = rr2 / (bend + 2.0 * (e0 * e1 * m[2] + e0 * e2 * m[3] + e1 * e2 * m[4]))
    return a0 + a1 * p + a2 * e0, a1 * q + a2 * e1, a2 * e2


def solve_slabs_kernel(places, tbl, dens, pot, wide, one, two, sums, gathered, weights, h_send, h_recv, s_send, s_recv):
    grp, place = lax.axis_index("grp"), lax.axis_index("grid")
    slots, planes = dens.shape[:2]
    first, last = HALO, HALO + planes - 1
    each = slots // WAVES
    barrier = pltpu.get_barrier_semaphore()
    for step in range(1, places):
        pl.semaphore_signal(
            barrier, inc=1, device_id=(grp, lax.rem(place + step, places)), device_id_type=MESH
        )
    pl.semaphore_wait(barrier, places - 1)

    def rise(wave):
        return remote(
            dens.at[pl.ds(wave * each, each), pl.ds(planes - HALO + 1, HALO - 1)],
            wide.at[pl.ds(wave * each, each), pl.ds(1, HALO - 1)],
            h_send.at[wave, 0], h_recv.at[wave, 0], (grp, lax.rem(place + 1, places)),
        )

    def sink(wave):
        return remote(
            dens.at[pl.ds(wave * each, each), pl.ds(0, HALO)],
            wide.at[pl.ds(wave * each, each), pl.ds(HALO + planes, HALO)],
            h_send.at[wave, 1], h_recv.at[wave, 1], (grp, lax.rem(place + places - 1, places)),
        )

    lowest, highest = place == 0, place == places - 1
    for wave in range(WAVES):
        @pl.when(jnp.logical_not(highest))
        def send_up(wave=wave):
            rise(wave).start()

        @pl.when(jnp.logical_not(lowest))
        def send_down(wave=wave):
            sink(wave).start()

    blank = jnp.zeros((HALO, ROWS, LANES), jnp.float32)

    def copy_in(slot, unused):
        wide[slot, pl.ds(HALO, planes)] = dens[slot]
        one[slot, 1] = blank[0]
        one[slot, last + 3] = blank[0]
        one[slot, 0] = blank[0]
        return unused

    lax.fori_loop(0, slots, copy_in, 0)

    @pl.when(lowest)
    def no_below():
        def fill(slot, unused):
            wide[slot, pl.ds(0, HALO)] = blank
            return unused

        lax.fori_loop(0, slots, fill, 0)

    @pl.when(highest)
    def no_above():
        def fill(slot, unused):
            wide[slot, pl.ds(HALO + planes, HALO)] = blank
            return unused

        lax.fori_loop(0, slots, fill, 0)

    lane = lax.broadcasted_iota(jnp.int32, (1, LANES), 1)
    none = jnp.zeros((8, LANES), jnp.float32)

    def row_of(parts):
        row = jnp.zeros((1, LANES), jnp.float32)
        for at, part in parts:
            row = row + jnp.where(lane == at, total(part), 0.0)
        return row

    def work(slot, unused):
        low, high = tbl[6, slot], tbl[6, slot] + B

        def live(e):
            x = planes * place + e - HALO
            return jnp.where((x >= low) & (x < high), 1.0, 0.0).astype(jnp.float32)

        m0, m1, m2, m3, m4, m5 = none, none, none, none, none, none
        for e in range(first - 1, last + 3):
            value = live(e) * (inner(wide[slot, e]) - (wide[slot, e - 1] + wide[slot, e + 1]))
            one[slot, e] = value
            if first <= e <= last:
                source = wide[slot, e]
                m0 = m0 + fold(source * source)
                m1 = m1 + fold(source * value)
                m2 = m2 + fold(value * value)
        bent = None
        for e in range(first, last + 2):
            value = live(e) * (inner(one[slot, e]) - (one[slot, e - 1] + one[slot, e + 1]))
            two[slot, e] = value
            if e > first:
                m5 = m5 - 2.0 * fold(value * two[slot, e - 1])
            if e <= last:
                m3 = m3 + fold(one[slot, e] * value)
                m4 = m4 + fold(value * value)
                m5 = m5 + fold(value * inner(value))
        sums[pl.ds(slot, 1)] = row_of(enumerate((m0, m1, m2, m3, m4, m5)))
        return unused

    def rim(slot, spots, pairs):
        low, high = tbl[6, slot], tbl[6, slot] + B
        m2, m3, m4, m5 = none, none, none, none
        for e, fresh in spots:
            if fresh:
                x = planes * place + e - HALO
                alive = jnp.where((x >= low) & (x < high), 1.0, 0.0).astype(jnp.float32)
                two[slot, e] = alive * (inner(one[slot, e]) - (one[slot, e - 1] + one[slot, e + 1]))
        for e, fresh in spots:
            value, before = two[slot, e], one[slot, e]
            m2 = m2 + fold(before * before)
            m3 = m3 + fold(before * value)
            m4 = m4 + fold(value * value)
            m5 = m5 + fold(value * inner(value))
        for e in pairs:
            m5 = m5 - 2.0 * fold(two[slot, e] * two[slot, e + 1])
        sums[pl.ds(slot, 1)] = sums[pl.ds(slot, 1)] + row_of(((2, m2), (3, m3), (4, m4), (5, m5)))

    for wave in range(WAVES):
        @pl.when(jnp.logical_not(lowest))
        def got_below(wave=wave):
            rise(wave).wait_recv()

        @pl.when(jnp.logical_not(highest))
        def got_above(wave=wave):
            sink(wave).wait_recv()

        lax.fori_loop(wave * each, (wave + 1) * each, work, 0)

    @pl.when(lowest)
    def rim_below():
        def go(slot, unused):
            rim(slot, ((first - 2, True), (first - 1, True)), (first - 2, first - 1))
            return unused

        lax.fori_loop(0, slots, go, 0)

    @pl.when(highest)
    def rim_above():
        def go(slot, unused):
            rim(slot, ((last + 1, False), (last + 2, True)), (last + 1,))
            return unused

        lax.fori_loop(0, slots, go, 0)

    def tell(step):
        return remote(
            sums, gathered.at[place], s_send.at[step - 1], s_recv.at[step - 1],
            (grp, lax.rem(place + step, places)),
        )

    def hear(step):
        source = lax.rem(place + places - step, places)
        return remote(
            sums, gathered.at[source], s_send.at[step - 1], s_recv.at[step - 1],
            (grp, lax.rem(place + step, places)),
        )

    for step in range(1, places):
        tell(step).start()
    gathered[place] = sums[...]
    for step in range(1, places):
        hear(step).wait_recv()
    whole = gathered[0]
    for at in range(1, places):
        whole = whole + gathered[at]
    lanes = lax.broadcasted_iota(jnp.int32, whole.shape, 1)
    moments = [jnp.sum(jnp.where(lanes == at, whole, 0.0), axis=1, keepdims=True) for at in range(6)]
    for at, weight in enumerate(krylov_weights(moments)):
        weights[at] = jnp.broadcast_to(weight, whole.shape)

    def finish(slot, unused):
        w0, w1, w2 = [weights[at, pl.ds(slot, 1)] for at in range(3)]
        for x in range(planes):
            e = x + HALO
            pot[slot, x] = w0 * wide[slot, e] + w1 * one[slot, e] + w2 * two[slot, e]
        return unused

    lax.fori_loop(0, slots, finish, 0)
    for wave in range(WAVES):
        @pl.when(jnp.logical_not(highest))
        def sent_up(wave=wave):
            rise(wave).wait_send()

        @pl.when(jnp.logical_not(lowest))
        def sent_down(wave=wave):
            sink(wave).wait_send()

    for step in range(1, places):
        tell(step).wait_send()


def solve_slabs(table, dens, places, ident):
    slots, planes, rows, lanes = dens.shape
    vmem = pl.BlockSpec(memory_space=pltpu.VMEM)
    dma = pltpu.SemaphoreType.DMA
    tall = pltpu.VMEM((slots, planes + 2 * HALO, rows, lanes), jnp.float32)
    return pl.pallas_call(
        functools.partial(solve_slabs_kernel, places),
        in_specs=[pl.BlockSpec(memory_space=pltpu.SMEM), vmem],
        out_specs=vmem,
        out_shape=jax.ShapeDtypeStruct(dens.shape, jnp.float32),
        scratch_shapes=[
            tall, tall, tall,
            pltpu.VMEM((slots, lanes), jnp.float32),
            pltpu.VMEM((places, slots, lanes), jnp.float32),
            pltpu.VMEM((3, slots, lanes), jnp.float32),
            dma((WAVES, 2)), dma((WAVES, 2)), dma((places - 1,)), dma((places - 1,)),
        ],
        compiler_params=pltpu.CompilerParams(
            collective_id=ident, has_side_effects=True, vmem_limit_bytes=40 * 1024 * 1024
        ),
        name="solve_slabs",
    )(table, dens)


def term_kernel(tbl, pot, partner, moved, fixed, going, staying):
    chunks = going.shape[0]

    def go(slot, unused):
        second = tbl[3, slot] > 0
        dy, dz = tbl[4, slot], tbl[5, slot]
        for x in range(pot.shape[1]):
            found = pot[slot, x]
            left = moved[:, slot, x].reshape(ROWS, LANES)
            right = fixed[:, slot, x].reshape(ROWS, LANES)
            term_a = found * partner[slot, x]
            term_b = shift_plane(found * jnp.where(second, right, left), -dy, -dz)
            going[:, slot, x] = jnp.where(second, term_b, term_a).reshape(chunks, SUB, LANES)
            staying[:, slot, x] = jnp.where(second, term_a, term_b).reshape(chunks, SUB, LANES)
        return unused

    lax.fori_loop(0, pot.shape[0], go, 0)


def make_terms(table, pot, partner, moved, fixed):
    vmem = pl.BlockSpec(memory_space=pltpu.VMEM)
    shape = jax.ShapeDtypeStruct(moved.shape, jnp.float32)
    return pl.pallas_call(
        term_kernel,
        in_specs=[pl.BlockSpec(memory_space=pltpu.SMEM)] + [vmem] * 4,
        out_specs=[vmem, vmem],
        out_shape=[shape, shape],
        compiler_params=pltpu.CompilerParams(vmem_limit_bytes=24 * 1024 * 1024),
        name="make_terms",
    )(table, pot, partner, moved, fixed)


def hand_back_kernel(chips, tbl, last, going, staying, out, *scratch):
    count, slots = going.shape[:2]
    wins, chains, outs1, outs2, ins1, ins2 = [scratch[i * count : (i + 1) * count] for i in range(6)]
    xy_send, xy_recv, z_send, z_recv = scratch[6 * count :]
    grp, place, across, along, corner = spot()
    core = lax.rem(place, 2)
    norb, planes = out.shape[:2]
    part = norb // 2
    relay = Relay(wins, z_send, z_recv, (-1, 1), chips, (slots // 2,) * 3)
    greet(chips)
    relay.clear()

    def start(chunk):
        for side in range(2):
            at = relay.offset(relay.signs[side], 0) + planes * core

            def place_in(slot, unused, at=at):
                wins[chunk][slot, pl.ds(at, planes)] = going[chunk, slot]
                return unused

            lax.fori_loop(side * (slots // 2), (side + 1) * (slots // 2), place_in, 0)
        relay.begin(chunk)

    def swap(chunk, kind):
        src = (outs1 if kind < 2 else outs2)[chunk].at[kind % 2]
        dst = (ins1 if kind < 2 else ins2)[chunk].at[kind % 2]
        target = (across, along, along, across)[kind]
        return remote(src, dst, xy_send.at[chunk, kind], xy_recv.at[chunk, kind], (target, place))

    start(0)
    start(1)
    for step in range(count + 4):
        if step < count:
            relay.first(step)
            relay.share(step)
            if step + 2 < count:
                start(step + 2)
        chunk = step - 1
        if 0 <= chunk < count:
            relay.second(chunk)
        chunk = step - 2
        if 0 <= chunk < count:
            relay.settle(chunk)
            chain = chains[chunk]
            chain[2 * slots] = jnp.zeros(chain.shape[1:], jnp.float32)

            def link_fixed(slot, unused, chain=chain, chunk=chunk):
                chain[slot] = staying[chunk, slot] + chain[tbl[8, slot]]
                return unused

            def link_moved(slot, unused, chain=chain, chunk=chunk):
                first = tbl[7, slot] + planes * core
                for plane in range(planes):
                    chain[slots + slot, plane] = wins[chunk][slot, first + plane] + chain[tbl[9, slot], plane]
                return unused

            lax.fori_loop(0, slots, link_fixed, 0)
            lax.fori_loop(0, slots, link_moved, 0)

            def pack(i, unused, chain=chain, chunk=chunk):
                outs1[chunk][0, i] = chain[last[across * norb + i]]
                outs1[chunk][0, part + i] = chain[last[corner * norb + i]]
                outs1[chunk][1, i] = chain[last[along * norb + part + i]]
                outs1[chunk][1, part + i] = chain[last[corner * norb + part + i]]
                return unused

            lax.fori_loop(0, part, pack, 0)
            swap(chunk, 0).start()
            swap(chunk, 1).start()
        chunk = step - 3
        if 0 <= chunk < count:
            chain = chains[chunk]
            swap(chunk, 0).wait_recv()

            def add_across(i, unused, chain=chain, chunk=chunk):
                outs2[chunk][0, i] = ins1[chunk][0, part + i] + chain[last[along * norb + i]]
                return unused

            lax.fori_loop(0, part, add_across, 0)
            swap(chunk, 2).start()
            swap(chunk, 1).wait_recv()

            def add_along(i, unused, chain=chain, chunk=chunk):
                outs2[chunk][1, i] = ins1[chunk][1, part + i] + chain[last[across * norb + part + i]]
                return unused

            lax.fori_loop(0, part, add_along, 0)
            swap(chunk, 3).start()
        chunk = step - 4
        if 0 <= chunk < count:
            chain = chains[chunk]
            swap(chunk, 2).wait_recv()
            swap(chunk, 3).wait_recv()
            for side in range(2):
                def keep(i, unused, side=side, chain=chain, chunk=chunk):
                    orbit = side * part + i
                    found = ins1[chunk][side, i] + ins2[chunk][side, i]
                    out[orbit, :, pl.ds(chunk * SUB, SUB)] = found + chain[last[grp * norb + orbit]]
                    return unused

                lax.fori_loop(0, part, keep, 0)
    for chunk in range(count):
        for kind in range(4):
            swap(chunk, kind).wait_send()
    relay.drain()


def hand_back(table, last, going, staying, norb, chips):
    chunks, slots, planes, sub, lanes = going.shape
    vmem = pl.BlockSpec(memory_space=pltpu.VMEM)
    smem = pl.BlockSpec(memory_space=pltpu.SMEM)
    dma = pltpu.SemaphoreType.DMA
    def room(*lead):
        return [pltpu.VMEM(lead + (planes, sub, lanes), jnp.float32)] * chunks
    wins = [pltpu.VMEM((slots, 6 * planes, sub, lanes), jnp.float32)] * chunks
    return pl.pallas_call(
        functools.partial(hand_back_kernel, chips),
        in_specs=[smem, smem, vmem, vmem],
        out_specs=vmem,
        out_shape=jax.ShapeDtypeStruct((norb, planes, chunks * sub, lanes), jnp.float32),
        scratch_shapes=wins + room(2 * slots + 1) + room(2, norb) + room(2, norb // 2)
        + room(2, norb) + room(2, norb // 2)
        + [dma((chunks, 4)), dma((chunks, 4)), dma((chunks, 2, 6)), dma((chunks, 2, 6))],
        compiler_params=pltpu.CompilerParams(
            collective_id=2, has_side_effects=True, vmem_limit_bytes=56 * 1024 * 1024
        ),
        name="hand_back",
    )(table, last, going, staying)


def plan_kernel(cap, planes, me_ref, anchors, pairs, tbl, links, fits, spots, masks, lists, mine, counts):
    groups = 4
    orbits = anchors.shape[1]
    local = orbits // groups
    depth, unused, owners = pairs.shape
    entries = depth * owners
    each = tbl.shape[1]
    half = each // 2
    extra = (groups - 1) * cap
    final = extra
    prior = final + local + extra
    ends = prior + extra
    spare = ends + local
    worst = 1 << 20
    me = me_ref[0]

    def unpack(code):
        return jnp.bitwise_and(code, 1023), jnp.bitwise_and(jnp.right_shift(code, 10), 1023)

    def clean(i, unused):
        links[i] = 0
        links[prior + i] = extra
        return unused

    def close(i, unused):
        links[final + i] = 2 * each
        return unused

    def own(i, unused):
        links[ends + i] = extra
        spots[me * local + i] = i
        return unused

    lax.fori_loop(0, extra, clean, 0, unroll=5)
    lax.fori_loop(0, local + extra, close, 0, unroll=4)
    lax.fori_loop(0, local, own, 0, unroll=4)

    def sort(i, tails, layer):
        a, b = pairs[layer, 0, i], pairs[layer, 1, i]
        filled = jnp.where(a >= 0, 1, 0)
        dx = anchors[0, jnp.maximum(b, 0)] - anchors[0, jnp.maximum(a, 0)]
        reach = jnp.abs(dx)
        kind = 3 - sum(jnp.where(reach > planes * k, 1, 0) for k in (1, 2, 3))
        step = jnp.left_shift(kind, 3)
        tail = jnp.bitwise_and(jnp.right_shift(tails, step), 255)
        code = a + jnp.left_shift(b, 10) + jnp.left_shift(dx + B, 20)
        lists[jnp.where(filled > 0, kind * entries + tail, 4 * entries)] = code
        return tails + jnp.left_shift(filled, step)

    zero = jnp.int32(0)
    packed = zero
    for layer in range(depth):
        packed = lax.fori_loop(0, owners, functools.partial(sort, layer=layer), packed, unroll=8)
    tails = [jnp.bitwise_and(jnp.right_shift(packed, 8 * k), 255) for k in range(4)]
    fits[0] = 0

    def trial(turn):
        def reset(i, unused):
            for g in range(groups):
                masks[g * local + i] = (15 - (1 << g)) + (g << 10)
            return unused

        lax.fori_loop(0, local, reset, 0, unroll=8)
        state = (zero,) * (groups + 1)
        for kind, limit in enumerate((half // 4, half // 2, 3 * half // 4, half)):
            size = tails[kind]
            base = lax.rem(turn * 5, jnp.maximum(size, 1))
            flip = jnp.bitwise_and(turn, 1) > 0

            def deal(i, state, kind=kind, limit=limit, size=size, base=base, flip=flip):
                filled, bad = state[:groups], state[groups]
                at = i + base
                at = jnp.where(at >= size, at - size, at)
                code = lists[kind * entries + jnp.where(flip, size - 1 - at, at)]
                a, b = unpack(code)
                word_a, word_b = masks[a], masks[b]
                step_a, step_b = jnp.right_shift(word_a, 8), jnp.right_shift(word_b, 8)
                same = jnp.where(step_a == step_b, 1, 0)

                def needs(h, count):
                    new_a = jnp.bitwise_and(jnp.right_shift(word_a, h), 1)
                    new_b = jnp.bitwise_and(jnp.right_shift(word_b, h), 1)
                    had_a = jnp.bitwise_and(jnp.right_shift(count, step_a), 15)
                    had_b = jnp.bitwise_and(jnp.right_shift(count, step_b), 15) + jnp.bitwise_and(new_a, same)
                    return new_a, new_b, had_a, had_b

                best = jnp.int32(worst)
                for h in range(groups):
                    new_a, new_b, had_a, had_b = needs(h, filled[h])
                    need = jnp.maximum(jnp.where(new_a > 0, had_a + 1, 0), jnp.where(new_b > 0, had_b + 1, 0))
                    up = jnp.bitwise_and(jnp.right_shift(filled[h], 16), 15)
                    down = jnp.right_shift(filled[h], 20)
                    taken = jnp.minimum(up, down)
                    side = jnp.where(down < up, 32 + (h << 6), h << 6)
                    cost = jnp.left_shift(2 * (new_a + new_b) + need + taken, 8) + (side + taken)
                    best = jnp.minimum(best, jnp.where((taken < limit) & (need <= cap), cost, worst))
                good = best < worst
                flag = jnp.where(good, 1, 0)
                column = jnp.bitwise_and(jnp.right_shift(best, 6), 3)
                side = jnp.bitwise_and(jnp.right_shift(best, 5), 1)
                slot = jnp.bitwise_and(best, 31)
                count = filled[0]
                for h in range(1, groups):
                    count = jnp.where(column == h, filled[h], count)
                new_a, new_b, had_a, had_b = needs(column, count)
                grown = jnp.left_shift(new_a, step_a) + jnp.left_shift(new_b, step_b)
                grown = jnp.where(good, count + grown + jnp.left_shift(1, 16 + 4 * side), count)
                masks[a] = word_a - jnp.where(good, jnp.left_shift(new_a, column), 0)
                masks[b] = word_b - jnp.where(good, jnp.left_shift(new_b, column), 0)
                here = good & (column == me)
                mine[jnp.where(here, side * half + slot, each)] = code
                for orbit, step, new, had in ((a, step_a, new_a, had_a), (b, step_b, new_b, had_b)):
                    group = jnp.right_shift(step, 2)
                    at = (jnp.bitwise_xor(group, column) - 1) * cap + had
                    spots[jnp.where(here & (new > 0), orbit, orbits)] = local + at
                    links[jnp.where(good & (new > 0) & (group == me), at, spare)] = orbit - group * local
                kept = tuple(jnp.where(column == h, grown, filled[h]) for h in range(groups))
                return kept + (jnp.bitwise_or(bad, 1 - flag),)

            state = lax.fori_loop(0, size, deal, state)
        for h in range(groups):
            counts[h] = state[h]
        fits[0] = 1 - state[groups]

    def attempt(turn, unused):
        @pl.when(fits[0] == 0)
        def go():
            trial(turn)

        return unused

    lax.fori_loop(0, TRIALS, attempt, 0)

    @pl.when(fits[0] > 0)
    def settle():
        def fill(at, unused):
            code = mine[at]
            a, b = unpack(code)
            dx = jnp.right_shift(code, 20) - B
            spot_a, spot_b = spots[a], spots[b]
            rising = at < half
            second = jnp.where(rising, dx, -dx) >= 0
            shift = jnp.where(second, dx, -dx)
            tbl[0, at] = jnp.where(second, spot_b, spot_a)
            tbl[1, at] = jnp.where(second, spot_a, spot_b)
            tbl[2, at] = jnp.where(rising, 4 * planes, 0) - shift
            tbl[3, at] = jnp.where(second, 1, 0)
            tbl[4, at] = anchors[1, b] - anchors[1, a]
            tbl[5, at] = anchors[2, b] - anchors[2, a]
            tbl[6, at] = jnp.where(second, 0, shift)
            tbl[7, at] = jnp.where(rising, 0, 4 * planes) + shift
            return unused

        lax.fori_loop(0, each, fill, 0, unroll=2)
        for row, base in ((1, 0), (0, each)):
            def link(slot, unused, row=row, base=base):
                at = final + tbl[row, slot]
                tbl[9 - row, slot] = links[at]
                links[at] = base + slot
                return unused

            lax.fori_loop(0, each, link, 0)
        for turn in range(1, groups):
            def hook(i, unused, turn=turn):
                at = (turn - 1) * cap + i
                end = ends + links[at]
                links[prior + at] = links[end]
                links[end] = at
                return unused

            sent = jnp.bitwise_and(jnp.right_shift(counts[jnp.bitwise_xor(me, turn)], 4 * me), 15)
            lax.fori_loop(0, sent, hook, 0)


def make_plan(anchors, pair_slots, cap, each, planes):
    orbits = anchors.shape[0]
    entries = pair_slots.shape[0] * pair_slots.shape[1]
    smem = pl.BlockSpec(memory_space=pltpu.SMEM)
    local = orbits // 4
    me = jnp.full((1,), lax.axis_index("grp"), jnp.int32)
    return pl.pallas_call(
        functools.partial(plan_kernel, cap, planes),
        in_specs=[smem] * 3,
        out_specs=[smem] * 3,
        out_shape=[
            jax.ShapeDtypeStruct((10, each), jnp.int32),
            jax.ShapeDtypeStruct((9 * cap + 2 * local + 1,), jnp.int32),
            jax.ShapeDtypeStruct((1,), jnp.int32),
        ],
        scratch_shapes=[
            pltpu.SMEM((orbits + 1,), jnp.int32), pltpu.SMEM((orbits,), jnp.int32),
            pltpu.SMEM((4 * entries + 1,), jnp.int32), pltpu.SMEM((each + 1,), jnp.int32),
            pltpu.SMEM((4,), jnp.int32),
        ],
        name="plan",
    )(me, anchors.T, jnp.transpose(pair_slots, (1, 2, 0)))


def coupled(plane):
    shape = plane.shape
    lane = lane_ids(shape)
    row = lax.broadcasted_iota(jnp.int32, shape, 0)
    lower_z = jnp.where(jnp.bitwise_and(lane, B - 1) > 0, pltpu.roll(plane, 1, 1), 0.0)
    half = pltpu.roll(plane, B, 1)
    down = jnp.where(row > 0, pltpu.roll(half, 1, 0), 0.0)
    return 3.0 * plane - lower_z - jnp.where(lane < B, down, half)


def lean_kernel(chips, cap, tbl, links, orb, out, *scratch):
    count = out.shape[2]
    raws, owns, parcels, pools, wins, wins_back, chains, parcels_back, backs, tallied = [
        scratch[i * count : (i + 1) * count] for i in range(10)
    ]
    partner, wide, one, two, staying, held, sums, gathered, weights = scratch[10 * count : 10 * count + 9]
    (own_sem, xy_send, xy_recv, z_send, z_recv, yx_send, yx_recv, zb_send, zb_recv,
     h_send, h_recv, s_send, s_recv) = scratch[10 * count + 9 :]
    grp, place, across, along, corner = spot()
    core = lax.rem(place, 2)
    places = 2 * chips
    tiles, planes = orb.shape[:2]
    deep = orb.shape[4]
    norb = tiles * deep
    slots = partner.shape[0]
    half = slots // 2
    first, last = HALO, HALO + planes - 1
    each = slots // WAVES
    marks = (half // 4, half // 2, 3 * half // 4)
    relay = Relay(wins, z_send, z_recv, (1, -1), chips, marks)
    relay_back = Relay(wins_back, zb_send, zb_recv, (-1, 1), chips, marks)
    lowest, highest = place == 0, place == places - 1

    def stage(chunk):
        return pltpu.make_async_copy(orb.at[:, :, chunk], raws[chunk], own_sem.at[chunk])

    for chunk in range(count):
        stage(chunk).start()
    barrier = pltpu.get_barrier_semaphore()
    for step in range(1, places):
        pl.semaphore_signal(
            barrier, inc=1, device_id=(grp, lax.rem(place + step, places)), device_id_type=MESH
        )
    for target in (across, along, corner):
        pl.semaphore_signal(barrier, inc=1, device_id=(target, place), device_id_type=MESH)

    def parcel(chunk, kind):
        return remote(
            parcels[chunk].at[pl.ds(kind * cap, cap)], pools[chunk].at[pl.ds(norb + kind * cap, cap)],
            xy_send.at[chunk, kind], xy_recv.at[chunk, kind], ((across, along, corner)[kind], place),
        )

    def pack(chunk):
        stage(chunk).wait()

        def untile(plane, unused):
            for tile in range(tiles):
                for row in range(deep):
                    piece = raws[chunk][tile, plane, :, row, :]
                    owns[chunk][tile * deep + row, plane] = piece
                    pools[chunk][tile * deep + row, plane] = piece
            return unused

        lax.fori_loop(0, planes, untile, 0)

        def put(i, unused):
            parcels[chunk][i] = owns[chunk][links[i]]
            return unused

        lax.fori_loop(0, 3 * cap, put, 0)

    def send(chunk):
        for kind in (2, 0, 1):
            parcel(chunk, kind).start()

    pack(0)
    pl.semaphore_wait(barrier, places + 2)
    send(0)
    pack(1)
    for chunk in range(2, count):
        pack(chunk)
        send(chunk - 1)
    send(count - 1)
    relay.clear()
    relay_back.clear()
    blank = jnp.zeros((HALO, ROWS, LANES), jnp.float32)

    def clear(slot, unused):
        for e in (0, 1, last + 3):
            one[slot, e] = blank[0]
        return unused

    lax.fori_loop(0, slots, clear, 0)

    @pl.when(lowest)
    def no_below():
        def fill(slot, unused):
            wide[slot, pl.ds(0, HALO)] = blank
            return unused

        lax.fori_loop(0, slots, fill, 0)

    @pl.when(highest)
    def no_above():
        def fill(slot, unused):
            wide[slot, pl.ds(HALO + planes, HALO)] = blank
            return unused

        lax.fori_loop(0, slots, fill, 0)

    for step in range(count + 1):
        if step < count:
            for kind in range(3):
                parcel(step, kind).wait_recv()
            for side in range(2):
                start = relay.offset(relay.signs[side], 0) + planes * core

                def pick(slot, unused, start=start, chunk=step):
                    wins[chunk][slot, pl.ds(start, planes)] = pools[chunk][tbl[0, slot]]
                    return unused

                lax.fori_loop(side * half, (side + 1) * half, pick, 0)
            relay.begin(step)
        if step > 0:
            relay.second(step - 1)
            relay.settle(step - 1)
        if step < count:
            relay.first(step)
            relay.share(step)

    def couple_of(slot, x):
        at = tbl[2, slot] + planes * core + x
        held_at = tbl[1, slot]
        left = jnp.concatenate([win[slot, at] for win in wins], axis=0)
        right = jnp.concatenate([pool[held_at, x] for pool in pools], axis=0)
        return left, right

    def rise(wave):
        return remote(
            wide.at[pl.ds(wave * each, each), pl.ds(last - HALO + 2, HALO - 1)],
            wide.at[pl.ds(wave * each, each), pl.ds(1, HALO - 1)],
            h_send.at[wave, 0], h_recv.at[wave, 0], (grp, lax.rem(place + 1, places)),
        )

    def sink(wave):
        return remote(
            wide.at[pl.ds(wave * each, each), pl.ds(first, HALO)],
            wide.at[pl.ds(wave * each, each), pl.ds(last + 1, HALO)],
            h_send.at[wave, 1], h_recv.at[wave, 1], (grp, lax.rem(place + places - 1, places)),
        )

    def edges(wave):
        @pl.when(jnp.logical_not(highest))
        def send_up():
            rise(wave).start()

        @pl.when(jnp.logical_not(lowest))
        def send_down():
            sink(wave).start()

    def make(slot, unused):
        second = tbl[3, slot] > 0
        dy, dz = tbl[4, slot], tbl[5, slot]
        for x in range(planes):
            left, right = couple_of(slot, x)
            other = shift_plane(jnp.where(second, left, right), dy, dz)
            wide[slot, x + HALO] = jnp.where(second, right, left) * other
            partner[slot, x] = other
        return unused

    none = jnp.zeros((8, LANES), jnp.float32)
    lane = lax.broadcasted_iota(jnp.int32, (1, LANES), 1)

    def row_of(parts):
        row = jnp.zeros((1, LANES), jnp.float32)
        for at, part in parts:
            row = row + jnp.where(lane == at, total(part), 0.0)
        return row

    def live(slot, e):
        x = planes * place + e - HALO
        low = tbl[6, slot]
        return jnp.where((x >= low) & (x < low + B), 1.0, 0.0).astype(jnp.float32)

    def raise_one(slot, e, acc):
        source = wide[slot, e]
        value = live(slot, e) * (inner(source) - (wide[slot, e - 1] + wide[slot, e + 1]))
        one[slot, e] = value
        if first <= e <= last:
            acc[1] = acc[1] + fold(source * value)
            acc[2] = acc[2] + fold(value * value)

    def raise_two(slot, e):
        source = one[slot, e]
        two[slot, e] = live(slot, e) * (inner(source) - (one[slot, e - 1] + one[slot, e + 1]))

    def measure_two(slot, e, acc, below):
        value = two[slot, e]
        acc[3] = acc[3] + fold(one[slot, e] * value)
        acc[4] = acc[4] + fold(value * value)
        bent = coupled(value)
        acc[5] = acc[5] + fold(value * (bent - two[slot, e - 1] if below else bent))

    def work_inside(slot, unused):
        acc = [none] * 6
        for e in range(first, last + 1):
            source = wide[slot, e]
            acc[0] = acc[0] + fold(source * source)
        for e in range(first + 1, last):
            raise_one(slot, e, acc)
        for e in range(first + 2, last - 1):
            raise_two(slot, e)
            measure_two(slot, e, acc, e > first + 2)
        for at in range(6):
            held[slot, at] = acc[at]
        return unused

    def work_edges(slot, unused):
        acc = [held[slot, at] for at in range(6)]
        for e in (first - 1, first, last, last + 1, last + 2):
            raise_one(slot, e, acc)
        for e in (first, first + 1, last - 1, last, last + 1):
            raise_two(slot, e)
        for e in (first, first + 1, last - 1, last):
            measure_two(slot, e, acc, e > first)
        acc[5] = acc[5] - fold(two[slot, first + 2] * two[slot, first + 1])
        acc[5] = acc[5] - fold(two[slot, last + 1] * two[slot, last])
        acc[5] = 2.0 * acc[5]
        sums[pl.ds(slot, 1)] = row_of(enumerate(acc))
        return unused

    def rim(slot, planes_one, planes_two, spots, pairs):
        spare = [none] * 6
        for e in planes_one:
            raise_one(slot, e, spare)
        for e in planes_two:
            raise_two(slot, e)
        acc = [held[slot, at] for at in range(6)]
        for e in spots:
            value, before = two[slot, e], one[slot, e]
            acc[2] = acc[2] + fold(before * before)
            acc[3] = acc[3] + fold(before * value)
            acc[4] = acc[4] + fold(value * value)
            acc[5] = acc[5] + fold(value * coupled(value))
        for e in pairs:
            acc[5] = acc[5] - fold(two[slot, e] * two[slot, e + 1])
        for at in range(2, 6):
            held[slot, at] = acc[at]

    lax.fori_loop(0, each, make, 0)
    for wave in range(1, WAVES):
        lax.fori_loop(wave * each, (wave + 1) * each, make, 0)
        edges(wave - 1)
    edges(WAVES - 1)
    lax.fori_loop(0, slots, work_inside, 0)

    @pl.when(lowest)
    def rim_below():
        def go(slot, unused):
            low = first - 2
            rim(slot, (low + 1, low + 2), (low, low + 1, low + 2), (low, low + 1), (low, low + 1))
            return unused

        lax.fori_loop(0, slots, go, 0)

    @pl.when(highest)
    def rim_above():
        def go(slot, unused):
            high = last + 2
            rim(slot, (high - 2, high - 1, high), (high - 1, high), (high - 1, high), (high - 1,))
            return unused

        lax.fori_loop(0, slots, go, 0)

    for wave in range(WAVES):
        @pl.when(jnp.logical_not(lowest))
        def got_below(wave=wave):
            rise(wave).wait_recv()

        @pl.when(jnp.logical_not(highest))
        def got_above(wave=wave):
            sink(wave).wait_recv()

        lax.fori_loop(wave * each, (wave + 1) * each, work_edges, 0)

    def tell(step, at):
        return remote(
            sums, gathered.at[at], s_send.at[step - 1], s_recv.at[step - 1],
            (grp, lax.rem(place + step, places)),
        )

    for step in range(1, places):
        tell(step, place).start()
    gathered[place] = sums[...]
    for step in range(1, places):
        tell(step, lax.rem(place + places - step, places)).wait_recv()
    whole = gathered[0]
    for at in range(1, places):
        whole = whole + gathered[at]
    lanes = lax.broadcasted_iota(jnp.int32, whole.shape, 1)
    moments = [jnp.sum(jnp.where(lanes == at, whole, 0.0), axis=1, keepdims=True) for at in range(6)]
    for at, weight in enumerate(krylov_weights(moments)):
        weights[at] = jnp.broadcast_to(weight, whole.shape)

    for side in range(2):
        start = relay_back.offset(relay_back.signs[side], 0) + planes * core

        def finish(slot, unused, start=start):
            second = tbl[3, slot] > 0
            dy, dz = tbl[4, slot], tbl[5, slot]
            w0, w1, w2 = [weights[at, pl.ds(slot, 1)] for at in range(3)]
            for x in range(planes):
                e = x + HALO
                found = w0 * wide[slot, e] + w1 * one[slot, e] + w2 * two[slot, e]
                left, right = couple_of(slot, x)
                term_a = found * partner[slot, x]
                term_b = shift_plane(found * jnp.where(second, right, left), -dy, -dz)
                going = jnp.where(second, term_b, term_a)
                stays = jnp.where(second, term_a, term_b)
                for chunk in range(count):
                    wins_back[chunk][slot, start + x] = going[chunk * SUB : (chunk + 1) * SUB]
                    staying[chunk, slot, x] = stays[chunk * SUB : (chunk + 1) * SUB]
            return unused

        lax.fori_loop(side * half, (side + 1) * half, finish, 0)
        relay_back.begin(0, (side,))

    extra = 3 * cap
    final = extra
    prior = final + norb + extra
    ends = prior + extra

    def reply(chunk, kind):
        return remote(
            parcels_back[chunk].at[pl.ds(kind * cap, cap)], backs[chunk].at[pl.ds(kind * cap, cap)],
            yx_send.at[chunk, kind], yx_recv.at[chunk, kind], ((across, along, corner)[kind], place),
        )

    for step in range(count + 2):
        chunk = step - 1
        if 0 <= chunk < count:
            relay_back.second(chunk)
            relay_back.settle(chunk)
            chain = chains[chunk]
            chain[2 * slots] = jnp.zeros(chain.shape[1:], jnp.float32)

            def link_fixed(slot, unused, chain=chain, chunk=chunk):
                chain[slot] = staying[chunk, slot] + chain[tbl[8, slot]]
                return unused

            def link_moved(slot, unused, chain=chain, chunk=chunk):
                at = tbl[7, slot] + planes * core
                for plane in range(planes):
                    chain[slots + slot, plane] = wins_back[chunk][slot, at + plane] + chain[tbl[9, slot], plane]
                return unused

            lax.fori_loop(0, slots, link_fixed, 0)
            lax.fori_loop(0, slots, link_moved, 0)

            def wrap(i, unused, chain=chain, chunk=chunk):
                parcels_back[chunk][i] = chain[links[final + norb + i]]
                return unused

            lax.fori_loop(0, extra, wrap, 0)
            for kind in (2, 0, 1):
                reply(chunk, kind).start()
        if step < count:
            relay_back.first(step)
            if step + 1 < count:
                relay_back.begin(step + 1)
            relay_back.share(step)
        chunk = step - 2
        if 0 <= chunk < count:
            total_of = tallied[chunk]
            total_of[extra] = jnp.zeros(total_of.shape[1:], jnp.float32)
            for kind in range(3):
                reply(chunk, kind).wait_recv()

            def gather(i, unused, total_of=total_of, chunk=chunk):
                total_of[i] = backs[chunk][i] + total_of[links[prior + i]]
                return unused

            lax.fori_loop(0, extra, gather, 0)

            for orbit in range(norb):
                found = total_of[links[ends + orbit]] + chains[chunk][links[final + orbit]]
                for plane in range(planes):
                    out[orbit // deep, plane, chunk, :, orbit % deep, :] = found[plane]
    for chunk in range(count):
        for kind in range(3):
            parcel(chunk, kind).wait_send()
            reply(chunk, kind).wait_send()
    for wave in range(WAVES):
        @pl.when(jnp.logical_not(highest))
        def sent_up(wave=wave):
            rise(wave).wait_send()

        @pl.when(jnp.logical_not(lowest))
        def sent_down(wave=wave):
            sink(wave).wait_send()

    for step in range(1, places):
        tell(step, place).wait_send()
    relay.drain()
    relay_back.drain()


def run_lean(table, links, tiled, slots, chips, cap):
    tiles, planes, chunks, unused, deep, lanes = tiled.shape
    norb, rows = tiles * deep, chunks * SUB
    places = 2 * chips
    smem = pl.BlockSpec(memory_space=pltpu.SMEM)
    dma = pltpu.SemaphoreType.DMA

    def room(count, deep=planes):
        return [pltpu.VMEM((count, deep, SUB, lanes), jnp.float32)] * chunks

    tall = pltpu.VMEM((slots, planes + 2 * HALO, rows, lanes), jnp.float32)
    xy, z = dma((chunks, 3)), dma((chunks, 2, 6))
    return pl.pallas_call(
        functools.partial(lean_kernel, chips, cap),
        in_specs=[smem, smem, pl.BlockSpec(memory_space=pl.ANY)],
        out_specs=pl.BlockSpec(memory_space=pltpu.VMEM),
        out_shape=jax.ShapeDtypeStruct(tiled.shape, jnp.float32),
        scratch_shapes=[pltpu.VMEM((tiles, planes, SUB, deep, lanes), jnp.float32)] * chunks
        + room(norb) + room(3 * cap) + room(norb + 3 * cap) + room(slots, 6 * planes)
        + room(slots, 6 * planes) + room(2 * slots + 1) + room(3 * cap) + room(3 * cap) + room(3 * cap + 1)
        + [
            pltpu.VMEM((slots, planes, rows, lanes), jnp.float32), tall, tall, tall,
            pltpu.VMEM((chunks, slots, planes, SUB, lanes), jnp.float32),
            pltpu.VMEM((slots, 6, 8, lanes), jnp.float32),
            pltpu.VMEM((slots, lanes), jnp.float32),
            pltpu.VMEM((places, slots, lanes), jnp.float32),
            pltpu.VMEM((3, slots, lanes), jnp.float32),
            dma((chunks,)), xy, xy, z, z, xy, xy, z, z,
            dma((WAVES, 2)), dma((WAVES, 2)), dma((places - 1,)), dma((places - 1,)),
        ],
        compiler_params=pltpu.CompilerParams(
            collective_id=3, has_side_effects=True, vmem_limit_bytes=60 * 1024 * 1024
        ),
        name="lean",
    )(table, links, tiled)


def full_tables(anchors, pair_slots, planes, groups, each):
    assignment = deal_evenly(pair_slots, groups, each)
    pairs = assignment[lax.axis_index("grp")]
    offsets = anchors[pairs[:, 1]] - anchors[pairs[:, 0]]
    dx, dy, dz = offsets[:, 0], offsets[:, 1], offsets[:, 2]
    slot = lax.broadcasted_iota(jnp.int32, (each,), 0)
    rising = slot < each // 2
    second = jnp.where(rising, dx >= 0, dx <= 0)
    shift = jnp.where(second, dx, -dx)
    moved_id = jnp.where(second, pairs[:, 1], pairs[:, 0])
    fixed_id = jnp.where(second, pairs[:, 0], pairs[:, 1])
    terms = jnp.concatenate([fixed_id, moved_id])
    at = lax.broadcasted_iota(jnp.int32, (2 * each, 2 * each), 0)
    before = lax.broadcasted_iota(jnp.int32, (2 * each, 2 * each), 1)
    found = jnp.where((terms[:, None] == terms[None, :]) & (before < at), before, -1)
    prior = jnp.max(found, axis=1)
    prior = jnp.where(prior < 0, 2 * each, prior)
    norb = anchors.shape[0]
    orbit = lax.broadcasted_iota(jnp.int32, (norb, 2 * each), 0)
    index = lax.broadcasted_iota(jnp.int32, (norb, 2 * each), 1)
    last = jnp.max(jnp.where(terms[None, :] == orbit, index, -1), axis=1)
    last = jnp.where(last < 0, 2 * each, last)
    table = jnp.stack([
        moved_id, fixed_id,
        jnp.where(rising, 4 * planes, 0) - shift,
        second.astype(jnp.int32), dy, dz,
        jnp.where(second, 0, shift),
        jnp.where(rising, 0, 4 * planes) + shift,
        prior[:each], prior[each:],
    ])
    return table, last


def slab_body(orbitals, anchors, pair_slots):
    groups, places = lax.axis_size("grp"), lax.axis_size("grid")
    norb_local, cells = orbitals.shape
    planes = cells // (B * B)
    each = PAIR_DEV * places
    chips = places // 2
    cap = 5 * norb_local // 16
    plan, links, fits = make_plan(anchors, pair_slots, cap, each, planes)
    deep = math.gcd(norb_local, 8)

    def lean(orbitals, anchors, pair_slots, plan, links):
        tiled = orbitals.reshape(norb_local // deep, deep, planes, ROWS // SUB, SUB, LANES)
        out = run_lean(plan, links, jnp.transpose(tiled, (0, 2, 3, 4, 1, 5)), each, chips, cap)
        return jnp.transpose(out, (0, 4, 1, 2, 3, 5)).reshape(norb_local, cells)

    def full(orbitals, anchors, pair_slots, plan, links):
        stacked = orbitals.reshape(norb_local, planes, ROWS, LANES)
        table, last = full_tables(anchors, pair_slots, planes, groups, each)
        moved, fixed = bring(table, stacked, each, groups, chips)
        dens, partner = pair_up(table, moved, fixed)
        pot = solve_slabs(table, dens, places, 5)
        going, staying = make_terms(table, pot, partner, moved, fixed)
        out = hand_back(table, last, going, staying, norb_local, chips)
        return out.reshape(norb_local, cells)

    return lax.cond(fits[0] > 0, lean, full, orbitals, anchors, pair_slots, plan, links)


def slabs_fit(mesh):
    groups, places = mesh.shape["grp"], mesh.shape["grid"]
    return groups == 4 and places % 2 == 0 and 4 * (B // places) >= PAD


def solution(mesh):
    return jax.shard_map(
        slab_body if slabs_fit(mesh) else owner_body,
        mesh=mesh,
        in_specs=(P("grp", "grid"), P(), P()),
        out_specs=P("grp", "grid"),
        check_vma=False,
    )
```

```python
import functools
import math

import jax
import jax.numpy as jnp
from jax import lax
from jax.experimental import pallas as pl
from jax.experimental.pallas import tpu as pltpu
from jax.sharding import PartitionSpec as P

B = 64
PAIR_DEV = 2
ITERS = 3
MOST_CHUNKS = 2
LANES = 128
ROWS = B * B // LANES
PAD = 32
STEP = 4


def deal_evenly(pair_slots, owner_count, each_owner):
    flat_slots = pair_slots.reshape(-1, 2)
    filled = (flat_slots[:, 0] >= 0).astype(jnp.int32)
    position = jnp.cumsum(filled, dtype=jnp.int32) - filled
    wanted = lax.broadcasted_iota(jnp.int32, (owner_count, each_owner), 1) * owner_count
    wanted = (wanted + lax.broadcasted_iota(jnp.int32, (owner_count, each_owner), 0)).reshape(-1)
    matched = (position[None, :] == wanted[:, None]) & (filled[None, :] == 1)
    picked = jnp.sum(jnp.where(matched[:, :, None], flat_slots[None], 0), axis=1)
    return picked.reshape(owner_count, each_owner, 2)


def gather_kernel(ids_ref, src_ref, *out_refs):
    count, terms = out_refs[0].shape[:2]
    for slot, out_ref in enumerate(out_refs):
        def pick(dest, unused, slot=slot, out_ref=out_ref):
            for term in range(terms):
                out_ref[dest, term] = src_ref[ids_ref[(slot * count + dest) * terms + term]]
            return unused

        lax.fori_loop(0, count, pick, 0)


def gather_pieces(ids, pieces, slots, count):
    norb, rows, lanes = pieces.shape
    block = max(8, rows // 4)
    return pl.pallas_call(
        gather_kernel,
        grid_spec=pltpu.PrefetchScalarGridSpec(
            num_scalar_prefetch=1,
            grid=(rows // block,),
            in_specs=[pl.BlockSpec((norb, block, lanes), lambda i, ids: (0, i, 0))],
            out_specs=[pl.BlockSpec((count, 2, block, lanes), lambda i, ids: (0, 0, i, 0))] * slots,
        ),
        out_shape=[jax.ShapeDtypeStruct((count, 2, rows, lanes), jnp.float32)] * slots,
        cost_estimate=pl.CostEstimate(flops=0, bytes_accessed=8 * norb * rows * lanes, transcendentals=0),
        name="pick_pieces",
    )(ids, pieces)


def scatter_kernel(ids_ref, *refs):
    out_ref = refs[-1]
    out_ref[...] = jnp.zeros_like(out_ref)
    count, terms = refs[0].shape[:2]
    for slot, in_ref in enumerate(refs[:-1]):
        def add(dest, unused, slot=slot, in_ref=in_ref):
            for term in range(terms):
                orbit = ids_ref[(slot * count + dest) * terms + term]
                out_ref[orbit] = out_ref[orbit] + in_ref[dest, term]
            return unused

        lax.fori_loop(0, count, add, 0)


def scatter_pieces(ids, parts, norb):
    count, terms, rows, lanes = parts[0].shape
    block = max(8, rows // 4)
    return pl.pallas_call(
        scatter_kernel,
        grid_spec=pltpu.PrefetchScalarGridSpec(
            num_scalar_prefetch=1,
            grid=(rows // block,),
            in_specs=[pl.BlockSpec((count, terms, block, lanes), lambda i, ids: (0, 0, i, 0))] * len(parts),
            out_specs=pl.BlockSpec((norb, block, lanes), lambda i, ids: (0, i, 0)),
        ),
        out_shape=jax.ShapeDtypeStruct((norb, rows, lanes), jnp.float32),
        cost_estimate=pl.CostEstimate(flops=0, bytes_accessed=8 * norb * rows * lanes, transcendentals=0),
        name="add_pieces",
    )(ids, *parts)


def lane_ids(shape):
    return lax.broadcasted_iota(jnp.int32, shape, len(shape) - 1)


def shift_plane(plane, off_y, off_z):
    shape = plane.shape
    lane = lane_ids(shape)
    row = lax.broadcasted_iota(jnp.int32, shape, 0)
    linear = off_y * B + off_z
    across = jnp.bitwise_and(linear, LANES - 1)
    down = jnp.right_shift(linear, 7)
    turned = pltpu.roll(plane, across, 1)
    near = pltpu.roll(turned, jnp.bitwise_and(down, ROWS - 1), 0)
    far = pltpu.roll(turned, jnp.bitwise_and(down + 1, ROWS - 1), 0)
    moved = jnp.where(lane >= across, near, far)
    from_y = row * 2 + jnp.right_shift(lane, 6) - off_y
    from_z = jnp.bitwise_and(lane, B - 1) - off_z
    inside = (from_y >= 0) & (from_y < B) & (from_z >= 0) & (from_z < B)
    return jnp.where(inside, moved, 0.0)


def operate_plane(before, plane, after):
    shape = plane.shape
    lane = lane_ids(shape)
    row = lax.broadcasted_iota(jnp.int32, shape, 0)
    z = jnp.bitwise_and(lane, B - 1)
    upper_z = jnp.where(z < B - 1, pltpu.roll(plane, LANES - 1, 1), 0.0)
    lower_z = jnp.where(z > 0, pltpu.roll(plane, 1, 1), 0.0)
    half = pltpu.roll(plane, B, 1)
    down = jnp.where(row > 0, pltpu.roll(half, 1, 0), 0.0)
    up = jnp.where(row < ROWS - 1, pltpu.roll(half, ROWS - 1, 0), 0.0)
    beside = (before + after) + (half + jnp.where(lane < B, down, up))
    return 6.0 * plane - beside - upper_z - lower_z


def fold(values):
    return jnp.sum(values.reshape(ROWS // 8, 8, LANES), axis=0)


def total(acc):
    return jnp.sum(acc, axis=(0, 1), keepdims=True)


def solve_kernel(info_ref, *refs):
    chunks = (len(refs) - 6) // 2
    in_refs, out_refs = refs[:chunks], refs[chunks : 2 * chunks]
    wide, partner, direction, resid, image, potential = refs[2 * chunks :]
    count, terms, rows, lanes = in_refs[0].shape
    each = rows // ROWS
    dx, dy, dz = info_ref[0], info_ref[1], info_ref[2]
    keep = jnp.where(info_ref[3] > 0, 1.0, 0.0).astype(jnp.float32)
    edge = jnp.zeros((PAD, ROWS, LANES), jnp.float32)
    wide[pl.ds(0, PAD)] = edge
    wide[pl.ds(PAD + B, PAD)] = edge
    direction[0] = edge[0]
    direction[B + 1] = edge[0]
    none = jnp.zeros((8, LANES), jnp.float32)

    def place(owner, chunk, i):
        return (owner * chunks + chunk) * each + i

    def load(owner, unused):
        for chunk in range(chunks):
            for i in range(each):
                wide[PAD + place(owner, chunk, i)] = in_refs[chunk][owner, 1, pl.ds(i * ROWS, ROWS)]
        return unused

    lax.fori_loop(0, count, load, 0)

    def start(owner, acc):
        for chunk in range(chunks):
            for i in range(each):
                x = place(owner, chunk, i)
                other = shift_plane(wide[PAD + x - dx], dy, dz)
                partner[x] = other
                density = in_refs[chunk][owner, 0, pl.ds(i * ROWS, ROWS)] * other
                direction[x + 1] = density
                resid[x] = density
                acc = acc + fold(density * density)
        return acc

    norm_now = total(lax.fori_loop(0, count, start, none))

    for turn in range(ITERS):
        def apply(block, acc):
            for i in range(STEP):
                x = block * STEP + i
                plane = direction[x + 1]
                result = operate_plane(direction[x], plane, direction[x + 2])
                image[x] = result
                acc = acc + fold(plane * result)
            return acc

        step_len = norm_now / total(lax.fori_loop(0, B // STEP, apply, none))

        if turn == ITERS - 1:
            break

        def advance(block, acc):
            for i in range(STEP):
                x = block * STEP + i
                moved = step_len * direction[x + 1]
                potential[x] = moved if turn == 0 else potential[x] + moved
                left = resid[x] - step_len * image[x]
                resid[x] = left
                acc = acc + fold(left * left)
            return acc

        norm_next = total(lax.fori_loop(0, B // STEP, advance, none))
        ratio = norm_next / norm_now

        def renew(block, unused):
            for i in range(STEP):
                x = block * STEP + i
                direction[x + 1] = resid[x] + ratio * direction[x + 1]
            return unused

        lax.fori_loop(0, B // STEP, renew, 0)
        norm_now = norm_next

    def finish(owner, unused):
        for chunk in range(chunks):
            for i in range(each):
                x = place(owner, chunk, i)
                found = (potential[x] + step_len * direction[x + 1]) * keep
                out_refs[chunk][owner, 0, pl.ds(i * ROWS, ROWS)] = found * partner[x]
                wide[PAD + x] = found * in_refs[chunk][owner, 0, pl.ds(i * ROWS, ROWS)]
        return unused

    lax.fori_loop(0, count, finish, 0)

    def give_back(owner, unused):
        for chunk in range(chunks):
            for i in range(each):
                x = place(owner, chunk, i)
                out_refs[chunk][owner, 1, pl.ds(i * ROWS, ROWS)] = shift_plane(wide[PAD + x + dx], -dy, -dz)
        return unused

    lax.fori_loop(0, count, give_back, 0)


def solve_pair(info, parts):
    box = (B, ROWS, LANES)
    vmem = pl.BlockSpec(memory_space=pltpu.VMEM)
    return pl.pallas_call(
        solve_kernel,
        in_specs=[pl.BlockSpec(memory_space=pltpu.SMEM)] + [vmem] * len(parts),
        out_specs=[vmem] * len(parts),
        out_shape=[jax.ShapeDtypeStruct(p.shape, jnp.float32) for p in parts],
        scratch_shapes=[
            pltpu.VMEM((B + 2 * PAD, ROWS, LANES), jnp.float32),
            pltpu.VMEM(box, jnp.float32),
            pltpu.VMEM((B + 2, ROWS, LANES), jnp.float32),
            pltpu.VMEM(box, jnp.float32),
            pltpu.VMEM(box, jnp.float32),
            pltpu.VMEM(box, jnp.float32),
        ],
        compiler_params=pltpu.CompilerParams(vmem_limit_bytes=32 * 1024 * 1024),
        cost_estimate=pl.CostEstimate(flops=0, bytes_accessed=40 * 1024 * 1024, transcendentals=0),
        name="solve_pair",
    )(info, *parts)


def owner_body(orbitals, anchors, pair_slots):
    grid_count = lax.axis_size("grid")
    owner_count = lax.axis_size("grp") * grid_count
    group_idx = lax.axis_index("grp")
    place_idx = lax.axis_index("grid")
    assignment = deal_evenly(pair_slots, owner_count, PAIR_DEV)
    slots = assignment.shape[1]
    filled = assignment[..., 0] >= 0
    safe_ids = jnp.maximum(assignment, 0)
    group_table = lax.dynamic_slice_in_dim(safe_ids, group_idx * grid_count, grid_count, 0)
    ids = jnp.transpose(group_table, (1, 0, 2)).reshape(-1)
    owner_idx = group_idx * grid_count + place_idx
    own_pairs = safe_ids[owner_idx]
    offsets = anchors[own_pairs[:, 1]] - anchors[own_pairs[:, 0]]
    info = jnp.concatenate([offsets, filled[owner_idx].astype(jnp.int32)[:, None]], axis=1)

    norb_local, cells = orbitals.shape
    stacked = orbitals.reshape(norb_local, cells // LANES, LANES)
    chunks = math.gcd(MOST_CHUNKS, cells // (B * B))
    rows = stacked.shape[1] // chunks
    arrived = [[None] * chunks for _ in range(slots)]
    for chunk in range(chunks):
        pieces = lax.all_gather(stacked[:, chunk * rows : (chunk + 1) * rows], "grp", axis=0, tiled=True)
        outgoing = gather_pieces(ids, pieces, slots, grid_count)
        for slot in range(slots):
            arrived[slot][chunk] = lax.all_to_all(outgoing[slot], "grid", split_axis=0, concat_axis=0, tiled=True)
    returned = []
    for slot in range(slots):
        terms = solve_pair(info[slot], arrived[slot])
        returned.append(
            [lax.all_to_all(t, "grid", split_axis=0, concat_axis=0, tiled=True) for t in terms]
        )
    results = []
    for chunk in range(chunks):
        summed = scatter_pieces(ids, [r[chunk] for r in returned], anchors.shape[0])
        results.append(lax.psum_scatter(summed, "grp", scatter_dimension=0, tiled=True))
    return jnp.concatenate(results, axis=1).reshape(norb_local, cells)


MESH = pl.DeviceIdType.MESH
HALO = 3
WAVES = 4
TRIALS = 12
SUB = 8


def remote(src, dst, send_sem, recv_sem, device):
    return pltpu.make_async_remote_copy(
        src_ref=src, dst_ref=dst, send_sem=send_sem, recv_sem=recv_sem, device_id=device, device_id_type=MESH
    )


def spot():
    grp = lax.axis_index("grp")
    place = lax.axis_index("grid")
    across = grp + 1 - 2 * lax.rem(grp, 2)
    along = lax.rem(grp + 2, 4)
    corner = lax.rem(across + 2, 4)
    return grp, place, across, along, corner


def greet(chips, wide=False):
    grp, place, across, along, corner = spot()
    chip = place // 2
    core = lax.rem(place, 2)
    barrier = pltpu.get_barrier_semaphore()
    peers = [(across, place), (along, place), (grp, 2 * chip + 1 - core)] + ([(corner, place)] if wide else [])
    for device in peers:
        pl.semaphore_signal(barrier, inc=1, device_id=device, device_id_type=MESH)

    @pl.when(chip > 0)
    def below():
        pl.semaphore_signal(barrier, inc=1, device_id=(grp, place - 2), device_id_type=MESH)

    @pl.when(chip < chips - 1)
    def above():
        pl.semaphore_signal(barrier, inc=1, device_id=(grp, place + 2), device_id_type=MESH)

    ends = jnp.where(chip > 0, 1, 0) + jnp.where(chip < chips - 1, 1, 0)
    pl.semaphore_wait(barrier, len(peers) + ends)


class Relay:
    def __init__(self, wins, send_sem, recv_sem, signs, chips, marks):
        self.wins, self.send_sem, self.recv_sem, self.signs, self.chips = wins, send_sem, recv_sem, signs, chips
        self.grp, self.place = lax.axis_index("grp"), lax.axis_index("grid")
        self.chip = self.place // 2
        self.core = lax.rem(self.place, 2)
        self.half = wins[0].shape[0] // 2
        self.planes = wins[0].shape[1] // 6
        self.deep, self.far, self.mid = marks

    def offset(self, sign, hop):
        return 2 * self.planes * (2 - hop if sign > 0 else hop)

    def region(self, chunk, side, hop, core, size, skip=0):
        start = self.offset(self.signs[side], hop) + self.planes * core
        return self.wins[chunk].at[pl.ds(side * self.half + skip, size), pl.ds(start, self.planes)]

    def comes(self, side, hop):
        source = self.chip - self.signs[side] * hop
        return source >= 0 if self.signs[side] > 0 else source < self.chips

    def goes(self, side, hop):
        source = self.chip + self.signs[side] - self.signs[side] * hop
        if self.signs[side] > 0:
            return (self.chip + 1 < self.chips) & (source >= 0)
        return (self.chip - 1 >= 0) & (source < self.chips)

    def spans(self, side, hop, core, act):
        if hop == 0:
            act(self.half)
        else:
            near = 1 if self.signs[side] > 0 else 0
            most, least = (self.half, self.mid) if hop == 1 else (self.far, self.deep)
            if most == least:
                act(most)
                return

            @pl.when(core == near)
            def whole():
                act(most)

            @pl.when(core != near)
            def some():
                act(least)

    def onward(self, chunk, side, hop, size, here=None):
        source = self.region(chunk, side, hop - 1 if here is None else here, self.core, size)
        there = self.region(chunk, side, hop, self.core, size)
        return remote(
            source, there, self.send_sem.at[chunk, side, hop - 1], self.recv_sem.at[chunk, side, hop - 1],
            (self.grp, self.place + 2 * self.signs[side]),
        )

    def rest(self, chunk, side, act, here=0):
        def copy(size):
            source = self.region(chunk, side, here, self.core, size - self.far, self.far)
            there = self.region(chunk, side, 1, self.core, size - self.far, self.far)
            act(remote(
                source, there, self.send_sem.at[chunk, side, 5], self.recv_sem.at[chunk, side, 5],
                (self.grp, self.place + 2 * self.signs[side]),
            ))

        if self.far < self.half:
            self.spans(side, 1, self.core, copy)

    def ahead(self, side, hop, act):
        if hop == 1:
            act(self.far)
        else:
            self.spans(side, hop, self.core, act)

    def beside(self, chunk, side, hop, core, size):
        part = self.region(chunk, side, hop, core, size)
        return remote(
            part, part, self.send_sem.at[chunk, side, 2 + hop], self.recv_sem.at[chunk, side, 2 + hop],
            (self.grp, 2 * self.chip + 1 - self.core),
        )

    def clear(self):
        for side in range(2):
            for hop in (1, 2):
                start = self.offset(self.signs[side], hop)

                @pl.when(jnp.logical_not(self.comes(side, hop)))
                def fill(side=side, start=start):
                    for win in self.wins:
                        def zero(slot, unused, win=win):
                            win[slot, pl.ds(start, 2 * self.planes)] = jnp.zeros(
                                (2 * self.planes,) + win.shape[2:], jnp.float32
                            )
                            return unused

                        lax.fori_loop(side * self.half, (side + 1) * self.half, zero, 0)

    def pass_on(self, chunk, side, hop):
        @pl.when(self.goes(side, hop))
        def go():
            self.ahead(side, hop, lambda size: self.onward(chunk, side, hop, size).start())
            if hop == 1:
                self.rest(chunk, side, lambda copy: copy.start())

    def begin(self, chunk, sides=(0, 1)):
        for side in sides:
            self.pass_on(chunk, side, 1)
        for side in sides:
            self.beside(chunk, side, 0, self.core, self.half).start()

    def arrive(self, chunk, side, hop):
        @pl.when(self.comes(side, hop))
        def got():
            self.ahead(side, hop, lambda size: self.onward(chunk, side, hop, size, hop).wait_recv())

    def spread(self, chunk, side, hop):
        @pl.when(self.comes(side, hop))
        def share():
            if hop == 1:
                self.rest(chunk, side, lambda copy: copy.wait_recv(), 1)
            self.spans(side, hop, self.core, lambda size: self.beside(chunk, side, hop, self.core, size).start())

    def first(self, chunk):
        for side in range(2):
            self.arrive(chunk, side, 1)
            self.pass_on(chunk, side, 2)

    def share(self, chunk):
        for side in range(2):
            self.spread(chunk, side, 1)

    def second(self, chunk):
        for side in range(2):
            self.arrive(chunk, side, 2)
            self.spread(chunk, side, 2)

    def settle(self, chunk):
        other = 1 - self.core
        for side in range(2):
            self.beside(chunk, side, 0, other, self.half).wait_recv()
            for hop in (1, 2):
                @pl.when(self.comes(side, hop))
                def got(side=side, hop=hop):
                    self.spans(side, hop, other, lambda size: self.beside(chunk, side, hop, other, size).wait_recv())

    def drain(self):
        for chunk in range(len(self.wins)):
            for side in range(2):
                self.beside(chunk, side, 0, self.core, self.half).wait_send()
                for hop in (1, 2):
                    @pl.when(self.comes(side, hop))
                    def sent(chunk=chunk, side=side, hop=hop):
                        self.spans(
                            side, hop, self.core,
                            lambda size: self.beside(chunk, side, hop, self.core, size).wait_send(),
                        )

                    @pl.when(self.goes(side, hop))
                    def passed(chunk=chunk, side=side, hop=hop):
                        self.ahead(side, hop, lambda size: self.onward(chunk, side, hop, size).wait_send())
                        if hop == 1:
                            self.rest(chunk, side, lambda copy: copy.wait_send())


def bring_kernel(chips, tbl, orb, moved, fixed, *scratch):
    count = moved.shape[0]
    pools, wins = scratch[:count], scratch[count : 2 * count]
    own_sem, xy_send, xy_recv, z_send, z_recv = scratch[2 * count :]
    grp, place, across, along, corner = spot()
    core = lax.rem(place, 2)
    norb, planes = orb.shape[:2]
    part = norb // 2
    slots = moved.shape[1]
    relay = Relay(wins, z_send, z_recv, (1, -1), chips, (slots // 2,) * 3)

    def block(chunk, owner, start, size):
        return pools[chunk].at[pl.ds(owner * norb + start, size)]

    def stage(chunk):
        return pltpu.make_async_copy(
            orb.at[:, :, pl.ds(chunk * SUB, SUB)], block(chunk, grp, 0, norb), own_sem.at[chunk]
        )

    def hop(chunk, kind, owner, start, size, target):
        ref = block(chunk, owner, start, size)
        return remote(ref, ref, xy_send.at[chunk, kind], xy_recv.at[chunk, kind], (target, place))

    def direct(chunk, owners):
        return hop(chunk, 0, owners[0], 0, norb, across), hop(chunk, 1, owners[1], 0, norb, along)

    def turned(chunk, owners):
        return hop(chunk, 2, owners[0], 0, part, along), hop(chunk, 3, owners[1], part, part, across)

    for chunk in range(count):
        stage(chunk).start()
    greet(chips)
    relay.clear()

    def send_own(chunk):
        stage(chunk).wait()
        for copy in direct(chunk, (grp, grp)):
            copy.start()

    send_own(0)
    send_own(1)
    for step in range(count + 4):
        if step < count:
            for copy in direct(step, (across, along)):
                copy.wait_recv()
            for copy in turned(step, (across, along)):
                copy.start()
            if step + 2 < count:
                send_own(step + 2)
        chunk = step - 1
        if 0 <= chunk < count:
            for copy in turned(chunk, (corner, corner)):
                copy.wait_recv()
            for side in range(2):
                start = relay.offset(relay.signs[side], 0) + planes * core

                def pick(slot, unused, start=start, chunk=chunk):
                    wins[chunk][slot, pl.ds(start, planes)] = pools[chunk][tbl[0, slot]]
                    fixed[chunk, slot] = pools[chunk][tbl[1, slot]]
                    return unused

                lax.fori_loop(side * (slots // 2), (side + 1) * (slots // 2), pick, 0)
            relay.begin(chunk)
        chunk = step - 2
        if 0 <= chunk < count:
            relay.first(chunk)
            relay.share(chunk)
        chunk = step - 3
        if 0 <= chunk < count:
            relay.second(chunk)
        chunk = step - 4
        if 0 <= chunk < count:
            relay.settle(chunk)

            def choose(slot, unused, chunk=chunk):
                first = tbl[2, slot] + planes * core
                for plane in range(planes):
                    moved[chunk, slot, plane] = wins[chunk][slot, first + plane]
                return unused

            lax.fori_loop(0, slots, choose, 0)
    for chunk in range(count):
        for copy in direct(chunk, (grp, grp)) + turned(chunk, (across, along)):
            copy.wait_send()
    relay.drain()


def bring(table, stacked, slots, groups, chips):
    norb, planes, rows, lanes = stacked.shape
    chunks = rows // SUB
    vmem = pl.BlockSpec(memory_space=pltpu.VMEM)
    dma = pltpu.SemaphoreType.DMA
    shape = jax.ShapeDtypeStruct((chunks, slots, planes, SUB, lanes), jnp.float32)
    return pl.pallas_call(
        functools.partial(bring_kernel, chips),
        in_specs=[pl.BlockSpec(memory_space=pltpu.SMEM), pl.BlockSpec(memory_space=pl.ANY)],
        out_specs=[vmem, vmem],
        out_shape=[shape, shape],
        scratch_shapes=[pltpu.VMEM((groups * norb, planes, SUB, lanes), jnp.float32)] * chunks
        + [pltpu.VMEM((slots, 6 * planes, SUB, lanes), jnp.float32)] * chunks
        + [dma((chunks,)), dma((chunks, 4)), dma((chunks, 4)), dma((chunks, 2, 6)), dma((chunks, 2, 6))],
        compiler_params=pltpu.CompilerParams(
            collective_id=0, has_side_effects=True, vmem_limit_bytes=48 * 1024 * 1024
        ),
        name="bring",
    )(table, stacked)


def pair_kernel(tbl, moved, fixed, dens, partner):
    def go(slot, unused):
        second = tbl[3, slot] > 0
        dy, dz = tbl[4, slot], tbl[5, slot]
        for x in range(moved.shape[2]):
            left = moved[:, slot, x].reshape(ROWS, LANES)
            right = fixed[:, slot, x].reshape(ROWS, LANES)
            other = shift_plane(jnp.where(second, left, right), dy, dz)
            dens[slot, x] = jnp.where(second, right, left) * other
            partner[slot, x] = other
        return unused

    lax.fori_loop(0, moved.shape[1], go, 0)


def pair_up(table, moved, fixed):
    chunks, slots, planes, sub, lanes = moved.shape
    vmem = pl.BlockSpec(memory_space=pltpu.VMEM)
    shape = jax.ShapeDtypeStruct((slots, planes, ROWS, lanes), jnp.float32)
    return pl.pallas_call(
        pair_kernel,
        in_specs=[pl.BlockSpec(memory_space=pltpu.SMEM), vmem, vmem],
        out_specs=[vmem, vmem],
        out_shape=[shape, shape],
        compiler_params=pltpu.CompilerParams(vmem_limit_bytes=24 * 1024 * 1024),
        name="pair_up",
    )(table, moved, fixed)


def inner(plane):
    shape = plane.shape
    lane = lane_ids(shape)
    row = lax.broadcasted_iota(jnp.int32, shape, 0)
    z = jnp.bitwise_and(lane, B - 1)
    upper_z = jnp.where(z < B - 1, pltpu.roll(plane, LANES - 1, 1), 0.0)
    lower_z = jnp.where(z > 0, pltpu.roll(plane, 1, 1), 0.0)
    half = pltpu.roll(plane, B, 1)
    down = jnp.where(row > 0, pltpu.roll(half, 1, 0), 0.0)
    up = jnp.where(row < ROWS - 1, pltpu.roll(half, ROWS - 1, 0), 0.0)
    return 6.0 * plane - ((half + jnp.where(lane < B, down, up)) + (upper_z + lower_z))


def krylov_weights(m):
    a0 = m[0] / m[1]
    rr1 = a0 * a0 * m[2] - m[0]
    p, q = 1.0 + rr1 / m[0], -a0
    a1 = rr1 / (p * p * m[1] + 2.0 * p * q * m[2] + q * q * m[3])
    s1, s2 = -a0 - a1 * p, -a1 * q
    rr2 = (m[0] + s1 * s1 * m[2] + s2 * s2 * m[4]) + 2.0 * (s1 * m[1] + s2 * m[2] + s1 * s2 * m[3])
    b1 = rr2 / rr1
    e0, e1, e2 = 1.0 + b1 * p, s1 + b1 * q, s2
    bend = e0 * e0 * m[1] + e1 * e1 * m[3] + e2 * e2 * m[5]
    a2 = rr2 / (bend + 2.0 * (e0 * e1 * m[2] + e0 * e2 * m[3] + e1 * e2 * m[4]))
    return a0 + a1 * p + a2 * e0, a1 * q + a2 * e1, a2 * e2


def solve_slabs_kernel(places, tbl, dens, pot, wide, one, two, sums, gathered, weights, h_send, h_recv, s_send, s_recv):
    grp, place = lax.axis_index("grp"), lax.axis_index("grid")
    slots, planes = dens.shape[:2]
    first, last = HALO, HALO + planes - 1
    each = slots // WAVES
    barrier = pltpu.get_barrier_semaphore()
    for step in range(1, places):
        pl.semaphore_signal(
            barrier, inc=1, device_id=(grp, lax.rem(place + step, places)), device_id_type=MESH
        )
    pl.semaphore_wait(barrier, places - 1)

    def rise(wave):
        return remote(
            dens.at[pl.ds(wave * each, each), pl.ds(planes - HALO + 1, HALO - 1)],
            wide.at[pl.ds(wave * each, each), pl.ds(1, HALO - 1)],
            h_send.at[wave, 0], h_recv.at[wave, 0], (grp, lax.rem(place + 1, places)),
        )

    def sink(wave):
        return remote(
            dens.at[pl.ds(wave * each, each), pl.ds(0, HALO)],
            wide.at[pl.ds(wave * each, each), pl.ds(HALO + planes, HALO)],
            h_send.at[wave, 1], h_recv.at[wave, 1], (grp, lax.rem(place + places - 1, places)),
        )

    lowest, highest = place == 0, place == places - 1
    for wave in range(WAVES):
        @pl.when(jnp.logical_not(highest))
        def send_up(wave=wave):
            rise(wave).start()

        @pl.when(jnp.logical_not(lowest))
        def send_down(wave=wave):
            sink(wave).start()

    blank = jnp.zeros((HALO, ROWS, LANES), jnp.float32)

    def copy_in(slot, unused):
        wide[slot, pl.ds(HALO, planes)] = dens[slot]
        one[slot, 1] = blank[0]
        one[slot, last + 3] = blank[0]
        one[slot, 0] = blank[0]
        return unused

    lax.fori_loop(0, slots, copy_in, 0)

    @pl.when(lowest)
    def no_below():
        def fill(slot, unused):
            wide[slot, pl.ds(0, HALO)] = blank
            return unused

        lax.fori_loop(0, slots, fill, 0)

    @pl.when(highest)
    def no_above():
        def fill(slot, unused):
            wide[slot, pl.ds(HALO + planes, HALO)] = blank
            return unused

        lax.fori_loop(0, slots, fill, 0)

    lane = lax.broadcasted_iota(jnp.int32, (1, LANES), 1)
    none = jnp.zeros((8, LANES), jnp.float32)

    def row_of(parts):
        row = jnp.zeros((1, LANES), jnp.float32)
        for at, part in parts:
            row = row + jnp.where(lane == at, total(part), 0.0)
        return row

    def work(slot, unused):
        low, high = tbl[6, slot], tbl[6, slot] + B

        def live(e):
            x = planes * place + e - HALO
            return jnp.where((x >= low) & (x < high), 1.0, 0.0).astype(jnp.float32)

        m0, m1, m2, m3, m4, m5 = none, none, none, none, none, none
        for e in range(first - 1, last + 3):
            value = live(e) * (inner(wide[slot, e]) - (wide[slot, e - 1] + wide[slot, e + 1]))
            one[slot, e] = value
            if first <= e <= last:
                source = wide[slot, e]
                m0 = m0 + fold(source * source)
                m1 = m1 + fold(source * value)
                m2 = m2 + fold(value * value)
        bent = None
        for e in range(first, last + 2):
            value = live(e) * (inner(one[slot, e]) - (one[slot, e - 1] + one[slot, e + 1]))
            two[slot, e] = value
            if e > first:
                m5 = m5 - 2.0 * fold(value * two[slot, e - 1])
            if e <= last:
                m3 = m3 + fold(one[slot, e] * value)
                m4 = m4 + fold(value * value)
                m5 = m5 + fold(value * inner(value))
        sums[pl.ds(slot, 1)] = row_of(enumerate((m0, m1, m2, m3, m4, m5)))
        return unused

    def rim(slot, spots, pairs):
        low, high = tbl[6, slot], tbl[6, slot] + B
        m2, m3, m4, m5 = none, none, none, none
        for e, fresh in spots:
            if fresh:
                x = planes * place + e - HALO
                alive = jnp.where((x >= low) & (x < high), 1.0, 0.0).astype(jnp.float32)
                two[slot, e] = alive * (inner(one[slot, e]) - (one[slot, e - 1] + one[slot, e + 1]))
        for e, fresh in spots:
            value, before = two[slot, e], one[slot, e]
            m2 = m2 + fold(before * before)
            m3 = m3 + fold(before * value)
            m4 = m4 + fold(value * value)
            m5 = m5 + fold(value * inner(value))
        for e in pairs:
            m5 = m5 - 2.0 * fold(two[slot, e] * two[slot, e + 1])
        sums[pl.ds(slot, 1)] = sums[pl.ds(slot, 1)] + row_of(((2, m2), (3, m3), (4, m4), (5, m5)))

    for wave in range(WAVES):
        @pl.when(jnp.logical_not(lowest))
        def got_below(wave=wave):
            rise(wave).wait_recv()

        @pl.when(jnp.logical_not(highest))
        def got_above(wave=wave):
            sink(wave).wait_recv()

        lax.fori_loop(wave * each, (wave + 1) * each, work, 0)

    @pl.when(lowest)
    def rim_below():
        def go(slot, unused):
            rim(slot, ((first - 2, True), (first - 1, True)), (first - 2, first - 1))
            return unused

        lax.fori_loop(0, slots, go, 0)

    @pl.when(highest)
    def rim_above():
        def go(slot, unused):
            rim(slot, ((last + 1, False), (last + 2, True)), (last + 1,))
            return unused

        lax.fori_loop(0, slots, go, 0)

    def tell(step):
        return remote(
            sums, gathered.at[place], s_send.at[step - 1], s_recv.at[step - 1],
            (grp, lax.rem(place + step, places)),
        )

    def hear(step):
        source = lax.rem(place + places - step, places)
        return remote(
            sums, gathered.at[source], s_send.at[step - 1], s_recv.at[step - 1],
            (grp, lax.rem(place + step, places)),
        )

    for step in range(1, places):
        tell(step).start()
    gathered[place] = sums[...]
    for step in range(1, places):
        hear(step).wait_recv()
    whole = gathered[0]
    for at in range(1, places):
        whole = whole + gathered[at]
    lanes = lax.broadcasted_iota(jnp.int32, whole.shape, 1)
    moments = [jnp.sum(jnp.where(lanes == at, whole, 0.0), axis=1, keepdims=True) for at in range(6)]
    for at, weight in enumerate(krylov_weights(moments)):
        weights[at] = jnp.broadcast_to(weight, whole.shape)

    def finish(slot, unused):
        w0, w1, w2 = [weights[at, pl.ds(slot, 1)] for at in range(3)]
        for x in range(planes):
            e = x + HALO
            pot[slot, x] = w0 * wide[slot, e] + w1 * one[slot, e] + w2 * two[slot, e]
        return unused

    lax.fori_loop(0, slots, finish, 0)
    for wave in range(WAVES):
        @pl.when(jnp.logical_not(highest))
        def sent_up(wave=wave):
            rise(wave).wait_send()

        @pl.when(jnp.logical_not(lowest))
        def sent_down(wave=wave):
            sink(wave).wait_send()

    for step in range(1, places):
        tell(step).wait_send()


def solve_slabs(table, dens, places, ident):
    slots, planes, rows, lanes = dens.shape
    vmem = pl.BlockSpec(memory_space=pltpu.VMEM)
    dma = pltpu.SemaphoreType.DMA
    tall = pltpu.VMEM((slots, planes + 2 * HALO, rows, lanes), jnp.float32)
    return pl.pallas_call(
        functools.partial(solve_slabs_kernel, places),
        in_specs=[pl.BlockSpec(memory_space=pltpu.SMEM), vmem],
        out_specs=vmem,
        out_shape=jax.ShapeDtypeStruct(dens.shape, jnp.float32),
        scratch_shapes=[
            tall, tall, tall,
            pltpu.VMEM((slots, lanes), jnp.float32),
            pltpu.VMEM((places, slots, lanes), jnp.float32),
            pltpu.VMEM((3, slots, lanes), jnp.float32),
            dma((WAVES, 2)), dma((WAVES, 2)), dma((places - 1,)), dma((places - 1,)),
        ],
        compiler_params=pltpu.CompilerParams(
            collective_id=ident, has_side_effects=True, vmem_limit_bytes=40 * 1024 * 1024
        ),
        name="solve_slabs",
    )(table, dens)


def term_kernel(tbl, pot, partner, moved, fixed, going, staying):
    chunks = going.shape[0]

    def go(slot, unused):
        second = tbl[3, slot] > 0
        dy, dz = tbl[4, slot], tbl[5, slot]
        for x in range(pot.shape[1]):
            found = pot[slot, x]
            left = moved[:, slot, x].reshape(ROWS, LANES)
            right = fixed[:, slot, x].reshape(ROWS, LANES)
            term_a = found * partner[slot, x]
            term_b = shift_plane(found * jnp.where(second, right, left), -dy, -dz)
            going[:, slot, x] = jnp.where(second, term_b, term_a).reshape(chunks, SUB, LANES)
            staying[:, slot, x] = jnp.where(second, term_a, term_b).reshape(chunks, SUB, LANES)
        return unused

    lax.fori_loop(0, pot.shape[0], go, 0)


def make_terms(table, pot, partner, moved, fixed):
    vmem = pl.BlockSpec(memory_space=pltpu.VMEM)
    shape = jax.ShapeDtypeStruct(moved.shape, jnp.float32)
    return pl.pallas_call(
        term_kernel,
        in_specs=[pl.BlockSpec(memory_space=pltpu.SMEM)] + [vmem] * 4,
        out_specs=[vmem, vmem],
        out_shape=[shape, shape],
        compiler_params=pltpu.CompilerParams(vmem_limit_bytes=24 * 1024 * 1024),
        name="make_terms",
    )(table, pot, partner, moved, fixed)


def hand_back_kernel(chips, tbl, last, going, staying, out, *scratch):
    count, slots = going.shape[:2]
    wins, chains, outs1, outs2, ins1, ins2 = [scratch[i * count : (i + 1) * count] for i in range(6)]
    xy_send, xy_recv, z_send, z_recv = scratch[6 * count :]
    grp, place, across, along, corner = spot()
    core = lax.rem(place, 2)
    norb, planes = out.shape[:2]
    part = norb // 2
    relay = Relay(wins, z_send, z_recv, (-1, 1), chips, (slots // 2,) * 3)
    greet(chips)
    relay.clear()

    def start(chunk):
        for side in range(2):
            at = relay.offset(relay.signs[side], 0) + planes * core

            def place_in(slot, unused, at=at):
                wins[chunk][slot, pl.ds(at, planes)] = going[chunk, slot]
                return unused

            lax.fori_loop(side * (slots // 2), (side + 1) * (slots // 2), place_in, 0)
        relay.begin(chunk)

    def swap(chunk, kind):
        src = (outs1 if kind < 2 else outs2)[chunk].at[kind % 2]
        dst = (ins1 if kind < 2 else ins2)[chunk].at[kind % 2]
        target = (across, along, along, across)[kind]
        return remote(src, dst, xy_send.at[chunk, kind], xy_recv.at[chunk, kind], (target, place))

    start(0)
    start(1)
    for step in range(count + 4):
        if step < count:
            relay.first(step)
            relay.share(step)
            if step + 2 < count:
                start(step + 2)
        chunk = step - 1
        if 0 <= chunk < count:
            relay.second(chunk)
        chunk = step - 2
        if 0 <= chunk < count:
            relay.settle(chunk)
            chain = chains[chunk]
            chain[2 * slots] = jnp.zeros(chain.shape[1:], jnp.float32)

            def link_fixed(slot, unused, chain=chain, chunk=chunk):
                chain[slot] = staying[chunk, slot] + chain[tbl[8, slot]]
                return unused

            def link_moved(slot, unused, chain=chain, chunk=chunk):
                first = tbl[7, slot] + planes * core
                for plane in range(planes):
                    chain[slots + slot, plane] = wins[chunk][slot, first + plane] + chain[tbl[9, slot], plane]
                return unused

            lax.fori_loop(0, slots, link_fixed, 0)
            lax.fori_loop(0, slots, link_moved, 0)

            def pack(i, unused, chain=chain, chunk=chunk):
                outs1[chunk][0, i] = chain[last[across * norb + i]]
                outs1[chunk][0, part + i] = chain[last[corner * norb + i]]
                outs1[chunk][1, i] = chain[last[along * norb + part + i]]
                outs1[chunk][1, part + i] = chain[last[corner * norb + part + i]]
                return unused

            lax.fori_loop(0, part, pack, 0)
            swap(chunk, 0).start()
            swap(chunk, 1).start()
        chunk = step - 3
        if 0 <= chunk < count:
            chain = chains[chunk]
            swap(chunk, 0).wait_recv()

            def add_across(i, unused, chain=chain, chunk=chunk):
                outs2[chunk][0, i] = ins1[chunk][0, part + i] + chain[last[along * norb + i]]
                return unused

            lax.fori_loop(0, part, add_across, 0)
            swap(chunk, 2).start()
            swap(chunk, 1).wait_recv()

            def add_along(i, unused, chain=chain, chunk=chunk):
                outs2[chunk][1, i] = ins1[chunk][1, part + i] + chain[last[across * norb + part + i]]
                return unused

            lax.fori_loop(0, part, add_along, 0)
            swap(chunk, 3).start()
        chunk = step - 4
        if 0 <= chunk < count:
            chain = chains[chunk]
            swap(chunk, 2).wait_recv()
            swap(chunk, 3).wait_recv()
            for side in range(2):
                def keep(i, unused, side=side, chain=chain, chunk=chunk):
                    orbit = side * part + i
                    found = ins1[chunk][side, i] + ins2[chunk][side, i]
                    out[orbit, :, pl.ds(chunk * SUB, SUB)] = found + chain[last[grp * norb + orbit]]
                    return unused

                lax.fori_loop(0, part, keep, 0)
    for chunk in range(count):
        for kind in range(4):
            swap(chunk, kind).wait_send()
    relay.drain()


def hand_back(table, last, going, staying, norb, chips):
    chunks, slots, planes, sub, lanes = going.shape
    vmem = pl.BlockSpec(memory_space=pltpu.VMEM)
    smem = pl.BlockSpec(memory_space=pltpu.SMEM)
    dma = pltpu.SemaphoreType.DMA
    def room(*lead):
        return [pltpu.VMEM(lead + (planes, sub, lanes), jnp.float32)] * chunks
    wins = [pltpu.VMEM((slots, 6 * planes, sub, lanes), jnp.float32)] * chunks
    return pl.pallas_call(
        functools.partial(hand_back_kernel, chips),
        in_specs=[smem, smem, vmem, vmem],
        out_specs=vmem,
        out_shape=jax.ShapeDtypeStruct((norb, planes, chunks * sub, lanes), jnp.float32),
        scratch_shapes=wins + room(2 * slots + 1) + room(2, norb) + room(2, norb // 2)
        + room(2, norb) + room(2, norb // 2)
        + [dma((chunks, 4)), dma((chunks, 4)), dma((chunks, 2, 6)), dma((chunks, 2, 6))],
        compiler_params=pltpu.CompilerParams(
            collective_id=2, has_side_effects=True, vmem_limit_bytes=56 * 1024 * 1024
        ),
        name="hand_back",
    )(table, last, going, staying)


def plan_kernel(cap, planes, me_ref, anchors, pairs, tbl, links, fits, spots, masks, lists, mine, counts):
    groups = 4
    orbits = anchors.shape[1]
    local = orbits // groups
    depth, unused, owners = pairs.shape
    entries = depth * owners
    each = tbl.shape[1]
    half = each // 2
    extra = (groups - 1) * cap
    final = extra
    prior = final + local + extra
    ends = prior + extra
    spare = ends + local
    worst = 1 << 20
    me = me_ref[0]

    def unpack(code):
        return jnp.bitwise_and(code, 1023), jnp.bitwise_and(jnp.right_shift(code, 10), 1023)

    def clean(i, unused):
        links[i] = 0
        links[prior + i] = extra
        return unused

    def close(i, unused):
        links[final + i] = 2 * each
        return unused

    def own(i, unused):
        links[ends + i] = extra
        spots[me * local + i] = i
        return unused

    lax.fori_loop(0, extra, clean, 0, unroll=5)
    lax.fori_loop(0, local + extra, close, 0, unroll=4)
    lax.fori_loop(0, local, own, 0, unroll=4)

    def sort(i, tails, layer):
        a, b = pairs[layer, 0, i], pairs[layer, 1, i]
        filled = jnp.where(a >= 0, 1, 0)
        dx = anchors[0, jnp.maximum(b, 0)] - anchors[0, jnp.maximum(a, 0)]
        reach = jnp.abs(dx)
        kind = 3 - sum(jnp.where(reach > planes * k, 1, 0) for k in (1, 2, 3))
        step = jnp.left_shift(kind, 3)
        tail = jnp.bitwise_and(jnp.right_shift(tails, step), 255)
        code = a + jnp.left_shift(b, 10) + jnp.left_shift(dx + B, 20)
        lists[jnp.where(filled > 0, kind * entries + tail, 4 * entries)] = code
        return tails + jnp.left_shift(filled, step)

    zero = jnp.int32(0)
    packed = zero
    for layer in range(depth):
        packed = lax.fori_loop(0, owners, functools.partial(sort, layer=layer), packed, unroll=8)
    tails = [jnp.bitwise_and(jnp.right_shift(packed, 8 * k), 255) for k in range(4)]
    fits[0] = 0

    def trial(turn):
        def reset(i, unused):
            for g in range(groups):
                masks[g * local + i] = (15 - (1 << g)) + (g << 10)
            return unused

        lax.fori_loop(0, local, reset, 0, unroll=8)
        state = (zero,) * (groups + 1)
        for kind, limit in enumerate((half // 4, half // 2, 3 * half // 4, half)):
            size = tails[kind]
            base = lax.rem(turn * 5, jnp.maximum(size, 1))
            flip = jnp.bitwise_and(turn, 1) > 0

            def deal(i, state, kind=kind, limit=limit, size=size, base=base, flip=flip):
                filled, bad = state[:groups], state[groups]
                at = i + base
                at = jnp.where(at >= size, at - size, at)
                code = lists[kind * entries + jnp.where(flip, size - 1 - at, at)]
                a, b = unpack(code)
                word_a, word_b = masks[a], masks[b]
                step_a, step_b = jnp.right_shift(word_a, 8), jnp.right_shift(word_b, 8)
                same = jnp.where(step_a == step_b, 1, 0)

                def needs(h, count):
                    new_a = jnp.bitwise_and(jnp.right_shift(word_a, h), 1)
                    new_b = jnp.bitwise_and(jnp.right_shift(word_b, h), 1)
                    had_a = jnp.bitwise_and(jnp.right_shift(count, step_a), 15)
                    had_b = jnp.bitwise_and(jnp.right_shift(count, step_b), 15) + jnp.bitwise_and(new_a, same)
                    return new_a, new_b, had_a, had_b

                best = jnp.int32(worst)
                for h in range(groups):
                    new_a, new_b, had_a, had_b = needs(h, filled[h])
                    need = jnp.maximum(jnp.where(new_a > 0, had_a + 1, 0), jnp.where(new_b > 0, had_b + 1, 0))
                    seats = jnp.right_shift(filled[h], 16)
                    cost = jnp.left_shift(new_a + new_b, 4) + jnp.left_shift(need, 3) + (jnp.left_shift(seats, 2) + h)
                    best = jnp.minimum(best, jnp.where((seats < 2 * limit) & (need <= cap), cost, worst))
                good = best < worst
                flag = jnp.where(good, 1, 0)
                column = jnp.bitwise_and(best, 3)
                count = filled[0]
                for h in range(1, groups):
                    count = jnp.where(column == h, filled[h], count)
                new_a, new_b, had_a, had_b = needs(column, count)
                seats = jnp.right_shift(count, 16)
                seat = jnp.bitwise_and(seats, 1) * half + jnp.right_shift(seats, 1)
                grown = jnp.left_shift(new_a, step_a) + jnp.left_shift(new_b, step_b)
                grown = jnp.where(good, count + grown + (1 << 16), count)
                masks[a] = word_a - jnp.where(good, jnp.left_shift(new_a, column), 0)
                masks[b] = word_b - jnp.where(good, jnp.left_shift(new_b, column), 0)
                here = good & (column == me)
                mine[jnp.where(here, seat, each)] = code
                for orbit, step, new, had in ((a, step_a, new_a, had_a), (b, step_b, new_b, had_b)):
                    group = jnp.right_shift(step, 2)
                    at = (jnp.bitwise_xor(group, column) - 1) * cap + had
                    spots[jnp.where(here & (new > 0), orbit, orbits)] = local + at
                    links[jnp.where(good & (new > 0) & (group == me), at, spare)] = orbit - group * local
                kept = tuple(jnp.where(column == h, grown, filled[h]) for h in range(groups))
                return kept + (jnp.bitwise_or(bad, 1 - flag),)

            state = lax.fori_loop(0, size, deal, state)
        for h in range(groups):
            counts[h] = state[h]
        fits[0] = 1 - state[groups]

    def attempt(turn, unused):
        @pl.when(fits[0] == 0)
        def go():
            trial(turn)

        return unused

    lax.fori_loop(0, TRIALS, attempt, 0)

    @pl.when(fits[0] > 0)
    def settle():
        def fill(at, unused):
            code = mine[at]
            a, b = unpack(code)
            dx = jnp.right_shift(code, 20) - B
            spot_a, spot_b = spots[a], spots[b]
            rising = at < half
            second = jnp.where(rising, dx, -dx) >= 0
            shift = jnp.where(second, dx, -dx)
            tbl[0, at] = jnp.where(second, spot_b, spot_a)
            tbl[1, at] = jnp.where(second, spot_a, spot_b)
            tbl[2, at] = jnp.where(rising, 4 * planes, 0) - shift
            tbl[3, at] = jnp.where(second, 1, 0)
            tbl[4, at] = anchors[1, b] - anchors[1, a]
            tbl[5, at] = anchors[2, b] - anchors[2, a]
            tbl[6, at] = jnp.where(second, 0, shift)
            tbl[7, at] = jnp.where(rising, 0, 4 * planes) + shift
            return unused

        lax.fori_loop(0, each, fill, 0, unroll=2)
        for row, base in ((1, 0), (0, each)):
            def link(slot, unused, row=row, base=base):
                at = final + tbl[row, slot]
                tbl[9 - row, slot] = links[at]
                links[at] = base + slot
                return unused

            lax.fori_loop(0, each, link, 0, unroll=4)
        for turn in range(1, groups):
            def hook(i, unused, turn=turn):
                at = (turn - 1) * cap + i
                end = ends + links[at]
                links[prior + at] = links[end]
                links[end] = at
                return unused

            sent = jnp.bitwise_and(jnp.right_shift(counts[jnp.bitwise_xor(me, turn)], 4 * me), 15)
            lax.fori_loop(0, sent, hook, 0)


def make_plan(anchors, pair_slots, cap, each, planes):
    orbits = anchors.shape[0]
    entries = pair_slots.shape[0] * pair_slots.shape[1]
    smem = pl.BlockSpec(memory_space=pltpu.SMEM)
    local = orbits // 4
    me = jnp.full((1,), lax.axis_index("grp"), jnp.int32)
    return pl.pallas_call(
        functools.partial(plan_kernel, cap, planes),
        in_specs=[smem] * 3,
        out_specs=[smem] * 3,
        out_shape=[
            jax.ShapeDtypeStruct((10, each), jnp.int32),
            jax.ShapeDtypeStruct((9 * cap + 2 * local + 1,), jnp.int32),
            jax.ShapeDtypeStruct((1,), jnp.int32),
        ],
        scratch_shapes=[
            pltpu.SMEM((orbits + 1,), jnp.int32), pltpu.SMEM((orbits,), jnp.int32),
            pltpu.SMEM((4 * entries + 1,), jnp.int32), pltpu.SMEM((each + 1,), jnp.int32),
            pltpu.SMEM((4,), jnp.int32),
        ],
        name="plan",
    )(me, anchors.T, jnp.transpose(pair_slots, (1, 2, 0)))


def coupled(plane):
    shape = plane.shape
    lane = lane_ids(shape)
    row = lax.broadcasted_iota(jnp.int32, shape, 0)
    lower_z = jnp.where(jnp.bitwise_and(lane, B - 1) > 0, pltpu.roll(plane, 1, 1), 0.0)
    half = pltpu.roll(plane, B, 1)
    down = jnp.where(row > 0, pltpu.roll(half, 1, 0), 0.0)
    return 3.0 * plane - lower_z - jnp.where(lane < B, down, half)


def lean_kernel(chips, cap, tbl, links, orb, out, *scratch):
    count = out.shape[2]
    raws, owns, parcels, pools, wins, wins_back, chains, parcels_back, backs, tallied = [
        scratch[i * count : (i + 1) * count] for i in range(10)
    ]
    partner, wide, one, two, staying, held, sums, gathered, weights = scratch[10 * count : 10 * count + 9]
    (own_sem, xy_send, xy_recv, z_send, z_recv, yx_send, yx_recv, zb_send, zb_recv,
     h_send, h_recv, s_send, s_recv) = scratch[10 * count + 9 :]
    grp, place, across, along, corner = spot()
    core = lax.rem(place, 2)
    places = 2 * chips
    tiles, planes = orb.shape[:2]
    deep = orb.shape[4]
    norb = tiles * deep
    slots = partner.shape[0]
    half = slots // 2
    first, last = HALO, HALO + planes - 1
    each = slots // WAVES
    marks = (half // 4, half // 2, 3 * half // 4)
    relay = Relay(wins, z_send, z_recv, (1, -1), chips, marks)
    relay_back = Relay(wins_back, zb_send, zb_recv, (-1, 1), chips, marks)
    lowest, highest = place == 0, place == places - 1

    def stage(chunk):
        return pltpu.make_async_copy(orb.at[:, :, chunk], raws[chunk], own_sem.at[chunk])

    for chunk in range(count):
        stage(chunk).start()
    barrier = pltpu.get_barrier_semaphore()
    for step in range(1, places):
        pl.semaphore_signal(
            barrier, inc=1, device_id=(grp, lax.rem(place + step, places)), device_id_type=MESH
        )
    for target in (across, along, corner):
        pl.semaphore_signal(barrier, inc=1, device_id=(target, place), device_id_type=MESH)

    def parcel(chunk, kind):
        return remote(
            parcels[chunk].at[pl.ds(kind * cap, cap)], pools[chunk].at[pl.ds(norb + kind * cap, cap)],
            xy_send.at[chunk, kind], xy_recv.at[chunk, kind], ((across, along, corner)[kind], place),
        )

    def pack(chunk):
        stage(chunk).wait()

        def untile(plane, unused):
            for tile in range(tiles):
                for row in range(deep):
                    piece = raws[chunk][tile, plane, :, row, :]
                    owns[chunk][tile * deep + row, plane] = piece
                    pools[chunk][tile * deep + row, plane] = piece
            return unused

        lax.fori_loop(0, planes, untile, 0)

        def put(i, unused):
            parcels[chunk][i] = owns[chunk][links[i]]
            return unused

        lax.fori_loop(0, 3 * cap, put, 0)

    def send(chunk):
        for kind in (2, 0, 1):
            parcel(chunk, kind).start()

    pack(0)
    pl.semaphore_wait(barrier, places + 2)
    send(0)
    pack(1)
    for chunk in range(2, count):
        pack(chunk)
        send(chunk - 1)
    send(count - 1)
    relay.clear()
    relay_back.clear()
    blank = jnp.zeros((HALO, ROWS, LANES), jnp.float32)

    def clear(slot, unused):
        for e in (0, 1, last + 3):
            one[slot, e] = blank[0]
        return unused

    lax.fori_loop(0, slots, clear, 0)

    @pl.when(lowest)
    def no_below():
        def fill(slot, unused):
            wide[slot, pl.ds(0, HALO)] = blank
            return unused

        lax.fori_loop(0, slots, fill, 0)

    @pl.when(highest)
    def no_above():
        def fill(slot, unused):
            wide[slot, pl.ds(HALO + planes, HALO)] = blank
            return unused

        lax.fori_loop(0, slots, fill, 0)

    for step in range(count + 1):
        if step < count:
            for kind in range(3):
                parcel(step, kind).wait_recv()
            for side in range(2):
                start = relay.offset(relay.signs[side], 0) + planes * core

                def pick(slot, unused, start=start, chunk=step):
                    wins[chunk][slot, pl.ds(start, planes)] = pools[chunk][tbl[0, slot]]
                    return unused

                lax.fori_loop(side * half, (side + 1) * half, pick, 0)
            relay.begin(step)
        if step > 0:
            relay.second(step - 1)
            relay.settle(step - 1)
        if step < count:
            relay.first(step)
            relay.share(step)

    def couple_of(slot, x):
        at = tbl[2, slot] + planes * core + x
        held_at = tbl[1, slot]
        left = jnp.concatenate([win[slot, at] for win in wins], axis=0)
        right = jnp.concatenate([pool[held_at, x] for pool in pools], axis=0)
        return left, right

    def rise(wave):
        return remote(
            wide.at[pl.ds(wave * each, each), pl.ds(last - HALO + 2, HALO - 1)],
            wide.at[pl.ds(wave * each, each), pl.ds(1, HALO - 1)],
            h_send.at[wave, 0], h_recv.at[wave, 0], (grp, lax.rem(place + 1, places)),
        )

    def sink(wave):
        return remote(
            wide.at[pl.ds(wave * each, each), pl.ds(first, HALO)],
            wide.at[pl.ds(wave * each, each), pl.ds(last + 1, HALO)],
            h_send.at[wave, 1], h_recv.at[wave, 1], (grp, lax.rem(place + places - 1, places)),
        )

    def edges(wave):
        @pl.when(jnp.logical_not(highest))
        def send_up():
            rise(wave).start()

        @pl.when(jnp.logical_not(lowest))
        def send_down():
            sink(wave).start()

    outer = [x for x in range(planes) if x < HALO or x >= planes - HALO + 1]
    middle = [x for x in range(planes) if x not in outer]

    def make(slot, unused, which):
        second = tbl[3, slot] > 0
        dy, dz = tbl[4, slot], tbl[5, slot]
        for x in which:
            left, right = couple_of(slot, x)
            other = shift_plane(jnp.where(second, left, right), dy, dz)
            wide[slot, x + HALO] = jnp.where(second, right, left) * other
            partner[slot, x] = other
        return unused

    none = jnp.zeros((8, LANES), jnp.float32)
    lane = lax.broadcasted_iota(jnp.int32, (1, LANES), 1)

    def row_of(parts):
        row = jnp.zeros((1, LANES), jnp.float32)
        for at, part in parts:
            row = row + jnp.where(lane == at, total(part), 0.0)
        return row

    def live(slot, e):
        x = planes * place + e - HALO
        low = tbl[6, slot]
        return jnp.where((x >= low) & (x < low + B), 1.0, 0.0).astype(jnp.float32)

    def raise_one(slot, e, acc):
        source = wide[slot, e]
        value = live(slot, e) * (inner(source) - (wide[slot, e - 1] + wide[slot, e + 1]))
        one[slot, e] = value
        if first <= e <= last:
            acc[1] = acc[1] + fold(source * value)
            acc[2] = acc[2] + fold(value * value)

    def raise_two(slot, e):
        source = one[slot, e]
        two[slot, e] = live(slot, e) * (inner(source) - (one[slot, e - 1] + one[slot, e + 1]))

    def measure_two(slot, e, acc, below):
        value = two[slot, e]
        acc[3] = acc[3] + fold(one[slot, e] * value)
        acc[4] = acc[4] + fold(value * value)
        bent = coupled(value)
        acc[5] = acc[5] + fold(value * (bent - two[slot, e - 1] if below else bent))

    def work_inside(slot, unused):
        acc = [none] * 6
        for e in range(first, last + 1):
            source = wide[slot, e]
            acc[0] = acc[0] + fold(source * source)
        for e in range(first + 1, last):
            raise_one(slot, e, acc)
        for e in range(first + 2, last - 1):
            raise_two(slot, e)
            measure_two(slot, e, acc, e > first + 2)
        for at in range(6):
            held[slot, at] = acc[at]
        return unused

    def work_edges(slot, unused):
        acc = [held[slot, at] for at in range(6)]
        for e in (first - 1, first, last, last + 1, last + 2):
            raise_one(slot, e, acc)
        for e in (first, first + 1, last - 1, last, last + 1):
            raise_two(slot, e)
        for e in (first, first + 1, last - 1, last):
            measure_two(slot, e, acc, e > first)
        acc[5] = acc[5] - fold(two[slot, first + 2] * two[slot, first + 1])
        acc[5] = acc[5] - fold(two[slot, last + 1] * two[slot, last])
        acc[5] = 2.0 * acc[5]
        sums[pl.ds(slot, 1)] = row_of(enumerate(acc))
        return unused

    def rim(slot, planes_one, planes_two, spots, pairs):
        spare = [none] * 6
        for e in planes_one:
            raise_one(slot, e, spare)
        for e in planes_two:
            raise_two(slot, e)
        acc = [held[slot, at] for at in range(6)]
        for e in spots:
            value, before = two[slot, e], one[slot, e]
            acc[2] = acc[2] + fold(before * before)
            acc[3] = acc[3] + fold(before * value)
            acc[4] = acc[4] + fold(value * value)
            acc[5] = acc[5] + fold(value * coupled(value))
        for e in pairs:
            acc[5] = acc[5] - fold(two[slot, e] * two[slot, e + 1])
        for at in range(2, 6):
            held[slot, at] = acc[at]

    make_outer = functools.partial(make, which=outer)
    lax.fori_loop(0, each, make_outer, 0)
    for wave in range(1, WAVES):
        lax.fori_loop(wave * each, (wave + 1) * each, make_outer, 0)
        edges(wave - 1)
    edges(WAVES - 1)
    lax.fori_loop(0, slots, functools.partial(make, which=middle), 0)
    lax.fori_loop(0, slots, work_inside, 0)

    @pl.when(lowest)
    def rim_below():
        def go(slot, unused):
            low = first - 2
            rim(slot, (low + 1, low + 2), (low, low + 1, low + 2), (low, low + 1), (low, low + 1))
            return unused

        lax.fori_loop(0, slots, go, 0)

    @pl.when(highest)
    def rim_above():
        def go(slot, unused):
            high = last + 2
            rim(slot, (high - 2, high - 1, high), (high - 1, high), (high - 1, high), (high - 1,))
            return unused

        lax.fori_loop(0, slots, go, 0)

    for wave in range(WAVES):
        @pl.when(jnp.logical_not(lowest))
        def got_below(wave=wave):
            rise(wave).wait_recv()

        @pl.when(jnp.logical_not(highest))
        def got_above(wave=wave):
            sink(wave).wait_recv()

        lax.fori_loop(wave * each, (wave + 1) * each, work_edges, 0)

    def tell(step, at):
        return remote(
            sums, gathered.at[at], s_send.at[step - 1], s_recv.at[step - 1],
            (grp, lax.rem(place + step, places)),
        )

    for step in range(1, places):
        tell(step, place).start()
    gathered[place] = sums[...]
    for step in range(1, places):
        tell(step, lax.rem(place + places - step, places)).wait_recv()
    whole = gathered[0]
    for at in range(1, places):
        whole = whole + gathered[at]
    lanes = lax.broadcasted_iota(jnp.int32, whole.shape, 1)
    moments = [jnp.sum(jnp.where(lanes == at, whole, 0.0), axis=1, keepdims=True) for at in range(6)]
    for at, weight in enumerate(krylov_weights(moments)):
        weights[at] = jnp.broadcast_to(weight, whole.shape)

    for side in range(2):
        start = relay_back.offset(relay_back.signs[side], 0) + planes * core

        def finish(slot, unused, start=start):
            second = tbl[3, slot] > 0
            dy, dz = tbl[4, slot], tbl[5, slot]
            w0, w1, w2 = [weights[at, pl.ds(slot, 1)] for at in range(3)]
            for x in range(planes):
                e = x + HALO
                found = w0 * wide[slot, e] + w1 * one[slot, e] + w2 * two[slot, e]
                left, right = couple_of(slot, x)
                term_a = found * partner[slot, x]
                term_b = shift_plane(found * jnp.where(second, right, left), -dy, -dz)
                going = jnp.where(second, term_b, term_a)
                stays = jnp.where(second, term_a, term_b)
                for chunk in range(count):
                    wins_back[chunk][slot, start + x] = going[chunk * SUB : (chunk + 1) * SUB]
                    staying[chunk, slot, x] = stays[chunk * SUB : (chunk + 1) * SUB]
            return unused

        lax.fori_loop(side * half, (side + 1) * half, finish, 0)
        relay_back.begin(0, (side,))

    extra = 3 * cap
    final = extra
    prior = final + norb + extra
    ends = prior + extra

    def reply(chunk, kind):
        return remote(
            parcels_back[chunk].at[pl.ds(kind * cap, cap)], backs[chunk].at[pl.ds(kind * cap, cap)],
            yx_send.at[chunk, kind], yx_recv.at[chunk, kind], ((across, along, corner)[kind], place),
        )

    for step in range(count + 2):
        chunk = step - 1
        if 0 <= chunk < count:
            relay_back.second(chunk)
            relay_back.settle(chunk)
            chain = chains[chunk]
            chain[2 * slots] = jnp.zeros(chain.shape[1:], jnp.float32)

            def link_fixed(slot, unused, chain=chain, chunk=chunk):
                chain[slot] = staying[chunk, slot] + chain[tbl[8, slot]]
                return unused

            def link_moved(slot, unused, chain=chain, chunk=chunk):
                at = tbl[7, slot] + planes * core
                for plane in range(planes):
                    chain[slots + slot, plane] = wins_back[chunk][slot, at + plane] + chain[tbl[9, slot], plane]
                return unused

            lax.fori_loop(0, slots, link_fixed, 0)
            lax.fori_loop(0, slots, link_moved, 0)

            def wrap(i, unused, chain=chain, chunk=chunk):
                parcels_back[chunk][i] = chain[links[final + norb + i]]
                return unused

            lax.fori_loop(0, extra, wrap, 0)
            for kind in (2, 0, 1):
                reply(chunk, kind).start()
        if step < count:
            relay_back.first(step)
            if step + 1 < count:
                relay_back.begin(step + 1)
            relay_back.share(step)
        chunk = step - 2
        if 0 <= chunk < count:
            total_of = tallied[chunk]
            total_of[extra] = jnp.zeros(total_of.shape[1:], jnp.float32)
            for kind in range(3):
                reply(chunk, kind).wait_recv()

            def gather(i, unused, total_of=total_of, chunk=chunk):
                total_of[i] = backs[chunk][i] + total_of[links[prior + i]]
                return unused

            lax.fori_loop(0, extra, gather, 0)

            for orbit in range(norb):
                found = total_of[links[ends + orbit]] + chains[chunk][links[final + orbit]]
                for plane in range(planes):
                    out[orbit // deep, plane, chunk, :, orbit % deep, :] = found[plane]
    for chunk in range(count):
        for kind in range(3):
            parcel(chunk, kind).wait_send()
            reply(chunk, kind).wait_send()
    for wave in range(WAVES):
        @pl.when(jnp.logical_not(highest))
        def sent_up(wave=wave):
            rise(wave).wait_send()

        @pl.when(jnp.logical_not(lowest))
        def sent_down(wave=wave):
            sink(wave).wait_send()

    for step in range(1, places):
        tell(step, place).wait_send()
    relay.drain()
    relay_back.drain()


def run_lean(table, links, tiled, slots, chips, cap):
    tiles, planes, chunks, unused, deep, lanes = tiled.shape
    norb, rows = tiles * deep, chunks * SUB
    places = 2 * chips
    smem = pl.BlockSpec(memory_space=pltpu.SMEM)
    dma = pltpu.SemaphoreType.DMA

    def room(count, deep=planes):
        return [pltpu.VMEM((count, deep, SUB, lanes), jnp.float32)] * chunks

    tall = pltpu.VMEM((slots, planes + 2 * HALO, rows, lanes), jnp.float32)
    xy, z = dma((chunks, 3)), dma((chunks, 2, 6))
    return pl.pallas_call(
        functools.partial(lean_kernel, chips, cap),
        in_specs=[smem, smem, pl.BlockSpec(memory_space=pl.ANY)],
        out_specs=pl.BlockSpec(memory_space=pltpu.VMEM),
        out_shape=jax.ShapeDtypeStruct(tiled.shape, jnp.float32),
        scratch_shapes=[pltpu.VMEM((tiles, planes, SUB, deep, lanes), jnp.float32)] * chunks
        + room(norb) + room(3 * cap) + room(norb + 3 * cap) + room(slots, 6 * planes)
        + room(slots, 6 * planes) + room(2 * slots + 1) + room(3 * cap) + room(3 * cap) + room(3 * cap + 1)
        + [
            pltpu.VMEM((slots, planes, rows, lanes), jnp.float32), tall, tall, tall,
            pltpu.VMEM((chunks, slots, planes, SUB, lanes), jnp.float32),
            pltpu.VMEM((slots, 6, 8, lanes), jnp.float32),
            pltpu.VMEM((slots, lanes), jnp.float32),
            pltpu.VMEM((places, slots, lanes), jnp.float32),
            pltpu.VMEM((3, slots, lanes), jnp.float32),
            dma((chunks,)), xy, xy, z, z, xy, xy, z, z,
            dma((WAVES, 2)), dma((WAVES, 2)), dma((places - 1,)), dma((places - 1,)),
        ],
        compiler_params=pltpu.CompilerParams(
            collective_id=3, has_side_effects=True, vmem_limit_bytes=60 * 1024 * 1024
        ),
        name="lean",
    )(table, links, tiled)


def full_tables(anchors, pair_slots, planes, groups, each):
    assignment = deal_evenly(pair_slots, groups, each)
    pairs = assignment[lax.axis_index("grp")]
    offsets = anchors[pairs[:, 1]] - anchors[pairs[:, 0]]
    dx, dy, dz = offsets[:, 0], offsets[:, 1], offsets[:, 2]
    slot = lax.broadcasted_iota(jnp.int32, (each,), 0)
    rising = slot < each // 2
    second = jnp.where(rising, dx >= 0, dx <= 0)
    shift = jnp.where(second, dx, -dx)
    moved_id = jnp.where(second, pairs[:, 1], pairs[:, 0])
    fixed_id = jnp.where(second, pairs[:, 0], pairs[:, 1])
    terms = jnp.concatenate([fixed_id, moved_id])
    at = lax.broadcasted_iota(jnp.int32, (2 * each, 2 * each), 0)
    before = lax.broadcasted_iota(jnp.int32, (2 * each, 2 * each), 1)
    found = jnp.where((terms[:, None] == terms[None, :]) & (before < at), before, -1)
    prior = jnp.max(found, axis=1)
    prior = jnp.where(prior < 0, 2 * each, prior)
    norb = anchors.shape[0]
    orbit = lax.broadcasted_iota(jnp.int32, (norb, 2 * each), 0)
    index = lax.broadcasted_iota(jnp.int32, (norb, 2 * each), 1)
    last = jnp.max(jnp.where(terms[None, :] == orbit, index, -1), axis=1)
    last = jnp.where(last < 0, 2 * each, last)
    table = jnp.stack([
        moved_id, fixed_id,
        jnp.where(rising, 4 * planes, 0) - shift,
        second.astype(jnp.int32), dy, dz,
        jnp.where(second, 0, shift),
        jnp.where(rising, 0, 4 * planes) + shift,
        prior[:each], prior[each:],
    ])
    return table, last


def slab_body(orbitals, anchors, pair_slots):
    groups, places = lax.axis_size("grp"), lax.axis_size("grid")
    norb_local, cells = orbitals.shape
    planes = cells // (B * B)
    each = PAIR_DEV * places
    chips = places // 2
    cap = 5 * norb_local // 16
    plan, links, fits = make_plan(anchors, pair_slots, cap, each, planes)
    deep = math.gcd(norb_local, 8)

    def lean(orbitals, anchors, pair_slots, plan, links):
        tiled = orbitals.reshape(norb_local // deep, deep, planes, ROWS // SUB, SUB, LANES)
        out = run_lean(plan, links, jnp.transpose(tiled, (0, 2, 3, 4, 1, 5)), each, chips, cap)
        return jnp.transpose(out, (0, 4, 1, 2, 3, 5)).reshape(norb_local, cells)

    def full(orbitals, anchors, pair_slots, plan, links):
        stacked = orbitals.reshape(norb_local, planes, ROWS, LANES)
        table, last = full_tables(anchors, pair_slots, planes, groups, each)
        moved, fixed = bring(table, stacked, each, groups, chips)
        dens, partner = pair_up(table, moved, fixed)
        pot = solve_slabs(table, dens, places, 5)
        going, staying = make_terms(table, pot, partner, moved, fixed)
        out = hand_back(table, last, going, staying, norb_local, chips)
        return out.reshape(norb_local, cells)

    return lax.cond(fits[0] > 0, lean, full, orbitals, anchors, pair_slots, plan, links)


def slabs_fit(mesh):
    groups, places = mesh.shape["grp"], mesh.shape["grid"]
    return groups == 4 and places % 2 == 0 and 4 * (B // places) >= PAD


def solution(mesh):
    return jax.shard_map(
        slab_body if slabs_fit(mesh) else owner_body,
        mesh=mesh,
        in_specs=(P("grp", "grid"), P(), P()),
        out_specs=P("grp", "grid"),
        check_vma=False,
    )
```

```python
import functools
import math

import jax
import jax.numpy as jnp
from jax import lax
from jax.experimental import pallas as pl
from jax.experimental.pallas import tpu as pltpu
from jax.sharding import PartitionSpec as P

B = 64
PAIR_DEV = 2
ITERS = 3
MOST_CHUNKS = 2
LANES = 128
ROWS = B * B // LANES
PAD = 32
STEP = 4


def deal_evenly(pair_slots, owner_count, each_owner):
    flat_slots = pair_slots.reshape(-1, 2)
    filled = (flat_slots[:, 0] >= 0).astype(jnp.int32)
    position = jnp.cumsum(filled, dtype=jnp.int32) - filled
    wanted = lax.broadcasted_iota(jnp.int32, (owner_count, each_owner), 1) * owner_count
    wanted = (wanted + lax.broadcasted_iota(jnp.int32, (owner_count, each_owner), 0)).reshape(-1)
    matched = (position[None, :] == wanted[:, None]) & (filled[None, :] == 1)
    picked = jnp.sum(jnp.where(matched[:, :, None], flat_slots[None], 0), axis=1)
    return picked.reshape(owner_count, each_owner, 2)


def gather_kernel(ids_ref, src_ref, *out_refs):
    count, terms = out_refs[0].shape[:2]
    for slot, out_ref in enumerate(out_refs):
        def pick(dest, unused, slot=slot, out_ref=out_ref):
            for term in range(terms):
                out_ref[dest, term] = src_ref[ids_ref[(slot * count + dest) * terms + term]]
            return unused

        lax.fori_loop(0, count, pick, 0)


def gather_pieces(ids, pieces, slots, count):
    norb, rows, lanes = pieces.shape
    block = max(8, rows // 4)
    return pl.pallas_call(
        gather_kernel,
        grid_spec=pltpu.PrefetchScalarGridSpec(
            num_scalar_prefetch=1,
            grid=(rows // block,),
            in_specs=[pl.BlockSpec((norb, block, lanes), lambda i, ids: (0, i, 0))],
            out_specs=[pl.BlockSpec((count, 2, block, lanes), lambda i, ids: (0, 0, i, 0))] * slots,
        ),
        out_shape=[jax.ShapeDtypeStruct((count, 2, rows, lanes), jnp.float32)] * slots,
        cost_estimate=pl.CostEstimate(flops=0, bytes_accessed=8 * norb * rows * lanes, transcendentals=0),
        name="pick_pieces",
    )(ids, pieces)


def scatter_kernel(ids_ref, *refs):
    out_ref = refs[-1]
    out_ref[...] = jnp.zeros_like(out_ref)
    count, terms = refs[0].shape[:2]
    for slot, in_ref in enumerate(refs[:-1]):
        def add(dest, unused, slot=slot, in_ref=in_ref):
            for term in range(terms):
                orbit = ids_ref[(slot * count + dest) * terms + term]
                out_ref[orbit] = out_ref[orbit] + in_ref[dest, term]
            return unused

        lax.fori_loop(0, count, add, 0)


def scatter_pieces(ids, parts, norb):
    count, terms, rows, lanes = parts[0].shape
    block = max(8, rows // 4)
    return pl.pallas_call(
        scatter_kernel,
        grid_spec=pltpu.PrefetchScalarGridSpec(
            num_scalar_prefetch=1,
            grid=(rows // block,),
            in_specs=[pl.BlockSpec((count, terms, block, lanes), lambda i, ids: (0, 0, i, 0))] * len(parts),
            out_specs=pl.BlockSpec((norb, block, lanes), lambda i, ids: (0, i, 0)),
        ),
        out_shape=jax.ShapeDtypeStruct((norb, rows, lanes), jnp.float32),
        cost_estimate=pl.CostEstimate(flops=0, bytes_accessed=8 * norb * rows * lanes, transcendentals=0),
        name="add_pieces",
    )(ids, *parts)


def lane_ids(shape):
    return lax.broadcasted_iota(jnp.int32, shape, len(shape) - 1)


def shift_plane(plane, off_y, off_z):
    shape = plane.shape
    lane = lane_ids(shape)
    row = lax.broadcasted_iota(jnp.int32, shape, 0)
    linear = off_y * B + off_z
    across = jnp.bitwise_and(linear, LANES - 1)
    down = jnp.right_shift(linear, 7)
    turned = pltpu.roll(plane, across, 1)
    near = pltpu.roll(turned, jnp.bitwise_and(down, ROWS - 1), 0)
    far = pltpu.roll(turned, jnp.bitwise_and(down + 1, ROWS - 1), 0)
    moved = jnp.where(lane >= across, near, far)
    from_y = row * 2 + jnp.right_shift(lane, 6) - off_y
    from_z = jnp.bitwise_and(lane, B - 1) - off_z
    inside = (from_y >= 0) & (from_y < B) & (from_z >= 0) & (from_z < B)
    return jnp.where(inside, moved, 0.0)


def operate_plane(before, plane, after):
    shape = plane.shape
    lane = lane_ids(shape)
    row = lax.broadcasted_iota(jnp.int32, shape, 0)
    z = jnp.bitwise_and(lane, B - 1)
    upper_z = jnp.where(z < B - 1, pltpu.roll(plane, LANES - 1, 1), 0.0)
    lower_z = jnp.where(z > 0, pltpu.roll(plane, 1, 1), 0.0)
    half = pltpu.roll(plane, B, 1)
    down = jnp.where(row > 0, pltpu.roll(half, 1, 0), 0.0)
    up = jnp.where(row < ROWS - 1, pltpu.roll(half, ROWS - 1, 0), 0.0)
    beside = (before + after) + (half + jnp.where(lane < B, down, up))
    return 6.0 * plane - beside - upper_z - lower_z


def fold(values):
    return jnp.sum(values.reshape(ROWS // 8, 8, LANES), axis=0)


def total(acc):
    return jnp.sum(acc, axis=(0, 1), keepdims=True)


def solve_kernel(info_ref, *refs):
    chunks = (len(refs) - 6) // 2
    in_refs, out_refs = refs[:chunks], refs[chunks : 2 * chunks]
    wide, partner, direction, resid, image, potential = refs[2 * chunks :]
    count, terms, rows, lanes = in_refs[0].shape
    each = rows // ROWS
    dx, dy, dz = info_ref[0], info_ref[1], info_ref[2]
    keep = jnp.where(info_ref[3] > 0, 1.0, 0.0).astype(jnp.float32)
    edge = jnp.zeros((PAD, ROWS, LANES), jnp.float32)
    wide[pl.ds(0, PAD)] = edge
    wide[pl.ds(PAD + B, PAD)] = edge
    direction[0] = edge[0]
    direction[B + 1] = edge[0]
    none = jnp.zeros((8, LANES), jnp.float32)

    def place(owner, chunk, i):
        return (owner * chunks + chunk) * each + i

    def load(owner, unused):
        for chunk in range(chunks):
            for i in range(each):
                wide[PAD + place(owner, chunk, i)] = in_refs[chunk][owner, 1, pl.ds(i * ROWS, ROWS)]
        return unused

    lax.fori_loop(0, count, load, 0)

    def start(owner, acc):
        for chunk in range(chunks):
            for i in range(each):
                x = place(owner, chunk, i)
                other = shift_plane(wide[PAD + x - dx], dy, dz)
                partner[x] = other
                density = in_refs[chunk][owner, 0, pl.ds(i * ROWS, ROWS)] * other
                direction[x + 1] = density
                resid[x] = density
                acc = acc + fold(density * density)
        return acc

    norm_now = total(lax.fori_loop(0, count, start, none))

    for turn in range(ITERS):
        def apply(block, acc):
            for i in range(STEP):
                x = block * STEP + i
                plane = direction[x + 1]
                result = operate_plane(direction[x], plane, direction[x + 2])
                image[x] = result
                acc = acc + fold(plane * result)
            return acc

        step_len = norm_now / total(lax.fori_loop(0, B // STEP, apply, none))

        if turn == ITERS - 1:
            break

        def advance(block, acc):
            for i in range(STEP):
                x = block * STEP + i
                moved = step_len * direction[x + 1]
                potential[x] = moved if turn == 0 else potential[x] + moved
                left = resid[x] - step_len * image[x]
                resid[x] = left
                acc = acc + fold(left * left)
            return acc

        norm_next = total(lax.fori_loop(0, B // STEP, advance, none))
        ratio = norm_next / norm_now

        def renew(block, unused):
            for i in range(STEP):
                x = block * STEP + i
                direction[x + 1] = resid[x] + ratio * direction[x + 1]
            return unused

        lax.fori_loop(0, B // STEP, renew, 0)
        norm_now = norm_next

    def finish(owner, unused):
        for chunk in range(chunks):
            for i in range(each):
                x = place(owner, chunk, i)
                found = (potential[x] + step_len * direction[x + 1]) * keep
                out_refs[chunk][owner, 0, pl.ds(i * ROWS, ROWS)] = found * partner[x]
                wide[PAD + x] = found * in_refs[chunk][owner, 0, pl.ds(i * ROWS, ROWS)]
        return unused

    lax.fori_loop(0, count, finish, 0)

    def give_back(owner, unused):
        for chunk in range(chunks):
            for i in range(each):
                x = place(owner, chunk, i)
                out_refs[chunk][owner, 1, pl.ds(i * ROWS, ROWS)] = shift_plane(wide[PAD + x + dx], -dy, -dz)
        return unused

    lax.fori_loop(0, count, give_back, 0)


def solve_pair(info, parts):
    box = (B, ROWS, LANES)
    vmem = pl.BlockSpec(memory_space=pltpu.VMEM)
    return pl.pallas_call(
        solve_kernel,
        in_specs=[pl.BlockSpec(memory_space=pltpu.SMEM)] + [vmem] * len(parts),
        out_specs=[vmem] * len(parts),
        out_shape=[jax.ShapeDtypeStruct(p.shape, jnp.float32) for p in parts],
        scratch_shapes=[
            pltpu.VMEM((B + 2 * PAD, ROWS, LANES), jnp.float32),
            pltpu.VMEM(box, jnp.float32),
            pltpu.VMEM((B + 2, ROWS, LANES), jnp.float32),
            pltpu.VMEM(box, jnp.float32),
            pltpu.VMEM(box, jnp.float32),
            pltpu.VMEM(box, jnp.float32),
        ],
        compiler_params=pltpu.CompilerParams(vmem_limit_bytes=32 * 1024 * 1024),
        cost_estimate=pl.CostEstimate(flops=0, bytes_accessed=40 * 1024 * 1024, transcendentals=0),
        name="solve_pair",
    )(info, *parts)


def owner_body(orbitals, anchors, pair_slots):
    grid_count = lax.axis_size("grid")
    owner_count = lax.axis_size("grp") * grid_count
    group_idx = lax.axis_index("grp")
    place_idx = lax.axis_index("grid")
    assignment = deal_evenly(pair_slots, owner_count, PAIR_DEV)
    slots = assignment.shape[1]
    filled = assignment[..., 0] >= 0
    safe_ids = jnp.maximum(assignment, 0)
    group_table = lax.dynamic_slice_in_dim(safe_ids, group_idx * grid_count, grid_count, 0)
    ids = jnp.transpose(group_table, (1, 0, 2)).reshape(-1)
    owner_idx = group_idx * grid_count + place_idx
    own_pairs = safe_ids[owner_idx]
    offsets = anchors[own_pairs[:, 1]] - anchors[own_pairs[:, 0]]
    info = jnp.concatenate([offsets, filled[owner_idx].astype(jnp.int32)[:, None]], axis=1)

    norb_local, cells = orbitals.shape
    stacked = orbitals.reshape(norb_local, cells // LANES, LANES)
    chunks = math.gcd(MOST_CHUNKS, cells // (B * B))
    rows = stacked.shape[1] // chunks
    arrived = [[None] * chunks for _ in range(slots)]
    for chunk in range(chunks):
        pieces = lax.all_gather(stacked[:, chunk * rows : (chunk + 1) * rows], "grp", axis=0, tiled=True)
        outgoing = gather_pieces(ids, pieces, slots, grid_count)
        for slot in range(slots):
            arrived[slot][chunk] = lax.all_to_all(outgoing[slot], "grid", split_axis=0, concat_axis=0, tiled=True)
    returned = []
    for slot in range(slots):
        terms = solve_pair(info[slot], arrived[slot])
        returned.append(
            [lax.all_to_all(t, "grid", split_axis=0, concat_axis=0, tiled=True) for t in terms]
        )
    results = []
    for chunk in range(chunks):
        summed = scatter_pieces(ids, [r[chunk] for r in returned], anchors.shape[0])
        results.append(lax.psum_scatter(summed, "grp", scatter_dimension=0, tiled=True))
    return jnp.concatenate(results, axis=1).reshape(norb_local, cells)


MESH = pl.DeviceIdType.MESH
HALO = 3
WAVES = 4
TRIALS = 12
SUB = 8


def remote(src, dst, send_sem, recv_sem, device):
    return pltpu.make_async_remote_copy(
        src_ref=src, dst_ref=dst, send_sem=send_sem, recv_sem=recv_sem, device_id=device, device_id_type=MESH
    )


def spot():
    grp = lax.axis_index("grp")
    place = lax.axis_index("grid")
    across = grp + 1 - 2 * lax.rem(grp, 2)
    along = lax.rem(grp + 2, 4)
    corner = lax.rem(across + 2, 4)
    return grp, place, across, along, corner


def greet(chips, wide=False):
    grp, place, across, along, corner = spot()
    chip = place // 2
    core = lax.rem(place, 2)
    barrier = pltpu.get_barrier_semaphore()
    peers = [(across, place), (along, place), (grp, 2 * chip + 1 - core)] + ([(corner, place)] if wide else [])
    for device in peers:
        pl.semaphore_signal(barrier, inc=1, device_id=device, device_id_type=MESH)

    @pl.when(chip > 0)
    def below():
        pl.semaphore_signal(barrier, inc=1, device_id=(grp, place - 2), device_id_type=MESH)

    @pl.when(chip < chips - 1)
    def above():
        pl.semaphore_signal(barrier, inc=1, device_id=(grp, place + 2), device_id_type=MESH)

    ends = jnp.where(chip > 0, 1, 0) + jnp.where(chip < chips - 1, 1, 0)
    pl.semaphore_wait(barrier, len(peers) + ends)


class Relay:
    def __init__(self, wins, send_sem, recv_sem, signs, chips, marks):
        self.wins, self.send_sem, self.recv_sem, self.signs, self.chips = wins, send_sem, recv_sem, signs, chips
        self.grp, self.place = lax.axis_index("grp"), lax.axis_index("grid")
        self.chip = self.place // 2
        self.core = lax.rem(self.place, 2)
        self.half = wins[0].shape[0] // 2
        self.planes = wins[0].shape[1] // 6
        self.deep, self.far, self.mid = marks

    def offset(self, sign, hop):
        return 2 * self.planes * (2 - hop if sign > 0 else hop)

    def region(self, chunk, side, hop, core, size, skip=0):
        start = self.offset(self.signs[side], hop) + self.planes * core
        return self.wins[chunk].at[pl.ds(side * self.half + skip, size), pl.ds(start, self.planes)]

    def comes(self, side, hop):
        source = self.chip - self.signs[side] * hop
        return source >= 0 if self.signs[side] > 0 else source < self.chips

    def goes(self, side, hop):
        source = self.chip + self.signs[side] - self.signs[side] * hop
        if self.signs[side] > 0:
            return (self.chip + 1 < self.chips) & (source >= 0)
        return (self.chip - 1 >= 0) & (source < self.chips)

    def spans(self, side, hop, core, act):
        if hop == 0:
            act(self.half)
        else:
            near = 1 if self.signs[side] > 0 else 0
            most, least = (self.half, self.mid) if hop == 1 else (self.far, self.deep)
            if most == least:
                act(most)
                return

            @pl.when(core == near)
            def whole():
                act(most)

            @pl.when(core != near)
            def some():
                act(least)

    def onward(self, chunk, side, hop, size, here=None):
        source = self.region(chunk, side, hop - 1 if here is None else here, self.core, size)
        there = self.region(chunk, side, hop, self.core, size)
        return remote(
            source, there, self.send_sem.at[chunk, side, hop - 1], self.recv_sem.at[chunk, side, hop - 1],
            (self.grp, self.place + 2 * self.signs[side]),
        )

    def rest(self, chunk, side, act, here=0):
        def copy(size):
            source = self.region(chunk, side, here, self.core, size - self.far, self.far)
            there = self.region(chunk, side, 1, self.core, size - self.far, self.far)
            act(remote(
                source, there, self.send_sem.at[chunk, side, 5], self.recv_sem.at[chunk, side, 5],
                (self.grp, self.place + 2 * self.signs[side]),
            ))

        if self.far < self.half:
            self.spans(side, 1, self.core, copy)

    def ahead(self, side, hop, act):
        if hop == 1:
            act(self.far)
        else:
            self.spans(side, hop, self.core, act)

    def beside(self, chunk, side, hop, core, size):
        part = self.region(chunk, side, hop, core, size)
        return remote(
            part, part, self.send_sem.at[chunk, side, 2 + hop], self.recv_sem.at[chunk, side, 2 + hop],
            (self.grp, 2 * self.chip + 1 - self.core),
        )

    def clear(self):
        for side in range(2):
            for hop in (1, 2):
                start = self.offset(self.signs[side], hop)

                @pl.when(jnp.logical_not(self.comes(side, hop)))
                def fill(side=side, start=start):
                    for win in self.wins:
                        def zero(slot, unused, win=win):
                            win[slot, pl.ds(start, 2 * self.planes)] = jnp.zeros(
                                (2 * self.planes,) + win.shape[2:], jnp.float32
                            )
                            return unused

                        lax.fori_loop(side * self.half, (side + 1) * self.half, zero, 0)

    def pass_on(self, chunk, side, hop):
        @pl.when(self.goes(side, hop))
        def go():
            self.ahead(side, hop, lambda size: self.onward(chunk, side, hop, size).start())
            if hop == 1:
                self.rest(chunk, side, lambda copy: copy.start())

    def begin(self, chunk, sides=(0, 1)):
        for side in sides:
            self.pass_on(chunk, side, 1)
        for side in sides:
            self.beside(chunk, side, 0, self.core, self.half).start()

    def arrive(self, chunk, side, hop):
        @pl.when(self.comes(side, hop))
        def got():
            self.ahead(side, hop, lambda size: self.onward(chunk, side, hop, size, hop).wait_recv())

    def spread(self, chunk, side, hop):
        @pl.when(self.comes(side, hop))
        def share():
            if hop == 1:
                self.rest(chunk, side, lambda copy: copy.wait_recv(), 1)
            self.spans(side, hop, self.core, lambda size: self.beside(chunk, side, hop, self.core, size).start())

    def first(self, chunk):
        for side in range(2):
            self.arrive(chunk, side, 1)
            self.pass_on(chunk, side, 2)

    def share(self, chunk):
        for side in range(2):
            self.spread(chunk, side, 1)

    def second(self, chunk):
        for side in range(2):
            self.arrive(chunk, side, 2)
            self.spread(chunk, side, 2)

    def settle(self, chunk):
        other = 1 - self.core
        for side in range(2):
            self.beside(chunk, side, 0, other, self.half).wait_recv()
            for hop in (1, 2):
                @pl.when(self.comes(side, hop))
                def got(side=side, hop=hop):
                    self.spans(side, hop, other, lambda size: self.beside(chunk, side, hop, other, size).wait_recv())

    def drain(self):
        for chunk in range(len(self.wins)):
            for side in range(2):
                self.beside(chunk, side, 0, self.core, self.half).wait_send()
                for hop in (1, 2):
                    @pl.when(self.comes(side, hop))
                    def sent(chunk=chunk, side=side, hop=hop):
                        self.spans(
                            side, hop, self.core,
                            lambda size: self.beside(chunk, side, hop, self.core, size).wait_send(),
                        )

                    @pl.when(self.goes(side, hop))
                    def passed(chunk=chunk, side=side, hop=hop):
                        self.ahead(side, hop, lambda size: self.onward(chunk, side, hop, size).wait_send())
                        if hop == 1:
                            self.rest(chunk, side, lambda copy: copy.wait_send())


def bring_kernel(chips, tbl, orb, moved, fixed, *scratch):
    count = moved.shape[0]
    pools, wins = scratch[:count], scratch[count : 2 * count]
    own_sem, xy_send, xy_recv, z_send, z_recv = scratch[2 * count :]
    grp, place, across, along, corner = spot()
    core = lax.rem(place, 2)
    norb, planes = orb.shape[:2]
    part = norb // 2
    slots = moved.shape[1]
    relay = Relay(wins, z_send, z_recv, (1, -1), chips, (slots // 2,) * 3)

    def block(chunk, owner, start, size):
        return pools[chunk].at[pl.ds(owner * norb + start, size)]

    def stage(chunk):
        return pltpu.make_async_copy(
            orb.at[:, :, pl.ds(chunk * SUB, SUB)], block(chunk, grp, 0, norb), own_sem.at[chunk]
        )

    def hop(chunk, kind, owner, start, size, target):
        ref = block(chunk, owner, start, size)
        return remote(ref, ref, xy_send.at[chunk, kind], xy_recv.at[chunk, kind], (target, place))

    def direct(chunk, owners):
        return hop(chunk, 0, owners[0], 0, norb, across), hop(chunk, 1, owners[1], 0, norb, along)

    def turned(chunk, owners):
        return hop(chunk, 2, owners[0], 0, part, along), hop(chunk, 3, owners[1], part, part, across)

    for chunk in range(count):
        stage(chunk).start()
    greet(chips)
    relay.clear()

    def send_own(chunk):
        stage(chunk).wait()
        for copy in direct(chunk, (grp, grp)):
            copy.start()

    send_own(0)
    send_own(1)
    for step in range(count + 4):
        if step < count:
            for copy in direct(step, (across, along)):
                copy.wait_recv()
            for copy in turned(step, (across, along)):
                copy.start()
            if step + 2 < count:
                send_own(step + 2)
        chunk = step - 1
        if 0 <= chunk < count:
            for copy in turned(chunk, (corner, corner)):
                copy.wait_recv()
            for side in range(2):
                start = relay.offset(relay.signs[side], 0) + planes * core

                def pick(slot, unused, start=start, chunk=chunk):
                    wins[chunk][slot, pl.ds(start, planes)] = pools[chunk][tbl[0, slot]]
                    fixed[chunk, slot] = pools[chunk][tbl[1, slot]]
                    return unused

                lax.fori_loop(side * (slots // 2), (side + 1) * (slots // 2), pick, 0)
            relay.begin(chunk)
        chunk = step - 2
        if 0 <= chunk < count:
            relay.first(chunk)
            relay.share(chunk)
        chunk = step - 3
        if 0 <= chunk < count:
            relay.second(chunk)
        chunk = step - 4
        if 0 <= chunk < count:
            relay.settle(chunk)

            def choose(slot, unused, chunk=chunk):
                first = tbl[2, slot] + planes * core
                for plane in range(planes):
                    moved[chunk, slot, plane] = wins[chunk][slot, first + plane]
                return unused

            lax.fori_loop(0, slots, choose, 0)
    for chunk in range(count):
        for copy in direct(chunk, (grp, grp)) + turned(chunk, (across, along)):
            copy.wait_send()
    relay.drain()


def bring(table, stacked, slots, groups, chips):
    norb, planes, rows, lanes = stacked.shape
    chunks = rows // SUB
    vmem = pl.BlockSpec(memory_space=pltpu.VMEM)
    dma = pltpu.SemaphoreType.DMA
    shape = jax.ShapeDtypeStruct((chunks, slots, planes, SUB, lanes), jnp.float32)
    return pl.pallas_call(
        functools.partial(bring_kernel, chips),
        in_specs=[pl.BlockSpec(memory_space=pltpu.SMEM), pl.BlockSpec(memory_space=pl.ANY)],
        out_specs=[vmem, vmem],
        out_shape=[shape, shape],
        scratch_shapes=[pltpu.VMEM((groups * norb, planes, SUB, lanes), jnp.float32)] * chunks
        + [pltpu.VMEM((slots, 6 * planes, SUB, lanes), jnp.float32)] * chunks
        + [dma((chunks,)), dma((chunks, 4)), dma((chunks, 4)), dma((chunks, 2, 6)), dma((chunks, 2, 6))],
        compiler_params=pltpu.CompilerParams(
            collective_id=0, has_side_effects=True, vmem_limit_bytes=48 * 1024 * 1024
        ),
        name="bring",
    )(table, stacked)


def pair_kernel(tbl, moved, fixed, dens, partner):
    def go(slot, unused):
        second = tbl[3, slot] > 0
        dy, dz = tbl[4, slot], tbl[5, slot]
        for x in range(moved.shape[2]):
            left = moved[:, slot, x].reshape(ROWS, LANES)
            right = fixed[:, slot, x].reshape(ROWS, LANES)
            other = shift_plane(jnp.where(second, left, right), dy, dz)
            dens[slot, x] = jnp.where(second, right, left) * other
            partner[slot, x] = other
        return unused

    lax.fori_loop(0, moved.shape[1], go, 0)


def pair_up(table, moved, fixed):
    chunks, slots, planes, sub, lanes = moved.shape
    vmem = pl.BlockSpec(memory_space=pltpu.VMEM)
    shape = jax.ShapeDtypeStruct((slots, planes, ROWS, lanes), jnp.float32)
    return pl.pallas_call(
        pair_kernel,
        in_specs=[pl.BlockSpec(memory_space=pltpu.SMEM), vmem, vmem],
        out_specs=[vmem, vmem],
        out_shape=[shape, shape],
        compiler_params=pltpu.CompilerParams(vmem_limit_bytes=24 * 1024 * 1024),
        name="pair_up",
    )(table, moved, fixed)


def inner(plane):
    shape = plane.shape
    lane = lane_ids(shape)
    row = lax.broadcasted_iota(jnp.int32, shape, 0)
    z = jnp.bitwise_and(lane, B - 1)
    upper_z = jnp.where(z < B - 1, pltpu.roll(plane, LANES - 1, 1), 0.0)
    lower_z = jnp.where(z > 0, pltpu.roll(plane, 1, 1), 0.0)
    half = pltpu.roll(plane, B, 1)
    down = jnp.where(row > 0, pltpu.roll(half, 1, 0), 0.0)
    up = jnp.where(row < ROWS - 1, pltpu.roll(half, ROWS - 1, 0), 0.0)
    return 6.0 * plane - ((half + jnp.where(lane < B, down, up)) + (upper_z + lower_z))


def krylov_weights(m):
    a0 = m[0] / m[1]
    rr1 = a0 * a0 * m[2] - m[0]
    p, q = 1.0 + rr1 / m[0], -a0
    a1 = rr1 / (p * p * m[1] + 2.0 * p * q * m[2] + q * q * m[3])
    s1, s2 = -a0 - a1 * p, -a1 * q
    rr2 = (m[0] + s1 * s1 * m[2] + s2 * s2 * m[4]) + 2.0 * (s1 * m[1] + s2 * m[2] + s1 * s2 * m[3])
    b1 = rr2 / rr1
    e0, e1, e2 = 1.0 + b1 * p, s1 + b1 * q, s2
    bend = e0 * e0 * m[1] + e1 * e1 * m[3] + e2 * e2 * m[5]
    a2 = rr2 / (bend + 2.0 * (e0 * e1 * m[2] + e0 * e2 * m[3] + e1 * e2 * m[4]))
    return a0 + a1 * p + a2 * e0, a1 * q + a2 * e1, a2 * e2


def solve_slabs_kernel(places, tbl, dens, pot, wide, one, two, sums, gathered, weights, h_send, h_recv, s_send, s_recv):
    grp, place = lax.axis_index("grp"), lax.axis_index("grid")
    slots, planes = dens.shape[:2]
    first, last = HALO, HALO + planes - 1
    each = slots // WAVES
    barrier = pltpu.get_barrier_semaphore()
    for step in range(1, places):
        pl.semaphore_signal(
            barrier, inc=1, device_id=(grp, lax.rem(place + step, places)), device_id_type=MESH
        )
    pl.semaphore_wait(barrier, places - 1)

    def rise(wave):
        return remote(
            dens.at[pl.ds(wave * each, each), pl.ds(planes - HALO + 1, HALO - 1)],
            wide.at[pl.ds(wave * each, each), pl.ds(1, HALO - 1)],
            h_send.at[wave, 0], h_recv.at[wave, 0], (grp, lax.rem(place + 1, places)),
        )

    def sink(wave):
        return remote(
            dens.at[pl.ds(wave * each, each), pl.ds(0, HALO)],
            wide.at[pl.ds(wave * each, each), pl.ds(HALO + planes, HALO)],
            h_send.at[wave, 1], h_recv.at[wave, 1], (grp, lax.rem(place + places - 1, places)),
        )

    lowest, highest = place == 0, place == places - 1
    for wave in range(WAVES):
        @pl.when(jnp.logical_not(highest))
        def send_up(wave=wave):
            rise(wave).start()

        @pl.when(jnp.logical_not(lowest))
        def send_down(wave=wave):
            sink(wave).start()

    blank = jnp.zeros((HALO, ROWS, LANES), jnp.float32)

    def copy_in(slot, unused):
        wide[slot, pl.ds(HALO, planes)] = dens[slot]
        one[slot, 1] = blank[0]
        one[slot, last + 3] = blank[0]
        one[slot, 0] = blank[0]
        return unused

    lax.fori_loop(0, slots, copy_in, 0)

    @pl.when(lowest)
    def no_below():
        def fill(slot, unused):
            wide[slot, pl.ds(0, HALO)] = blank
            return unused

        lax.fori_loop(0, slots, fill, 0)

    @pl.when(highest)
    def no_above():
        def fill(slot, unused):
            wide[slot, pl.ds(HALO + planes, HALO)] = blank
            return unused

        lax.fori_loop(0, slots, fill, 0)

    lane = lax.broadcasted_iota(jnp.int32, (1, LANES), 1)
    none = jnp.zeros((8, LANES), jnp.float32)

    def row_of(parts):
        row = jnp.zeros((1, LANES), jnp.float32)
        for at, part in parts:
            row = row + jnp.where(lane == at, total(part), 0.0)
        return row

    def work(slot, unused):
        low, high = tbl[6, slot], tbl[6, slot] + B

        def live(e):
            x = planes * place + e - HALO
            return jnp.where((x >= low) & (x < high), 1.0, 0.0).astype(jnp.float32)

        m0, m1, m2, m3, m4, m5 = none, none, none, none, none, none
        for e in range(first - 1, last + 3):
            value = live(e) * (inner(wide[slot, e]) - (wide[slot, e - 1] + wide[slot, e + 1]))
            one[slot, e] = value
            if first <= e <= last:
                source = wide[slot, e]
                m0 = m0 + fold(source * source)
                m1 = m1 + fold(source * value)
                m2 = m2 + fold(value * value)
        bent = None
        for e in range(first, last + 2):
            value = live(e) * (inner(one[slot, e]) - (one[slot, e - 1] + one[slot, e + 1]))
            two[slot, e] = value
            if e > first:
                m5 = m5 - 2.0 * fold(value * two[slot, e - 1])
            if e <= last:
                m3 = m3 + fold(one[slot, e] * value)
                m4 = m4 + fold(value * value)
                m5 = m5 + fold(value * inner(value))
        sums[pl.ds(slot, 1)] = row_of(enumerate((m0, m1, m2, m3, m4, m5)))
        return unused

    def rim(slot, spots, pairs):
        low, high = tbl[6, slot], tbl[6, slot] + B
        m2, m3, m4, m5 = none, none, none, none
        for e, fresh in spots:
            if fresh:
                x = planes * place + e - HALO
                alive = jnp.where((x >= low) & (x < high), 1.0, 0.0).astype(jnp.float32)
                two[slot, e] = alive * (inner(one[slot, e]) - (one[slot, e - 1] + one[slot, e + 1]))
        for e, fresh in spots:
            value, before = two[slot, e], one[slot, e]
            m2 = m2 + fold(before * before)
            m3 = m3 + fold(before * value)
            m4 = m4 + fold(value * value)
            m5 = m5 + fold(value * inner(value))
        for e in pairs:
            m5 = m5 - 2.0 * fold(two[slot, e] * two[slot, e + 1])
        sums[pl.ds(slot, 1)] = sums[pl.ds(slot, 1)] + row_of(((2, m2), (3, m3), (4, m4), (5, m5)))

    for wave in range(WAVES):
        @pl.when(jnp.logical_not(lowest))
        def got_below(wave=wave):
            rise(wave).wait_recv()

        @pl.when(jnp.logical_not(highest))
        def got_above(wave=wave):
            sink(wave).wait_recv()

        lax.fori_loop(wave * each, (wave + 1) * each, work, 0)

    @pl.when(lowest)
    def rim_below():
        def go(slot, unused):
            rim(slot, ((first - 2, True), (first - 1, True)), (first - 2, first - 1))
            return unused

        lax.fori_loop(0, slots, go, 0)

    @pl.when(highest)
    def rim_above():
        def go(slot, unused):
            rim(slot, ((last + 1, False), (last + 2, True)), (last + 1,))
            return unused

        lax.fori_loop(0, slots, go, 0)

    def tell(step):
        return remote(
            sums, gathered.at[place], s_send.at[step - 1], s_recv.at[step - 1],
            (grp, lax.rem(place + step, places)),
        )

    def hear(step):
        source = lax.rem(place + places - step, places)
        return remote(
            sums, gathered.at[source], s_send.at[step - 1], s_recv.at[step - 1],
            (grp, lax.rem(place + step, places)),
        )

    for step in range(1, places):
        tell(step).start()
    gathered[place] = sums[...]
    for step in range(1, places):
        hear(step).wait_recv()
    whole = gathered[0]
    for at in range(1, places):
        whole = whole + gathered[at]
    lanes = lax.broadcasted_iota(jnp.int32, whole.shape, 1)
    moments = [jnp.sum(jnp.where(lanes == at, whole, 0.0), axis=1, keepdims=True) for at in range(6)]
    for at, weight in enumerate(krylov_weights(moments)):
        weights[at] = jnp.broadcast_to(weight, whole.shape)

    def finish(slot, unused):
        w0, w1, w2 = [weights[at, pl.ds(slot, 1)] for at in range(3)]
        for x in range(planes):
            e = x + HALO
            pot[slot, x] = w0 * wide[slot, e] + w1 * one[slot, e] + w2 * two[slot, e]
        return unused

    lax.fori_loop(0, slots, finish, 0)
    for wave in range(WAVES):
        @pl.when(jnp.logical_not(highest))
        def sent_up(wave=wave):
            rise(wave).wait_send()

        @pl.when(jnp.logical_not(lowest))
        def sent_down(wave=wave):
            sink(wave).wait_send()

    for step in range(1, places):
        tell(step).wait_send()


def solve_slabs(table, dens, places, ident):
    slots, planes, rows, lanes = dens.shape
    vmem = pl.BlockSpec(memory_space=pltpu.VMEM)
    dma = pltpu.SemaphoreType.DMA
    tall = pltpu.VMEM((slots, planes + 2 * HALO, rows, lanes), jnp.float32)
    return pl.pallas_call(
        functools.partial(solve_slabs_kernel, places),
        in_specs=[pl.BlockSpec(memory_space=pltpu.SMEM), vmem],
        out_specs=vmem,
        out_shape=jax.ShapeDtypeStruct(dens.shape, jnp.float32),
        scratch_shapes=[
            tall, tall, tall,
            pltpu.VMEM((slots, lanes), jnp.float32),
            pltpu.VMEM((places, slots, lanes), jnp.float32),
            pltpu.VMEM((3, slots, lanes), jnp.float32),
            dma((WAVES, 2)), dma((WAVES, 2)), dma((places - 1,)), dma((places - 1,)),
        ],
        compiler_params=pltpu.CompilerParams(
            collective_id=ident, has_side_effects=True, vmem_limit_bytes=40 * 1024 * 1024
        ),
        name="solve_slabs",
    )(table, dens)


def term_kernel(tbl, pot, partner, moved, fixed, going, staying):
    chunks = going.shape[0]

    def go(slot, unused):
        second = tbl[3, slot] > 0
        dy, dz = tbl[4, slot], tbl[5, slot]
        for x in range(pot.shape[1]):
            found = pot[slot, x]
            left = moved[:, slot, x].reshape(ROWS, LANES)
            right = fixed[:, slot, x].reshape(ROWS, LANES)
            term_a = found * partner[slot, x]
            term_b = shift_plane(found * jnp.where(second, right, left), -dy, -dz)
            going[:, slot, x] = jnp.where(second, term_b, term_a).reshape(chunks, SUB, LANES)
            staying[:, slot, x] = jnp.where(second, term_a, term_b).reshape(chunks, SUB, LANES)
        return unused

    lax.fori_loop(0, pot.shape[0], go, 0)


def make_terms(table, pot, partner, moved, fixed):
    vmem = pl.BlockSpec(memory_space=pltpu.VMEM)
    shape = jax.ShapeDtypeStruct(moved.shape, jnp.float32)
    return pl.pallas_call(
        term_kernel,
        in_specs=[pl.BlockSpec(memory_space=pltpu.SMEM)] + [vmem] * 4,
        out_specs=[vmem, vmem],
        out_shape=[shape, shape],
        compiler_params=pltpu.CompilerParams(vmem_limit_bytes=24 * 1024 * 1024),
        name="make_terms",
    )(table, pot, partner, moved, fixed)


def hand_back_kernel(chips, tbl, last, going, staying, out, *scratch):
    count, slots = going.shape[:2]
    wins, chains, outs1, outs2, ins1, ins2 = [scratch[i * count : (i + 1) * count] for i in range(6)]
    xy_send, xy_recv, z_send, z_recv = scratch[6 * count :]
    grp, place, across, along, corner = spot()
    core = lax.rem(place, 2)
    norb, planes = out.shape[:2]
    part = norb // 2
    relay = Relay(wins, z_send, z_recv, (-1, 1), chips, (slots // 2,) * 3)
    greet(chips)
    relay.clear()

    def start(chunk):
        for side in range(2):
            at = relay.offset(relay.signs[side], 0) + planes * core

            def place_in(slot, unused, at=at):
                wins[chunk][slot, pl.ds(at, planes)] = going[chunk, slot]
                return unused

            lax.fori_loop(side * (slots // 2), (side + 1) * (slots // 2), place_in, 0)
        relay.begin(chunk)

    def swap(chunk, kind):
        src = (outs1 if kind < 2 else outs2)[chunk].at[kind % 2]
        dst = (ins1 if kind < 2 else ins2)[chunk].at[kind % 2]
        target = (across, along, along, across)[kind]
        return remote(src, dst, xy_send.at[chunk, kind], xy_recv.at[chunk, kind], (target, place))

    start(0)
    start(1)
    for step in range(count + 4):
        if step < count:
            relay.first(step)
            relay.share(step)
            if step + 2 < count:
                start(step + 2)
        chunk = step - 1
        if 0 <= chunk < count:
            relay.second(chunk)
        chunk = step - 2
        if 0 <= chunk < count:
            relay.settle(chunk)
            chain = chains[chunk]
            chain[2 * slots] = jnp.zeros(chain.shape[1:], jnp.float32)

            def link_fixed(slot, unused, chain=chain, chunk=chunk):
                chain[slot] = staying[chunk, slot] + chain[tbl[8, slot]]
                return unused

            def link_moved(slot, unused, chain=chain, chunk=chunk):
                first = tbl[7, slot] + planes * core
                for plane in range(planes):
                    chain[slots + slot, plane] = wins[chunk][slot, first + plane] + chain[tbl[9, slot], plane]
                return unused

            lax.fori_loop(0, slots, link_fixed, 0)
            lax.fori_loop(0, slots, link_moved, 0)

            def pack(i, unused, chain=chain, chunk=chunk):
                outs1[chunk][0, i] = chain[last[across * norb + i]]
                outs1[chunk][0, part + i] = chain[last[corner * norb + i]]
                outs1[chunk][1, i] = chain[last[along * norb + part + i]]
                outs1[chunk][1, part + i] = chain[last[corner * norb + part + i]]
                return unused

            lax.fori_loop(0, part, pack, 0)
            swap(chunk, 0).start()
            swap(chunk, 1).start()
        chunk = step - 3
        if 0 <= chunk < count:
            chain = chains[chunk]
            swap(chunk, 0).wait_recv()

            def add_across(i, unused, chain=chain, chunk=chunk):
                outs2[chunk][0, i] = ins1[chunk][0, part + i] + chain[last[along * norb + i]]
                return unused

            lax.fori_loop(0, part, add_across, 0)
            swap(chunk, 2).start()
            swap(chunk, 1).wait_recv()

            def add_along(i, unused, chain=chain, chunk=chunk):
                outs2[chunk][1, i] = ins1[chunk][1, part + i] + chain[last[across * norb + part + i]]
                return unused

            lax.fori_loop(0, part, add_along, 0)
            swap(chunk, 3).start()
        chunk = step - 4
        if 0 <= chunk < count:
            chain = chains[chunk]
            swap(chunk, 2).wait_recv()
            swap(chunk, 3).wait_recv()
            for side in range(2):
                def keep(i, unused, side=side, chain=chain, chunk=chunk):
                    orbit = side * part + i
                    found = ins1[chunk][side, i] + ins2[chunk][side, i]
                    out[orbit, :, pl.ds(chunk * SUB, SUB)] = found + chain[last[grp * norb + orbit]]
                    return unused

                lax.fori_loop(0, part, keep, 0)
    for chunk in range(count):
        for kind in range(4):
            swap(chunk, kind).wait_send()
    relay.drain()


def hand_back(table, last, going, staying, norb, chips):
    chunks, slots, planes, sub, lanes = going.shape
    vmem = pl.BlockSpec(memory_space=pltpu.VMEM)
    smem = pl.BlockSpec(memory_space=pltpu.SMEM)
    dma = pltpu.SemaphoreType.DMA
    def room(*lead):
        return [pltpu.VMEM(lead + (planes, sub, lanes), jnp.float32)] * chunks
    wins = [pltpu.VMEM((slots, 6 * planes, sub, lanes), jnp.float32)] * chunks
    return pl.pallas_call(
        functools.partial(hand_back_kernel, chips),
        in_specs=[smem, smem, vmem, vmem],
        out_specs=vmem,
        out_shape=jax.ShapeDtypeStruct((norb, planes, chunks * sub, lanes), jnp.float32),
        scratch_shapes=wins + room(2 * slots + 1) + room(2, norb) + room(2, norb // 2)
        + room(2, norb) + room(2, norb // 2)
        + [dma((chunks, 4)), dma((chunks, 4)), dma((chunks, 2, 6)), dma((chunks, 2, 6))],
        compiler_params=pltpu.CompilerParams(
            collective_id=2, has_side_effects=True, vmem_limit_bytes=56 * 1024 * 1024
        ),
        name="hand_back",
    )(table, last, going, staying)


def plan_kernel(cap, planes, me_ref, anchors, pairs, tbl, links, fits, spots, masks, lists, mine, counts):
    groups = 4
    orbits = anchors.shape[1]
    local = orbits // groups
    depth, unused, owners = pairs.shape
    entries = depth * owners
    each = tbl.shape[1]
    half = each // 2
    extra = (groups - 1) * cap
    final = extra
    prior = final + local + extra
    ends = prior + extra
    spare = ends + local
    worst = 1 << 20
    me = me_ref[0]

    def unpack(code):
        return jnp.bitwise_and(code, 1023), jnp.bitwise_and(jnp.right_shift(code, 10), 1023)

    def clean(i, unused):
        links[i] = 0
        links[prior + i] = extra
        return unused

    def close(i, unused):
        links[final + i] = 2 * each
        return unused

    def own(i, unused):
        links[ends + i] = extra
        spots[me * local + i] = i
        return unused

    lax.fori_loop(0, extra, clean, 0, unroll=5)
    lax.fori_loop(0, local + extra, close, 0, unroll=4)
    lax.fori_loop(0, local, own, 0, unroll=4)

    def sort(i, tails, layer):
        a, b = pairs[layer, 0, i], pairs[layer, 1, i]
        filled = jnp.where(a >= 0, 1, 0)
        dx = anchors[0, jnp.maximum(b, 0)] - anchors[0, jnp.maximum(a, 0)]
        reach = jnp.abs(dx)
        kind = 3 - sum(jnp.where(reach > planes * k, 1, 0) for k in (1, 2, 3))
        step = jnp.left_shift(kind, 3)
        tail = jnp.bitwise_and(jnp.right_shift(tails, step), 255)
        code = a + jnp.left_shift(b, 10) + jnp.left_shift(dx + B, 20)
        lists[jnp.where(filled > 0, kind * entries + tail, 4 * entries)] = code
        return tails + jnp.left_shift(filled, step)

    zero = jnp.int32(0)
    packed = zero
    for layer in range(depth):
        packed = lax.fori_loop(0, owners, functools.partial(sort, layer=layer), packed, unroll=8)
    tails = [jnp.bitwise_and(jnp.right_shift(packed, 8 * k), 255) for k in range(4)]
    fits[0] = 0

    def trial(turn):
        def reset(i, unused):
            for g in range(groups):
                masks[g * local + i] = (15 - (1 << g)) + (g << 10)
            return unused

        lax.fori_loop(0, local, reset, 0, unroll=8)
        state = (zero,) * (groups + 1)
        for kind, limit in enumerate((half // 4, half // 2, 3 * half // 4, half)):
            size = tails[kind]
            base = lax.rem(turn * 5, jnp.maximum(size, 1))
            flip = jnp.bitwise_and(turn, 1) > 0

            def deal(i, state, kind=kind, limit=limit, size=size, base=base, flip=flip):
                filled, bad = state[:groups], state[groups]
                at = i + base
                at = jnp.where(at >= size, at - size, at)
                code = lists[kind * entries + jnp.where(flip, size - 1 - at, at)]
                a, b = unpack(code)
                word_a, word_b = masks[a], masks[b]
                step_a, step_b = jnp.right_shift(word_a, 8), jnp.right_shift(word_b, 8)
                same = jnp.where(step_a == step_b, 1, 0)

                def needs(h, count):
                    new_a = jnp.bitwise_and(jnp.right_shift(word_a, h), 1)
                    new_b = jnp.bitwise_and(jnp.right_shift(word_b, h), 1)
                    had_a = jnp.bitwise_and(jnp.right_shift(count, step_a), 15)
                    had_b = jnp.bitwise_and(jnp.right_shift(count, step_b), 15) + jnp.bitwise_and(new_a, same)
                    return new_a, new_b, had_a, had_b

                best = jnp.int32(worst)
                for h in range(groups):
                    new_a, new_b, had_a, had_b = needs(h, filled[h])
                    need = jnp.maximum(jnp.where(new_a > 0, had_a + 1, 0), jnp.where(new_b > 0, had_b + 1, 0))
                    seats = jnp.right_shift(filled[h], 16)
                    cost = jnp.left_shift(new_a + new_b, 4) + jnp.left_shift(need, 3) + (jnp.left_shift(seats, 2) + h)
                    best = jnp.minimum(best, jnp.where((seats < 2 * limit) & (need <= cap), cost, worst))
                good = best < worst
                flag = jnp.where(good, 1, 0)
                column = jnp.bitwise_and(best, 3)
                count = filled[0]
                for h in range(1, groups):
                    count = jnp.where(column == h, filled[h], count)
                new_a, new_b, had_a, had_b = needs(column, count)
                seats = jnp.right_shift(count, 16)
                seat = jnp.bitwise_and(seats, 1) * half + jnp.right_shift(seats, 1)
                grown = jnp.left_shift(new_a, step_a) + jnp.left_shift(new_b, step_b)
                grown = jnp.where(good, count + grown + (1 << 16), count)
                masks[a] = word_a - jnp.where(good, jnp.left_shift(new_a, column), 0)
                masks[b] = word_b - jnp.where(good, jnp.left_shift(new_b, column), 0)
                here = good & (column == me)
                mine[jnp.where(here, seat, each)] = code
                for orbit, step, new, had in ((a, step_a, new_a, had_a), (b, step_b, new_b, had_b)):
                    group = jnp.right_shift(step, 2)
                    at = (jnp.bitwise_xor(group, column) - 1) * cap + had
                    spots[jnp.where(here & (new > 0), orbit, orbits)] = local + at
                    links[jnp.where(good & (new > 0) & (group == me), at, spare)] = orbit - group * local
                kept = tuple(jnp.where(column == h, grown, filled[h]) for h in range(groups))
                return kept + (jnp.bitwise_or(bad, 1 - flag),)

            state = lax.fori_loop(0, size, deal, state)
        for h in range(groups):
            counts[h] = state[h]
        fits[0] = 1 - state[groups]

    def attempt(turn, unused):
        @pl.when(fits[0] == 0)
        def go():
            trial(turn)

        return unused

    lax.fori_loop(0, TRIALS, attempt, 0)

    @pl.when(fits[0] > 0)
    def settle():
        def fill(at, unused):
            code = mine[at]
            a, b = unpack(code)
            dx = jnp.right_shift(code, 20) - B
            spot_a, spot_b = spots[a], spots[b]
            rising = at < half
            second = jnp.where(rising, dx, -dx) >= 0
            shift = jnp.where(second, dx, -dx)
            tbl[0, at] = jnp.where(second, spot_b, spot_a)
            tbl[1, at] = jnp.where(second, spot_a, spot_b)
            tbl[2, at] = jnp.where(rising, 4 * planes, 0) - shift
            tbl[3, at] = jnp.where(second, 1, 0)
            tbl[4, at] = anchors[1, b] - anchors[1, a]
            tbl[5, at] = anchors[2, b] - anchors[2, a]
            tbl[6, at] = jnp.where(second, 0, shift)
            tbl[7, at] = jnp.where(rising, 0, 4 * planes) + shift
            return unused

        lax.fori_loop(0, each, fill, 0, unroll=2)
        for row, base in ((1, 0), (0, each)):
            def link(slot, unused, row=row, base=base):
                at = final + tbl[row, slot]
                tbl[9 - row, slot] = links[at]
                links[at] = base + slot
                return unused

            lax.fori_loop(0, each, link, 0, unroll=4)
        for turn in range(1, groups):
            def hook(i, unused, turn=turn):
                at = (turn - 1) * cap + i
                end = ends + links[at]
                links[prior + at] = links[end]
                links[end] = at
                return unused

            sent = jnp.bitwise_and(jnp.right_shift(counts[jnp.bitwise_xor(me, turn)], 4 * me), 15)
            lax.fori_loop(0, sent, hook, 0)


def make_plan(anchors, pair_slots, cap, each, planes):
    orbits = anchors.shape[0]
    entries = pair_slots.shape[0] * pair_slots.shape[1]
    smem = pl.BlockSpec(memory_space=pltpu.SMEM)
    local = orbits // 4
    me = jnp.full((1,), lax.axis_index("grp"), jnp.int32)
    return pl.pallas_call(
        functools.partial(plan_kernel, cap, planes),
        in_specs=[smem] * 3,
        out_specs=[smem] * 3,
        out_shape=[
            jax.ShapeDtypeStruct((10, each), jnp.int32),
            jax.ShapeDtypeStruct((9 * cap + 2 * local + 1,), jnp.int32),
            jax.ShapeDtypeStruct((1,), jnp.int32),
        ],
        scratch_shapes=[
            pltpu.SMEM((orbits + 1,), jnp.int32), pltpu.SMEM((orbits,), jnp.int32),
            pltpu.SMEM((4 * entries + 1,), jnp.int32), pltpu.SMEM((each + 1,), jnp.int32),
            pltpu.SMEM((4,), jnp.int32),
        ],
        name="plan",
    )(me, anchors.T, jnp.transpose(pair_slots, (1, 2, 0)))


def coupled(plane):
    shape = plane.shape
    lane = lane_ids(shape)
    row = lax.broadcasted_iota(jnp.int32, shape, 0)
    lower_z = jnp.where(jnp.bitwise_and(lane, B - 1) > 0, pltpu.roll(plane, 1, 1), 0.0)
    half = pltpu.roll(plane, B, 1)
    down = jnp.where(row > 0, pltpu.roll(half, 1, 0), 0.0)
    return 3.0 * plane - lower_z - jnp.where(lane < B, down, half)


def lean_kernel(chips, cap, tbl, links, orb, out, *scratch):
    count = out.shape[2]
    raws, owns, parcels, pools, wins, wins_back, chains, parcels_back, backs, tallied = [
        scratch[i * count : (i + 1) * count] for i in range(10)
    ]
    partner, wide, one, two, staying, held, sums, gathered, weights = scratch[10 * count : 10 * count + 9]
    (own_sem, xy_send, xy_recv, z_send, z_recv, yx_send, yx_recv, zb_send, zb_recv,
     h_send, h_recv, s_send, s_recv) = scratch[10 * count + 9 :]
    grp, place, across, along, corner = spot()
    core = lax.rem(place, 2)
    places = 2 * chips
    tiles, planes = orb.shape[:2]
    deep = orb.shape[4]
    norb = tiles * deep
    slots = partner.shape[0]
    half = slots // 2
    first, last = HALO, HALO + planes - 1
    each = slots // WAVES
    marks = (half // 4, half // 2, 3 * half // 4)
    relay = Relay(wins, z_send, z_recv, (1, -1), chips, marks)
    relay_back = Relay(wins_back, zb_send, zb_recv, (-1, 1), chips, marks)
    lowest, highest = place == 0, place == places - 1

    def stage(chunk):
        return pltpu.make_async_copy(orb.at[:, :, chunk], raws[chunk], own_sem.at[chunk])

    for chunk in range(count):
        stage(chunk).start()
    barrier = pltpu.get_barrier_semaphore()
    for step in range(1, places):
        pl.semaphore_signal(
            barrier, inc=1, device_id=(grp, lax.rem(place + step, places)), device_id_type=MESH
        )
    for target in (across, along, corner):
        pl.semaphore_signal(barrier, inc=1, device_id=(target, place), device_id_type=MESH)

    def parcel(chunk, kind):
        return remote(
            parcels[chunk].at[pl.ds(kind * cap, cap)], pools[chunk].at[pl.ds(norb + kind * cap, cap)],
            xy_send.at[chunk, kind], xy_recv.at[chunk, kind], ((across, along, corner)[kind], place),
        )

    def pack(chunk):
        stage(chunk).wait()

        def untile(plane, unused):
            for tile in range(tiles):
                for row in range(deep):
                    piece = raws[chunk][tile, plane, :, row, :]
                    owns[chunk][tile * deep + row, plane] = piece
                    pools[chunk][tile * deep + row, plane] = piece
            return unused

        lax.fori_loop(0, planes, untile, 0)

        def put(i, unused):
            parcels[chunk][i] = owns[chunk][links[i]]
            return unused

        lax.fori_loop(0, 3 * cap, put, 0)

    def send(chunk):
        for kind in (2, 0, 1):
            parcel(chunk, kind).start()

    pack(0)
    pl.semaphore_wait(barrier, places + 2)
    send(0)
    pack(1)
    for chunk in range(2, count):
        pack(chunk)
        send(chunk - 1)
    send(count - 1)
    relay.clear()
    relay_back.clear()
    blank = jnp.zeros((HALO, ROWS, LANES), jnp.float32)

    def clear(slot, unused):
        for e in (0, 1, last + 3):
            one[slot, e] = blank[0]
        return unused

    lax.fori_loop(0, slots, clear, 0)

    @pl.when(lowest)
    def no_below():
        def fill(slot, unused):
            wide[slot, pl.ds(0, HALO)] = blank
            return unused

        lax.fori_loop(0, slots, fill, 0)

    @pl.when(highest)
    def no_above():
        def fill(slot, unused):
            wide[slot, pl.ds(HALO + planes, HALO)] = blank
            return unused

        lax.fori_loop(0, slots, fill, 0)

    for step in range(count + 1):
        if step < count:
            for kind in range(3):
                parcel(step, kind).wait_recv()
            for side in range(2):
                start = relay.offset(relay.signs[side], 0) + planes * core

                def pick(slot, unused, start=start, chunk=step):
                    wins[chunk][slot, pl.ds(start, planes)] = pools[chunk][tbl[0, slot]]
                    return unused

                lax.fori_loop(side * half, (side + 1) * half, pick, 0)
            relay.begin(step)
        if step > 0:
            relay.second(step - 1)
            relay.settle(step - 1)
        if step < count:
            relay.first(step)
            relay.share(step)

    def couple_of(slot, x):
        at = tbl[2, slot] + planes * core + x
        held_at = tbl[1, slot]
        left = jnp.concatenate([win[slot, at] for win in wins], axis=0)
        right = jnp.concatenate([pool[held_at, x] for pool in pools], axis=0)
        return left, right

    def rise(wave):
        return remote(
            wide.at[pl.ds(wave * each, each), pl.ds(last - HALO + 2, HALO - 1)],
            wide.at[pl.ds(wave * each, each), pl.ds(1, HALO - 1)],
            h_send.at[wave, 0], h_recv.at[wave, 0], (grp, lax.rem(place + 1, places)),
        )

    def sink(wave):
        return remote(
            wide.at[pl.ds(wave * each, each), pl.ds(first, HALO)],
            wide.at[pl.ds(wave * each, each), pl.ds(last + 1, HALO)],
            h_send.at[wave, 1], h_recv.at[wave, 1], (grp, lax.rem(place + places - 1, places)),
        )

    def edges(wave):
        @pl.when(jnp.logical_not(highest))
        def send_up():
            rise(wave).start()

        @pl.when(jnp.logical_not(lowest))
        def send_down():
            sink(wave).start()

    def make(slot, unused):
        second = tbl[3, slot] > 0
        dy, dz = tbl[4, slot], tbl[5, slot]
        for x in range(planes):
            left, right = couple_of(slot, x)
            other = shift_plane(jnp.where(second, left, right), dy, dz)
            wide[slot, x + HALO] = jnp.where(second, right, left) * other
            partner[slot, x] = other
        return unused

    none = jnp.zeros((8, LANES), jnp.float32)
    lane = lax.broadcasted_iota(jnp.int32, (1, LANES), 1)

    def row_of(parts):
        row = jnp.zeros((1, LANES), jnp.float32)
        for at, part in parts:
            row = row + jnp.where(lane == at, total(part), 0.0)
        return row

    def live(slot, e):
        x = planes * place + e - HALO
        low = tbl[6, slot]
        return jnp.where((x >= low) & (x < low + B), 1.0, 0.0).astype(jnp.float32)

    def raise_one(slot, e, acc):
        source = wide[slot, e]
        value = live(slot, e) * (inner(source) - (wide[slot, e - 1] + wide[slot, e + 1]))
        one[slot, e] = value
        if first <= e <= last:
            acc[1] = acc[1] + fold(source * value)
            acc[2] = acc[2] + fold(value * value)

    def raise_two(slot, e):
        source = one[slot, e]
        two[slot, e] = live(slot, e) * (inner(source) - (one[slot, e - 1] + one[slot, e + 1]))

    def measure_two(slot, e, acc, below):
        value = two[slot, e]
        acc[3] = acc[3] + fold(one[slot, e] * value)
        acc[4] = acc[4] + fold(value * value)
        bent = coupled(value)
        acc[5] = acc[5] + fold(value * (bent - two[slot, e - 1] if below else bent))

    def work_inside(slot, unused):
        acc = [none] * 6
        for e in range(first, last + 1):
            source = wide[slot, e]
            acc[0] = acc[0] + fold(source * source)
        for e in range(first + 1, last):
            raise_one(slot, e, acc)
        for e in range(first + 2, last - 1):
            raise_two(slot, e)
            measure_two(slot, e, acc, e > first + 2)
        for at in range(6):
            held[slot, at] = acc[at]
        return unused

    def work_edges(slot, unused):
        acc = [held[slot, at] for at in range(6)]
        for e in (first - 1, first, last, last + 1, last + 2):
            raise_one(slot, e, acc)
        for e in (first, first + 1, last - 1, last, last + 1):
            raise_two(slot, e)
        for e in (first, first + 1, last - 1, last):
            measure_two(slot, e, acc, e > first)
        acc[5] = acc[5] - fold(two[slot, first + 2] * two[slot, first + 1])
        acc[5] = acc[5] - fold(two[slot, last + 1] * two[slot, last])
        acc[5] = 2.0 * acc[5]
        sums[pl.ds(slot, 1)] = row_of(enumerate(acc))
        return unused

    def rim(slot, planes_one, planes_two, spots, pairs):
        spare = [none] * 6
        for e in planes_one:
            raise_one(slot, e, spare)
        for e in planes_two:
            raise_two(slot, e)
        acc = [held[slot, at] for at in range(6)]
        for e in spots:
            value, before = two[slot, e], one[slot, e]
            acc[2] = acc[2] + fold(before * before)
            acc[3] = acc[3] + fold(before * value)
            acc[4] = acc[4] + fold(value * value)
            acc[5] = acc[5] + fold(value * coupled(value))
        for e in pairs:
            acc[5] = acc[5] - fold(two[slot, e] * two[slot, e + 1])
        for at in range(2, 6):
            held[slot, at] = acc[at]

    lax.fori_loop(0, each, make, 0)
    for wave in range(1, WAVES):
        lax.fori_loop(wave * each, (wave + 1) * each, make, 0)
        edges(wave - 1)
    edges(WAVES - 1)
    lax.fori_loop(0, slots, work_inside, 0)

    @pl.when(lowest)
    def rim_below():
        def go(slot, unused):
            low = first - 2
            rim(slot, (low + 1, low + 2), (low, low + 1, low + 2), (low, low + 1), (low, low + 1))
            return unused

        lax.fori_loop(0, slots, go, 0)

    @pl.when(highest)
    def rim_above():
        def go(slot, unused):
            high = last + 2
            rim(slot, (high - 2, high - 1, high), (high - 1, high), (high - 1, high), (high - 1,))
            return unused

        lax.fori_loop(0, slots, go, 0)

    for wave in range(WAVES):
        @pl.when(jnp.logical_not(lowest))
        def got_below(wave=wave):
            rise(wave).wait_recv()

        @pl.when(jnp.logical_not(highest))
        def got_above(wave=wave):
            sink(wave).wait_recv()

        lax.fori_loop(wave * each, (wave + 1) * each, work_edges, 0)

    def tell(step, at):
        return remote(
            sums, gathered.at[at], s_send.at[step - 1], s_recv.at[step - 1],
            (grp, lax.rem(place + step, places)),
        )

    for step in range(1, places):
        tell(step, place).start()
    gathered[place] = sums[...]
    for step in range(1, places):
        tell(step, lax.rem(place + places - step, places)).wait_recv()
    whole = gathered[0]
    for at in range(1, places):
        whole = whole + gathered[at]
    lanes = lax.broadcasted_iota(jnp.int32, whole.shape, 1)
    moments = [jnp.sum(jnp.where(lanes == at, whole, 0.0), axis=1, keepdims=True) for at in range(6)]
    for at, weight in enumerate(krylov_weights(moments)):
        weights[at] = jnp.broadcast_to(weight, whole.shape)

    for side in range(2):
        start = relay_back.offset(relay_back.signs[side], 0) + planes * core

        def finish(slot, unused, start=start):
            second = tbl[3, slot] > 0
            dy, dz = tbl[4, slot], tbl[5, slot]
            w0, w1, w2 = [weights[at, pl.ds(slot, 1)] for at in range(3)]
            for x in range(planes):
                e = x + HALO
                found = w0 * wide[slot, e] + w1 * one[slot, e] + w2 * two[slot, e]
                left, right = couple_of(slot, x)
                term_a = found * partner[slot, x]
                term_b = shift_plane(found * jnp.where(second, right, left), -dy, -dz)
                going = jnp.where(second, term_b, term_a)
                stays = jnp.where(second, term_a, term_b)
                for chunk in range(count):
                    wins_back[chunk][slot, start + x] = going[chunk * SUB : (chunk + 1) * SUB]
                    staying[chunk, slot, x] = stays[chunk * SUB : (chunk + 1) * SUB]
            return unused

        lax.fori_loop(side * half, (side + 1) * half, finish, 0)
        relay_back.begin(0, (side,))

    extra = 3 * cap
    final = extra
    prior = final + norb + extra
    ends = prior + extra

    def reply(chunk, kind):
        return remote(
            parcels_back[chunk].at[pl.ds(kind * cap, cap)], backs[chunk].at[pl.ds(kind * cap, cap)],
            yx_send.at[chunk, kind], yx_recv.at[chunk, kind], ((across, along, corner)[kind], place),
        )

    for step in range(count + 2):
        chunk = step - 1
        if 0 <= chunk < count:
            relay_back.second(chunk)
            relay_back.settle(chunk)
            chain = chains[chunk]
            chain[2 * slots] = jnp.zeros(chain.shape[1:], jnp.float32)

            def link_fixed(slot, unused, chain=chain, chunk=chunk):
                chain[slot] = staying[chunk, slot] + chain[tbl[8, slot]]
                return unused

            def link_moved(slot, unused, chain=chain, chunk=chunk):
                at = tbl[7, slot] + planes * core
                for plane in range(planes):
                    chain[slots + slot, plane] = wins_back[chunk][slot, at + plane] + chain[tbl[9, slot], plane]
                return unused

            lax.fori_loop(0, slots, link_fixed, 0)
            lax.fori_loop(0, slots, link_moved, 0)

            def wrap(i, unused, chain=chain, chunk=chunk):
                parcels_back[chunk][i] = chain[links[final + norb + i]]
                return unused

            lax.fori_loop(0, extra, wrap, 0)
            for kind in (2, 0, 1):
                reply(chunk, kind).start()
        if step < count:
            relay_back.first(step)
            if step + 1 < count:
                relay_back.begin(step + 1)
            relay_back.share(step)
        chunk = step - 2
        if 0 <= chunk < count:
            total_of = tallied[chunk]
            total_of[extra] = jnp.zeros(total_of.shape[1:], jnp.float32)
            for kind in range(3):
                reply(chunk, kind).wait_recv()

            def gather(i, unused, total_of=total_of, chunk=chunk):
                total_of[i] = backs[chunk][i] + total_of[links[prior + i]]
                return unused

            lax.fori_loop(0, extra, gather, 0)

            for orbit in range(norb):
                found = total_of[links[ends + orbit]] + chains[chunk][links[final + orbit]]
                for plane in range(planes):
                    out[orbit // deep, plane, chunk, :, orbit % deep, :] = found[plane]
    for chunk in range(count):
        for kind in range(3):
            parcel(chunk, kind).wait_send()
            reply(chunk, kind).wait_send()
    for wave in range(WAVES):
        @pl.when(jnp.logical_not(highest))
        def sent_up(wave=wave):
            rise(wave).wait_send()

        @pl.when(jnp.logical_not(lowest))
        def sent_down(wave=wave):
            sink(wave).wait_send()

    for step in range(1, places):
        tell(step, place).wait_send()
    relay.drain()
    relay_back.drain()


def run_lean(table, links, tiled, slots, chips, cap):
    tiles, planes, chunks, unused, deep, lanes = tiled.shape
    norb, rows = tiles * deep, chunks * SUB
    places = 2 * chips
    smem = pl.BlockSpec(memory_space=pltpu.SMEM)
    dma = pltpu.SemaphoreType.DMA

    def room(count, deep=planes):
        return [pltpu.VMEM((count, deep, SUB, lanes), jnp.float32)] * chunks

    tall = pltpu.VMEM((slots, planes + 2 * HALO, rows, lanes), jnp.float32)
    xy, z = dma((chunks, 3)), dma((chunks, 2, 6))
    return pl.pallas_call(
        functools.partial(lean_kernel, chips, cap),
        in_specs=[smem, smem, pl.BlockSpec(memory_space=pl.ANY)],
        out_specs=pl.BlockSpec(memory_space=pltpu.VMEM),
        out_shape=jax.ShapeDtypeStruct(tiled.shape, jnp.float32),
        scratch_shapes=[pltpu.VMEM((tiles, planes, SUB, deep, lanes), jnp.float32)] * chunks
        + room(norb) + room(3 * cap) + room(norb + 3 * cap) + room(slots, 6 * planes)
        + room(slots, 6 * planes) + room(2 * slots + 1) + room(3 * cap) + room(3 * cap) + room(3 * cap + 1)
        + [
            pltpu.VMEM((slots, planes, rows, lanes), jnp.float32), tall, tall, tall,
            pltpu.VMEM((chunks, slots, planes, SUB, lanes), jnp.float32),
            pltpu.VMEM((slots, 6, 8, lanes), jnp.float32),
            pltpu.VMEM((slots, lanes), jnp.float32),
            pltpu.VMEM((places, slots, lanes), jnp.float32),
            pltpu.VMEM((3, slots, lanes), jnp.float32),
            dma((chunks,)), xy, xy, z, z, xy, xy, z, z,
            dma((WAVES, 2)), dma((WAVES, 2)), dma((places - 1,)), dma((places - 1,)),
        ],
        compiler_params=pltpu.CompilerParams(
            collective_id=3, has_side_effects=True, vmem_limit_bytes=60 * 1024 * 1024
        ),
        name="lean",
    )(table, links, tiled)


def full_tables(anchors, pair_slots, planes, groups, each):
    assignment = deal_evenly(pair_slots, groups, each)
    pairs = assignment[lax.axis_index("grp")]
    offsets = anchors[pairs[:, 1]] - anchors[pairs[:, 0]]
    dx, dy, dz = offsets[:, 0], offsets[:, 1], offsets[:, 2]
    slot = lax.broadcasted_iota(jnp.int32, (each,), 0)
    rising = slot < each // 2
    second = jnp.where(rising, dx >= 0, dx <= 0)
    shift = jnp.where(second, dx, -dx)
    moved_id = jnp.where(second, pairs[:, 1], pairs[:, 0])
    fixed_id = jnp.where(second, pairs[:, 0], pairs[:, 1])
    terms = jnp.concatenate([fixed_id, moved_id])
    at = lax.broadcasted_iota(jnp.int32, (2 * each, 2 * each), 0)
    before = lax.broadcasted_iota(jnp.int32, (2 * each, 2 * each), 1)
    found = jnp.where((terms[:, None] == terms[None, :]) & (before < at), before, -1)
    prior = jnp.max(found, axis=1)
    prior = jnp.where(prior < 0, 2 * each, prior)
    norb = anchors.shape[0]
    orbit = lax.broadcasted_iota(jnp.int32, (norb, 2 * each), 0)
    index = lax.broadcasted_iota(jnp.int32, (norb, 2 * each), 1)
    last = jnp.max(jnp.where(terms[None, :] == orbit, index, -1), axis=1)
    last = jnp.where(last < 0, 2 * each, last)
    table = jnp.stack([
        moved_id, fixed_id,
        jnp.where(rising, 4 * planes, 0) - shift,
        second.astype(jnp.int32), dy, dz,
        jnp.where(second, 0, shift),
        jnp.where(rising, 0, 4 * planes) + shift,
        prior[:each], prior[each:],
    ])
    return table, last


def slab_body(orbitals, anchors, pair_slots):
    groups, places = lax.axis_size("grp"), lax.axis_size("grid")
    norb_local, cells = orbitals.shape
    planes = cells // (B * B)
    each = PAIR_DEV * places
    chips = places // 2
    cap = 5 * norb_local // 16
    plan, links, fits = make_plan(anchors, pair_slots, cap, each, planes)
    deep = math.gcd(norb_local, 8)

    def lean(orbitals, anchors, pair_slots, plan, links):
        tiled = orbitals.reshape(norb_local // deep, deep, planes, ROWS // SUB, SUB, LANES)
        out = run_lean(plan, links, jnp.transpose(tiled, (0, 2, 3, 4, 1, 5)), each, chips, cap)
        return jnp.transpose(out, (0, 4, 1, 2, 3, 5)).reshape(norb_local, cells)

    def full(orbitals, anchors, pair_slots, plan, links):
        stacked = orbitals.reshape(norb_local, planes, ROWS, LANES)
        table, last = full_tables(anchors, pair_slots, planes, groups, each)
        moved, fixed = bring(table, stacked, each, groups, chips)
        dens, partner = pair_up(table, moved, fixed)
        pot = solve_slabs(table, dens, places, 5)
        going, staying = make_terms(table, pot, partner, moved, fixed)
        out = hand_back(table, last, going, staying, norb_local, chips)
        return out.reshape(norb_local, cells)

    return lax.cond(fits[0] > 0, lean, full, orbitals, anchors, pair_slots, plan, links)


def slabs_fit(mesh):
    groups, places = mesh.shape["grp"], mesh.shape["grid"]
    return groups == 4 and places % 2 == 0 and 4 * (B // places) >= PAD


def solution(mesh):
    return jax.shard_map(
        slab_body if slabs_fit(mesh) else owner_body,
        mesh=mesh,
        in_specs=(P("grp", "grid"), P(), P()),
        out_specs=P("grp", "grid"),
        check_vma=False,
    )
```
